256 devices in a mesh: gx: 32 (over z, x), gy: 8 (over y, core).
Axes of the slice: x: 4, y: 4, z: 8, core: 2. Of those that a mesh axis runs over, the one named last changes fastest.
Arguments:
- fine_disp: float32 [3, 512, 128, 128], P(None, 'gx', 'gy'), may hold values from -12 to 12
- fine_prev: float32 [3, 512, 128, 128], P(None, 'gx', 'gy'), may hold values from -12 to 12
- coarse_disp: float32 [3, 256, 64, 256], P(None, 'gx', 'gy'), may hold values from -12 to 12
- coarse_prev: float32 [3, 256, 64, 256], P(None, 'gx', 'gy'), may hold values from -12 to 12
- fine_density: float32 [512, 128, 128], P('gx', 'gy'), may hold values from 0.6 to 1.8
- fine_lame: float32 [512, 128, 128], P('gx', 'gy'), may hold values from 0.5 to 2
- fine_rigidity: float32 [512, 128, 128], P('gx', 'gy'), may hold values from 0.3 to 1.5
- fine_metric: float32 [512, 128, 128], P('gx', 'gy'), may hold values from 0.7 to 1.4
- coarse_density: float32 [256, 64, 256], P('gx', 'gy'), may hold values from 0.6 to 1.8
- coarse_lame: float32 [256, 64, 256], P('gx', 'gy'), may hold values from 0.5 to 2
- coarse_rigidity: float32 [256, 64, 256], P('gx', 'gy'), may hold values from 0.3 to 1.5
- coarse_metric: float32 [256, 64, 256], P('gx', 'gy'), may hold values from 0.7 to 1.4
- offsets: int32 [2, 512, 128], P(None, 'gx', 'gy'), may hold values from -1 to 1
Outputs:
- fine_final: float32 [3, 512, 128, 128], P(None, 'gx', 'gy')
- coarse_final: float32 [3, 256, 64, 256], P(None, 'gx', 'gy')
- energy: float32 [3, 2], replicated
The draws below stay inside these ranges and needn't reach their ends.
All inputs are finite; a program needn't handle non-finite values.
Results may differ from the reference program's by a relative error of at most 0.00021.
Values sent between devices are 32-bit elements; how exact they have to be, the bound alone decides.
No kernel may reach another device: no remote copies, remote signals or barrier semaphores. Data moves between devices by JAX's collectives and lax.ppermute only.
A program may use at most 64 MiB of HBM per device.

```python
import math
import jax
import jax.numpy as jnp

FZ = 128
STEPS = 3
CZ = 256
NXF = 512
NYF = 128
NXC = 256
NYC = 64


def rough_field(key, cells_x, cells_y, cells_z):
    key_scale, key_rough, key_common = jax.random.split(key, 3)
    blocks_x = (cells_x + 7) // 8
    blocks_y = (cells_y + 7) // 8
    log_scale = jax.random.uniform(key_scale, (blocks_x, blocks_y), jnp.float32, -1.1, 1.1)
    rough_part = jax.random.truncated_normal(key_rough, -4.0, 4.0, (3, cells_x, cells_y, cells_z), jnp.float32)
    amplitude = jnp.repeat(jnp.repeat(jnp.exp(log_scale), 8, axis=0), 8, axis=1)[:cells_x, :cells_y]
    return jnp.clip(rough_part * amplitude[None, :, :, None], -12.0, 12.0)


def draw_fine_disp(key, part):
    return rough_field(jax.random.fold_in(key, 11), NXF, NYF, FZ)


def draw_fine_prev(key, part):
    return rough_field(jax.random.fold_in(key, 12), NXF, NYF, FZ)


def draw_coarse_disp(key, part):
    return rough_field(jax.random.fold_in(key, 13), NXC, NYC, CZ)


def draw_coarse_prev(key, part):
    return rough_field(jax.random.fold_in(key, 14), NXC, NYC, CZ)


def touch_ends(drawn, key, least, top_value):
    spot = [jax.random.randint(jax.random.fold_in(key, axis), (), 0, length) for axis, length in enumerate(drawn.shape)]
    main_axis = drawn.shape.index(max(drawn.shape))
    next_to = spot[:main_axis] + [(spot[main_axis] + 1) % drawn.shape[main_axis]] + spot[main_axis + 1:]
    return drawn.at[tuple(spot)].set(least).at[tuple(next_to)].set(top_value)


def block_scale(own_key, shape, shards, least, top_value):
    loudness = 1.0
    for position, parts in shards:
        steps = jax.random.uniform(jax.random.fold_in(jax.random.fold_in(own_key, 6), position), (parts,), jnp.float32, least / len(shards), top_value / len(shards))
        loudness = loudness * jnp.repeat(jnp.exp(steps), shape[position] // parts).reshape((-1,) + (1,) * (len(shape) - 1 - position))
    return loudness


def setup_inputs(seed: int = 0) -> dict:
    key_of = jax.random.split(jax.random.key(seed), 14)
    return {
        "fine_disp": draw_fine_disp(jax.random.fold_in(key_of[13], 71), 0),
        "fine_prev": draw_fine_prev(jax.random.fold_in(key_of[13], 71), 0),
        "coarse_disp": draw_coarse_disp(jax.random.fold_in(key_of[13], 71), 0),
        "coarse_prev": draw_coarse_prev(jax.random.fold_in(key_of[13], 71), 0),
        "fine_density": jnp.clip(jnp.exp(math.log(1.8) - 1.0986122 * jax.random.uniform(key_of[4], (NXF, NYF, FZ), jnp.float32) ** block_scale(key_of[4], (NXF, NYF, FZ), ((0, 32), (1, 8)), -0.2, 0.2)), 0.6, 1.8),
        "fine_lame": jnp.clip(jnp.exp(math.log(2.0) - 1.3862944 * jax.random.uniform(key_of[5], (NXF, NYF, FZ), jnp.float32) ** block_scale(key_of[5], (NXF, NYF, FZ), ((0, 32), (1, 8)), -0.2, 0.2)), 0.5, 2.0),
        "fine_rigidity": jnp.clip(jnp.exp(math.log(1.5) - 1.60943787 * jax.random.uniform(key_of[6], (NXF, NYF, FZ), jnp.float32) ** block_scale(key_of[6], (NXF, NYF, FZ), ((0, 32), (1, 8)), -0.2, 0.2)), 0.3, 1.5),
        "fine_metric": jnp.clip(jnp.exp(math.log(1.4) - 0.6931472 * jax.random.uniform(key_of[7], (NXF, NYF, FZ), jnp.float32) ** block_scale(key_of[7], (NXF, NYF, FZ), ((0, 32), (1, 8)), -0.2, 0.2)), 0.7, 1.4),
        "coarse_density": jnp.clip(jnp.exp(math.log(1.8) - 1.0986122 * jax.random.uniform(key_of[8], (NXC, NYC, CZ), jnp.float32) ** block_scale(key_of[8], (NXC, NYC, CZ), ((0, 32), (1, 8)), -0.2, 0.2)), 0.6, 1.8),
        "coarse_lame": jnp.clip(jnp.exp(math.log(2.0) - 1.3862944 * jax.random.uniform(key_of[9], (NXC, NYC, CZ), jnp.float32) ** block_scale(key_of[9], (NXC, NYC, CZ), ((0, 32), (1, 8)), -0.2, 0.2)), 0.5, 2.0),
        "coarse_rigidity": jnp.clip(jnp.exp(math.log(1.5) - 1.60943787 * jax.random.uniform(key_of[10], (NXC, NYC, CZ), jnp.float32) ** block_scale(key_of[10], (NXC, NYC, CZ), ((0, 32), (1, 8)), -0.2, 0.2)), 0.3, 1.5),
        "coarse_metric": jnp.clip(jnp.exp(math.log(1.4) - 0.6931472 * jax.random.uniform(key_of[11], (NXC, NYC, CZ), jnp.float32) ** block_scale(key_of[11], (NXC, NYC, CZ), ((0, 32), (1, 8)), -0.2, 0.2)), 0.7, 1.4),
        "offsets": touch_ends(jax.random.randint(key_of[12], (2, NXF, NYF), -1, 2), jax.random.fold_in(key_of[12], 1), -1, 1).astype(jnp.int32),
    }


step_factor = 0.15


def vertical_slope(values):
    middle = 0.5 * (values[..., 2:] - values[..., :-2])
    first = values[..., 1:2] - values[..., 0:1]
    final = values[..., -1:] - values[..., -2:-1]
    return jnp.concatenate([first, middle, final], axis=-1)


def divergence(along_x, along_y, along_z, inverse):
    return 0.5 * (along_x[2:] - along_x[:-2]) + 0.5 * (along_y[:, 2:] - along_y[:, :-2]) + inverse * vertical_slope(along_z)


def interpolate(plane_ext, offsets):
    coarse_x = plane_ext.shape[1] - 4
    coarse_y = plane_ext.shape[2] - 4
    near_x = jnp.where((jnp.arange(2 * coarse_x) % 2) == 0, 0.75, 0.25)[:, None]
    near_y = jnp.where((jnp.arange(2 * coarse_y) % 2) == 0, 0.75, 0.25)[None, :]
    offset_x = offsets[0]
    offset_y = offsets[1]
    summed = jnp.zeros((3, 2 * coarse_x, 2 * coarse_y), plane_ext.dtype)
    for shift_x in (-1, 0, 1, 2):
        weight_x = jnp.where(offset_x == shift_x, near_x, 0.0) + jnp.where(offset_x + 1 == shift_x, 1.0 - near_x, 0.0)
        row_band = jnp.repeat(plane_ext[:, 2 + shift_x:2 + shift_x + coarse_x, :], 2, axis=1)
        for shift_y in (-1, 0, 1, 2):
            weight_y = jnp.where(offset_y == shift_y, near_y, 0.0) + jnp.where(offset_y + 1 == shift_y, 1.0 - near_y, 0.0)
            tile_band = jnp.repeat(row_band[:, :, 2 + shift_y:2 + shift_y + coarse_y], 2, axis=2)
            summed = summed + (weight_x * weight_y)[None] * tile_band
    return summed


def restrict(plane):
    half_x = plane.shape[1] // 2
    half_y = plane.shape[2] // 2
    return 0.25 * jnp.sum(plane.reshape(3, half_x, 2, half_y, 2), axis=(2, 4))


def elastic_rate(extended, mats_ext, div_ext, displace, top_ghost, bottom_ghost, density, lame_first, rigidity):
    wide_ext = mats_ext[0]
    inverse = mats_ext[1, 1:-1, 1:-1]
    face_x = 0.5 * (wide_ext[:-1, 1:-1] + wide_ext[1:, 1:-1])
    flux_x = face_x * (extended[:, 1:, 1:-1] - extended[:, :-1, 1:-1])
    face_y = 0.5 * (wide_ext[1:-1, :-1] + wide_ext[1:-1, 1:])
    flux_y = face_y * (extended[:, 1:-1, 1:] - extended[:, 1:-1, :-1])
    vertical = rigidity * inverse
    face_z = jnp.concatenate([vertical[:, :, :1], 0.5 * (vertical[:, :, :-1] + vertical[:, :, 1:]), vertical[:, :, -1:]], axis=2)
    column = jnp.concatenate([top_ghost[:, :, :, None], displace, bottom_ghost[:, :, :, None]], axis=3)
    flux_z = face_z * (column[:, :, :, 1:] - column[:, :, :, :-1])
    spread = (flux_x[:, 1:] - flux_x[:, :-1]) + (flux_y[:, :, 1:] - flux_y[:, :, :-1]) + (flux_z[:, :, :, 1:] - flux_z[:, :, :, :-1])
    grad_x = 0.5 * (div_ext[2:, 1:-1] - div_ext[:-2, 1:-1])
    grad_y = 0.5 * (div_ext[1:-1, 2:] - div_ext[1:-1, :-2])
    grad_z = inverse * vertical_slope(div_ext[1:-1, 1:-1])
    gradient = jnp.stack([grad_x, grad_y, grad_z])
    return spread * (inverse / density) + ((lame_first + rigidity) / density) * gradient


def energy_part(updated, displace, rate, density, metric, cell_count):
    change = updated - displace
    inner_sum = jnp.sum(change * change - step_factor * updated * rate, axis=0)
    return jnp.sum(density * metric * inner_sum) / cell_count


def reference(fine_disp, fine_prev, coarse_disp, coarse_prev, fine_density, fine_lame, fine_rigidity, fine_metric, coarse_density, coarse_lame, coarse_rigidity, coarse_metric, offsets):
    pad_cells = ((1, 1), (1, 1), (0, 0))
    pad_fields = ((0, 0), (1, 1), (1, 1), (0, 0))
    fine_mats = jnp.pad(jnp.stack([fine_rigidity * fine_metric, 1.0 / fine_metric]), pad_fields)
    coarse_mats = jnp.pad(jnp.stack([coarse_rigidity * coarse_metric, 1.0 / coarse_metric]), pad_fields)
    fine_cells = fine_disp.shape[1] * fine_disp.shape[2] * fine_disp.shape[3]
    coarse_cells = coarse_disp.shape[1] * coarse_disp.shape[2] * coarse_disp.shape[3]
    energies = []
    for step_index in range(STEPS):
        fine_ext = jnp.pad(fine_disp, pad_fields)
        coarse_ext = jnp.pad(coarse_disp, pad_fields)
        fine_div = divergence(fine_ext[0, :, 1:-1], fine_ext[1, 1:-1, :], fine_disp[2], fine_mats[1, 1:-1, 1:-1])
        coarse_div = divergence(coarse_ext[0, :, 1:-1], coarse_ext[1, 1:-1, :], coarse_disp[2], coarse_mats[1, 1:-1, 1:-1])
        fine_div_ext = jnp.pad(fine_div, pad_cells)
        coarse_div_ext = jnp.pad(coarse_div, pad_cells)
        plane_ext = jnp.pad(coarse_disp[:, :, :, 0], ((0, 0), (2, 2), (2, 2)))
        fine_bottom = interpolate(plane_ext, offsets)
        fine_top = fine_disp[:, :, :, 0]
        coarse_top = restrict(fine_disp[:, :, :, -1])
        coarse_bottom = jnp.zeros_like(coarse_top)
        fine_rate = elastic_rate(fine_ext, fine_mats, fine_div_ext, fine_disp, fine_top, fine_bottom, fine_density, fine_lame, fine_rigidity)
        coarse_rate = elastic_rate(coarse_ext, coarse_mats, coarse_div_ext, coarse_disp, coarse_top, coarse_bottom, coarse_density, coarse_lame, coarse_rigidity)
        fine_new = 2.0 * fine_disp - fine_prev + step_factor * fine_rate
        coarse_new = 2.0 * coarse_disp - coarse_prev + step_factor * coarse_rate
        energies.append(jnp.stack([
            energy_part(fine_new, fine_disp, fine_rate, fine_density, fine_metric, fine_cells),
            energy_part(coarse_new, coarse_disp, coarse_rate, coarse_density, coarse_metric, coarse_cells)]))
        fine_prev, fine_disp = fine_disp, fine_new
        coarse_prev, coarse_disp = coarse_disp, coarse_new
    return (fine_disp, coarse_disp, jnp.stack(energies))
```

```python
import functools

import jax
import jax.numpy as jnp
from jax import lax
from jax.experimental import pallas as pl
from jax.experimental.pallas import tpu as pltpu
from jax.sharding import Mesh
from jax.sharding import PartitionSpec as P

STEPS = 3
GX = ("gx_0", "gx_1")
GY = ("gy_0", "gy_1")
ALL = GX + GY
STEP = 0.15
LANES = 128
VMEM_LIMIT = 20 * 1024 * 1024

EVEN_X, HAS_XM, HAS_XP, EVEN_Y, HAS_YM, HAS_YP = range(6)


class Sizes:
    def __init__(self, fine, coarse):
        self.fx, self.fy, self.fz = fine
        self.cx, self.cy, self.cz = coarse
        self.halves = self.cz // LANES
        self.x_fine = 0
        self.x_coarse = 6 * self.fy
        self.x_rows = self.x_coarse + self.halves * 6 * self.cy
        self.x_fine_mats = self.x_rows
        self.x_coarse_mats = self.x_fine_mats + 2 * self.fy
        self.x_rows_mats = self.x_coarse_mats + 2 * self.halves * self.cy
        self.fe, self.ce = self.fx + 4, self.cx + 4
        self.y_coarse = 3 * self.fe
        self.y_rows = self.y_coarse + self.halves * 3 * self.ce
        self.y_fine_mats = self.y_rows
        self.y_coarse_mats = self.y_fine_mats + self.fx
        self.y_rows_mats = self.y_coarse_mats + self.halves * self.cx


def lanes_of(h):
    return slice(h * LANES, (h + 1) * LANES)


def put_x(s, flags, outs, fine, coarse, mats):
    even = flags[EVEN_X] == 1
    for k, out in enumerate(outs):
        far = even if k == 0 else jnp.logical_not(even)
        start_f = jnp.where(far, s.fx - 2, 0)
        start_c = jnp.where(far, s.cx - 2, 0)
        out[0 : s.x_coarse, :] = fine[:, pl.ds(start_f, 2), :, :].reshape(6 * s.fy, LANES)
        strip = coarse[:, pl.ds(start_c, 2), :, :]
        for h in range(s.halves):
            base = s.x_coarse + h * 6 * s.cy
            out[base : base + 6 * s.cy, :] = strip[:, :, :, lanes_of(h)].reshape(6 * s.cy, LANES)
        if mats is None:
            continue
        edge_f = jnp.where(far, s.fx - 1, 0)
        edge_c = jnp.where(far, s.cx - 1, 0)
        for m in range(2):
            base = s.x_fine_mats + m * s.fy
            out[base : base + s.fy, :] = mats[m][edge_f]
            line = mats[2 + m][edge_c]
            for h in range(s.halves):
                base = s.x_coarse_mats + (m * s.halves + h) * s.cy
                out[base : base + s.cy, :] = line[:, lanes_of(h)]


def first_kernel(s, flags, fine, coarse, rig_f, met_f, rig_c, met_c, out_a, out_b):
    put_x(s, flags, (out_a, out_b), fine, coarse, (rig_f, met_f, rig_c, met_c))


def sides(flags, even, has_low, has_high, a, b):
    low = jnp.where(flags[even] == 1, b, a)
    high = jnp.where(flags[even] == 1, a, b)
    low = jnp.where(flags[has_low] == 1, low, 0.0)
    high = jnp.where(flags[has_high] == 1, high, 0.0)
    return low, high


def middle_kernel(s, with_mats, flags, *refs):
    if with_mats:
        fine, coarse, rig_f, met_f, rig_c, met_c, in_a, in_b, out_a, out_b = refs
    else:
        fine, coarse, in_a, in_b, out_a, out_b = refs
    even = flags[EVEN_Y] == 1

    def put(index, low, high):
        out_a[index] = jnp.where(even, high, low)
        out_b[index] = jnp.where(even, low, high)

    for c in range(3):
        own = pl.ds(c * s.fe + 2, s.fx)
        put(own, fine[c, :, 0:2, :], fine[c, :, s.fy - 2 : s.fy, :])
        for k in range(2):
            base = (c * 2 + k) * s.fy
            pieces = []
            for first in (0, s.fy - 2):
                rows = slice(base + first, base + first + 2)
                pieces.append(sides(flags, EVEN_X, HAS_XM, HAS_XP, in_a[rows, :], in_b[rows, :]))
            for side in range(2):
                place = c * s.fe + (k if side == 0 else s.fx + 2 + k)
                put(place, pieces[0][side], pieces[1][side])
        for h in range(s.halves):
            origin = s.y_coarse + (h * 3 + c) * s.ce
            own = pl.ds(origin + 2, s.cx)
            put(own, coarse[c, :, 0:2, lanes_of(h)], coarse[c, :, s.cy - 2 : s.cy, lanes_of(h)])
            for k in range(2):
                base = s.x_coarse + (h * 6 + c * 2 + k) * s.cy
                pieces = []
                for first in (0, s.cy - 2):
                    rows = slice(base + first, base + first + 2)
                    pieces.append(
                        sides(flags, EVEN_X, HAS_XM, HAS_XP, in_a[rows, :], in_b[rows, :])
                    )
                for side in range(2):
                    place = origin + (k if side == 0 else s.cx + 2 + k)
                    put(place, pieces[0][side], pieces[1][side])
    if not with_mats:
        return
    for m, (of_f, of_c) in enumerate(((rig_f, rig_c), (met_f, met_c))):
        low, high = of_f[:, 0:1, :], of_f[:, s.fy - 1 : s.fy, :]
        where = pl.ds(s.y_fine_mats, s.fx)
        out_a[where, m : m + 1, :] = jnp.where(even, high, low)
        out_b[where, m : m + 1, :] = jnp.where(even, low, high)
        for h in range(s.halves):
            low, high = of_c[:, 0:1, lanes_of(h)], of_c[:, s.cy - 1 : s.cy, lanes_of(h)]
            where = pl.ds(s.y_coarse_mats + h * s.cx, s.cx)
            out_a[where, m : m + 1, :] = jnp.where(even, high, low)
            out_b[where, m : m + 1, :] = jnp.where(even, low, high)


def up_one(x):
    return pltpu.roll(x, x.shape[-1] - 1, x.ndim - 1)


def down_one(x):
    return pltpu.roll(x, 1, x.ndim - 1)


def own_kernel(density, lame, rigidity, metric, inverse, c1, c2, weight, above, below):
    inv = 1.0 / metric[...]
    inverse[...] = inv
    over = 1.0 / density[...]
    c1[...] = inv * over
    c2[...] = (lame[...] + rigidity[...]) * over
    weight[...] = density[...] * metric[...]
    v = rigidity[...] * inv
    lane = lax.broadcasted_iota(jnp.int32, v.shape, 2)
    above[...] = jnp.where(lane == v.shape[2] - 1, v, 0.5 * (v + up_one(v)))
    below[...] = jnp.where(lane == 0, v, 0.5 * (v + down_one(v)))


def slope(f, up, down, lane):
    last = f.shape[-1] - 1
    return jnp.where(lane == 0, up - f, jnp.where(lane == last, f - down, 0.5 * (up - down)))


def fill_displacement(s, flags, own, ext, x_in, y_in, fine):
    x, y, e = (s.fx, s.fy, s.fe) if fine else (s.cx, s.cy, s.ce)
    ext[:, 2 : 2 + x, 8 : 8 + y, :] = own[...]
    for h in range(1 if fine else s.halves):
        base = s.x_fine if fine else s.x_coarse + h * 6 * y
        rows = slice(base, base + 6 * y)
        low, high = sides(flags, EVEN_X, HAS_XM, HAS_XP, x_in[0][rows, :], x_in[1][rows, :])
        ext[:, 0:2, 8 : 8 + y, lanes_of(h)] = low.reshape(3, 2, y, LANES)
        ext[:, x + 2 : x + 4, 8 : 8 + y, lanes_of(h)] = high.reshape(3, 2, y, LANES)
        for c in range(3):
            start = c * e if fine else s.y_coarse + (h * 3 + c) * e
            rows = slice(start, start + e)
            low, high = sides(flags, EVEN_Y, HAS_YM, HAS_YP, y_in[0][rows], y_in[1][rows])
            ext[c, :, 6:8, lanes_of(h)] = low
            ext[c, :, 8 + y : 10 + y, lanes_of(h)] = high


def fill_materials(s, flags, rigidity, metric, inverse, wide_ext, inv_ext, x_in, y_in, fine):
    x, y = (s.fx, s.fy) if fine else (s.cx, s.cy)
    wide_ext[1 : 1 + x, 8 : 8 + y, :] = rigidity[...] * metric[...]
    inv_ext[1 : 1 + x, 8 : 8 + y, :] = inverse[...]
    for h in range(1 if fine else s.halves):
        at = lanes_of(h)
        got = []
        for m in range(2):
            base = s.x_fine_mats + m * y if fine else s.x_coarse_mats + (m * s.halves + h) * y
            rows = slice(base, base + y)
            even = flags[EVEN_X] == 1
            a, b = x_in[0][rows, :], x_in[1][rows, :]
            got.append((jnp.where(even, b, a), jnp.where(even, a, b)))
        for side, (flag, place) in enumerate(((HAS_XM, 0), (HAS_XP, x + 1))):
            rig, met = got[0][side], got[1][side]
            wide_ext[place, 8 : 8 + y, at] = jnp.where(flags[flag] == 1, rig * met, 0.0)
            inv_ext[place, 8 : 8 + y, at] = jnp.where(flags[flag] == 1, 1.0 / met, 0.0)
        start = s.y_fine_mats if fine else s.y_coarse_mats + h * x
        rows = slice(start, start + x)
        got = []
        for m in range(2):
            even = flags[EVEN_Y] == 1
            a, b = y_in[0][rows, m : m + 1, :], y_in[1][rows, m : m + 1, :]
            got.append((jnp.where(even, b, a), jnp.where(even, a, b)))
        for side, (flag, place) in enumerate(((HAS_YM, 7), (HAS_YP, 8 + y))):
            rig, met = got[0][side], got[1][side]
            wide_ext[1 : 1 + x, place : place + 1, at] = jnp.where(flags[flag] == 1, rig * met, 0.0)
            inv_ext[1 : 1 + x, place : place + 1, at] = jnp.where(flags[flag] == 1, 1.0 / met, 0.0)


def fill_divergence(x, y, ext, inv_ext, div):
    z = ext.shape[-1]
    lane = lax.broadcasted_iota(jnp.int32, (y + 2, z), 1)

    def row(r, carry):
        along_x = ext[0, r + 2, 7 : 9 + y, :] - ext[0, r, 7 : 9 + y, :]
        along_y = ext[1, r + 1, 8 : 10 + y, :] - ext[1, r + 1, 6 : 8 + y, :]
        f = ext[2, r + 1, 7 : 9 + y, :]
        inv = inv_ext[r, 7 : 9 + y, :]
        total = 0.5 * along_x + 0.5 * along_y + inv * slope(f, up_one(f), down_one(f), lane)
        div[r, 7 : 9 + y, :] = jnp.where(inv > 0.0, total, 0.0)
        return carry

    lax.fori_loop(0, x + 2, row, 0)


def update(x, y, ext, wide_ext, inv_ext, div, prev, coef, new, ghosts):
    c1, c2, weight, above, below = coef
    z = ext.shape[-1]
    lane = lax.broadcasted_iota(jnp.int32, (y, z), 1)
    mid, left, right = slice(8, 8 + y), slice(7, 7 + y), slice(9, 9 + y)

    def row(i, total):
        wide = wide_ext[i + 1, mid, :]
        w_xp = 0.5 * (wide + wide_ext[i + 2, mid, :])
        w_xm = 0.5 * (wide_ext[i, mid, :] + wide)
        w_yp = 0.5 * (wide + wide_ext[i + 1, right, :])
        w_ym = 0.5 * (wide_ext[i + 1, left, :] + wide)
        inv = inv_ext[i + 1, mid, :]
        f = div[i + 1, mid, :]
        gradient = (
            0.5 * (div[i + 2, mid, :] - div[i, mid, :]),
            0.5 * (div[i + 1, right, :] - div[i + 1, left, :]),
            inv * slope(f, up_one(f), down_one(f), lane),
        )
        top, bottom = ghosts(i)
        k1, k2, dm, va, vb = c1[i], c2[i], weight[i], above[i], below[i]
        inner = jnp.zeros((y, z), jnp.float32)
        for c in range(3):
            u = ext[c, i + 2, mid, :]
            up = jnp.where(lane == z - 1, bottom(c), up_one(u))
            down = jnp.where(lane == 0, u if top is None else top(c), down_one(u))
            flux = w_xp * (ext[c, i + 3, mid, :] - u) - w_xm * (u - ext[c, i + 1, mid, :])
            flux += w_yp * (ext[c, i + 2, right, :] - u) - w_ym * (u - ext[c, i + 2, left, :])
            flux += va * (up - u) - vb * (u - down)
            rate = flux * k1 + k2 * gradient[c]
            updated = 2.0 * u - prev[c, i] + STEP * rate
            change = updated - u
            inner += change * change - STEP * updated * rate
            new[c, i] = updated
        return total + dm * inner

    return lax.fori_loop(0, x, row, jnp.zeros((y, z), jnp.float32))


def step_kernel(s, step, flags, *refs):
    refs = list(refs)

    def take(n):
        out = refs[:n]
        del refs[:n]
        return out

    fine, coarse, fine_prev, coarse_prev, offs = take(5)
    coef_f, coef_c = take(5), take(5)
    first, final = step == 0, step == STEPS - 1
    if first:
        rig_f, met_f, inverse_f, rig_c, met_c, inverse_c = take(6)
    else:
        wide_f, inv_f, wide_c, inv_c, energy_in = take(5)
    x_in, y_in = take(2), take(2)
    new_f, new_c, energy = take(3)
    if not final:
        x_out = take(2)
    if first:
        wide_f, inv_f, wide_c, inv_c = take(4)
    ext_f, ext_c, div_f, div_c, double, pairs = take(6)

    fill_displacement(s, flags, fine, ext_f, x_in, y_in, True)
    fill_displacement(s, flags, coarse, ext_c, x_in, y_in, False)
    if first:
        fill_materials(s, flags, rig_f, met_f, inverse_f, wide_f, inv_f, x_in, y_in, True)
        fill_materials(s, flags, rig_c, met_c, inverse_c, wide_c, inv_c, x_in, y_in, False)

    lane = lax.broadcasted_iota(jnp.int32, (s.cy + 4, LANES), 1)
    for i in range(s.ce):
        e0, e1, e2 = (ext_c[c, i, 6 : 10 + s.cy, 0:LANES] for c in range(3))
        e1, e2 = pltpu.roll(e1, 1, 1), pltpu.roll(e2, 2, 1)
        plane = jnp.where(lane == 0, e0, jnp.where(lane == 1, e1, e2))
        for j in range(s.cy + 4):
            double[i, 2 * j : 2 * j + 2, :] = jnp.broadcast_to(plane[j : j + 1, :], (2, LANES))
    for c in range(3):
        for i in range(s.cx):
            pairs[c, i] = fine[c, 2 * i] + fine[c, 2 * i + 1]

    fill_divergence(s.fx, s.fy, ext_f, inv_f, div_f)
    fill_divergence(s.cx, s.cy, ext_c, inv_c, div_c)

    odd_y = lax.broadcasted_iota(jnp.int32, (s.fy, LANES), 0) % 2
    near_y = jnp.where(odd_y == 0, 0.75, 0.25)

    def fine_ghosts(i):
        half = i // 2
        near_x = jnp.where(i % 2 == 0, 0.75, 0.25)
        off_x, off_y = offs[0, i], offs[1, i]
        total = jnp.zeros((s.fy, LANES), jnp.float32)
        weights = []
        for shift in (-1, 0, 1, 2):
            weights.append(
                jnp.where(off_y == shift, near_y, 0.0)
                + jnp.where(off_y == shift - 1, 1.0 - near_y, 0.0)
            )
        for shift in (-1, 0, 1, 2):
            weight_x = jnp.where(off_x == shift, near_x, 0.0) + jnp.where(
                off_x == shift - 1, 1.0 - near_x, 0.0
            )
            line = jnp.zeros((s.fy, LANES), jnp.float32)
            for k in range(4):
                line += weights[k] * double[half + 2 + shift, 2 * k + 2 : 2 * k + 2 + s.fy, :]
            total += weight_x * line
        return None, lambda c: pltpu.roll(total, LANES - 1 - c, 1)

    def coarse_ghosts(i):
        def top(c):
            both = pairs[c, i, pl.ds(0, s.cy, stride=2), :] + pairs[c, i, pl.ds(1, s.cy, stride=2), :]
            column = pltpu.roll(0.25 * both, 1, 1)
            return jnp.concatenate([column] * s.halves, axis=1)

        return top, lambda c: jnp.zeros((s.cy, s.cz), jnp.float32)

    sum_f = update(s.fx, s.fy, ext_f, wide_f, inv_f, div_f, fine_prev, coef_f, new_f, fine_ghosts)
    sum_c = update(
        s.cx, s.cy, ext_c, wide_c, inv_c, div_c, coarse_prev, coef_c, new_c, coarse_ghosts
    )
    place = lax.broadcasted_iota(jnp.int32, (8, LANES), 0)
    before = jnp.zeros((8, LANES), jnp.float32) if first else energy_in[...]
    before = jnp.where(place == 2 * step, jnp.sum(sum_f), before)
    energy[...] = jnp.where(place == 2 * step + 1, jnp.sum(sum_c), before)
    if not final:
        put_x(s, flags, x_out, new_f, new_c, None)


VMEM = pl.BlockSpec(memory_space=pltpu.VMEM)
SMEM = pl.BlockSpec(memory_space=pltpu.SMEM)


def call(kernel, shapes, flops, *args, scratch=(), name=None, table=True):
    shapes = [jax.ShapeDtypeStruct(shape, jnp.float32) for shape in shapes]
    return pl.pallas_call(
        kernel,
        out_shape=shapes,
        in_specs=([SMEM] if table else []) + [VMEM] * (len(args) - table),
        out_specs=[VMEM] * len(shapes),
        scratch_shapes=[pltpu.VMEM(shape, jnp.float32) for shape in scratch],
        compiler_params=pltpu.CompilerParams(vmem_limit_bytes=VMEM_LIMIT),
        cost_estimate=pl.CostEstimate(flops=flops, bytes_accessed=1 << 20, transcendentals=0),
        name=name,
    )(*args)


def across(i, n):
    return (i + 1) % n if i % 2 else (i - 1) % n


def opposite(i, n):
    return (i - 3) % n if i % 2 else (i + 3) % n


def device_pairs(mesh, axes, move):
    sizes = dict(mesh.shape)
    names = list(sizes)
    total = 1
    for name in names:
        total *= sizes[name]
    count = 1
    for name in axes:
        count *= sizes[name]
    pairs = []
    for source in range(total):
        rest, at = source, {}
        for name in reversed(names):
            at[name] = rest % sizes[name]
            rest //= sizes[name]
        index = 0
        for name in axes:
            index = index * sizes[name] + at[name]
        index = move(index, count)
        for name in reversed(axes):
            at[name] = index % sizes[name]
            index //= sizes[name]
        target = 0
        for name in names:
            target = target * sizes[name] + at[name]
        pairs.append((source, target))
    return pairs


def beside(i, n):
    return i ^ 1


def total_over_mesh(value, swap):
    lane = lax.broadcasted_iota(jnp.int32, (8, LANES), 1)

    def ring_of_eight(value, axes):
        value = value + swap(value, axes, beside)
        pair = lax.axis_index(axes) // 2
        slots = jnp.where(lane == pair, value, 0.0)
        slots = slots + swap(slots, axes, across)
        slots = slots + swap(slots, axes, opposite)
        return jnp.broadcast_to(jnp.sum(slots[:, 0:4], axis=1, keepdims=True), (8, LANES))

    value = ring_of_eight(value, GY)
    value = value + swap(value, ("gx_1",), beside)
    value = value + swap(value, ("gx_1",), across)
    return ring_of_eight(value, ("gx_0",))


def per_device(
    mesh,
    fine_disp,
    fine_prev,
    coarse_disp,
    coarse_prev,
    fine_density,
    fine_lame,
    fine_rigidity,
    fine_metric,
    coarse_density,
    coarse_lame,
    coarse_rigidity,
    coarse_metric,
    offsets,
):
    fine_shape, coarse_shape = fine_metric.shape, coarse_metric.shape
    s = Sizes(fine_shape, coarse_shape)
    count_x, count_y = lax.axis_size(GX), lax.axis_size(GY)
    place_x, place_y = lax.axis_index(GX), lax.axis_index(GY)
    flags = jnp.stack(
        [
            (place_x % 2 == 0).astype(jnp.int32),
            (place_x > 0).astype(jnp.int32),
            (place_x < count_x - 1).astype(jnp.int32),
            (place_y % 2 == 0).astype(jnp.int32),
            (place_y > 0).astype(jnp.int32),
            (place_y < count_y - 1).astype(jnp.int32),
        ]
    )

    def swap(value, axes, move):
        return lax.ppermute(value, ALL, device_pairs(mesh, axes, move))

    def swap_both(pair, axes):
        second = swap(pair[1], axes, across)
        return swap(pair[0], axes, beside), second

    offs = jnp.broadcast_to(offsets[..., None], offsets.shape + (LANES,))
    x_out = call(
        functools.partial(first_kernel, s),
        [(s.x_rows_mats, LANES)] * 2,
        1000,
        flags,
        fine_disp,
        coarse_disp,
        fine_rigidity,
        fine_metric,
        coarse_rigidity,
        coarse_metric,
        name="first_strips",
    )
    own = []
    for tag, density, lame, rigidity, metric in (
        ("fine", fine_density, fine_lame, fine_rigidity, fine_metric),
        ("coarse", coarse_density, coarse_lame, coarse_rigidity, coarse_metric),
    ):
        own.append(
            call(
                own_kernel,
                [metric.shape] * 6,
                2_000_000,
                density,
                lame,
                rigidity,
                metric,
                name=f"own_{tag}",
                table=False,
            )
        )
    inverse_f, *coef_f = own[0]
    inverse_c, *coef_c = own[1]

    fine, coarse = fine_disp, coarse_disp
    fine_ext = (s.fx + 2, s.fy + 16, s.fz)
    coarse_ext = (s.cx + 2, s.cy + 16, s.cz)
    scratch = [
        (3, s.fe, s.fy + 16, s.fz),
        (3, s.ce, s.cy + 16, s.cz),
        fine_ext,
        coarse_ext,
        (s.ce, 2 * (s.cy + 4), LANES),
        (3, s.cx, s.fy, LANES),
    ]
    energy = None
    for step in range(STEPS):
        first, final = step == 0, step == STEPS - 1
        raw = [fine_rigidity, fine_metric, coarse_rigidity, coarse_metric] if first else []
        x_in = swap_both(x_out, GX)
        y_out = call(
            functools.partial(middle_kernel, s, first),
            [(s.y_rows_mats if first else s.y_rows, 2, LANES)] * 2,
            1000,
            flags,
            fine,
            coarse,
            *raw,
            *x_in,
            name=f"corner_strips_{step}",
        )
        y_in = swap_both(y_out, GY)
        if first:
            extra = [fine_rigidity, fine_metric, inverse_f, coarse_rigidity, coarse_metric, inverse_c]
        else:
            extra = [*ext_mats, energy]
        shapes = [fine.shape, coarse.shape, (8, LANES)]
        if not final:
            shapes += [(s.x_rows, LANES)] * 2
        if first:
            shapes += [fine_ext, fine_ext, coarse_ext, coarse_ext]
        outs = call(
            functools.partial(step_kernel, s, step),
            shapes,
            4_000_000,
            flags,
            fine,
            coarse,
            fine_prev,
            coarse_prev,
            offs,
            *coef_f,
            *coef_c,
            *extra,
            *x_in,
            *y_in,
            scratch=scratch,
            name=f"step_{step}",
        )
        fine_prev, coarse_prev = fine, coarse
        fine, coarse, energy = outs[:3]
        if not final:
            x_out = outs[3:5]
        if first:
            ext_mats = outs[5:9]
    total = total_over_mesh(energy, swap)
    cells = [count_x * count_y * s.fx * s.fy * s.fz, count_x * count_y * s.cx * s.cy * s.cz]
    energy = total[: 2 * STEPS, 0].reshape(STEPS, 2) / jnp.array(cells, jnp.float32)
    return fine, coarse, energy


def solution(mesh):
    finer = Mesh(mesh.devices.reshape(8, 4, 4, 2), ALL)
    level, cell = P(None, GX, GY, None), P(GX, GY, None)
    in_specs = (level,) * 4 + (cell,) * 8 + (P(None, GX, GY),)
    return jax.shard_map(
        functools.partial(per_device, finer),
        mesh=finer,
        in_specs=in_specs,
        out_specs=(level, level, P()),
        check_vma=False,
    )
```

```python
import functools

import jax
import jax.numpy as jnp
from jax import lax
from jax.experimental import pallas as pl
from jax.experimental.pallas import tpu as pltpu
from jax.sharding import Mesh
from jax.sharding import PartitionSpec as P

STEPS = 3
GX = ("gx_0", "gx_1")
GY = ("gy_0", "gy_1")
ALL = GX + GY
STEP = 0.15
LANES = 128
VMEM_LIMIT = 20 * 1024 * 1024

EVEN_X, HAS_XM, HAS_XP, EVEN_Y, HAS_YM, HAS_YP = range(6)


class Sizes:
    def __init__(self, fine, coarse):
        self.fx, self.fy, self.fz = fine
        self.cx, self.cy, self.cz = coarse
        self.halves = self.cz // LANES
        self.x_fine = 0
        self.x_coarse = 6 * self.fy
        self.x_rows = self.x_coarse + self.halves * 6 * self.cy
        self.x_fine_mats = self.x_rows
        self.x_coarse_mats = self.x_fine_mats + 2 * self.fy
        self.x_rows_mats = self.x_coarse_mats + 2 * self.halves * self.cy
        self.fe, self.ce = self.fx + 4, self.cx + 4
        self.y_coarse = 3 * self.fe
        self.y_rows = self.y_coarse + self.halves * 3 * self.ce
        self.y_fine_mats = self.y_rows
        self.y_coarse_mats = self.y_fine_mats + self.fx
        self.y_rows_mats = self.y_coarse_mats + self.halves * self.cx


def lanes_of(h):
    return slice(h * LANES, (h + 1) * LANES)


def put_x(s, flags, outs, fine, coarse):
    even = flags[EVEN_X] == 1
    for k, out in enumerate(outs):
        far = even if k == 0 else jnp.logical_not(even)
        start_f = jnp.where(far, s.fx - 2, 0)
        start_c = jnp.where(far, s.cx - 2, 0)
        out[0 : s.x_coarse, :] = fine[:, pl.ds(start_f, 2), :, :].reshape(6 * s.fy, LANES)
        strip = coarse[:, pl.ds(start_c, 2), :, :]
        for h in range(s.halves):
            base = s.x_coarse + h * 6 * s.cy
            out[base : base + 6 * s.cy, :] = strip[:, :, :, lanes_of(h)].reshape(6 * s.cy, LANES)


def first_kernel(s, flags, fine, coarse, rig_f, met_f, rig_c, met_c, out_a, out_b, *scratch):
    strip_f, strip_c, line_f, line_c, sems = scratch
    copies = []

    def fetch(source, target):
        copies.append(pltpu.make_async_copy(source, target, sems.at[len(copies)]))
        copies[-1].start()

    even = flags[EVEN_X] == 1
    for k in range(2):
        far = even if k == 0 else jnp.logical_not(even)
        fetch(fine.at[:, pl.ds(jnp.where(far, s.fx - 2, 0), 2)], strip_f.at[k])
        fetch(coarse.at[:, pl.ds(jnp.where(far, s.cx - 2, 0), 2)], strip_c.at[k])
        for m, (of_f, of_c) in enumerate(((rig_f, rig_c), (met_f, met_c))):
            fetch(of_f.at[jnp.where(far, s.fx - 1, 0)], line_f.at[k, m])
            fetch(of_c.at[jnp.where(far, s.cx - 1, 0)], line_c.at[k, m])
    for copy in copies:
        copy.wait()
    for k, out in enumerate((out_a, out_b)):
        out[0 : s.x_coarse, :] = strip_f[k].reshape(6 * s.fy, LANES)
        for m in range(2):
            base = s.x_fine_mats + m * s.fy
            out[base : base + s.fy, :] = line_f[k, m]
        for h in range(s.halves):
            base = s.x_coarse + h * 6 * s.cy
            out[base : base + 6 * s.cy, :] = strip_c[k, :, :, :, lanes_of(h)].reshape(6 * s.cy, LANES)
            for m in range(2):
                base = s.x_coarse_mats + (m * s.halves + h) * s.cy
                out[base : base + s.cy, :] = line_c[k, m, :, lanes_of(h)]


def sides(flags, even, has_low, has_high, a, b):
    low = jnp.where(flags[even] == 1, b, a)
    high = jnp.where(flags[even] == 1, a, b)
    low = jnp.where(flags[has_low] == 1, low, 0.0)
    high = jnp.where(flags[has_high] == 1, high, 0.0)
    return low, high


def middle_kernel(s, with_mats, flags, *refs):
    if with_mats:
        fine, coarse, rig_f, met_f, rig_c, met_c, in_a, in_b, out_a, out_b = refs
    else:
        fine, coarse, in_a, in_b, out_a, out_b = refs
    even = flags[EVEN_Y] == 1

    def put(index, low, high):
        out_a[index] = jnp.where(even, high, low)
        out_b[index] = jnp.where(even, low, high)

    for c in range(3):
        own = pl.ds(c * s.fe + 2, s.fx)
        put(own, fine[c, :, 0:2, :], fine[c, :, s.fy - 2 : s.fy, :])
        for k in range(2):
            base = (c * 2 + k) * s.fy
            pieces = []
            for first in (0, s.fy - 2):
                rows = slice(base + first, base + first + 2)
                pieces.append(sides(flags, EVEN_X, HAS_XM, HAS_XP, in_a[rows, :], in_b[rows, :]))
            for side in range(2):
                place = c * s.fe + (k if side == 0 else s.fx + 2 + k)
                put(place, pieces[0][side], pieces[1][side])
        for h in range(s.halves):
            origin = s.y_coarse + (h * 3 + c) * s.ce
            own = pl.ds(origin + 2, s.cx)
            put(own, coarse[c, :, 0:2, lanes_of(h)], coarse[c, :, s.cy - 2 : s.cy, lanes_of(h)])
            for k in range(2):
                base = s.x_coarse + (h * 6 + c * 2 + k) * s.cy
                pieces = []
                for first in (0, s.cy - 2):
                    rows = slice(base + first, base + first + 2)
                    pieces.append(
                        sides(flags, EVEN_X, HAS_XM, HAS_XP, in_a[rows, :], in_b[rows, :])
                    )
                for side in range(2):
                    place = origin + (k if side == 0 else s.cx + 2 + k)
                    put(place, pieces[0][side], pieces[1][side])
    if not with_mats:
        return
    for m, (of_f, of_c) in enumerate(((rig_f, rig_c), (met_f, met_c))):
        low, high = of_f[:, 0:1, :], of_f[:, s.fy - 1 : s.fy, :]
        where = pl.ds(s.y_fine_mats, s.fx)
        out_a[where, m : m + 1, :] = jnp.where(even, high, low)
        out_b[where, m : m + 1, :] = jnp.where(even, low, high)
        for h in range(s.halves):
            low, high = of_c[:, 0:1, lanes_of(h)], of_c[:, s.cy - 1 : s.cy, lanes_of(h)]
            where = pl.ds(s.y_coarse_mats + h * s.cx, s.cx)
            out_a[where, m : m + 1, :] = jnp.where(even, high, low)
            out_b[where, m : m + 1, :] = jnp.where(even, low, high)


def up_one(x):
    return pltpu.roll(x, x.shape[-1] - 1, x.ndim - 1)


def down_one(x):
    return pltpu.roll(x, 1, x.ndim - 1)


def own_kernel(density, lame, rigidity, metric, inverse, c1, c2, weight, above, first):
    inv = 1.0 / metric[...]
    inverse[...] = inv
    over = 1.0 / density[...]
    c1[...] = inv * over
    c2[...] = (lame[...] + rigidity[...]) * over
    weight[...] = density[...] * metric[...]
    v = rigidity[...] * inv
    lane = lax.broadcasted_iota(jnp.int32, v.shape, 2)
    above[...] = jnp.where(lane == v.shape[2] - 1, v, 0.5 * (v + up_one(v)))
    first[...] = v[:, :, 0:LANES]


def slope(f, up, down, lane):
    last = f.shape[-1] - 1
    return jnp.where(lane == 0, up - f, jnp.where(lane == last, f - down, 0.5 * (up - down)))


def fill_displacement(s, flags, own, ext, x_in, y_in, fine):
    x, y, e = (s.fx, s.fy, s.fe) if fine else (s.cx, s.cy, s.ce)
    ext[:, 2 : 2 + x, 8 : 8 + y, :] = own[...]
    for h in range(1 if fine else s.halves):
        base = s.x_fine if fine else s.x_coarse + h * 6 * y
        rows = slice(base, base + 6 * y)
        low, high = sides(flags, EVEN_X, HAS_XM, HAS_XP, x_in[0][rows, :], x_in[1][rows, :])
        ext[:, 0:2, 8 : 8 + y, lanes_of(h)] = low.reshape(3, 2, y, LANES)
        ext[:, x + 2 : x + 4, 8 : 8 + y, lanes_of(h)] = high.reshape(3, 2, y, LANES)
        for c in range(3):
            start = c * e if fine else s.y_coarse + (h * 3 + c) * e
            rows = slice(start, start + e)
            low, high = sides(flags, EVEN_Y, HAS_YM, HAS_YP, y_in[0][rows], y_in[1][rows])
            ext[c, :, 6:8, lanes_of(h)] = low
            ext[c, :, 8 + y : 10 + y, lanes_of(h)] = high


def fill_materials(s, flags, rigidity, metric, inverse, wide_ext, inv_ext, x_in, y_in, fine):
    x, y = (s.fx, s.fy) if fine else (s.cx, s.cy)
    wide_ext[1 : 1 + x, 1 : 1 + y, :] = rigidity[...] * metric[...]
    inv_ext[1 : 1 + x, 1 : 1 + y, :] = inverse[...]
    for h in range(1 if fine else s.halves):
        at = lanes_of(h)
        got = []
        for m in range(2):
            base = s.x_fine_mats + m * y if fine else s.x_coarse_mats + (m * s.halves + h) * y
            rows = slice(base, base + y)
            even = flags[EVEN_X] == 1
            a, b = x_in[0][rows, :], x_in[1][rows, :]
            got.append((jnp.where(even, b, a), jnp.where(even, a, b)))
        for side, (flag, place) in enumerate(((HAS_XM, 0), (HAS_XP, x + 1))):
            rig, met = got[0][side], got[1][side]
            wide_ext[place, 1 : 1 + y, at] = jnp.where(flags[flag] == 1, rig * met, 0.0)
            inv_ext[place, 1 : 1 + y, at] = jnp.where(flags[flag] == 1, 1.0 / met, 0.0)
        start = s.y_fine_mats if fine else s.y_coarse_mats + h * x
        rows = slice(start, start + x)
        got = []
        for m in range(2):
            even = flags[EVEN_Y] == 1
            a, b = y_in[0][rows, m : m + 1, :], y_in[1][rows, m : m + 1, :]
            got.append((jnp.where(even, b, a), jnp.where(even, a, b)))
        for side, (flag, place) in enumerate(((HAS_YM, 0), (HAS_YP, 1 + y))):
            rig, met = got[0][side], got[1][side]
            wide_ext[1 : 1 + x, place : place + 1, at] = jnp.where(flags[flag] == 1, rig * met, 0.0)
            inv_ext[1 : 1 + x, place : place + 1, at] = jnp.where(flags[flag] == 1, 1.0 / met, 0.0)


def fill_divergence(x, y, ext, inv_ext, div):
    z = ext.shape[-1]
    lane = lax.broadcasted_iota(jnp.int32, (y + 2, z), 1)

    def row(r, carry):
        along_x = ext[0, r + 2, 7 : 9 + y, :] - ext[0, r, 7 : 9 + y, :]
        along_y = ext[1, r + 1, 8 : 10 + y, :] - ext[1, r + 1, 6 : 8 + y, :]
        f = ext[2, r + 1, 7 : 9 + y, :]
        inv = inv_ext[r, 0 : 2 + y, :]
        total = 0.5 * along_x + 0.5 * along_y + inv * slope(f, up_one(f), down_one(f), lane)
        div[r, 7 : 9 + y, :] = jnp.where(inv > 0.0, total, 0.0)
        return carry

    lax.fori_loop(0, x + 2, row, 0, unroll=True)


def update(x, y, ext, wide_ext, inv_ext, div, prev, coef, new, ghosts):
    c1, c2, weight, above, vertical = coef
    z = ext.shape[-1]
    lane = lax.broadcasted_iota(jnp.int32, (y, z), 1)
    mid, left, right, own = slice(8, 8 + y), slice(7, 7 + y), slice(9, 9 + y), slice(1, 1 + y)

    def row(i, total):
        wide = wide_ext[i + 1, own, :]
        w_xp = 0.5 * (wide + wide_ext[i + 2, own, :])
        w_xm = 0.5 * (wide_ext[i, own, :] + wide)
        w_yp = 0.5 * (wide + wide_ext[i + 1, 2 : 2 + y, :])
        w_ym = 0.5 * (wide_ext[i + 1, 0:y, :] + wide)
        inv = inv_ext[i + 1, own, :]
        f = div[i + 1, mid, :]
        gradient = (
            0.5 * (div[i + 2, mid, :] - div[i, mid, :]),
            0.5 * (div[i + 1, right, :] - div[i + 1, left, :]),
            inv * slope(f, up_one(f), down_one(f), lane),
        )
        top, bottom = ghosts(i)
        k1, k2, dm, va = c1[i], c2[i], weight[i], above[i]
        inner = jnp.zeros((y, z), jnp.float32)
        for c in range(3):
            u = ext[c, i + 2, mid, :]
            up = jnp.where(lane == z - 1, bottom(c), up_one(u))
            flux = w_xp * (ext[c, i + 3, mid, :] - u) - w_xm * (u - ext[c, i + 1, mid, :])
            flux += w_yp * (ext[c, i + 2, right, :] - u) - w_ym * (u - ext[c, i + 2, left, :])
            over = va * (up - u)
            entry = 0.0 if top is None else vertical[i, :, 0:1] * (u[:, 0:1] - top(c))
            flux += over - jnp.where(lane == 0, entry, down_one(over))
            rate = flux * k1 + k2 * gradient[c]
            updated = 2.0 * u - prev[c, i] + STEP * rate
            change = updated - u
            inner += change * change - STEP * updated * rate
            new[c, i] = updated
        return total + dm * inner

    return lax.fori_loop(0, x, row, jnp.zeros((y, z), jnp.float32), unroll=4)


def step_kernel(s, step, cells, flags, *refs):
    refs = list(refs)

    def take(n):
        out = refs[:n]
        del refs[:n]
        return out

    fine, coarse, fine_prev, coarse_prev, offs = take(5)
    coef_f, coef_c = take(5), take(5)
    first, final = step == 0, step == STEPS - 1
    if first:
        rig_f, met_f, inverse_f, rig_c, met_c, inverse_c = take(6)
    else:
        wide_f, inv_f, wide_c, inv_c, energy_in = take(5)
    x_in, y_in = take(2), take(2)
    new_f, new_c, energy = take(3)
    if not final:
        x_out = take(2)
    if first:
        wide_f, inv_f, wide_c, inv_c = take(4)
    ext_f, ext_c, div_f, div_c, double, pairs = take(6)

    fill_displacement(s, flags, fine, ext_f, x_in, y_in, True)
    fill_displacement(s, flags, coarse, ext_c, x_in, y_in, False)
    if first:
        fill_materials(s, flags, rig_f, met_f, inverse_f, wide_f, inv_f, x_in, y_in, True)
        fill_materials(s, flags, rig_c, met_c, inverse_c, wide_c, inv_c, x_in, y_in, False)

    lane = lax.broadcasted_iota(jnp.int32, (s.cy + 4, LANES), 1)
    for i in range(s.ce):
        e0, e1, e2 = (ext_c[c, i, 6 : 10 + s.cy, 0:LANES] for c in range(3))
        e1, e2 = pltpu.roll(e1, 1, 1), pltpu.roll(e2, 2, 1)
        plane = jnp.where(lane == 0, e0, jnp.where(lane == 1, e1, e2))
        for j in range(s.cy + 4):
            double[i, 2 * j : 2 * j + 2, :] = jnp.broadcast_to(plane[j : j + 1, :], (2, LANES))
    for c in range(3):
        for i in range(s.cx):
            pairs[c, i] = fine[c, 2 * i] + fine[c, 2 * i + 1]

    fill_divergence(s.fx, s.fy, ext_f, inv_f, div_f)
    fill_divergence(s.cx, s.cy, ext_c, inv_c, div_c)

    odd_y = lax.broadcasted_iota(jnp.int32, (s.fy, LANES), 0) % 2
    near_y = jnp.where(odd_y == 0, 0.75, 0.25)

    def fine_ghosts(i):
        half = i // 2
        near_x = jnp.where(i % 2 == 0, 0.75, 0.25)
        off_x, off_y = offs[i] // 4 - 1, offs[i] % 4 - 1
        total = jnp.zeros((s.fy, LANES), jnp.float32)
        weights = []
        for shift in (-1, 0, 1, 2):
            weights.append(
                jnp.where(off_y == shift, near_y, 0.0)
                + jnp.where(off_y == shift - 1, 1.0 - near_y, 0.0)
            )
        for shift in (-1, 0, 1, 2):
            weight_x = jnp.where(off_x == shift, near_x, 0.0) + jnp.where(
                off_x == shift - 1, 1.0 - near_x, 0.0
            )
            line = jnp.zeros((s.fy, LANES), jnp.float32)
            for k in range(4):
                line += weights[k] * double[half + 2 + shift, 2 * k + 2 : 2 * k + 2 + s.fy, :]
            total += weight_x * line
        return None, lambda c: pltpu.roll(total, LANES - 1 - c, 1)

    def coarse_ghosts(i):
        def top(c):
            both = pairs[c, i, pl.ds(0, s.cy, stride=2), :] + pairs[c, i, pl.ds(1, s.cy, stride=2), :]
            return 0.25 * both[:, LANES - 1 :]

        return top, lambda c: jnp.zeros((s.cy, s.cz), jnp.float32)

    sum_f = update(s.fx, s.fy, ext_f, wide_f, inv_f, div_f, fine_prev, coef_f, new_f, fine_ghosts)
    sum_c = update(
        s.cx, s.cy, ext_c, wide_c, inv_c, div_c, coarse_prev, coef_c, new_c, coarse_ghosts
    )
    place = lax.broadcasted_iota(jnp.int32, (8, LANES), 0)
    before = jnp.zeros((8, LANES), jnp.float32) if first else energy_in[...]
    before = jnp.where(place == step, jnp.sum(sum_f) / cells[0], before)
    energy[...] = jnp.where(place == STEPS + step, jnp.sum(sum_c) / cells[1], before)
    if not final:
        put_x(s, flags, x_out, new_f, new_c)


VMEM = pl.BlockSpec(memory_space=pltpu.VMEM)
SMEM = pl.BlockSpec(memory_space=pltpu.SMEM)
HBM = pl.BlockSpec(memory_space=pltpu.HBM)


def call(kernel, shapes, flops, *args, scratch=(), name=None, specs=None, sems=0):
    shapes = [jax.ShapeDtypeStruct(shape, jnp.float32) for shape in shapes]
    scratch = [pltpu.VMEM(shape, jnp.float32) for shape in scratch]
    if sems:
        scratch.append(pltpu.SemaphoreType.DMA((sems,)))
    return pl.pallas_call(
        kernel,
        out_shape=shapes,
        in_specs=specs or [SMEM] + [VMEM] * (len(args) - 1),
        out_specs=[VMEM] * len(shapes),
        scratch_shapes=scratch,
        compiler_params=pltpu.CompilerParams(vmem_limit_bytes=VMEM_LIMIT),
        cost_estimate=pl.CostEstimate(flops=flops, bytes_accessed=1 << 20, transcendentals=0),
        name=name,
    )(*args)


def across(i, n):
    return (i + 1) % n if i % 2 else (i - 1) % n


def opposite(i, n):
    return (i - 3) % n if i % 2 else (i + 3) % n


def device_pairs(mesh, axes, move):
    sizes = dict(mesh.shape)
    names = list(sizes)
    total = 1
    for name in names:
        total *= sizes[name]
    count = 1
    for name in axes:
        count *= sizes[name]
    pairs = []
    for source in range(total):
        rest, at = source, {}
        for name in reversed(names):
            at[name] = rest % sizes[name]
            rest //= sizes[name]
        index = 0
        for name in axes:
            index = index * sizes[name] + at[name]
        index = move(index, count)
        for name in reversed(axes):
            at[name] = index % sizes[name]
            index //= sizes[name]
        target = 0
        for name in names:
            target = target * sizes[name] + at[name]
        pairs.append((source, target))
    return pairs


def beside(i, n):
    return i ^ 1


def total_over_mesh(value, swap):
    lane = lax.broadcasted_iota(jnp.int32, (8, LANES), 1)

    def ring_of_eight(value, axes):
        value = value + swap(value, axes, beside)
        pair = lax.axis_index(axes) // 2
        slots = jnp.where(lane == pair, value, 0.0)
        slots = slots + swap(slots, axes, across)
        slots = slots + swap(slots, axes, opposite)
        return jnp.broadcast_to(jnp.sum(slots[:, 0:4], axis=1, keepdims=True), (8, LANES))

    value = ring_of_eight(value, GY)
    value = value + swap(value, ("gx_1",), beside)
    value = value + swap(value, ("gx_1",), across)
    return ring_of_eight(value, ("gx_0",))


def per_device(
    mesh,
    fine_disp,
    fine_prev,
    coarse_disp,
    coarse_prev,
    fine_density,
    fine_lame,
    fine_rigidity,
    fine_metric,
    coarse_density,
    coarse_lame,
    coarse_rigidity,
    coarse_metric,
    offsets,
):
    fine_shape, coarse_shape = fine_metric.shape, coarse_metric.shape
    s = Sizes(fine_shape, coarse_shape)
    count_x, count_y = lax.axis_size(GX), lax.axis_size(GY)
    place_x, place_y = lax.axis_index(GX), lax.axis_index(GY)
    flags = jnp.stack(
        [
            (place_x % 2 == 0).astype(jnp.int32),
            (place_x > 0).astype(jnp.int32),
            (place_x < count_x - 1).astype(jnp.int32),
            (place_y % 2 == 0).astype(jnp.int32),
            (place_y > 0).astype(jnp.int32),
            (place_y < count_y - 1).astype(jnp.int32),
        ]
    )

    def swap(value, axes, move):
        return lax.ppermute(value, ALL, device_pairs(mesh, axes, move))

    def swap_both(pair, axes):
        second = swap(pair[1], axes, across)
        first = swap(pair[0], axes, beside)
        return [pltpu.with_memory_space_constraint(x, pltpu.VMEM) for x in (first, second)]

    offs = offsets[0] * 4 + offsets[1] + 5
    offs = jnp.broadcast_to(offs[..., None], offs.shape + (LANES,))
    x_out = call(
        functools.partial(first_kernel, s),
        [(s.x_rows_mats, LANES)] * 2,
        1000,
        flags,
        *(
            pltpu.with_memory_space_constraint(x, pltpu.HBM)
            for x in (
                fine_disp,
                coarse_disp,
                fine_rigidity,
                fine_metric,
                coarse_rigidity,
                coarse_metric,
            )
        ),
        scratch=[
            (2, 3, 2, s.fy, s.fz),
            (2, 3, 2, s.cy, s.cz),
            (2, 2, s.fy, s.fz),
            (2, 2, s.cy, s.cz),
        ],
        specs=[SMEM] + [HBM] * 6,
        sems=12,
        name="first_strips",
    )
    own = []
    for tag, density, lame, rigidity, metric in (
        ("fine", fine_density, fine_lame, fine_rigidity, fine_metric),
        ("coarse", coarse_density, coarse_lame, coarse_rigidity, coarse_metric),
    ):
        own.append(
            call(
                own_kernel,
                [metric.shape] * 5 + [metric.shape[:2] + (LANES,)],
                2_000_000,
                density,
                lame,
                rigidity,
                metric,
                name=f"own_{tag}",
                specs=[VMEM] * 4,
            )
        )
    inverse_f, *coef_f = own[0]
    inverse_c, *coef_c = own[1]

    fine, coarse = fine_disp, coarse_disp
    fine_ext = (s.fx + 2, s.fy + 2, s.fz)
    coarse_ext = (s.cx + 2, s.cy + 2, s.cz)
    scratch = [
        (3, s.fe, s.fy + 16, s.fz),
        (3, s.ce, s.cy + 16, s.cz),
        (s.fx + 2, s.fy + 16, s.fz),
        (s.cx + 2, s.cy + 16, s.cz),
        (s.ce, 2 * (s.cy + 4), LANES),
        (3, s.cx, s.fy, LANES),
    ]
    cells = [count_x * count_y * s.fx * s.fy * s.fz, count_x * count_y * s.cx * s.cy * s.cz]
    energy = None
    for step in range(STEPS):
        first, final = step == 0, step == STEPS - 1
        raw = [fine_rigidity, fine_metric, coarse_rigidity, coarse_metric] if first else []
        x_in = swap_both(x_out, GX)
        y_out = call(
            functools.partial(middle_kernel, s, first),
            [(s.y_rows_mats if first else s.y_rows, 2, LANES)] * 2,
            1000,
            flags,
            fine,
            coarse,
            *raw,
            *x_in,
            name=f"corner_strips_{step}",
        )
        y_in = swap_both(y_out, GY)
        if first:
            extra = [fine_rigidity, fine_metric, inverse_f, coarse_rigidity, coarse_metric, inverse_c]
        else:
            extra = [*ext_mats, energy]
        shapes = [fine.shape, coarse.shape, (8, LANES)]
        if not final:
            shapes += [(s.x_rows, LANES)] * 2
        if first:
            shapes += [fine_ext, fine_ext, coarse_ext, coarse_ext]
        outs = call(
            functools.partial(step_kernel, s, step, cells),
            shapes,
            4_000_000,
            flags,
            fine,
            coarse,
            fine_prev,
            coarse_prev,
            offs,
            *coef_f,
            *coef_c,
            *extra,
            *x_in,
            *y_in,
            scratch=scratch,
            name=f"step_{step}",
        )
        fine_prev, coarse_prev = fine, coarse
        fine, coarse, energy = outs[:3]
        if not final:
            x_out = outs[3:5]
        if first:
            ext_mats = outs[5:9]
    total = total_over_mesh(energy, swap)
    energy = total[: 2 * STEPS, 0].reshape(2, STEPS).T
    return fine, coarse, energy


def solution(mesh):
    finer = Mesh(mesh.devices.reshape(8, 4, 4, 2), ALL)
    level, cell = P(None, GX, GY, None), P(GX, GY, None)
    in_specs = (level,) * 4 + (cell,) * 8 + (P(None, GX, GY),)
    return jax.shard_map(
        functools.partial(per_device, finer),
        mesh=finer,
        in_specs=in_specs,
        out_specs=(level, level, P()),
        check_vma=False,
    )
```

```python
import functools
import math

import jax
import jax.numpy as jnp
from jax import lax
from jax.experimental import pallas as pl
from jax.experimental.pallas import tpu as pltpu
from jax.sharding import Mesh
from jax.sharding import PartitionSpec as P

STEPS = 3
GX = ("gx_0", "gx_1")
GY = ("gy_0", "gy_1")
ALL = GX + GY
STEP = 0.15
LANES = 128
VMEM_LIMIT = 20 * 1024 * 1024

EVEN_X, HAS_XM, HAS_XP, EVEN_Y, HAS_YM, HAS_YP = range(6)


class Sizes:
    def __init__(self, fine, coarse):
        self.fx, self.fy, self.fz = fine
        self.cx, self.cy, self.cz = coarse
        self.halves = self.cz // LANES
        self.x_fine = 0
        self.x_coarse = 6 * self.fy
        self.x_rows = self.x_coarse + self.halves * 6 * self.cy
        self.x_fine_mats = self.x_rows
        self.x_coarse_mats = self.x_fine_mats + 2 * self.fy
        self.x_rows_mats = self.x_coarse_mats + 2 * self.halves * self.cy
        self.fe, self.ce = self.fx + 4, self.cx + 4
        self.y_coarse = 3 * self.fe
        self.y_rows = self.y_coarse + self.halves * 3 * self.ce
        self.y_fine_mats = self.y_rows
        self.y_coarse_mats = self.y_fine_mats + self.fx
        self.y_rows_mats = self.y_coarse_mats + self.halves * self.cx


def lanes_of(h):
    return slice(h * LANES, (h + 1) * LANES)


def put_x(s, flags, outs, fine, coarse):
    even = flags[EVEN_X] == 1
    for k, out in enumerate(outs):
        far = even if k == 0 else jnp.logical_not(even)
        start_f = jnp.where(far, s.fx - 2, 0)
        start_c = jnp.where(far, s.cx - 2, 0)
        out[0 : s.x_coarse, :] = fine[:, pl.ds(start_f, 2), :, :].reshape(6 * s.fy, LANES)
        strip = coarse[:, pl.ds(start_c, 2), :, :]
        for h in range(s.halves):
            base = s.x_coarse + h * 6 * s.cy
            out[base : base + 6 * s.cy, :] = strip[:, :, :, lanes_of(h)].reshape(6 * s.cy, LANES)


def first_kernel(s, flags, fine, coarse, rig_f, met_f, rig_c, met_c, out_a, out_b, *scratch):
    strip_f, strip_c, line_f, line_c, sems = scratch
    copies = []

    def fetch(source, target):
        copies.append(pltpu.make_async_copy(source, target, sems.at[len(copies)]))
        copies[-1].start()

    even = flags[EVEN_X] == 1
    for k in range(2):
        far = even if k == 0 else jnp.logical_not(even)
        fetch(fine.at[:, pl.ds(jnp.where(far, s.fx - 2, 0), 2)], strip_f.at[k])
        fetch(coarse.at[:, pl.ds(jnp.where(far, s.cx - 2, 0), 2)], strip_c.at[k])
        for m, (of_f, of_c) in enumerate(((rig_f, rig_c), (met_f, met_c))):
            fetch(of_f.at[jnp.where(far, s.fx - 1, 0)], line_f.at[k, m])
            fetch(of_c.at[jnp.where(far, s.cx - 1, 0)], line_c.at[k, m])
    for copy in copies:
        copy.wait()
    for k, out in enumerate((out_a, out_b)):
        out[0 : s.x_coarse, :] = strip_f[k].reshape(6 * s.fy, LANES)
        for m in range(2):
            base = s.x_fine_mats + m * s.fy
            out[base : base + s.fy, :] = line_f[k, m]
        for h in range(s.halves):
            base = s.x_coarse + h * 6 * s.cy
            out[base : base + 6 * s.cy, :] = strip_c[k, :, :, :, lanes_of(h)].reshape(6 * s.cy, LANES)
            for m in range(2):
                base = s.x_coarse_mats + (m * s.halves + h) * s.cy
                out[base : base + s.cy, :] = line_c[k, m, :, lanes_of(h)]


def sides(flags, even, has_low, has_high, a, b):
    low = jnp.where(flags[even] == 1, b, a)
    high = jnp.where(flags[even] == 1, a, b)
    low = jnp.where(flags[has_low] == 1, low, 0.0)
    high = jnp.where(flags[has_high] == 1, high, 0.0)
    return low, high


def middle_kernel(s, with_mats, flags, *refs):
    if with_mats:
        fine, coarse, rig_f, met_f, rig_c, met_c, in_a, in_b, out_a, out_b = refs
    else:
        fine, coarse, in_a, in_b, out_a, out_b = refs
    even = flags[EVEN_Y] == 1

    def put(index, low, high):
        out_a[index] = jnp.where(even, high, low)
        out_b[index] = jnp.where(even, low, high)

    for c in range(3):
        own = pl.ds(c * s.fe + 2, s.fx)
        put(own, fine[c, :, 0:2, :], fine[c, :, s.fy - 2 : s.fy, :])
        for k in range(2):
            base = (c * 2 + k) * s.fy
            pieces = []
            for first in (0, s.fy - 2):
                rows = slice(base + first, base + first + 2)
                pieces.append(sides(flags, EVEN_X, HAS_XM, HAS_XP, in_a[rows, :], in_b[rows, :]))
            for side in range(2):
                place = c * s.fe + (k if side == 0 else s.fx + 2 + k)
                put(place, pieces[0][side], pieces[1][side])
        for h in range(s.halves):
            origin = s.y_coarse + (h * 3 + c) * s.ce
            own = pl.ds(origin + 2, s.cx)
            put(own, coarse[c, :, 0:2, lanes_of(h)], coarse[c, :, s.cy - 2 : s.cy, lanes_of(h)])
            for k in range(2):
                base = s.x_coarse + (h * 6 + c * 2 + k) * s.cy
                pieces = []
                for first in (0, s.cy - 2):
                    rows = slice(base + first, base + first + 2)
                    pieces.append(
                        sides(flags, EVEN_X, HAS_XM, HAS_XP, in_a[rows, :], in_b[rows, :])
                    )
                for side in range(2):
                    place = origin + (k if side == 0 else s.cx + 2 + k)
                    put(place, pieces[0][side], pieces[1][side])
    if not with_mats:
        return
    for m, (of_f, of_c) in enumerate(((rig_f, rig_c), (met_f, met_c))):
        low, high = of_f[:, 0:1, :], of_f[:, s.fy - 1 : s.fy, :]
        where = pl.ds(s.y_fine_mats, s.fx)
        out_a[where, m : m + 1, :] = jnp.where(even, high, low)
        out_b[where, m : m + 1, :] = jnp.where(even, low, high)
        for h in range(s.halves):
            low, high = of_c[:, 0:1, lanes_of(h)], of_c[:, s.cy - 1 : s.cy, lanes_of(h)]
            where = pl.ds(s.y_coarse_mats + h * s.cx, s.cx)
            out_a[where, m : m + 1, :] = jnp.where(even, high, low)
            out_b[where, m : m + 1, :] = jnp.where(even, low, high)


def up_one(x):
    return pltpu.roll(x, x.shape[-1] - 1, x.ndim - 1)


def down_one(x):
    return pltpu.roll(x, 1, x.ndim - 1)


def own_kernel(density, lame, rigidity, metric, inverse, c1, c2, weight, above, first):
    inv = 1.0 / metric[...]
    inverse[...] = inv
    over = 1.0 / density[...]
    c1[...] = inv * over
    c2[...] = (lame[...] + rigidity[...]) * over
    weight[...] = density[...] * metric[...]
    v = rigidity[...] * inv
    lane = lax.broadcasted_iota(jnp.int32, v.shape, 2)
    above[...] = jnp.where(lane == v.shape[2] - 1, v, 0.5 * (v + up_one(v)))
    first[...] = v[:, :, 0:LANES]


def slope(f, up, down, lane):
    last = f.shape[-1] - 1
    return jnp.where(lane == 0, up - f, jnp.where(lane == last, f - down, 0.5 * (up - down)))


def fill_displacement(s, flags, own, ext, x_in, y_in, fine):
    x, y, e = (s.fx, s.fy, s.fe) if fine else (s.cx, s.cy, s.ce)
    ext[:, 2 : 2 + x, 8 : 8 + y, :] = own[...]
    for h in range(1 if fine else s.halves):
        base = s.x_fine if fine else s.x_coarse + h * 6 * y
        rows = slice(base, base + 6 * y)
        low, high = sides(flags, EVEN_X, HAS_XM, HAS_XP, x_in[0][rows, :], x_in[1][rows, :])
        ext[:, 0:2, 8 : 8 + y, lanes_of(h)] = low.reshape(3, 2, y, LANES)
        ext[:, x + 2 : x + 4, 8 : 8 + y, lanes_of(h)] = high.reshape(3, 2, y, LANES)
        for c in range(3):
            start = c * e if fine else s.y_coarse + (h * 3 + c) * e
            rows = slice(start, start + e)
            low, high = sides(flags, EVEN_Y, HAS_YM, HAS_YP, y_in[0][rows], y_in[1][rows])
            ext[c, :, 6:8, lanes_of(h)] = low
            ext[c, :, 8 + y : 10 + y, lanes_of(h)] = high


def fill_materials(s, flags, rigidity, metric, inverse, wide_ext, inv_ext, x_in, y_in, fine):
    x, y = (s.fx, s.fy) if fine else (s.cx, s.cy)
    wide_ext[1 : 1 + x, 1 : 1 + y, :] = rigidity[...] * metric[...]
    inv_ext[1 : 1 + x, 1 : 1 + y, :] = inverse[...]
    for h in range(1 if fine else s.halves):
        at = lanes_of(h)
        got = []
        for m in range(2):
            base = s.x_fine_mats + m * y if fine else s.x_coarse_mats + (m * s.halves + h) * y
            rows = slice(base, base + y)
            even = flags[EVEN_X] == 1
            a, b = x_in[0][rows, :], x_in[1][rows, :]
            got.append((jnp.where(even, b, a), jnp.where(even, a, b)))
        for side, (flag, place) in enumerate(((HAS_XM, 0), (HAS_XP, x + 1))):
            rig, met = got[0][side], got[1][side]
            wide_ext[place, 1 : 1 + y, at] = jnp.where(flags[flag] == 1, rig * met, 0.0)
            inv_ext[place, 1 : 1 + y, at] = jnp.where(flags[flag] == 1, 1.0 / met, 0.0)
        start = s.y_fine_mats if fine else s.y_coarse_mats + h * x
        rows = slice(start, start + x)
        got = []
        for m in range(2):
            even = flags[EVEN_Y] == 1
            a, b = y_in[0][rows, m : m + 1, :], y_in[1][rows, m : m + 1, :]
            got.append((jnp.where(even, b, a), jnp.where(even, a, b)))
        for side, (flag, place) in enumerate(((HAS_YM, 0), (HAS_YP, 1 + y))):
            rig, met = got[0][side], got[1][side]
            wide_ext[1 : 1 + x, place : place + 1, at] = jnp.where(flags[flag] == 1, rig * met, 0.0)
            inv_ext[1 : 1 + x, place : place + 1, at] = jnp.where(flags[flag] == 1, 1.0 / met, 0.0)


def fill_divergence(x, y, ext, inv_ext, div):
    z = ext.shape[-1]
    lane = lax.broadcasted_iota(jnp.int32, (y + 2, z), 1)

    def row(r, carry):
        along_x = ext[0, r + 2, 7 : 9 + y, :] - ext[0, r, 7 : 9 + y, :]
        along_y = ext[1, r + 1, 8 : 10 + y, :] - ext[1, r + 1, 6 : 8 + y, :]
        f = ext[2, r + 1, 7 : 9 + y, :]
        inv = inv_ext[r, 0 : 2 + y, :]
        total = 0.5 * along_x + 0.5 * along_y + inv * slope(f, up_one(f), down_one(f), lane)
        div[r, 7 : 9 + y, :] = jnp.where(inv > 0.0, total, 0.0)
        return carry

    lax.fori_loop(0, x + 2, row, 0, unroll=True)


def update(x, y, ext, wide_ext, inv_ext, div, prev, coef, new, ghosts):
    c1, c2, weight, above, vertical = coef
    z = ext.shape[-1]
    lane = lax.broadcasted_iota(jnp.int32, (y, z), 1)
    mid, left, right, own = slice(8, 8 + y), slice(7, 7 + y), slice(9, 9 + y), slice(1, 1 + y)

    def row(i, total):
        wide = wide_ext[i + 1, own, :]
        w_xp = 0.5 * (wide + wide_ext[i + 2, own, :])
        w_xm = 0.5 * (wide_ext[i, own, :] + wide)
        w_yp = 0.5 * (wide + wide_ext[i + 1, 2 : 2 + y, :])
        w_ym = 0.5 * (wide_ext[i + 1, 0:y, :] + wide)
        inv = inv_ext[i + 1, own, :]
        f = div[i + 1, mid, :]
        gradient = (
            0.5 * (div[i + 2, mid, :] - div[i, mid, :]),
            0.5 * (div[i + 1, right, :] - div[i + 1, left, :]),
            inv * slope(f, up_one(f), down_one(f), lane),
        )
        top, bottom = ghosts(i)
        k1, k2, dm, va = c1[i], c2[i], weight[i], above[i]
        inner = jnp.zeros((y, z), jnp.float32)
        for c in range(3):
            u = ext[c, i + 2, mid, :]
            up = jnp.where(lane == z - 1, bottom(c), up_one(u))
            flux = w_xp * (ext[c, i + 3, mid, :] - u) - w_xm * (u - ext[c, i + 1, mid, :])
            flux += w_yp * (ext[c, i + 2, right, :] - u) - w_ym * (u - ext[c, i + 2, left, :])
            over = va * (up - u)
            entry = 0.0 if top is None else vertical[i, :, 0:1] * (u[:, 0:1] - top(c))
            flux += over - jnp.where(lane == 0, entry, down_one(over))
            rate = flux * k1 + k2 * gradient[c]
            updated = 2.0 * u - prev[c, i] + STEP * rate
            change = updated - u
            inner += change * change - STEP * updated * rate
            new[c, i] = updated
        return total + dm * inner

    return lax.fori_loop(0, x, row, jnp.zeros((y, z), jnp.float32), unroll=4)


def step_kernel(s, step, cells, flags, *refs):
    refs = list(refs)

    def take(n):
        out = refs[:n]
        del refs[:n]
        return out

    fine, coarse, fine_prev, coarse_prev, offs = take(5)
    coef_f, coef_c = take(5), take(5)
    first, final = step == 0, step == STEPS - 1
    if first:
        rig_f, met_f, inverse_f, rig_c, met_c, inverse_c = take(6)
    else:
        wide_f, inv_f, wide_c, inv_c, energy_in = take(5)
    x_in, y_in = take(2), take(2)
    new_f, new_c, energy = take(3)
    if not final:
        x_out = take(2)
    if first:
        wide_f, inv_f, wide_c, inv_c = take(4)
    ext_f, ext_c, div_f, div_c, double, pairs = take(6)

    fill_displacement(s, flags, fine, ext_f, x_in, y_in, True)
    fill_displacement(s, flags, coarse, ext_c, x_in, y_in, False)
    if first:
        fill_materials(s, flags, rig_f, met_f, inverse_f, wide_f, inv_f, x_in, y_in, True)
        fill_materials(s, flags, rig_c, met_c, inverse_c, wide_c, inv_c, x_in, y_in, False)

    lane = lax.broadcasted_iota(jnp.int32, (s.cy + 4, LANES), 1)
    for i in range(s.ce):
        e0, e1, e2 = (ext_c[c, i, 6 : 10 + s.cy, 0:LANES] for c in range(3))
        e1, e2 = pltpu.roll(e1, 1, 1), pltpu.roll(e2, 2, 1)
        plane = jnp.where(lane == 0, e0, jnp.where(lane == 1, e1, e2))
        for j in range(s.cy + 4):
            double[i, 2 * j : 2 * j + 2, :] = jnp.broadcast_to(plane[j : j + 1, :], (2, LANES))
    for c in range(3):
        for i in range(s.cx):
            pairs[c, i] = fine[c, 2 * i] + fine[c, 2 * i + 1]

    fill_divergence(s.fx, s.fy, ext_f, inv_f, div_f)
    fill_divergence(s.cx, s.cy, ext_c, inv_c, div_c)

    odd_y = lax.broadcasted_iota(jnp.int32, (s.fy, LANES), 0) % 2
    near_y = jnp.where(odd_y == 0, 0.75, 0.25)

    def fine_ghosts(i):
        half = i // 2
        near_x = jnp.where(i % 2 == 0, 0.75, 0.25)
        off_x, off_y = offs[i] // 4 - 1, offs[i] % 4 - 1
        total = jnp.zeros((s.fy, LANES), jnp.float32)
        weights = []
        for shift in (-1, 0, 1, 2):
            weights.append(
                jnp.where(off_y == shift, near_y, 0.0)
                + jnp.where(off_y == shift - 1, 1.0 - near_y, 0.0)
            )
        for shift in (-1, 0, 1, 2):
            weight_x = jnp.where(off_x == shift, near_x, 0.0) + jnp.where(
                off_x == shift - 1, 1.0 - near_x, 0.0
            )
            line = jnp.zeros((s.fy, LANES), jnp.float32)
            for k in range(4):
                line += weights[k] * double[half + 2 + shift, 2 * k + 2 : 2 * k + 2 + s.fy, :]
            total += weight_x * line
        return None, lambda c: pltpu.roll(total, LANES - 1 - c, 1)

    def coarse_ghosts(i):
        def top(c):
            both = pairs[c, i, pl.ds(0, s.cy, stride=2), :] + pairs[c, i, pl.ds(1, s.cy, stride=2), :]
            return 0.25 * both[:, LANES - 1 :]

        return top, lambda c: jnp.zeros((s.cy, s.cz), jnp.float32)

    sum_f = update(s.fx, s.fy, ext_f, wide_f, inv_f, div_f, fine_prev, coef_f, new_f, fine_ghosts)
    sum_c = update(
        s.cx, s.cy, ext_c, wide_c, inv_c, div_c, coarse_prev, coef_c, new_c, coarse_ghosts
    )
    place = lax.broadcasted_iota(jnp.int32, (8, LANES), 0)
    before = jnp.zeros((8, LANES), jnp.float32) if first else energy_in[...]
    before = jnp.where(place == step, jnp.sum(sum_f) / cells[0], before)
    energy[...] = jnp.where(place == STEPS + step, jnp.sum(sum_c) / cells[1], before)
    if not final:
        put_x(s, flags, x_out, new_f, new_c)


VMEM = pl.BlockSpec(memory_space=pltpu.VMEM)
SMEM = pl.BlockSpec(memory_space=pltpu.SMEM)
HBM = pl.BlockSpec(memory_space=pltpu.HBM)


def call(kernel, shapes, flops, *args, scratch=(), name=None, specs=None, sems=0):
    shapes = [jax.ShapeDtypeStruct(shape, jnp.float32) for shape in shapes]
    scratch = [pltpu.VMEM(shape, jnp.float32) for shape in scratch]
    if sems:
        scratch.append(pltpu.SemaphoreType.DMA((sems,)))
    return pl.pallas_call(
        kernel,
        out_shape=shapes,
        in_specs=specs or [SMEM] + [VMEM] * (len(args) - 1),
        out_specs=[VMEM] * len(shapes),
        scratch_shapes=scratch,
        compiler_params=pltpu.CompilerParams(vmem_limit_bytes=VMEM_LIMIT),
        cost_estimate=pl.CostEstimate(flops=flops, bytes_accessed=1 << 20, transcendentals=0),
        name=name,
    )(*args)


def swap_pairs(mesh, move):
    sizes = list(mesh.shape.values())
    pairs = []
    for source in range(math.prod(sizes)):
        rest, at = source, []
        for size in reversed(sizes):
            at.insert(0, rest % size)
            rest //= size
        target = 0
        for index, size in zip(move(*at), sizes, strict=True):
            target = target * size + index
        pairs.append((source, target))
    return pairs


def beside_x(z, x, y, core):
    return z, x ^ 1, y, core


def across_x(z, x, y, core):
    place = 4 * z + x
    if place in (0, 31):
        return z, x, y, core ^ 1
    place += 1 if place % 2 else -1
    return place // 4, place % 4, y, core


def beside_y(z, x, y, core):
    return z, x, y, core ^ 1


def across_y(z, x, y, core):
    place = (2 * y + core + (1 if core else -1)) % 8
    return z, x, place // 2, place % 2


TOTAL = (
    lambda z, x, y, core: (z, x, y, core ^ 1),
    lambda z, x, y, core: (z, x, y ^ 1, core ^ 1),
    lambda z, x, y, core: (z, x, y ^ 3, core ^ 1),
    lambda z, x, y, core: (z, x ^ 1, y, core ^ 1),
    lambda z, x, y, core: (z, x ^ 3, y, core ^ 1),
    lambda z, x, y, core: (z ^ 1, x, y, core ^ 1),
    lambda z, x, y, core: (z ^ 2, x, y, core ^ 1),
    lambda z, x, y, core: (z ^ 7, x, y, core ^ 1),
)


def per_device(
    mesh,
    fine_disp,
    fine_prev,
    coarse_disp,
    coarse_prev,
    fine_density,
    fine_lame,
    fine_rigidity,
    fine_metric,
    coarse_density,
    coarse_lame,
    coarse_rigidity,
    coarse_metric,
    offsets,
):
    fine_shape, coarse_shape = fine_metric.shape, coarse_metric.shape
    s = Sizes(fine_shape, coarse_shape)
    count_x, count_y = lax.axis_size(GX), lax.axis_size(GY)
    place_x, place_y = lax.axis_index(GX), lax.axis_index(GY)
    flags = jnp.stack(
        [
            (place_x % 2 == 0).astype(jnp.int32),
            (place_x > 0).astype(jnp.int32),
            (place_x < count_x - 1).astype(jnp.int32),
            (place_y % 2 == 0).astype(jnp.int32),
            (place_y > 0).astype(jnp.int32),
            (place_y < count_y - 1).astype(jnp.int32),
        ]
    )

    def swap(value, move):
        return lax.ppermute(value, ALL, swap_pairs(mesh, move))

    def swap_both(pair, beside, across):
        second = swap(pair[1], across)
        first = swap(pair[0], beside)
        return [pltpu.with_memory_space_constraint(x, pltpu.VMEM) for x in (first, second)]

    offs = offsets[0] * 4 + offsets[1] + 5
    offs = jnp.broadcast_to(offs[..., None], offs.shape + (LANES,))
    x_out = call(
        functools.partial(first_kernel, s),
        [(s.x_rows_mats, LANES)] * 2,
        1000,
        flags,
        *(
            pltpu.with_memory_space_constraint(x, pltpu.HBM)
            for x in (
                fine_disp,
                coarse_disp,
                fine_rigidity,
                fine_metric,
                coarse_rigidity,
                coarse_metric,
            )
        ),
        scratch=[
            (2, 3, 2, s.fy, s.fz),
            (2, 3, 2, s.cy, s.cz),
            (2, 2, s.fy, s.fz),
            (2, 2, s.cy, s.cz),
        ],
        specs=[SMEM] + [HBM] * 6,
        sems=12,
        name="first_strips",
    )
    own = []
    for tag, density, lame, rigidity, metric in (
        ("fine", fine_density, fine_lame, fine_rigidity, fine_metric),
        ("coarse", coarse_density, coarse_lame, coarse_rigidity, coarse_metric),
    ):
        own.append(
            call(
                own_kernel,
                [metric.shape] * 5 + [metric.shape[:2] + (LANES,)],
                2_000_000,
                density,
                lame,
                rigidity,
                metric,
                name=f"own_{tag}",
                specs=[VMEM] * 4,
            )
        )
    inverse_f, *coef_f = own[0]
    inverse_c, *coef_c = own[1]

    fine, coarse = fine_disp, coarse_disp
    fine_ext = (s.fx + 2, s.fy + 2, s.fz)
    coarse_ext = (s.cx + 2, s.cy + 2, s.cz)
    scratch = [
        (3, s.fe, s.fy + 16, s.fz),
        (3, s.ce, s.cy + 16, s.cz),
        (s.fx + 2, s.fy + 16, s.fz),
        (s.cx + 2, s.cy + 16, s.cz),
        (s.ce, 2 * (s.cy + 4), LANES),
        (3, s.cx, s.fy, LANES),
    ]
    cells = [count_x * count_y * s.fx * s.fy * s.fz, count_x * count_y * s.cx * s.cy * s.cz]
    energy = None
    for step in range(STEPS):
        first, final = step == 0, step == STEPS - 1
        raw = [fine_rigidity, fine_metric, coarse_rigidity, coarse_metric] if first else []
        x_in = swap_both(x_out, beside_x, across_x)
        y_out = call(
            functools.partial(middle_kernel, s, first),
            [(s.y_rows_mats if first else s.y_rows, 2, LANES)] * 2,
            1000,
            flags,
            fine,
            coarse,
            *raw,
            *x_in,
            name=f"corner_strips_{step}",
        )
        y_in = swap_both(y_out, beside_y, across_y)
        if first:
            extra = [fine_rigidity, fine_metric, inverse_f, coarse_rigidity, coarse_metric, inverse_c]
        else:
            extra = [*ext_mats, energy]
        shapes = [fine.shape, coarse.shape, (8, LANES)]
        if not final:
            shapes += [(s.x_rows, LANES)] * 2
        if first:
            shapes += [fine_ext, fine_ext, coarse_ext, coarse_ext]
        outs = call(
            functools.partial(step_kernel, s, step, cells),
            shapes,
            4_000_000,
            flags,
            fine,
            coarse,
            fine_prev,
            coarse_prev,
            offs,
            *coef_f,
            *coef_c,
            *extra,
            *x_in,
            *y_in,
            scratch=scratch,
            name=f"step_{step}",
        )
        fine_prev, coarse_prev = fine, coarse
        fine, coarse, energy = outs[:3]
        if not final:
            x_out = outs[3:5]
        if first:
            ext_mats = outs[5:9]
    for move in TOTAL:
        energy = energy + swap(energy, move)
    energy = energy[: 2 * STEPS, 0].reshape(2, STEPS).T
    return fine, coarse, energy


def solution(mesh):
    finer = Mesh(mesh.devices.reshape(8, 4, 4, 2), ALL)
    level, cell = P(None, GX, GY, None), P(GX, GY, None)
    in_specs = (level,) * 4 + (cell,) * 8 + (P(None, GX, GY),)
    return jax.shard_map(
        functools.partial(per_device, finer),
        mesh=finer,
        in_specs=in_specs,
        out_specs=(level, level, P()),
        check_vma=False,
    )
```

```python
import functools
import math

import jax
import jax.numpy as jnp
from jax import lax
from jax.experimental import pallas as pl
from jax.experimental.pallas import tpu as pltpu
from jax.sharding import Mesh
from jax.sharding import PartitionSpec as P

STEPS = 3
GX = ("gx_0", "gx_1")
GY = ("gy_0", "gy_1")
ALL = GX + GY
STEP = 0.15
LANES = 128
VMEM_LIMIT = 20 * 1024 * 1024

EVEN_X, HAS_XM, HAS_XP, EVEN_Y, HAS_YM, HAS_YP = range(6)


class Sizes:
    def __init__(self, fine, coarse):
        self.fx, self.fy, self.fz = fine
        self.cx, self.cy, self.cz = coarse
        self.halves = self.cz // LANES
        self.x_fine = 0
        self.x_coarse = 6 * self.fy
        self.x_rows = self.x_coarse + self.halves * 6 * self.cy
        self.x_fine_mats = self.x_rows
        self.x_coarse_mats = self.x_fine_mats + 2 * self.fy
        self.x_rows_mats = self.x_coarse_mats + 2 * self.halves * self.cy
        self.x_fine_beta = self.x_rows
        self.x_coarse_beta = self.x_fine_beta + 2 * self.fy
        self.x_spread = self.x_coarse_beta + self.halves * 2 * self.cy
        self.spread = self.cy + 8
        self.x_rows_beta = self.x_spread + 2 * self.spread
        self.fe, self.ce = self.fx + 4, self.cx + 4
        self.y_coarse = 3 * self.fe
        self.y_rows = self.y_coarse + self.halves * 3 * self.ce
        self.y_fine_mats = self.y_rows
        self.y_coarse_mats = self.y_fine_mats + self.fx
        self.y_rows_mats = self.y_coarse_mats + self.halves * self.cx
        self.y_fine_beta = self.y_rows
        self.y_coarse_beta = self.y_fine_beta + self.fe
        self.y_spread = self.y_coarse_beta + self.halves * self.ce
        self.y_rows_beta = self.y_spread + self.cx


def lanes_of(h):
    return slice(h * LANES, (h + 1) * LANES)


def put_x(s, flags, outs, fine, coarse, betas=None, spread=None):
    even = flags[EVEN_X] == 1
    for k, out in enumerate(outs):
        far = even if k == 0 else jnp.logical_not(even)
        start_f = jnp.where(far, s.fx - 2, 0)
        start_c = jnp.where(far, s.cx - 2, 0)
        out[0 : s.x_coarse, :] = fine[:, pl.ds(start_f, 2), :, :].reshape(6 * s.fy, LANES)
        strip = coarse[:, pl.ds(start_c, 2), :, :]
        for h in range(s.halves):
            base = s.x_coarse + h * 6 * s.cy
            out[base : base + 6 * s.cy, :] = strip[:, :, :, lanes_of(h)].reshape(6 * s.cy, LANES)
        if betas is None:
            continue
        strip = betas[0][pl.ds(start_f, 2), :, :]
        out[s.x_fine_beta : s.x_coarse_beta, :] = strip.reshape(2 * s.fy, LANES)
        strip = betas[1][pl.ds(start_c, 2), :, :]
        for h in range(s.halves):
            base = s.x_coarse_beta + h * 2 * s.cy
            out[base : base + 2 * s.cy, :] = strip[:, :, lanes_of(h)].reshape(2 * s.cy, LANES)
        start = jnp.where(far, s.cx + 2, 0)
        out[s.x_spread : s.x_rows_beta, :] = spread[pl.ds(start, 2)].reshape(2 * s.spread, LANES)


def first_kernel(s, flags, fine, coarse, rig_f, met_f, rig_c, met_c, out_a, out_b, *scratch):
    strip_f, strip_c, line_f, line_c, sems = scratch
    copies = []

    def fetch(source, target):
        copies.append(pltpu.make_async_copy(source, target, sems.at[len(copies)]))
        copies[-1].start()

    even = flags[EVEN_X] == 1
    for k in range(2):
        far = even if k == 0 else jnp.logical_not(even)
        fetch(fine.at[:, pl.ds(jnp.where(far, s.fx - 2, 0), 2)], strip_f.at[k])
        fetch(coarse.at[:, pl.ds(jnp.where(far, s.cx - 2, 0), 2)], strip_c.at[k])
        for m, (of_f, of_c) in enumerate(((rig_f, rig_c), (met_f, met_c))):
            fetch(of_f.at[jnp.where(far, s.fx - 1, 0)], line_f.at[k, m])
            fetch(of_c.at[jnp.where(far, s.cx - 1, 0)], line_c.at[k, m])
    for copy in copies:
        copy.wait()
    for k, out in enumerate((out_a, out_b)):
        out[0 : s.x_coarse, :] = strip_f[k].reshape(6 * s.fy, LANES)
        for m in range(2):
            base = s.x_fine_mats + m * s.fy
            out[base : base + s.fy, :] = line_f[k, m]
        for h in range(s.halves):
            base = s.x_coarse + h * 6 * s.cy
            out[base : base + 6 * s.cy, :] = strip_c[k, :, :, :, lanes_of(h)].reshape(6 * s.cy, LANES)
            for m in range(2):
                base = s.x_coarse_mats + (m * s.halves + h) * s.cy
                out[base : base + s.cy, :] = line_c[k, m, :, lanes_of(h)]


def sides(flags, even, has_low, has_high, a, b):
    low = jnp.where(flags[even] == 1, b, a)
    high = jnp.where(flags[even] == 1, a, b)
    low = jnp.where(flags[has_low] == 1, low, 0.0)
    high = jnp.where(flags[has_high] == 1, high, 0.0)
    return low, high


def middle_kernel(s, step, flags, *refs):
    fine, coarse, *mats, in_a, in_b = refs[:-2] if step != 1 else refs[:-3]
    out_a, out_b = refs[-2:] if step != 1 else refs[-3:-1]
    even = flags[EVEN_Y] == 1

    def put(index, low, high):
        out_a[index] = jnp.where(even, high, low)
        out_b[index] = jnp.where(even, low, high)

    def field(own, x, y, x_base, y_base):
        put(pl.ds(y_base + 2, x), own(slice(0, 2)), own(slice(y - 2, y)))
        for k in range(2):
            pieces = []
            for first in (0, y - 2):
                rows = slice(x_base + k * y + first, x_base + k * y + first + 2)
                pieces.append(sides(flags, EVEN_X, HAS_XM, HAS_XP, in_a[rows, :], in_b[rows, :]))
            for side in range(2):
                place = y_base + (k if side == 0 else x + 2 + k)
                put(place, pieces[0][side], pieces[1][side])

    for c in range(3):
        field(lambda r: fine[c, :, r, :], s.fx, s.fy, c * 2 * s.fy, c * s.fe)
        for h in range(s.halves):
            at = lanes_of(h)
            x_base, y_base = s.x_coarse + (h * 6 + c * 2) * s.cy, s.y_coarse + (h * 3 + c) * s.ce
            field(lambda r: coarse[c, :, r, at], s.cx, s.cy, x_base, y_base)
    if step == 0:
        rig_f, met_f, rig_c, met_c = mats
        for m, (of_f, of_c) in enumerate(((rig_f, rig_c), (met_f, met_c))):
            low, high = of_f[:, 0:1, :], of_f[:, s.fy - 1 : s.fy, :]
            where = pl.ds(s.y_fine_mats, s.fx)
            out_a[where, m : m + 1, :] = jnp.where(even, high, low)
            out_b[where, m : m + 1, :] = jnp.where(even, low, high)
            for h in range(s.halves):
                low, high = of_c[:, 0:1, lanes_of(h)], of_c[:, s.cy - 1 : s.cy, lanes_of(h)]
                where = pl.ds(s.y_coarse_mats + h * s.cx, s.cx)
                out_a[where, m : m + 1, :] = jnp.where(even, high, low)
                out_b[where, m : m + 1, :] = jnp.where(even, low, high)
    if step == 1:
        beta_f, beta_c, spread = mats
        field(lambda r: beta_f[:, r, :], s.fx, s.fy, s.x_fine_beta, s.y_fine_beta)
        for h in range(s.halves):
            at = lanes_of(h)
            x_base, y_base = s.x_coarse_beta + h * 2 * s.cy, s.y_coarse_beta + h * s.ce
            field(lambda r: beta_c[:, r, at], s.cx, s.cy, x_base, y_base)
        total = refs[-1]
        total[...] = spread[2 : 2 + s.cx]
        for k in range(2):
            rows = slice(s.x_spread + k * s.spread, s.x_spread + (k + 1) * s.spread)
            low, high = sides(flags, EVEN_X, HAS_XM, HAS_XP, in_a[rows, :], in_b[rows, :])
            total[k] += low
            total[s.cx - 2 + k] += high
        put(pl.ds(s.y_spread, s.cx), total[:, 0:2, :], total[:, s.cy + 2 : s.cy + 4, :])


def up_one(x):
    return pltpu.roll(x, x.shape[-1] - 1, x.ndim - 1)


def down_one(x):
    return pltpu.roll(x, 1, x.ndim - 1)


def own_kernel(density, lame, rigidity, metric, inverse, c1, c2, weight, above, first, beta):
    inv = 1.0 / metric[...]
    inverse[...] = inv
    over = 1.0 / density[...]
    c1[...] = inv * over
    c2[...] = (lame[...] + rigidity[...]) * over
    weight[...] = density[...] * metric[...]
    v = rigidity[...] * inv
    lane = lax.broadcasted_iota(jnp.int32, v.shape, 2)
    above[...] = jnp.where(lane == v.shape[2] - 1, v, 0.5 * (v + up_one(v)))
    first[...] = v[:, :, 0:LANES]
    beta[...] = (lame[...] + rigidity[...]) * metric[...]


def slope(f, up, down, lane):
    last = f.shape[-1] - 1
    return jnp.where(lane == 0, up - f, jnp.where(lane == last, f - down, 0.5 * (up - down)))


def slope_transposed(q, lane):
    last = q.shape[-1] - 1
    half = jnp.where((lane == 0) | (lane == last), q, 0.5 * q)
    down = jnp.where(lane == 0, -half, down_one(half))
    return down - jnp.where(lane == last, -half, up_one(half))


def fill_beta(s, flags, own, ext, x_in, y_in, fine):
    x, y, e = (s.fx, s.fy, s.fe) if fine else (s.cx, s.cy, s.ce)
    ext[2 : 2 + x, 8 : 8 + y, :] = own[...]
    for h in range(1 if fine else s.halves):
        at = lanes_of(h)
        base = s.x_fine_beta if fine else s.x_coarse_beta + h * 2 * y
        rows = slice(base, base + 2 * y)
        low, high = sides(flags, EVEN_X, HAS_XM, HAS_XP, x_in[0][rows, :], x_in[1][rows, :])
        ext[0:2, 8 : 8 + y, at] = low.reshape(2, y, LANES)
        ext[x + 2 : x + 4, 8 : 8 + y, at] = high.reshape(2, y, LANES)
        start = s.y_fine_beta if fine else s.y_coarse_beta + h * e
        rows = slice(start, start + e)
        low, high = sides(flags, EVEN_Y, HAS_YM, HAS_YP, y_in[0][rows], y_in[1][rows])
        ext[:, 6:8, at] = low
        ext[:, 8 + y : 10 + y, at] = high


def fill_transposed(x, y, ext, beta, inv_ext, psi):
    z = ext.shape[-1]
    lane = lax.broadcasted_iota(jnp.int32, (y + 2, z), 1)
    wide, low, high = slice(7, 9 + y), slice(6, 8 + y), slice(8, 10 + y)

    def row(r, carry):
        along_x = ext[0, r, wide, :] * beta[r, wide, :]
        along_x -= ext[0, r + 2, wide, :] * beta[r + 2, wide, :]
        along_y = ext[1, r + 1, low, :] * beta[r + 1, low, :]
        along_y -= ext[1, r + 1, high, :] * beta[r + 1, high, :]
        inv = inv_ext[r, 0 : 2 + y, :]
        column = inv * beta[r + 1, wide, :] * ext[2, r + 1, wide, :]
        total = 0.5 * along_x + 0.5 * along_y + slope_transposed(column, lane)
        psi[r, wide, :] = jnp.where(inv > 0.0, total, 0.0)
        return carry

    lax.fori_loop(0, x + 2, row, 0, unroll=True)


def fill_displacement(s, flags, own, ext, x_in, y_in, fine):
    x, y, e = (s.fx, s.fy, s.fe) if fine else (s.cx, s.cy, s.ce)
    ext[:, 2 : 2 + x, 8 : 8 + y, :] = own[...]
    for h in range(1 if fine else s.halves):
        base = s.x_fine if fine else s.x_coarse + h * 6 * y
        rows = slice(base, base + 6 * y)
        low, high = sides(flags, EVEN_X, HAS_XM, HAS_XP, x_in[0][rows, :], x_in[1][rows, :])
        ext[:, 0:2, 8 : 8 + y, lanes_of(h)] = low.reshape(3, 2, y, LANES)
        ext[:, x + 2 : x + 4, 8 : 8 + y, lanes_of(h)] = high.reshape(3, 2, y, LANES)
        for c in range(3):
            start = c * e if fine else s.y_coarse + (h * 3 + c) * e
            rows = slice(start, start + e)
            low, high = sides(flags, EVEN_Y, HAS_YM, HAS_YP, y_in[0][rows], y_in[1][rows])
            ext[c, :, 6:8, lanes_of(h)] = low
            ext[c, :, 8 + y : 10 + y, lanes_of(h)] = high


def fill_materials(s, flags, rigidity, metric, inverse, wide_ext, inv_ext, x_in, y_in, fine):
    x, y = (s.fx, s.fy) if fine else (s.cx, s.cy)
    wide_ext[1 : 1 + x, 1 : 1 + y, :] = rigidity[...] * metric[...]
    inv_ext[1 : 1 + x, 1 : 1 + y, :] = inverse[...]
    for h in range(1 if fine else s.halves):
        at = lanes_of(h)
        got = []
        for m in range(2):
            base = s.x_fine_mats + m * y if fine else s.x_coarse_mats + (m * s.halves + h) * y
            rows = slice(base, base + y)
            even = flags[EVEN_X] == 1
            a, b = x_in[0][rows, :], x_in[1][rows, :]
            got.append((jnp.where(even, b, a), jnp.where(even, a, b)))
        for side, (flag, place) in enumerate(((HAS_XM, 0), (HAS_XP, x + 1))):
            rig, met = got[0][side], got[1][side]
            wide_ext[place, 1 : 1 + y, at] = jnp.where(flags[flag] == 1, rig * met, 0.0)
            inv_ext[place, 1 : 1 + y, at] = jnp.where(flags[flag] == 1, 1.0 / met, 0.0)
        start = s.y_fine_mats if fine else s.y_coarse_mats + h * x
        rows = slice(start, start + x)
        got = []
        for m in range(2):
            even = flags[EVEN_Y] == 1
            a, b = y_in[0][rows, m : m + 1, :], y_in[1][rows, m : m + 1, :]
            got.append((jnp.where(even, b, a), jnp.where(even, a, b)))
        for side, (flag, place) in enumerate(((HAS_YM, 0), (HAS_YP, 1 + y))):
            rig, met = got[0][side], got[1][side]
            wide_ext[1 : 1 + x, place : place + 1, at] = jnp.where(flags[flag] == 1, rig * met, 0.0)
            inv_ext[1 : 1 + x, place : place + 1, at] = jnp.where(flags[flag] == 1, 1.0 / met, 0.0)


def fill_divergence(x, y, ext, inv_ext, div):
    z = ext.shape[-1]
    lane = lax.broadcasted_iota(jnp.int32, (y + 2, z), 1)

    def row(r, carry):
        along_x = ext[0, r + 2, 7 : 9 + y, :] - ext[0, r, 7 : 9 + y, :]
        along_y = ext[1, r + 1, 8 : 10 + y, :] - ext[1, r + 1, 6 : 8 + y, :]
        f = ext[2, r + 1, 7 : 9 + y, :]
        inv = inv_ext[r, 0 : 2 + y, :]
        total = 0.5 * along_x + 0.5 * along_y + inv * slope(f, up_one(f), down_one(f), lane)
        div[r, 7 : 9 + y, :] = jnp.where(inv > 0.0, total, 0.0)
        return carry

    lax.fori_loop(0, x + 2, row, 0, unroll=True)


def update(x, y, ext, wide_ext, inv_ext, div, prev, coef, new, ghosts, psi=None):
    c1, c2, weight, above, vertical = coef
    z = ext.shape[-1]
    lane = lax.broadcasted_iota(jnp.int32, (y, z), 1)
    mid, left, right, own = slice(8, 8 + y), slice(7, 7 + y), slice(9, 9 + y), slice(1, 1 + y)

    def row(i, totals):
        wide = wide_ext[i + 1, own, :]
        w_xp = 0.5 * (wide + wide_ext[i + 2, own, :])
        w_xm = 0.5 * (wide_ext[i, own, :] + wide)
        w_yp = 0.5 * (wide + wide_ext[i + 1, 2 : 2 + y, :])
        w_ym = 0.5 * (wide_ext[i + 1, 0:y, :] + wide)
        inv = inv_ext[i + 1, own, :]
        f = div[i + 1, mid, :]
        gradient = (
            0.5 * (div[i + 2, mid, :] - div[i, mid, :]),
            0.5 * (div[i + 1, right, :] - div[i + 1, left, :]),
            inv * slope(f, up_one(f), down_one(f), lane),
        )
        if psi is not None:
            transposed = (
                0.5 * (psi[i, mid, :] - psi[i + 2, mid, :]),
                0.5 * (psi[i + 1, left, :] - psi[i + 1, right, :]),
                slope_transposed(inv * psi[i + 1, mid, :], lane),
            )
        top, bottom, top_next = ghosts(i)
        k1, k2, dm, va = c1[i], c2[i], weight[i], above[i]
        first = vertical[i, :, 0:1]
        inner, squares, cross = (jnp.zeros((y, z), jnp.float32) for _ in range(3))
        for c in range(3):
            u = ext[c, i + 2, mid, :]
            flux = w_xp * (ext[c, i + 3, mid, :] - u) - w_xm * (u - ext[c, i + 1, mid, :])
            flux += w_yp * (ext[c, i + 2, right, :] - u) - w_ym * (u - ext[c, i + 2, left, :])
            over = va * (jnp.where(lane == z - 1, 0.0, up_one(u)) - u)
            entry = 0.0 if top is None else first * u[:, 0:1]
            flux += over - jnp.where(lane == 0, entry, down_one(over))
            if top is None:
                ghost = jnp.where(lane == z - 1, va * bottom(c), 0.0)
            else:
                ghost = jnp.where(lane == 0, first * top(c), 0.0)
            rate = (flux + ghost) * k1 + k2 * gradient[c]
            updated = 2.0 * u - prev[c, i] + STEP * rate
            change = updated - u
            inner += change * change - STEP * updated * rate
            new[c, i] = updated
            if psi is not None:
                squares += change * change
                cross += updated * (flux + transposed[c])
                if top is not None:
                    cross += jnp.where(lane == 0, first * u[:, 0:1] * top_next(c), 0.0)
        total = totals[0] + dm * inner
        if psi is None:
            return (total,)
        return total, totals[1] + (dm * squares - STEP * cross)

    start = (jnp.zeros((y, z), jnp.float32),) * (1 if psi is None else 2)
    return lax.fori_loop(0, x, row, start, unroll=4)


def step_kernel(s, step, cells, flags, *refs):
    refs = list(refs)

    def take(n):
        out = refs[:n]
        del refs[:n]
        return out

    fine, coarse, fine_prev, coarse_prev, offs = take(5)
    coef_f, coef_c = take(5), take(5)
    if step == 0:
        rig_f, met_f, inverse_f, rig_c, met_c, inverse_c = take(6)
    else:
        wide_f, inv_f, wide_c, inv_c = take(4)
    if step < 2:
        beta_own = take(2)
    if step == 1:
        energy_in, spread_in = take(2)
    x_in, y_in = take(2), take(2)
    new_f, new_c = take(2)
    if step < 2:
        (energy,) = take(1)
        x_out = take(2)
    if step == 0:
        wide_f, inv_f, wide_c, inv_c, spread_out = take(5)
    ext_f, ext_c, div_f, div_c, double, pairs = take(6)

    fill_displacement(s, flags, fine, ext_f, x_in, y_in, True)
    fill_displacement(s, flags, coarse, ext_c, x_in, y_in, False)
    if step == 0:
        fill_materials(s, flags, rig_f, met_f, inverse_f, wide_f, inv_f, x_in, y_in, True)
        fill_materials(s, flags, rig_c, met_c, inverse_c, wide_c, inv_c, x_in, y_in, False)

    lane = lax.broadcasted_iota(jnp.int32, (s.cy + 4, LANES), 1)
    for i in range(s.ce):
        e0, e1, e2 = (ext_c[c, i, 6 : 10 + s.cy, 0:LANES] for c in range(3))
        e1, e2 = pltpu.roll(e1, 1, 1), pltpu.roll(e2, 2, 1)
        plane = jnp.where(lane == 0, e0, jnp.where(lane == 1, e1, e2))
        for j in range(s.cy + 4):
            double[i, 2 * j : 2 * j + 2, :] = jnp.broadcast_to(plane[j : j + 1, :], (2, LANES))
    for c in range(3):
        for i in range(s.cx):
            pairs[c, i] = fine[c, 2 * i] + fine[c, 2 * i + 1]

    fill_divergence(s.fx, s.fy, ext_f, inv_f, div_f)
    fill_divergence(s.cx, s.cy, ext_c, inv_c, div_c)
    psi_f = psi_c = None
    if step == 1:
        psi_f, psi_c, all_beta_f, all_beta_c, pairs_next, spread = take(6)
        fill_beta(s, flags, beta_own[0], all_beta_f, x_in, y_in, True)
        fill_beta(s, flags, beta_own[1], all_beta_c, x_in, y_in, False)
        fill_transposed(s.fx, s.fy, ext_f, all_beta_f, inv_f, psi_f)
        fill_transposed(s.cx, s.cy, ext_c, all_beta_c, inv_c, psi_c)

    odd_y = lax.broadcasted_iota(jnp.int32, (s.fy, LANES), 0) % 2
    near_y = jnp.where(odd_y == 0, 0.75, 0.25)

    def node_weights(i):
        near_x = jnp.where(i % 2 == 0, 0.75, 0.25)
        off_x, off_y = offs[i] // 4 - 1, offs[i] % 4 - 1
        out = []
        for off, near in ((off_x, near_x), (off_y, near_y)):
            out.append(
                [
                    jnp.where(off == shift, near, 0.0)
                    + jnp.where(off == shift - 1, 1.0 - near, 0.0)
                    for shift in (-1, 0, 1, 2)
                ]
            )
        return out

    def fine_ghosts(i):
        weights_x, weights_y = node_weights(i)
        total = jnp.zeros((s.fy, LANES), jnp.float32)
        for a in range(4):
            line = jnp.zeros((s.fy, LANES), jnp.float32)
            for b in range(4):
                line += weights_y[b] * double[i // 2 + 1 + a, 2 * b + 2 : 2 * b + 2 + s.fy, :]
            total += weights_x[a] * line
        return None, lambda c: pltpu.roll(total, LANES - 1 - c, 1), None

    def coarse_ghosts(i):
        def mean(of):
            def top(c):
                both = of[c, i, pl.ds(0, s.cy, stride=2), :] + of[c, i, pl.ds(1, s.cy, stride=2), :]
                return 0.25 * both[:, LANES - 1 :]

            return top

        return mean(pairs), None, mean(pairs_next) if step == 1 else None

    sums_f = update(
        s.fx, s.fy, ext_f, wide_f, inv_f, div_f, fine_prev, coef_f, new_f, fine_ghosts, psi_f
    )
    if step == 1:
        for c in range(3):
            for i in range(s.cx):
                pairs_next[c, i] = new_f[c, 2 * i] + new_f[c, 2 * i + 1]
    sums_c = update(
        s.cx, s.cy, ext_c, wide_c, inv_c, div_c, coarse_prev, coef_c, new_c, coarse_ghosts, psi_c
    )
    if step == 2:
        return
    place = lax.broadcasted_iota(jnp.int32, (8, LANES), 0)
    table = jnp.zeros((8, LANES), jnp.float32) if step == 0 else energy_in[...]
    table = jnp.where(place == step, jnp.sum(sums_f[0]) / cells[0], table)
    table = jnp.where(place == STEPS + step, jnp.sum(sums_c[0]) / cells[1], table)
    if step == 0:
        line_lane = lax.broadcasted_iota(jnp.int32, (s.fy, LANES), 1)
        double[...] = jnp.zeros(double.shape, jnp.float32)

        def scatter(i, carry):
            weights_x, weights_y = node_weights(i)
            face = coef_f[3][i]
            q = jnp.zeros((s.fy, LANES), jnp.float32)
            for c in range(3):
                q = jnp.where(line_lane == c, pltpu.roll(face * new_f[c, i], c + 1, 1), q)
            for b in range(4):
                part = weights_y[b] * q
                for a in range(4):
                    rows = slice(2 * b + 2, 2 * b + 2 + s.fy)
                    double[i // 2 + 1 + a, rows, :] += weights_x[a] * part
            return carry

        lax.fori_loop(0, s.fx, scatter, 0, unroll=4)
        rows = s.cy + 4
        for i in range(s.ce):
            evens = double[i, pl.ds(0, rows, stride=2), :]
            spread_out[i, 0:rows, :] = evens + double[i, pl.ds(1, rows, stride=2), :]
            spread_out[i, rows:, :] = jnp.zeros((s.spread - rows, LANES), jnp.float32)
        put_x(s, flags, x_out, new_f, new_c, beta_own, spread_out)
    if step == 1:
        spread[...] = spread_in[:, 2 : 2 + s.cy, :]
        rows = pl.ds(s.y_spread, s.cx)
        low, high = sides(flags, EVEN_Y, HAS_YM, HAS_YP, y_in[0][rows], y_in[1][rows])
        spread[:, 0:2, :] += low
        spread[:, s.cy - 2 : s.cy, :] += high
        joined = jnp.zeros((s.cy, LANES), jnp.float32)
        for i in range(s.cx):
            for c in range(3):
                weights = spread[i] if c == 0 else pltpu.roll(spread[i], LANES - c, 1)
                joined += new_c[c, i, :, 0:LANES] * weights
        joined = jnp.sum(joined[:, 0:1])
        table = jnp.where(place == 2, (jnp.sum(sums_f[1]) - STEP * joined) / cells[0], table)
        table = jnp.where(place == STEPS + 2, jnp.sum(sums_c[1]) / cells[1], table)
        put_x(s, flags, x_out, new_f, new_c)
    energy[...] = table


VMEM = pl.BlockSpec(memory_space=pltpu.VMEM)
SMEM = pl.BlockSpec(memory_space=pltpu.SMEM)
HBM = pl.BlockSpec(memory_space=pltpu.HBM)


def call(kernel, shapes, flops, *args, scratch=(), name=None, specs=None, sems=0):
    shapes = [jax.ShapeDtypeStruct(shape, jnp.float32) for shape in shapes]
    scratch = [pltpu.VMEM(shape, jnp.float32) for shape in scratch]
    if sems:
        scratch.append(pltpu.SemaphoreType.DMA((sems,)))
    return pl.pallas_call(
        kernel,
        out_shape=shapes,
        in_specs=specs or [SMEM] + [VMEM] * (len(args) - 1),
        out_specs=[VMEM] * len(shapes),
        scratch_shapes=scratch,
        compiler_params=pltpu.CompilerParams(vmem_limit_bytes=VMEM_LIMIT),
        cost_estimate=pl.CostEstimate(flops=flops, bytes_accessed=1 << 20, transcendentals=0),
        name=name,
    )(*args)


def swap_pairs(mesh, move):
    sizes = list(mesh.shape.values())
    pairs = []
    for source in range(math.prod(sizes)):
        rest, at = source, []
        for size in reversed(sizes):
            at.insert(0, rest % size)
            rest //= size
        target = 0
        for index, size in zip(move(*at), sizes, strict=True):
            target = target * size + index
        pairs.append((source, target))
    return pairs


def beside_x(z, x, y, core):
    return z, x ^ 1, y, core


def across_x(z, x, y, core):
    place = 4 * z + x
    if place in (0, 31):
        return z, x, y, core ^ 1
    place += 1 if place % 2 else -1
    return place // 4, place % 4, y, core


def beside_y(z, x, y, core):
    return z, x, y, core ^ 1


def across_y(z, x, y, core):
    place = (2 * y + core + (1 if core else -1)) % 8
    return z, x, place // 2, place % 2


TOTAL = (
    lambda z, x, y, core: (z, x, y, core ^ 1),
    lambda z, x, y, core: (z, x, y ^ 1, core ^ 1),
    lambda z, x, y, core: (z, x, y ^ 3, core ^ 1),
    lambda z, x, y, core: (z, x ^ 1, y, core ^ 1),
    lambda z, x, y, core: (z, x ^ 3, y, core ^ 1),
    lambda z, x, y, core: (z ^ 1, x, y, core ^ 1),
    lambda z, x, y, core: (z ^ 2, x, y, core ^ 1),
    lambda z, x, y, core: (z ^ 7, x, y, core ^ 1),
)


def per_device(
    mesh,
    fine_disp,
    fine_prev,
    coarse_disp,
    coarse_prev,
    fine_density,
    fine_lame,
    fine_rigidity,
    fine_metric,
    coarse_density,
    coarse_lame,
    coarse_rigidity,
    coarse_metric,
    offsets,
):
    fine_shape, coarse_shape = fine_metric.shape, coarse_metric.shape
    s = Sizes(fine_shape, coarse_shape)
    count_x, count_y = lax.axis_size(GX), lax.axis_size(GY)
    place_x, place_y = lax.axis_index(GX), lax.axis_index(GY)
    flags = jnp.stack(
        [
            (place_x % 2 == 0).astype(jnp.int32),
            (place_x > 0).astype(jnp.int32),
            (place_x < count_x - 1).astype(jnp.int32),
            (place_y % 2 == 0).astype(jnp.int32),
            (place_y > 0).astype(jnp.int32),
            (place_y < count_y - 1).astype(jnp.int32),
        ]
    )

    def swap(value, move):
        return lax.ppermute(value, ALL, swap_pairs(mesh, move))

    def swap_both(pair, beside, across):
        second = swap(pair[1], across)
        first = swap(pair[0], beside)
        return [pltpu.with_memory_space_constraint(x, pltpu.VMEM) for x in (first, second)]

    offs = offsets[0] * 4 + offsets[1] + 5
    offs = jnp.broadcast_to(offs[..., None], offs.shape + (LANES,))
    x_out = call(
        functools.partial(first_kernel, s),
        [(s.x_rows_mats, LANES)] * 2,
        1000,
        flags,
        *(
            pltpu.with_memory_space_constraint(x, pltpu.HBM)
            for x in (
                fine_disp,
                coarse_disp,
                fine_rigidity,
                fine_metric,
                coarse_rigidity,
                coarse_metric,
            )
        ),
        scratch=[
            (2, 3, 2, s.fy, s.fz),
            (2, 3, 2, s.cy, s.cz),
            (2, 2, s.fy, s.fz),
            (2, 2, s.cy, s.cz),
        ],
        specs=[SMEM] + [HBM] * 6,
        sems=12,
        name="first_strips",
    )
    own = []
    for tag, density, lame, rigidity, metric in (
        ("fine", fine_density, fine_lame, fine_rigidity, fine_metric),
        ("coarse", coarse_density, coarse_lame, coarse_rigidity, coarse_metric),
    ):
        own.append(
            call(
                own_kernel,
                [metric.shape] * 5 + [metric.shape[:2] + (LANES,), metric.shape],
                2_000_000,
                density,
                lame,
                rigidity,
                metric,
                name=f"own_{tag}",
                specs=[VMEM] * 4,
            )
        )
    inverse_f, *coef_f, beta_f = own[0]
    inverse_c, *coef_c, beta_c = own[1]

    fine, coarse = fine_disp, coarse_disp
    fine_ext = (s.fx + 2, s.fy + 2, s.fz)
    coarse_ext = (s.cx + 2, s.cy + 2, s.cz)
    scratch = [
        (3, s.fe, s.fy + 16, s.fz),
        (3, s.ce, s.cy + 16, s.cz),
        (s.fx + 2, s.fy + 16, s.fz),
        (s.cx + 2, s.cy + 16, s.cz),
        (s.ce, 2 * (s.cy + 4), LANES),
        (3, s.cx, s.fy, LANES),
    ]
    cells = [count_x * count_y * s.fx * s.fy * s.fz, count_x * count_y * s.cx * s.cy * s.cz]
    spread = (s.ce, s.spread, LANES)
    for step in range(STEPS):
        x_in = swap_both(x_out, beside_x, across_x)
        if step == 2:
            for move in TOTAL[:2]:
                energy = energy + swap(energy, move)
            energy, *x_in = lax.optimization_barrier((energy, *x_in))
            for move in TOTAL[2:-1]:
                energy = energy + swap(energy, move)
            other = swap(energy, TOTAL[-1])
        shapes = [((s.y_rows_mats, s.y_rows_beta, s.y_rows)[step], 2, LANES)] * 2
        if step == 0:
            mats = [fine_rigidity, fine_metric, coarse_rigidity, coarse_metric]
        if step == 1:
            mats = [beta_f, beta_c, spread_own]
            shapes.append((s.cx,) + spread[1:])
        y_out = call(
            functools.partial(middle_kernel, s, step),
            shapes,
            1000,
            flags,
            fine,
            coarse,
            *(mats if step < 2 else ()),
            *x_in,
            name=f"corner_strips_{step}",
        )
        y_in = swap_both(y_out[:2], beside_y, across_y)
        shapes = [fine.shape, coarse.shape]
        more_scratch = []
        if step < 2:
            shapes += [(8, LANES)] + [((s.x_rows_beta, s.x_rows)[step], LANES)] * 2
        if step == 0:
            extra = [fine_rigidity, fine_metric, inverse_f, coarse_rigidity, coarse_metric, inverse_c]
            extra += [beta_f, beta_c]
            shapes += [fine_ext, fine_ext, coarse_ext, coarse_ext, spread]
        else:
            extra = list(ext_mats)
        if step == 1:
            extra += [beta_f, beta_c, energy, y_out[2]]
            more_scratch = [
                scratch[2],
                scratch[3],
                scratch[0][1:],
                scratch[1][1:],
                scratch[5],
                (s.cx, s.cy, LANES),
            ]
        outs = call(
            functools.partial(step_kernel, s, step, cells),
            shapes,
            4_000_000,
            flags,
            fine,
            coarse,
            fine_prev,
            coarse_prev,
            offs,
            *coef_f,
            *coef_c,
            *extra,
            *x_in,
            *y_in,
            scratch=scratch + more_scratch,
            name=f"step_{step}",
        )
        fine_prev, coarse_prev = fine, coarse
        fine, coarse = outs[:2]
        if step < 2:
            energy, x_out = outs[2], outs[3:5]
        if step == 0:
            *ext_mats, spread_own = outs[5:]
    other, fine, coarse = lax.optimization_barrier((other, fine, coarse))
    energy = energy + other
    energy = energy[: 2 * STEPS, 0].reshape(2, STEPS).T
    return fine, coarse, energy


def solution(mesh):
    finer = Mesh(mesh.devices.reshape(8, 4, 4, 2), ALL)
    level, cell = P(None, GX, GY, None), P(GX, GY, None)
    in_specs = (level,) * 4 + (cell,) * 8 + (P(None, GX, GY),)
    return jax.shard_map(
        functools.partial(per_device, finer),
        mesh=finer,
        in_specs=in_specs,
        out_specs=(level, level, P()),
        check_vma=False,
    )
```

```python
import functools
import math

import jax
import jax.numpy as jnp
from jax import lax
from jax.experimental import pallas as pl
from jax.experimental.pallas import tpu as pltpu
from jax.sharding import Mesh
from jax.sharding import PartitionSpec as P

STEPS = 3
GX = ("gx_0", "gx_1")
GY = ("gy_0", "gy_1")
ALL = GX + GY
STEP = 0.15
LANES = 128
VMEM_LIMIT = 20 * 1024 * 1024

EVEN_X, HAS_XM, HAS_XP, EVEN_Y, HAS_YM, HAS_YP = range(6)


def where_am_i():
    x = 4 * lax.axis_index("gx_0") + lax.axis_index("gx_1")
    y = 2 * lax.axis_index("gy_0") + lax.axis_index("gy_1")
    return x % 2 == 0, x > 0, x < 31, y % 2 == 0, y > 0, y < 7


class Sizes:
    def __init__(self, fine, coarse):
        self.fx, self.fy, self.fz = fine
        self.cx, self.cy, self.cz = coarse
        self.halves = self.cz // LANES
        self.x_fine = 0
        self.x_coarse = 6 * self.fy
        self.x_rows = self.x_coarse + self.halves * 6 * self.cy
        self.x_fine_mats = self.x_rows
        self.x_coarse_mats = self.x_fine_mats + 2 * self.fy
        self.x_rows_mats = self.x_coarse_mats + 2 * self.halves * self.cy
        self.x_fine_beta = self.x_rows
        self.x_coarse_beta = self.x_fine_beta + 2 * self.fy
        self.x_spread = self.x_coarse_beta + self.halves * 2 * self.cy
        self.spread = self.cy + 8
        self.x_rows_beta = self.x_spread + 2 * self.spread
        self.fe, self.ce = self.fx + 4, self.cx + 4
        self.y_coarse = 3 * self.fe
        self.y_rows = self.y_coarse + self.halves * 3 * self.ce
        self.y_fine_mats = self.y_rows
        self.y_coarse_mats = self.y_fine_mats + self.fx
        self.y_rows_mats = self.y_coarse_mats + self.halves * self.cx
        self.y_fine_beta = self.y_rows
        self.y_coarse_beta = self.y_fine_beta + self.fe
        self.y_spread = self.y_coarse_beta + self.halves * self.ce
        self.y_rows_beta = self.y_spread + self.cx


def lanes_of(h):
    return slice(h * LANES, (h + 1) * LANES)


def put_x(s, flags, outs, fine, coarse, betas=None, spread=None):
    even = flags[EVEN_X]
    for k, out in enumerate(outs):
        far = even if k == 0 else jnp.logical_not(even)
        start_f = jnp.where(far, s.fx - 2, 0)
        start_c = jnp.where(far, s.cx - 2, 0)
        out[0 : s.x_coarse, :] = fine[:, pl.ds(start_f, 2), :, :].reshape(6 * s.fy, LANES)
        strip = coarse[:, pl.ds(start_c, 2), :, :]
        for h in range(s.halves):
            base = s.x_coarse + h * 6 * s.cy
            out[base : base + 6 * s.cy, :] = strip[:, :, :, lanes_of(h)].reshape(6 * s.cy, LANES)
        if betas is None:
            continue
        strip = betas[0][pl.ds(start_f, 2), :, :]
        out[s.x_fine_beta : s.x_coarse_beta, :] = strip.reshape(2 * s.fy, LANES)
        strip = betas[1][pl.ds(start_c, 2), :, :]
        for h in range(s.halves):
            base = s.x_coarse_beta + h * 2 * s.cy
            out[base : base + 2 * s.cy, :] = strip[:, :, lanes_of(h)].reshape(2 * s.cy, LANES)
        start = jnp.where(far, s.cx + 2, 0)
        out[s.x_spread : s.x_rows_beta, :] = spread[pl.ds(start, 2)].reshape(2 * s.spread, LANES)


def first_kernel(s, fine, coarse, rig_f, met_f, rig_c, met_c, out_a, out_b, *scratch):
    strip_f, strip_c, line_f, line_c, sems = scratch
    flags = where_am_i()
    copies = []

    def fetch(source, target):
        copies.append(pltpu.make_async_copy(source, target, sems.at[len(copies)]))
        copies[-1].start()

    even = flags[EVEN_X]
    for k in range(2):
        far = even if k == 0 else jnp.logical_not(even)
        fetch(fine.at[:, pl.ds(jnp.where(far, s.fx - 2, 0), 2)], strip_f.at[k])
        fetch(coarse.at[:, pl.ds(jnp.where(far, s.cx - 2, 0), 2)], strip_c.at[k])
        for m, (of_f, of_c) in enumerate(((rig_f, rig_c), (met_f, met_c))):
            fetch(of_f.at[jnp.where(far, s.fx - 1, 0)], line_f.at[k, m])
            fetch(of_c.at[jnp.where(far, s.cx - 1, 0)], line_c.at[k, m])
    for copy in copies:
        copy.wait()
    for k, out in enumerate((out_a, out_b)):
        out[0 : s.x_coarse, :] = strip_f[k].reshape(6 * s.fy, LANES)
        for m in range(2):
            base = s.x_fine_mats + m * s.fy
            out[base : base + s.fy, :] = line_f[k, m]
        for h in range(s.halves):
            base = s.x_coarse + h * 6 * s.cy
            out[base : base + 6 * s.cy, :] = strip_c[k, :, :, :, lanes_of(h)].reshape(6 * s.cy, LANES)
            for m in range(2):
                base = s.x_coarse_mats + (m * s.halves + h) * s.cy
                out[base : base + s.cy, :] = line_c[k, m, :, lanes_of(h)]


def sides(flags, even, has_low, has_high, a, b):
    low = jnp.where(flags[even], b, a)
    high = jnp.where(flags[even], a, b)
    low = jnp.where(flags[has_low], low, 0.0)
    high = jnp.where(flags[has_high], high, 0.0)
    return low, high


def middle_kernel(s, step, *refs):
    flags = where_am_i()
    fine, coarse, *mats, in_a, in_b = refs[:-2] if step != 1 else refs[:-3]
    out_a, out_b = refs[-2:] if step != 1 else refs[-3:-1]
    even = flags[EVEN_Y]

    def put(index, low, high):
        out_a[index] = jnp.where(even, high, low)
        out_b[index] = jnp.where(even, low, high)

    def field(own, x, y, x_base, y_base):
        put(pl.ds(y_base + 2, x), own(slice(0, 2)), own(slice(y - 2, y)))
        for k in range(2):
            pieces = []
            for first in (0, y - 2):
                rows = slice(x_base + k * y + first, x_base + k * y + first + 2)
                pieces.append(sides(flags, EVEN_X, HAS_XM, HAS_XP, in_a[rows, :], in_b[rows, :]))
            for side in range(2):
                place = y_base + (k if side == 0 else x + 2 + k)
                put(place, pieces[0][side], pieces[1][side])

    for c in range(3):
        field(lambda r: fine[c, :, r, :], s.fx, s.fy, c * 2 * s.fy, c * s.fe)
        for h in range(s.halves):
            at = lanes_of(h)
            x_base, y_base = s.x_coarse + (h * 6 + c * 2) * s.cy, s.y_coarse + (h * 3 + c) * s.ce
            field(lambda r: coarse[c, :, r, at], s.cx, s.cy, x_base, y_base)
    if step == 0:
        rig_f, met_f, rig_c, met_c = mats
        for m, (of_f, of_c) in enumerate(((rig_f, rig_c), (met_f, met_c))):
            low, high = of_f[:, 0:1, :], of_f[:, s.fy - 1 : s.fy, :]
            where = pl.ds(s.y_fine_mats, s.fx)
            out_a[where, m : m + 1, :] = jnp.where(even, high, low)
            out_b[where, m : m + 1, :] = jnp.where(even, low, high)
            for h in range(s.halves):
                low, high = of_c[:, 0:1, lanes_of(h)], of_c[:, s.cy - 1 : s.cy, lanes_of(h)]
                where = pl.ds(s.y_coarse_mats + h * s.cx, s.cx)
                out_a[where, m : m + 1, :] = jnp.where(even, high, low)
                out_b[where, m : m + 1, :] = jnp.where(even, low, high)
    if step == 1:
        beta_f, beta_c, spread = mats
        field(lambda r: beta_f[:, r, :], s.fx, s.fy, s.x_fine_beta, s.y_fine_beta)
        for h in range(s.halves):
            at = lanes_of(h)
            x_base, y_base = s.x_coarse_beta + h * 2 * s.cy, s.y_coarse_beta + h * s.ce
            field(lambda r: beta_c[:, r, at], s.cx, s.cy, x_base, y_base)
        total = refs[-1]
        total[...] = spread[2 : 2 + s.cx]
        for k in range(2):
            rows = slice(s.x_spread + k * s.spread, s.x_spread + (k + 1) * s.spread)
            low, high = sides(flags, EVEN_X, HAS_XM, HAS_XP, in_a[rows, :], in_b[rows, :])
            total[k] += low
            total[s.cx - 2 + k] += high
        put(pl.ds(s.y_spread, s.cx), total[:, 0:2, :], total[:, s.cy + 2 : s.cy + 4, :])


def up_one(x):
    return pltpu.roll(x, x.shape[-1] - 1, x.ndim - 1)


def down_one(x):
    return pltpu.roll(x, 1, x.ndim - 1)


def own_kernel(density, lame, rigidity, metric, inverse, c1, c2, weight, above, first, beta):
    inv = 1.0 / metric[...]
    inverse[...] = inv
    over = 1.0 / density[...]
    c1[...] = inv * over
    c2[...] = (lame[...] + rigidity[...]) * over
    weight[...] = density[...] * metric[...]
    v = rigidity[...] * inv
    lane = lax.broadcasted_iota(jnp.int32, v.shape, 2)
    above[...] = jnp.where(lane == v.shape[2] - 1, v, 0.5 * (v + up_one(v)))
    first[...] = v[:, :, 0:LANES]
    beta[...] = (lame[...] + rigidity[...]) * metric[...]


def slope(f, up, down, lane):
    last = f.shape[-1] - 1
    return jnp.where(lane == 0, up - f, jnp.where(lane == last, f - down, 0.5 * (up - down)))


def slope_transposed(q, lane):
    last = q.shape[-1] - 1
    half = jnp.where((lane == 0) | (lane == last), q, 0.5 * q)
    down = jnp.where(lane == 0, -half, down_one(half))
    return down - jnp.where(lane == last, -half, up_one(half))


def fill_beta(s, flags, own, ext, x_in, y_in, fine):
    x, y, e = (s.fx, s.fy, s.fe) if fine else (s.cx, s.cy, s.ce)
    ext[2 : 2 + x, 8 : 8 + y, :] = own[...]
    for h in range(1 if fine else s.halves):
        at = lanes_of(h)
        base = s.x_fine_beta if fine else s.x_coarse_beta + h * 2 * y
        rows = slice(base, base + 2 * y)
        low, high = sides(flags, EVEN_X, HAS_XM, HAS_XP, x_in[0][rows, :], x_in[1][rows, :])
        ext[0:2, 8 : 8 + y, at] = low.reshape(2, y, LANES)
        ext[x + 2 : x + 4, 8 : 8 + y, at] = high.reshape(2, y, LANES)
        start = s.y_fine_beta if fine else s.y_coarse_beta + h * e
        rows = slice(start, start + e)
        low, high = sides(flags, EVEN_Y, HAS_YM, HAS_YP, y_in[0][rows], y_in[1][rows])
        ext[:, 6:8, at] = low
        ext[:, 8 + y : 10 + y, at] = high


def fill_transposed(x, y, ext, beta, inv_ext, psi):
    z = ext.shape[-1]
    lane = lax.broadcasted_iota(jnp.int32, (y + 2, z), 1)
    wide, low, high = slice(7, 9 + y), slice(6, 8 + y), slice(8, 10 + y)

    def row(r, carry):
        along_x = ext[0, r, wide, :] * beta[r, wide, :]
        along_x -= ext[0, r + 2, wide, :] * beta[r + 2, wide, :]
        along_y = ext[1, r + 1, low, :] * beta[r + 1, low, :]
        along_y -= ext[1, r + 1, high, :] * beta[r + 1, high, :]
        inv = inv_ext[r, 0 : 2 + y, :]
        column = inv * beta[r + 1, wide, :] * ext[2, r + 1, wide, :]
        total = 0.5 * along_x + 0.5 * along_y + slope_transposed(column, lane)
        psi[r, wide, :] = jnp.where(inv > 0.0, total, 0.0)
        return carry

    lax.fori_loop(0, x + 2, row, 0, unroll=True)


def fill_displacement(s, flags, own, ext, x_in, y_in, fine):
    x, y, e = (s.fx, s.fy, s.fe) if fine else (s.cx, s.cy, s.ce)
    ext[:, 2 : 2 + x, 8 : 8 + y, :] = own[...]
    for h in range(1 if fine else s.halves):
        base = s.x_fine if fine else s.x_coarse + h * 6 * y
        rows = slice(base, base + 6 * y)
        low, high = sides(flags, EVEN_X, HAS_XM, HAS_XP, x_in[0][rows, :], x_in[1][rows, :])
        ext[:, 0:2, 8 : 8 + y, lanes_of(h)] = low.reshape(3, 2, y, LANES)
        ext[:, x + 2 : x + 4, 8 : 8 + y, lanes_of(h)] = high.reshape(3, 2, y, LANES)
        for c in range(3):
            start = c * e if fine else s.y_coarse + (h * 3 + c) * e
            rows = slice(start, start + e)
            low, high = sides(flags, EVEN_Y, HAS_YM, HAS_YP, y_in[0][rows], y_in[1][rows])
            ext[c, :, 6:8, lanes_of(h)] = low
            ext[c, :, 8 + y : 10 + y, lanes_of(h)] = high


def fill_materials(s, flags, rigidity, metric, inverse, wide_ext, inv_ext, x_in, y_in, fine):
    x, y = (s.fx, s.fy) if fine else (s.cx, s.cy)
    wide_ext[1 : 1 + x, 1 : 1 + y, :] = rigidity[...] * metric[...]
    inv_ext[1 : 1 + x, 1 : 1 + y, :] = inverse[...]
    for h in range(1 if fine else s.halves):
        at = lanes_of(h)
        got = []
        for m in range(2):
            base = s.x_fine_mats + m * y if fine else s.x_coarse_mats + (m * s.halves + h) * y
            rows = slice(base, base + y)
            even = flags[EVEN_X]
            a, b = x_in[0][rows, :], x_in[1][rows, :]
            got.append((jnp.where(even, b, a), jnp.where(even, a, b)))
        for side, (flag, place) in enumerate(((HAS_XM, 0), (HAS_XP, x + 1))):
            rig, met = got[0][side], got[1][side]
            wide_ext[place, 1 : 1 + y, at] = jnp.where(flags[flag], rig * met, 0.0)
            inv_ext[place, 1 : 1 + y, at] = jnp.where(flags[flag], 1.0 / met, 0.0)
        start = s.y_fine_mats if fine else s.y_coarse_mats + h * x
        rows = slice(start, start + x)
        got = []
        for m in range(2):
            even = flags[EVEN_Y]
            a, b = y_in[0][rows, m : m + 1, :], y_in[1][rows, m : m + 1, :]
            got.append((jnp.where(even, b, a), jnp.where(even, a, b)))
        for side, (flag, place) in enumerate(((HAS_YM, 0), (HAS_YP, 1 + y))):
            rig, met = got[0][side], got[1][side]
            wide_ext[1 : 1 + x, place : place + 1, at] = jnp.where(flags[flag], rig * met, 0.0)
            inv_ext[1 : 1 + x, place : place + 1, at] = jnp.where(flags[flag], 1.0 / met, 0.0)


def fill_divergence(x, y, ext, inv_ext, div):
    z = ext.shape[-1]
    lane = lax.broadcasted_iota(jnp.int32, (y + 2, z), 1)

    def row(r, carry):
        along_x = ext[0, r + 2, 7 : 9 + y, :] - ext[0, r, 7 : 9 + y, :]
        along_y = ext[1, r + 1, 8 : 10 + y, :] - ext[1, r + 1, 6 : 8 + y, :]
        f = ext[2, r + 1, 7 : 9 + y, :]
        inv = inv_ext[r, 0 : 2 + y, :]
        total = 0.5 * along_x + 0.5 * along_y + inv * slope(f, up_one(f), down_one(f), lane)
        div[r, 7 : 9 + y, :] = jnp.where(inv > 0.0, total, 0.0)
        return carry

    lax.fori_loop(0, x + 2, row, 0, unroll=True)


def update(x, y, ext, wide_ext, inv_ext, div, prev, coef, new, ghosts, psi=None):
    c1, c2, weight, above, vertical = coef
    z = ext.shape[-1]
    lane = lax.broadcasted_iota(jnp.int32, (y, z), 1)
    mid, left, right, own = slice(8, 8 + y), slice(7, 7 + y), slice(9, 9 + y), slice(1, 1 + y)

    def row(i, totals):
        wide = wide_ext[i + 1, own, :]
        w_xp = 0.5 * (wide + wide_ext[i + 2, own, :])
        w_xm = 0.5 * (wide_ext[i, own, :] + wide)
        w_yp = 0.5 * (wide + wide_ext[i + 1, 2 : 2 + y, :])
        w_ym = 0.5 * (wide_ext[i + 1, 0:y, :] + wide)
        inv = inv_ext[i + 1, own, :]
        f = div[i + 1, mid, :]
        gradient = (
            0.5 * (div[i + 2, mid, :] - div[i, mid, :]),
            0.5 * (div[i + 1, right, :] - div[i + 1, left, :]),
            inv * slope(f, up_one(f), down_one(f), lane),
        )
        if psi is not None:
            transposed = (
                0.5 * (psi[i, mid, :] - psi[i + 2, mid, :]),
                0.5 * (psi[i + 1, left, :] - psi[i + 1, right, :]),
                slope_transposed(inv * psi[i + 1, mid, :], lane),
            )
        top, bottom, top_next = ghosts(i)
        k1, k2, dm, va = c1[i], c2[i], weight[i], above[i]
        first = vertical[i, :, 0:1]
        inner, squares, cross = (jnp.zeros((y, z), jnp.float32) for _ in range(3))
        for c in range(3):
            u = ext[c, i + 2, mid, :]
            flux = w_xp * (ext[c, i + 3, mid, :] - u) - w_xm * (u - ext[c, i + 1, mid, :])
            flux += w_yp * (ext[c, i + 2, right, :] - u) - w_ym * (u - ext[c, i + 2, left, :])
            over = va * (jnp.where(lane == z - 1, 0.0, up_one(u)) - u)
            entry = 0.0 if top is None else first * u[:, 0:1]
            flux += over - jnp.where(lane == 0, entry, down_one(over))
            if top is None:
                ghost = jnp.where(lane == z - 1, va * bottom(c), 0.0)
            else:
                ghost = jnp.where(lane == 0, first * top(c), 0.0)
            rate = (flux + ghost) * k1 + k2 * gradient[c]
            updated = 2.0 * u - prev[c, i] + STEP * rate
            change = updated - u
            inner += change * change - STEP * updated * rate
            new[c, i] = updated
            if psi is not None:
                squares += change * change
                cross += updated * (flux + transposed[c])
                if top is not None:
                    cross += jnp.where(lane == 0, first * u[:, 0:1] * top_next(c), 0.0)
        total = totals[0] + dm * inner
        if psi is None:
            return (total,)
        return total, totals[1] + (dm * squares - STEP * cross)

    start = (jnp.zeros((y, z), jnp.float32),) * (1 if psi is None else 2)
    return lax.fori_loop(0, x, row, start, unroll=4)


def step_kernel(s, step, cells, *refs):
    flags = where_am_i()
    refs = list(refs)

    def take(n):
        out = refs[:n]
        del refs[:n]
        return out

    fine, coarse, fine_prev, coarse_prev, offs = take(5)
    coef_f, coef_c = take(5), take(5)
    if step == 0:
        rig_f, met_f, inverse_f, rig_c, met_c, inverse_c = take(6)
    else:
        wide_f, inv_f, wide_c, inv_c = take(4)
    if step < 2:
        beta_own = take(2)
    if step == 1:
        energy_in, spread_in = take(2)
    x_in, y_in = take(2), take(2)
    new_f, new_c = take(2)
    if step < 2:
        (energy,) = take(1)
        x_out = take(2)
    if step == 0:
        wide_f, inv_f, wide_c, inv_c, spread_out = take(5)
    ext_f, ext_c, div_f, div_c, double, pairs = take(6)

    fill_displacement(s, flags, fine, ext_f, x_in, y_in, True)
    fill_displacement(s, flags, coarse, ext_c, x_in, y_in, False)
    if step == 0:
        fill_materials(s, flags, rig_f, met_f, inverse_f, wide_f, inv_f, x_in, y_in, True)
        fill_materials(s, flags, rig_c, met_c, inverse_c, wide_c, inv_c, x_in, y_in, False)

    lane = lax.broadcasted_iota(jnp.int32, (s.cy + 4, LANES), 1)
    for i in range(s.ce):
        e0, e1, e2 = (ext_c[c, i, 6 : 10 + s.cy, 0:LANES] for c in range(3))
        e1, e2 = pltpu.roll(e1, 1, 1), pltpu.roll(e2, 2, 1)
        plane = jnp.where(lane == 0, e0, jnp.where(lane == 1, e1, e2))
        for j in range(s.cy + 4):
            double[i, 2 * j : 2 * j + 2, :] = jnp.broadcast_to(plane[j : j + 1, :], (2, LANES))
    for c in range(3):
        for i in range(s.cx):
            pairs[c, i] = fine[c, 2 * i] + fine[c, 2 * i + 1]

    fill_divergence(s.fx, s.fy, ext_f, inv_f, div_f)
    fill_divergence(s.cx, s.cy, ext_c, inv_c, div_c)
    psi_f = psi_c = None
    if step == 1:
        psi_f, psi_c, all_beta_f, all_beta_c, pairs_next, spread = take(6)
        fill_beta(s, flags, beta_own[0], all_beta_f, x_in, y_in, True)
        fill_beta(s, flags, beta_own[1], all_beta_c, x_in, y_in, False)
        fill_transposed(s.fx, s.fy, ext_f, all_beta_f, inv_f, psi_f)
        fill_transposed(s.cx, s.cy, ext_c, all_beta_c, inv_c, psi_c)

    odd_y = lax.broadcasted_iota(jnp.int32, (s.fy, LANES), 0) % 2
    near_y = jnp.where(odd_y == 0, 0.75, 0.25)

    def node_weights(i):
        near_x = jnp.where(i % 2 == 0, 0.75, 0.25)
        off_x, off_y = offs[i] // 4 - 1, offs[i] % 4 - 1
        out = []
        for off, near in ((off_x, near_x), (off_y, near_y)):
            out.append(
                [
                    jnp.where(off == shift, near, 0.0)
                    + jnp.where(off == shift - 1, 1.0 - near, 0.0)
                    for shift in (-1, 0, 1, 2)
                ]
            )
        return out

    def fine_ghosts(i):
        weights_x, weights_y = node_weights(i)
        total = jnp.zeros((s.fy, LANES), jnp.float32)
        for a in range(4):
            line = jnp.zeros((s.fy, LANES), jnp.float32)
            for b in range(4):
                line += weights_y[b] * double[i // 2 + 1 + a, 2 * b + 2 : 2 * b + 2 + s.fy, :]
            total += weights_x[a] * line
        return None, lambda c: pltpu.roll(total, LANES - 1 - c, 1), None

    def coarse_ghosts(i):
        def mean(of):
            def top(c):
                both = of[c, i, pl.ds(0, s.cy, stride=2), :] + of[c, i, pl.ds(1, s.cy, stride=2), :]
                return 0.25 * both[:, LANES - 1 :]

            return top

        return mean(pairs), None, mean(pairs_next) if step == 1 else None

    sums_f = update(
        s.fx, s.fy, ext_f, wide_f, inv_f, div_f, fine_prev, coef_f, new_f, fine_ghosts, psi_f
    )
    if step == 1:
        for c in range(3):
            for i in range(s.cx):
                pairs_next[c, i] = new_f[c, 2 * i] + new_f[c, 2 * i + 1]
    sums_c = update(
        s.cx, s.cy, ext_c, wide_c, inv_c, div_c, coarse_prev, coef_c, new_c, coarse_ghosts, psi_c
    )
    if step == 2:
        return
    place = lax.broadcasted_iota(jnp.int32, (8, LANES), 0)
    table = jnp.zeros((8, LANES), jnp.float32) if step == 0 else energy_in[...]
    table = jnp.where(place == step, jnp.sum(sums_f[0]) / cells[0], table)
    table = jnp.where(place == STEPS + step, jnp.sum(sums_c[0]) / cells[1], table)
    if step == 0:
        line_lane = lax.broadcasted_iota(jnp.int32, (s.fy, LANES), 1)
        double[...] = jnp.zeros(double.shape, jnp.float32)

        def scatter(i, carry):
            weights_x, weights_y = node_weights(i)
            face = coef_f[3][i]
            q = jnp.zeros((s.fy, LANES), jnp.float32)
            for c in range(3):
                q = jnp.where(line_lane == c, pltpu.roll(face * new_f[c, i], c + 1, 1), q)
            for b in range(4):
                part = weights_y[b] * q
                for a in range(4):
                    rows = slice(2 * b + 2, 2 * b + 2 + s.fy)
                    double[i // 2 + 1 + a, rows, :] += weights_x[a] * part
            return carry

        lax.fori_loop(0, s.fx, scatter, 0, unroll=4)
        rows = s.cy + 4
        for i in range(s.ce):
            evens = double[i, pl.ds(0, rows, stride=2), :]
            spread_out[i, 0:rows, :] = evens + double[i, pl.ds(1, rows, stride=2), :]
            spread_out[i, rows:, :] = jnp.zeros((s.spread - rows, LANES), jnp.float32)
        put_x(s, flags, x_out, new_f, new_c, beta_own, spread_out)
    if step == 1:
        spread[...] = spread_in[:, 2 : 2 + s.cy, :]
        rows = pl.ds(s.y_spread, s.cx)
        low, high = sides(flags, EVEN_Y, HAS_YM, HAS_YP, y_in[0][rows], y_in[1][rows])
        spread[:, 0:2, :] += low
        spread[:, s.cy - 2 : s.cy, :] += high
        joined = jnp.zeros((s.cy, LANES), jnp.float32)
        for i in range(s.cx):
            for c in range(3):
                weights = spread[i] if c == 0 else pltpu.roll(spread[i], LANES - c, 1)
                joined += new_c[c, i, :, 0:LANES] * weights
        joined = jnp.sum(joined[:, 0:1])
        table = jnp.where(place == 2, (jnp.sum(sums_f[1]) - STEP * joined) / cells[0], table)
        table = jnp.where(place == STEPS + 2, jnp.sum(sums_c[1]) / cells[1], table)
        put_x(s, flags, x_out, new_f, new_c)
    energy[...] = table


VMEM = pl.BlockSpec(memory_space=pltpu.VMEM)
HBM = pl.BlockSpec(memory_space=pltpu.HBM)


def call(kernel, shapes, flops, *args, scratch=(), spec=VMEM, sems=0):
    shapes = [jax.ShapeDtypeStruct(shape, jnp.float32) for shape in shapes]
    scratch = [pltpu.VMEM(shape, jnp.float32) for shape in scratch]
    if sems:
        scratch.append(pltpu.SemaphoreType.DMA((sems,)))
    return pl.pallas_call(
        kernel,
        out_shape=shapes,
        in_specs=[spec] * len(args),
        out_specs=[VMEM] * len(shapes),
        scratch_shapes=scratch,
        compiler_params=pltpu.CompilerParams(vmem_limit_bytes=VMEM_LIMIT),
        cost_estimate=pl.CostEstimate(flops=flops, bytes_accessed=1 << 20, transcendentals=0),
    )(*args)


def swap_pairs(mesh, move):
    sizes = list(mesh.shape.values())
    pairs = []
    for source in range(math.prod(sizes)):
        rest, at = source, []
        for size in reversed(sizes):
            at.insert(0, rest % size)
            rest //= size
        target = 0
        for index, size in zip(move(*at), sizes, strict=True):
            target = target * size + index
        pairs.append((source, target))
    return pairs


def beside_x(z, x, y, core):
    return z, x ^ 1, y, core


def across_x(z, x, y, core):
    place = 4 * z + x
    if place in (0, 31):
        return z, x, y, core ^ 1
    place += 1 if place % 2 else -1
    return place // 4, place % 4, y, core


def beside_y(z, x, y, core):
    return z, x, y, core ^ 1


def across_y(z, x, y, core):
    place = (2 * y + core + (1 if core else -1)) % 8
    return z, x, place // 2, place % 2


TOTAL = (
    lambda z, x, y, core: (z, x, y, core ^ 1),
    lambda z, x, y, core: (z, x, y ^ 1, core ^ 1),
    lambda z, x, y, core: (z, x, y ^ 3, core ^ 1),
    lambda z, x, y, core: (z, x ^ 1, y, core ^ 1),
    lambda z, x, y, core: (z, x ^ 3, y, core ^ 1),
    lambda z, x, y, core: (z ^ 1, x, y, core ^ 1),
    lambda z, x, y, core: (z ^ 2, x, y, core ^ 1),
    lambda z, x, y, core: (z ^ 7, x, y, core ^ 1),
)


def per_device(
    mesh,
    fine_disp,
    fine_prev,
    coarse_disp,
    coarse_prev,
    fine_density,
    fine_lame,
    fine_rigidity,
    fine_metric,
    coarse_density,
    coarse_lame,
    coarse_rigidity,
    coarse_metric,
    offsets,
):
    fine_shape, coarse_shape = fine_metric.shape, coarse_metric.shape
    s = Sizes(fine_shape, coarse_shape)
    count_x, count_y = lax.axis_size(GX), lax.axis_size(GY)

    def swap(value, move):
        return lax.ppermute(value, ALL, swap_pairs(mesh, move))

    def swap_both(pair, beside, across):
        second = swap(pair[1], across)
        first = swap(pair[0], beside)
        return [pltpu.with_memory_space_constraint(x, pltpu.VMEM) for x in (first, second)]

    offs = offsets[0] * 4 + offsets[1] + 5
    offs = jnp.broadcast_to(offs[..., None], offs.shape + (LANES,))
    x_out = call(
        functools.partial(first_kernel, s),
        [(s.x_rows_mats, LANES)] * 2,
        1000,
        *(
            pltpu.with_memory_space_constraint(x, pltpu.HBM)
            for x in (
                fine_disp,
                coarse_disp,
                fine_rigidity,
                fine_metric,
                coarse_rigidity,
                coarse_metric,
            )
        ),
        scratch=[
            (2, 3, 2, s.fy, s.fz),
            (2, 3, 2, s.cy, s.cz),
            (2, 2, s.fy, s.fz),
            (2, 2, s.cy, s.cz),
        ],
        spec=HBM,
        sems=12,
    )
    own = []
    for density, lame, rigidity, metric in (
        (fine_density, fine_lame, fine_rigidity, fine_metric),
        (coarse_density, coarse_lame, coarse_rigidity, coarse_metric),
    ):
        own.append(
            call(
                own_kernel,
                [metric.shape] * 5 + [metric.shape[:2] + (LANES,), metric.shape],
                2_000_000,
                density,
                lame,
                rigidity,
                metric,
            )
        )
    inverse_f, *coef_f, beta_f = own[0]
    inverse_c, *coef_c, beta_c = own[1]

    fine, coarse = fine_disp, coarse_disp
    fine_ext = (s.fx + 2, s.fy + 2, s.fz)
    coarse_ext = (s.cx + 2, s.cy + 2, s.cz)
    scratch = [
        (3, s.fe, s.fy + 16, s.fz),
        (3, s.ce, s.cy + 16, s.cz),
        (s.fx + 2, s.fy + 16, s.fz),
        (s.cx + 2, s.cy + 16, s.cz),
        (s.ce, 2 * (s.cy + 4), LANES),
        (3, s.cx, s.fy, LANES),
    ]
    cells = [count_x * count_y * s.fx * s.fy * s.fz, count_x * count_y * s.cx * s.cy * s.cz]
    spread = (s.ce, s.spread, LANES)
    for step in range(STEPS):
        x_in = swap_both(x_out, beside_x, across_x)
        if step == 2:
            for k, move in enumerate(TOTAL):
                other = swap(energy, move)
                if k < len(TOTAL) - 1:
                    energy = energy + other
        shapes = [((s.y_rows_mats, s.y_rows_beta, s.y_rows)[step], 2, LANES)] * 2
        if step == 0:
            mats = [fine_rigidity, fine_metric, coarse_rigidity, coarse_metric]
        if step == 1:
            mats = [beta_f, beta_c, spread_own]
            shapes.append((s.cx,) + spread[1:])
        y_out = call(
            functools.partial(middle_kernel, s, step),
            shapes,
            1000,
            fine,
            coarse,
            *(mats if step < 2 else ()),
            *x_in,
        )
        y_in = swap_both(y_out[:2], beside_y, across_y)
        shapes = [fine.shape, coarse.shape]
        more_scratch = []
        if step < 2:
            shapes += [(8, LANES)] + [((s.x_rows_beta, s.x_rows)[step], LANES)] * 2
        if step == 0:
            extra = [fine_rigidity, fine_metric, inverse_f, coarse_rigidity, coarse_metric, inverse_c]
            extra += [beta_f, beta_c]
            shapes += [fine_ext, fine_ext, coarse_ext, coarse_ext, spread]
        else:
            extra = list(ext_mats)
        if step == 1:
            extra += [beta_f, beta_c, energy, y_out[2]]
            more_scratch = [
                scratch[2],
                scratch[3],
                scratch[0][1:],
                scratch[1][1:],
                scratch[5],
                (s.cx, s.cy, LANES),
            ]
        outs = call(
            functools.partial(step_kernel, s, step, cells),
            shapes,
            4_000_000,
            fine,
            coarse,
            fine_prev,
            coarse_prev,
            offs,
            *coef_f,
            *coef_c,
            *extra,
            *x_in,
            *y_in,
            scratch=scratch + more_scratch,
        )
        fine_prev, coarse_prev = fine, coarse
        fine, coarse = outs[:2]
        if step < 2:
            energy, x_out = outs[2], outs[3:5]
        if step == 0:
            *ext_mats, spread_own = outs[5:]
    other, fine, coarse = lax.optimization_barrier((other, fine, coarse))
    energy = energy + other
    energy = energy[: 2 * STEPS, 0].reshape(2, STEPS).T
    return fine, coarse, energy


def solution(mesh):
    finer = Mesh(mesh.devices.reshape(8, 4, 4, 2), ALL)
    level, cell = P(None, GX, GY, None), P(GX, GY, None)
    in_specs = (level,) * 4 + (cell,) * 8 + (P(None, GX, GY),)

    def body(*args):
        return per_device(finer, *args)

    return jax.shard_map(
        body, mesh=finer, in_specs=in_specs, out_specs=(level, level, P()), check_vma=False
    )
```

```python
import functools
import math

import jax
import jax.numpy as jnp
from jax import lax
from jax.experimental import pallas as pl
from jax.experimental.pallas import tpu as pltpu
from jax.sharding import Mesh
from jax.sharding import PartitionSpec as P

STEPS = 3
GX = ("gx_0", "gx_1")
GY = ("gy_0", "gy_1")
ALL = GX + GY
STEP = 0.15
LANES = 128
VMEM_LIMIT = 20 * 1024 * 1024

EVEN_X, HAS_XM, HAS_XP, EVEN_Y, HAS_YM, HAS_YP = range(6)


def where_am_i():
    x = 4 * lax.axis_index("gx_0") + lax.axis_index("gx_1")
    y = 2 * lax.axis_index("gy_0") + lax.axis_index("gy_1")
    return x % 2 == 0, x > 0, x < 31, y % 2 == 0, y > 0, y < 7


class Sizes:
    def __init__(self, fine, coarse):
        self.fx, self.fy, self.fz = fine
        self.cx, self.cy, self.cz = coarse
        self.halves = self.cz // LANES
        self.x_fine = 0
        self.x_coarse = 6 * self.fy
        self.x_rows = self.x_coarse + self.halves * 6 * self.cy
        self.x_fine_mats = self.x_rows
        self.x_coarse_mats = self.x_fine_mats + 2 * self.fy
        self.x_rows_mats = self.x_coarse_mats + 2 * self.halves * self.cy
        self.x_fine_beta = self.x_rows
        self.x_coarse_beta = self.x_fine_beta + 2 * self.fy
        self.x_spread = self.x_coarse_beta + self.halves * 2 * self.cy
        self.spread = self.cy + 8
        self.x_rows_beta = self.x_spread + 2 * self.spread
        self.fe, self.ce = self.fx + 4, self.cx + 4
        self.y_coarse = 3 * self.fe
        self.y_rows = self.y_coarse + self.halves * 3 * self.ce
        self.y_fine_mats = self.y_rows
        self.y_coarse_mats = self.y_fine_mats + self.fx
        self.y_rows_mats = self.y_coarse_mats + self.halves * self.cx
        self.y_fine_beta = self.y_rows
        self.y_coarse_beta = self.y_fine_beta + self.fe
        self.y_spread = self.y_coarse_beta + self.halves * self.ce
        self.y_rows_beta = self.y_spread + self.cx


def lanes_of(h):
    return slice(h * LANES, (h + 1) * LANES)


def put_x(s, flags, outs, fine, coarse, betas=None, spread=None):
    even = flags[EVEN_X]
    for k, out in enumerate(outs):
        far = even if k == 0 else jnp.logical_not(even)
        start_f = jnp.where(far, s.fx - 2, 0)
        start_c = jnp.where(far, s.cx - 2, 0)
        out[0 : s.x_coarse, :] = fine[:, pl.ds(start_f, 2), :, :].reshape(6 * s.fy, LANES)
        strip = coarse[:, pl.ds(start_c, 2), :, :]
        for h in range(s.halves):
            base = s.x_coarse + h * 6 * s.cy
            out[base : base + 6 * s.cy, :] = strip[:, :, :, lanes_of(h)].reshape(6 * s.cy, LANES)
        if betas is None:
            continue
        strip = betas[0][pl.ds(start_f, 2), :, :]
        out[s.x_fine_beta : s.x_coarse_beta, :] = strip.reshape(2 * s.fy, LANES)
        strip = betas[1][pl.ds(start_c, 2), :, :]
        for h in range(s.halves):
            base = s.x_coarse_beta + h * 2 * s.cy
            out[base : base + 2 * s.cy, :] = strip[:, :, lanes_of(h)].reshape(2 * s.cy, LANES)
        start = jnp.where(far, s.cx + 2, 0)
        out[s.x_spread : s.x_rows_beta, :] = spread[pl.ds(start, 2)].reshape(2 * s.spread, LANES)


def first_kernel(s, fine, coarse, rig_f, met_f, rig_c, met_c, out_a, out_b, *scratch):
    strip_f, strip_c, line_f, line_c, sems = scratch
    flags = where_am_i()
    copies = []

    def fetch(source, target):
        copies.append(pltpu.make_async_copy(source, target, sems.at[len(copies)]))
        copies[-1].start()

    even = flags[EVEN_X]
    for k in range(2):
        far = even if k == 0 else jnp.logical_not(even)
        fetch(fine.at[:, pl.ds(jnp.where(far, s.fx - 2, 0), 2)], strip_f.at[k])
        fetch(coarse.at[:, pl.ds(jnp.where(far, s.cx - 2, 0), 2)], strip_c.at[k])
        for m, (of_f, of_c) in enumerate(((rig_f, rig_c), (met_f, met_c))):
            fetch(of_f.at[jnp.where(far, s.fx - 1, 0)], line_f.at[k, m])
            fetch(of_c.at[jnp.where(far, s.cx - 1, 0)], line_c.at[k, m])
    for copy in copies:
        copy.wait()
    for k, out in enumerate((out_a, out_b)):
        out[0 : s.x_coarse, :] = strip_f[k].reshape(6 * s.fy, LANES)
        for m in range(2):
            base = s.x_fine_mats + m * s.fy
            out[base : base + s.fy, :] = line_f[k, m]
        for h in range(s.halves):
            base = s.x_coarse + h * 6 * s.cy
            out[base : base + 6 * s.cy, :] = strip_c[k, :, :, :, lanes_of(h)].reshape(6 * s.cy, LANES)
            for m in range(2):
                base = s.x_coarse_mats + (m * s.halves + h) * s.cy
                out[base : base + s.cy, :] = line_c[k, m, :, lanes_of(h)]


def sides(flags, even, has_low, has_high, a, b):
    low = jnp.where(flags[even], b, a)
    high = jnp.where(flags[even], a, b)
    low = jnp.where(flags[has_low], low, 0.0)
    high = jnp.where(flags[has_high], high, 0.0)
    return low, high


def middle_kernel(s, step, *refs):
    flags = where_am_i()
    fine, coarse, *mats, in_a, in_b = refs[:-2] if step != 1 else refs[:-3]
    out_a, out_b = refs[-2:] if step != 1 else refs[-3:-1]
    even = flags[EVEN_Y]

    def put(index, low, high):
        out_a[index] = jnp.where(even, high, low)
        out_b[index] = jnp.where(even, low, high)

    def field(own, x, y, x_base, y_base):
        put(pl.ds(y_base + 2, x), own(slice(0, 2)), own(slice(y - 2, y)))
        for k in range(2):
            pieces = []
            for first in (0, y - 2):
                rows = slice(x_base + k * y + first, x_base + k * y + first + 2)
                pieces.append(sides(flags, EVEN_X, HAS_XM, HAS_XP, in_a[rows, :], in_b[rows, :]))
            for side in range(2):
                place = y_base + (k if side == 0 else x + 2 + k)
                put(place, pieces[0][side], pieces[1][side])

    for c in range(3):
        field(lambda r: fine[c, :, r, :], s.fx, s.fy, c * 2 * s.fy, c * s.fe)
        for h in range(s.halves):
            at = lanes_of(h)
            x_base, y_base = s.x_coarse + (h * 6 + c * 2) * s.cy, s.y_coarse + (h * 3 + c) * s.ce
            field(lambda r: coarse[c, :, r, at], s.cx, s.cy, x_base, y_base)
    if step == 0:
        rig_f, met_f, rig_c, met_c = mats
        for m, (of_f, of_c) in enumerate(((rig_f, rig_c), (met_f, met_c))):
            low, high = of_f[:, 0:1, :], of_f[:, s.fy - 1 : s.fy, :]
            where = pl.ds(s.y_fine_mats, s.fx)
            out_a[where, m : m + 1, :] = jnp.where(even, high, low)
            out_b[where, m : m + 1, :] = jnp.where(even, low, high)
            for h in range(s.halves):
                low, high = of_c[:, 0:1, lanes_of(h)], of_c[:, s.cy - 1 : s.cy, lanes_of(h)]
                where = pl.ds(s.y_coarse_mats + h * s.cx, s.cx)
                out_a[where, m : m + 1, :] = jnp.where(even, high, low)
                out_b[where, m : m + 1, :] = jnp.where(even, low, high)
    if step == 1:
        beta_f, beta_c, spread = mats
        field(lambda r: beta_f[:, r, :], s.fx, s.fy, s.x_fine_beta, s.y_fine_beta)
        for h in range(s.halves):
            at = lanes_of(h)
            x_base, y_base = s.x_coarse_beta + h * 2 * s.cy, s.y_coarse_beta + h * s.ce
            field(lambda r: beta_c[:, r, at], s.cx, s.cy, x_base, y_base)
        total = refs[-1]
        total[...] = spread[2 : 2 + s.cx]
        for k in range(2):
            rows = slice(s.x_spread + k * s.spread, s.x_spread + (k + 1) * s.spread)
            low, high = sides(flags, EVEN_X, HAS_XM, HAS_XP, in_a[rows, :], in_b[rows, :])
            total[k] += low
            total[s.cx - 2 + k] += high
        put(pl.ds(s.y_spread, s.cx), total[:, 0:2, :], total[:, s.cy + 2 : s.cy + 4, :])


def up_one(x):
    return pltpu.roll(x, x.shape[-1] - 1, x.ndim - 1)


def down_one(x):
    return pltpu.roll(x, 1, x.ndim - 1)


def own_kernel(density, lame, rigidity, metric, inverse, c1, c2, weight, above, first, beta):
    inv = 1.0 / metric[...]
    inverse[...] = inv
    over = 1.0 / density[...]
    c1[...] = inv * over
    c2[...] = (lame[...] + rigidity[...]) * over
    weight[...] = density[...] * metric[...]
    v = rigidity[...] * inv
    lane = lax.broadcasted_iota(jnp.int32, v.shape, 2)
    above[...] = jnp.where(lane == v.shape[2] - 1, v, 0.5 * (v + up_one(v)))
    first[...] = v[:, :, 0:LANES]
    beta[...] = (lame[...] + rigidity[...]) * metric[...]


def slope(f, up, down, lane):
    last = f.shape[-1] - 1
    return jnp.where(lane == 0, up - f, jnp.where(lane == last, f - down, 0.5 * (up - down)))


def slope_transposed(q, lane):
    last = q.shape[-1] - 1
    half = jnp.where((lane == 0) | (lane == last), q, 0.5 * q)
    down = jnp.where(lane == 0, -half, down_one(half))
    return down - jnp.where(lane == last, -half, up_one(half))


def fill_beta(s, flags, own, ext, x_in, y_in, fine):
    x, y, e = (s.fx, s.fy, s.fe) if fine else (s.cx, s.cy, s.ce)
    ext[2 : 2 + x, 8 : 8 + y, :] = own[...]
    for h in range(1 if fine else s.halves):
        at = lanes_of(h)
        base = s.x_fine_beta if fine else s.x_coarse_beta + h * 2 * y
        rows = slice(base, base + 2 * y)
        low, high = sides(flags, EVEN_X, HAS_XM, HAS_XP, x_in[0][rows, :], x_in[1][rows, :])
        ext[0:2, 8 : 8 + y, at] = low.reshape(2, y, LANES)
        ext[x + 2 : x + 4, 8 : 8 + y, at] = high.reshape(2, y, LANES)
        start = s.y_fine_beta if fine else s.y_coarse_beta + h * e
        rows = slice(start, start + e)
        low, high = sides(flags, EVEN_Y, HAS_YM, HAS_YP, y_in[0][rows], y_in[1][rows])
        ext[:, 6:8, at] = low
        ext[:, 8 + y : 10 + y, at] = high


def fill_transposed(x, y, ext, beta, inv_ext, psi):
    z = ext.shape[-1]
    lane = lax.broadcasted_iota(jnp.int32, (y + 2, z), 1)
    wide, low, high = slice(7, 9 + y), slice(6, 8 + y), slice(8, 10 + y)

    def row(r, carry):
        along_x = ext[0, r, wide, :] * beta[r, wide, :]
        along_x -= ext[0, r + 2, wide, :] * beta[r + 2, wide, :]
        along_y = ext[1, r + 1, low, :] * beta[r + 1, low, :]
        along_y -= ext[1, r + 1, high, :] * beta[r + 1, high, :]
        inv = inv_ext[r, 0 : 2 + y, :]
        column = inv * beta[r + 1, wide, :] * ext[2, r + 1, wide, :]
        total = 0.5 * along_x + 0.5 * along_y + slope_transposed(column, lane)
        psi[r, wide, :] = jnp.where(inv > 0.0, total, 0.0)
        return carry

    lax.fori_loop(0, x + 2, row, 0, unroll=True)


def fill_displacement(s, flags, own, ext, x_in, y_in, fine):
    x, y, e = (s.fx, s.fy, s.fe) if fine else (s.cx, s.cy, s.ce)
    ext[:, 2 : 2 + x, 8 : 8 + y, :] = own[...]
    for h in range(1 if fine else s.halves):
        base = s.x_fine if fine else s.x_coarse + h * 6 * y
        rows = slice(base, base + 6 * y)
        low, high = sides(flags, EVEN_X, HAS_XM, HAS_XP, x_in[0][rows, :], x_in[1][rows, :])
        ext[:, 0:2, 8 : 8 + y, lanes_of(h)] = low.reshape(3, 2, y, LANES)
        ext[:, x + 2 : x + 4, 8 : 8 + y, lanes_of(h)] = high.reshape(3, 2, y, LANES)
        for c in range(3):
            start = c * e if fine else s.y_coarse + (h * 3 + c) * e
            rows = slice(start, start + e)
            low, high = sides(flags, EVEN_Y, HAS_YM, HAS_YP, y_in[0][rows], y_in[1][rows])
            ext[c, :, 6:8, lanes_of(h)] = low
            ext[c, :, 8 + y : 10 + y, lanes_of(h)] = high


def fill_materials(s, flags, rigidity, metric, inverse, wide_ext, inv_ext, x_in, y_in, fine):
    x, y = (s.fx, s.fy) if fine else (s.cx, s.cy)
    wide_ext[1 : 1 + x, 1 : 1 + y, :] = rigidity[...] * metric[...]
    inv_ext[1 : 1 + x, 1 : 1 + y, :] = inverse[...]
    for h in range(1 if fine else s.halves):
        at = lanes_of(h)
        got = []
        for m in range(2):
            base = s.x_fine_mats + m * y if fine else s.x_coarse_mats + (m * s.halves + h) * y
            rows = slice(base, base + y)
            even = flags[EVEN_X]
            a, b = x_in[0][rows, :], x_in[1][rows, :]
            got.append((jnp.where(even, b, a), jnp.where(even, a, b)))
        for side, (flag, place) in enumerate(((HAS_XM, 0), (HAS_XP, x + 1))):
            rig, met = got[0][side], got[1][side]
            wide_ext[place, 1 : 1 + y, at] = jnp.where(flags[flag], rig * met, 0.0)
            inv_ext[place, 1 : 1 + y, at] = jnp.where(flags[flag], 1.0 / met, 0.0)
        start = s.y_fine_mats if fine else s.y_coarse_mats + h * x
        rows = slice(start, start + x)
        got = []
        for m in range(2):
            even = flags[EVEN_Y]
            a, b = y_in[0][rows, m : m + 1, :], y_in[1][rows, m : m + 1, :]
            got.append((jnp.where(even, b, a), jnp.where(even, a, b)))
        for side, (flag, place) in enumerate(((HAS_YM, 0), (HAS_YP, 1 + y))):
            rig, met = got[0][side], got[1][side]
            wide_ext[1 : 1 + x, place : place + 1, at] = jnp.where(flags[flag], rig * met, 0.0)
            inv_ext[1 : 1 + x, place : place + 1, at] = jnp.where(flags[flag], 1.0 / met, 0.0)


def fill_divergence(x, y, ext, inv_ext, div):
    z = ext.shape[-1]
    lane = lax.broadcasted_iota(jnp.int32, (y + 2, z), 1)

    def row(r, carry):
        along_x = ext[0, r + 2, 7 : 9 + y, :] - ext[0, r, 7 : 9 + y, :]
        along_y = ext[1, r + 1, 8 : 10 + y, :] - ext[1, r + 1, 6 : 8 + y, :]
        f = ext[2, r + 1, 7 : 9 + y, :]
        inv = inv_ext[r, 0 : 2 + y, :]
        total = 0.5 * along_x + 0.5 * along_y + inv * slope(f, up_one(f), down_one(f), lane)
        div[r, 7 : 9 + y, :] = jnp.where(inv > 0.0, total, 0.0)
        return carry

    lax.fori_loop(0, x + 2, row, 0, unroll=True)


def update(x, y, ext, wide_ext, inv_ext, div, prev, coef, new, ghosts, psi=None):
    c1, c2, weight, above, vertical = coef
    z = ext.shape[-1]
    lane = lax.broadcasted_iota(jnp.int32, (y, z), 1)
    mid, left, right, own = slice(8, 8 + y), slice(7, 7 + y), slice(9, 9 + y), slice(1, 1 + y)

    def row(i, totals):
        wide = wide_ext[i + 1, own, :]
        w_xp = 0.5 * (wide + wide_ext[i + 2, own, :])
        w_xm = 0.5 * (wide_ext[i, own, :] + wide)
        w_yp = 0.5 * (wide + wide_ext[i + 1, 2 : 2 + y, :])
        w_ym = 0.5 * (wide_ext[i + 1, 0:y, :] + wide)
        inv = inv_ext[i + 1, own, :]
        f = div[i + 1, mid, :]
        gradient = (
            0.5 * (div[i + 2, mid, :] - div[i, mid, :]),
            0.5 * (div[i + 1, right, :] - div[i + 1, left, :]),
            inv * slope(f, up_one(f), down_one(f), lane),
        )
        if psi is not None:
            transposed = (
                0.5 * (psi[i, mid, :] - psi[i + 2, mid, :]),
                0.5 * (psi[i + 1, left, :] - psi[i + 1, right, :]),
                slope_transposed(inv * psi[i + 1, mid, :], lane),
            )
        top, bottom, top_next = ghosts(i)
        k1, k2, dm, va = c1[i], c2[i], weight[i], above[i]
        first = vertical[i, :, 0:1]
        inner, squares, cross = (jnp.zeros((y, z), jnp.float32) for _ in range(3))
        for c in range(3):
            u = ext[c, i + 2, mid, :]
            flux = w_xp * (ext[c, i + 3, mid, :] - u) - w_xm * (u - ext[c, i + 1, mid, :])
            flux += w_yp * (ext[c, i + 2, right, :] - u) - w_ym * (u - ext[c, i + 2, left, :])
            over = va * (jnp.where(lane == z - 1, 0.0, up_one(u)) - u)
            entry = 0.0 if top is None else first * u[:, 0:1]
            flux += over - jnp.where(lane == 0, entry, down_one(over))
            if top is None:
                ghost = jnp.where(lane == z - 1, va * bottom(c), 0.0)
            else:
                ghost = jnp.where(lane == 0, first * top(c), 0.0)
            rate = (flux + ghost) * k1 + k2 * gradient[c]
            updated = 2.0 * u - prev[c, i] + STEP * rate
            change = updated - u
            inner += change * change - STEP * updated * rate
            new[c, i] = updated
            if psi is not None:
                squares += change * change
                cross += updated * (flux + transposed[c])
                if top is not None:
                    cross += jnp.where(lane == 0, first * u[:, 0:1] * top_next(c), 0.0)
        total = totals[0] + dm * inner
        if psi is None:
            return (total,)
        return total, totals[1] + (dm * squares - STEP * cross)

    start = (jnp.zeros((y, z), jnp.float32),) * (1 if psi is None else 2)
    return lax.fori_loop(0, x, row, start, unroll=4)


def step_kernel(s, step, cells, *refs):
    flags = where_am_i()
    refs = list(refs)

    def take(n):
        out = refs[:n]
        del refs[:n]
        return out

    fine, coarse, fine_prev, coarse_prev, offs = take(5)
    coef_f, coef_c = take(5), take(5)
    if step == 0:
        rig_f, met_f, inverse_f, rig_c, met_c, inverse_c = take(6)
    else:
        wide_f, inv_f, wide_c, inv_c = take(4)
    if step < 2:
        beta_own = take(2)
    if step == 1:
        energy_in, spread_in = take(2)
    x_in, y_in = take(2), take(2)
    new_f, new_c = take(2)
    if step < 2:
        (energy,) = take(1)
        x_out = take(2)
    if step == 0:
        wide_f, inv_f, wide_c, inv_c, spread_out = take(5)
    ext_f, ext_c, div_f, div_c, double, moved, pairs = take(7)

    fill_displacement(s, flags, fine, ext_f, x_in, y_in, True)
    fill_displacement(s, flags, coarse, ext_c, x_in, y_in, False)
    if step == 0:
        fill_materials(s, flags, rig_f, met_f, inverse_f, wide_f, inv_f, x_in, y_in, True)
        fill_materials(s, flags, rig_c, met_c, inverse_c, wide_c, inv_c, x_in, y_in, False)

    lane = lax.broadcasted_iota(jnp.int32, (s.cy + 4, LANES), 1)
    table = jnp.zeros((s.cy + 4, LANES), jnp.float32)
    for i in range(s.ce):
        e0, e1, e2 = (ext_c[c, i, 6 : 10 + s.cy, 0:LANES] for c in range(3))
        e1, e2 = pltpu.roll(e1, 1, 1), pltpu.roll(e2, 2, 1)
        plane = jnp.where(lane == 0, e0, jnp.where(lane == 1, e1, e2))
        for k in (2 * i, 2 * i + 1):
            there = pltpu.roll(plane, 4 * k, 1) if k else plane
            table = jnp.where(lane // 4 == k, there, table)
    for j in range(s.cy + 4):
        double[2 * j : 2 * j + 2, :] = jnp.broadcast_to(table[j : j + 1, :], (2, LANES))
    for c in range(3):
        for i in range(s.cx):
            pairs[c, i] = fine[c, 2 * i] + fine[c, 2 * i + 1]

    fill_divergence(s.fx, s.fy, ext_f, inv_f, div_f)
    fill_divergence(s.cx, s.cy, ext_c, inv_c, div_c)
    psi_f = psi_c = None
    if step == 1:
        psi_f, psi_c, all_beta_f, all_beta_c, pairs_next, spread = take(6)
        fill_beta(s, flags, beta_own[0], all_beta_f, x_in, y_in, True)
        fill_beta(s, flags, beta_own[1], all_beta_c, x_in, y_in, False)
        fill_transposed(s.fx, s.fy, ext_f, all_beta_f, inv_f, psi_f)
        fill_transposed(s.cx, s.cy, ext_c, all_beta_c, inv_c, psi_c)

    node = (s.fy, LANES)
    node_lane = lax.broadcasted_iota(jnp.int32, node, 1)
    near_x = jnp.where(node_lane // 4 % 2 == 0, 0.75, 0.25)
    near_y = jnp.where(lax.broadcasted_iota(jnp.int32, node, 0) % 2 == 0, 0.75, 0.25)
    code = offs[...]
    weights_x, weights_y = (
        [
            jnp.where(off == shift, near, 0.0) + jnp.where(off == shift - 1, 1.0 - near, 0.0)
            for shift in (-1, 0, 1, 2)
        ]
        for off, near in ((code // 4 - 1, near_x), (code % 4 - 1, near_y))
    )
    ghosts = jnp.zeros(node, jnp.float32)
    for a in range(4):
        moved[a] = pltpu.roll(double[...], LANES - 8 * (1 + a), 1)
        line = jnp.zeros(node, jnp.float32)
        for b in range(4):
            line += weights_y[b] * moved[a, 2 * b + 2 : 2 * b + 2 + s.fy, :]
        ghosts += weights_x[a] * line

    def fine_ghosts(i):
        return None, lambda c: pltpu.roll(ghosts, LANES - 1 - c - 4 * i, 1), None

    def coarse_ghosts(i):
        def mean(of):
            def top(c):
                both = of[c, i, pl.ds(0, s.cy, stride=2), :] + of[c, i, pl.ds(1, s.cy, stride=2), :]
                return 0.25 * both[:, LANES - 1 :]

            return top

        return mean(pairs), None, mean(pairs_next) if step == 1 else None

    sums_f = update(
        s.fx, s.fy, ext_f, wide_f, inv_f, div_f, fine_prev, coef_f, new_f, fine_ghosts, psi_f
    )
    if step == 1:
        for c in range(3):
            for i in range(s.cx):
                pairs_next[c, i] = new_f[c, 2 * i] + new_f[c, 2 * i + 1]
    sums_c = update(
        s.cx, s.cy, ext_c, wide_c, inv_c, div_c, coarse_prev, coef_c, new_c, coarse_ghosts, psi_c
    )
    if step == 2:
        return
    place = lax.broadcasted_iota(jnp.int32, (8, LANES), 0)
    table = jnp.zeros((8, LANES), jnp.float32) if step == 0 else energy_in[...]
    table = jnp.where(place == step, jnp.sum(sums_f[0]) / cells[0], table)
    table = jnp.where(place == STEPS + step, jnp.sum(sums_c[0]) / cells[1], table)
    if step == 0:
        q = jnp.zeros(node, jnp.float32)
        for i in range(s.fx):
            for c in range(3):
                there = pltpu.roll(coef_f[3][i] * new_f[c, i], 4 * i + c + 1, 1)
                q = jnp.where(node_lane == 4 * i + c, there, q)
        moved[...] = jnp.zeros(moved.shape, jnp.float32)
        for a in range(4):
            part = weights_x[a] * q
            for b in range(4):
                moved[a, 2 * b + 2 : 2 * b + 2 + s.fy, :] += weights_y[b] * part
        double[...] = sum(pltpu.roll(moved[a], 8 * (1 + a), 1) for a in range(4))
        rows = s.cy + 4
        both = double[pl.ds(0, rows, stride=2), :] + double[pl.ds(1, rows, stride=2), :]
        for i in range(s.ce):
            there = pltpu.roll(both, LANES - 8 * i, 1) if i else both
            spread_out[i, 0:rows, :] = there + pltpu.roll(there, LANES - 4, 1)
            spread_out[i, rows:, :] = jnp.zeros((s.spread - rows, LANES), jnp.float32)
        put_x(s, flags, x_out, new_f, new_c, beta_own, spread_out)
    if step == 1:
        spread[...] = spread_in[:, 2 : 2 + s.cy, :]
        rows = pl.ds(s.y_spread, s.cx)
        low, high = sides(flags, EVEN_Y, HAS_YM, HAS_YP, y_in[0][rows], y_in[1][rows])
        spread[:, 0:2, :] += low
        spread[:, s.cy - 2 : s.cy, :] += high
        joined = jnp.zeros((s.cy, LANES), jnp.float32)
        for i in range(s.cx):
            for c in range(3):
                weights = spread[i] if c == 0 else pltpu.roll(spread[i], LANES - c, 1)
                joined += new_c[c, i, :, 0:LANES] * weights
        joined = jnp.sum(joined[:, 0:1])
        table = jnp.where(place == 2, (jnp.sum(sums_f[1]) - STEP * joined) / cells[0], table)
        table = jnp.where(place == STEPS + 2, jnp.sum(sums_c[1]) / cells[1], table)
        put_x(s, flags, x_out, new_f, new_c)
    energy[...] = table


VMEM = pl.BlockSpec(memory_space=pltpu.VMEM)
HBM = pl.BlockSpec(memory_space=pltpu.HBM)


def call(kernel, shapes, flops, *args, scratch=(), spec=VMEM, sems=0):
    shapes = [jax.ShapeDtypeStruct(shape, jnp.float32) for shape in shapes]
    scratch = [pltpu.VMEM(shape, jnp.float32) for shape in scratch]
    if sems:
        scratch.append(pltpu.SemaphoreType.DMA((sems,)))
    return pl.pallas_call(
        kernel,
        out_shape=shapes,
        in_specs=[spec] * len(args),
        out_specs=[VMEM] * len(shapes),
        scratch_shapes=scratch,
        compiler_params=pltpu.CompilerParams(vmem_limit_bytes=VMEM_LIMIT),
        cost_estimate=pl.CostEstimate(flops=flops, bytes_accessed=1 << 20, transcendentals=0),
    )(*args)


def swap_pairs(mesh, move):
    sizes = list(mesh.shape.values())
    pairs = []
    for source in range(math.prod(sizes)):
        rest, at = source, []
        for size in reversed(sizes):
            at.insert(0, rest % size)
            rest //= size
        target = 0
        for index, size in zip(move(*at), sizes, strict=True):
            target = target * size + index
        pairs.append((source, target))
    return pairs


def beside_x(z, x, y, core):
    return z, x ^ 1, y, core


def across_x(z, x, y, core):
    place = 4 * z + x
    if place in (0, 31):
        return z, x, y, core ^ 1
    place += 1 if place % 2 else -1
    return place // 4, place % 4, y, core


def beside_y(z, x, y, core):
    return z, x, y, core ^ 1


def across_y(z, x, y, core):
    place = (2 * y + core + (1 if core else -1)) % 8
    return z, x, place // 2, place % 2


TOTAL = (
    lambda z, x, y, core: (z ^ 7, x, y, core),
    lambda z, x, y, core: (z, x, y, core ^ 1),
    lambda z, x, y, core: (z ^ 2, x, y, core ^ 1),
    lambda z, x, y, core: (z, x, y ^ 1, core ^ 1),
    lambda z, x, y, core: (z, x ^ 1, y, core ^ 1),
    lambda z, x, y, core: (z ^ 1, x, y, core ^ 1),
    lambda z, x, y, core: (z, x ^ 3, y, core ^ 1),
    lambda z, x, y, core: (z, x, y ^ 3, core ^ 1),
)


def per_device(
    mesh,
    fine_disp,
    fine_prev,
    coarse_disp,
    coarse_prev,
    fine_density,
    fine_lame,
    fine_rigidity,
    fine_metric,
    coarse_density,
    coarse_lame,
    coarse_rigidity,
    coarse_metric,
    offsets,
):
    fine_shape, coarse_shape = fine_metric.shape, coarse_metric.shape
    s = Sizes(fine_shape, coarse_shape)
    count_x, count_y = lax.axis_size(GX), lax.axis_size(GY)

    def swap(value, move):
        return lax.ppermute(value, ALL, swap_pairs(mesh, move))

    def swap_both(pair, beside, across):
        second = swap(pair[1], across)
        first = swap(pair[0], beside)
        return [pltpu.with_memory_space_constraint(x, pltpu.VMEM) for x in (first, second)]

    offs = offsets[0] * 4 + offsets[1] + 5
    offs = jnp.pad(jnp.repeat(offs.T, 4, axis=1), ((0, 0), (0, LANES - 4 * s.fx)))
    x_out = call(
        functools.partial(first_kernel, s),
        [(s.x_rows_mats, LANES)] * 2,
        1000,
        *(
            pltpu.with_memory_space_constraint(x, pltpu.HBM)
            for x in (
                fine_disp,
                coarse_disp,
                fine_rigidity,
                fine_metric,
                coarse_rigidity,
                coarse_metric,
            )
        ),
        scratch=[
            (2, 3, 2, s.fy, s.fz),
            (2, 3, 2, s.cy, s.cz),
            (2, 2, s.fy, s.fz),
            (2, 2, s.cy, s.cz),
        ],
        spec=HBM,
        sems=12,
    )
    own = []
    for density, lame, rigidity, metric in (
        (fine_density, fine_lame, fine_rigidity, fine_metric),
        (coarse_density, coarse_lame, coarse_rigidity, coarse_metric),
    ):
        own.append(
            call(
                own_kernel,
                [metric.shape] * 5 + [metric.shape[:2] + (LANES,), metric.shape],
                2_000_000,
                density,
                lame,
                rigidity,
                metric,
            )
        )
    inverse_f, *coef_f, beta_f = own[0]
    inverse_c, *coef_c, beta_c = own[1]

    fine, coarse = fine_disp, coarse_disp
    fine_ext = (s.fx + 2, s.fy + 2, s.fz)
    coarse_ext = (s.cx + 2, s.cy + 2, s.cz)
    scratch = [
        (3, s.fe, s.fy + 16, s.fz),
        (3, s.ce, s.cy + 16, s.cz),
        (s.fx + 2, s.fy + 16, s.fz),
        (s.cx + 2, s.cy + 16, s.cz),
        (2 * (s.cy + 4), LANES),
        (4, 2 * (s.cy + 4), LANES),
        (3, s.cx, s.fy, LANES),
    ]
    cells = [count_x * count_y * s.fx * s.fy * s.fz, count_x * count_y * s.cx * s.cy * s.cz]
    spread = (s.ce, s.spread, LANES)
    for step in range(STEPS):
        x_in = swap_both(x_out, beside_x, across_x)
        if step == 2:
            for k, move in enumerate(TOTAL):
                other = swap(energy, move)
                if k < len(TOTAL) - 1:
                    energy = energy + other
        shapes = [((s.y_rows_mats, s.y_rows_beta, s.y_rows)[step], 2, LANES)] * 2
        if step == 0:
            mats = [fine_rigidity, fine_metric, coarse_rigidity, coarse_metric]
        if step == 1:
            mats = [beta_f, beta_c, spread_own]
            shapes.append((s.cx,) + spread[1:])
        y_out = call(
            functools.partial(middle_kernel, s, step),
            shapes,
            1000,
            fine,
            coarse,
            *(mats if step < 2 else ()),
            *x_in,
        )
        y_in = swap_both(y_out[:2], beside_y, across_y)
        shapes = [fine.shape, coarse.shape]
        more_scratch = []
        if step < 2:
            shapes += [(8, LANES)] + [((s.x_rows_beta, s.x_rows)[step], LANES)] * 2
        if step == 0:
            extra = [fine_rigidity, fine_metric, inverse_f, coarse_rigidity, coarse_metric, inverse_c]
            extra += [beta_f, beta_c]
            shapes += [fine_ext, fine_ext, coarse_ext, coarse_ext, spread]
        else:
            extra = list(ext_mats)
        if step == 1:
            extra += [beta_f, beta_c, energy, y_out[2]]
            more_scratch = [
                scratch[2],
                scratch[3],
                scratch[0][1:],
                scratch[1][1:],
                scratch[6],
                (s.cx, s.cy, LANES),
            ]
        outs = call(
            functools.partial(step_kernel, s, step, cells),
            shapes,
            4_000_000,
            fine,
            coarse,
            fine_prev,
            coarse_prev,
            offs,
            *coef_f,
            *coef_c,
            *extra,
            *x_in,
            *y_in,
            scratch=scratch + more_scratch,
        )
        fine_prev, coarse_prev = fine, coarse
        fine, coarse = outs[:2]
        if step < 2:
            energy, x_out = outs[2], outs[3:5]
        if step == 0:
            *ext_mats, spread_own = outs[5:]
    other, fine, coarse = lax.optimization_barrier((other, fine, coarse))
    energy = energy + other
    energy = energy[: 2 * STEPS, 0].reshape(2, STEPS).T
    return fine, coarse, energy


def solution(mesh):
    finer = Mesh(mesh.devices.reshape(8, 4, 4, 2), ALL)
    level, cell = P(None, GX, GY, None), P(GX, GY, None)
    in_specs = (level,) * 4 + (cell,) * 8 + (P(None, GX, GY),)

    def body(*args):
        return per_device(finer, *args)

    return jax.shard_map(
        body, mesh=finer, in_specs=in_specs, out_specs=(level, level, P()), check_vma=False
    )
```

```python
import functools
import math

import jax
import jax.numpy as jnp
from jax import lax
from jax.experimental import pallas as pl
from jax.experimental.pallas import tpu as pltpu
from jax.sharding import Mesh
from jax.sharding import PartitionSpec as P

STEPS = 3
GX = ("gx_0", "gx_1")
GY = ("gy_0", "gy_1")
ALL = GX + GY
STEP = 0.15
LANES = 128
VMEM_LIMIT = 20 * 1024 * 1024

EVEN_X, HAS_XM, HAS_XP, EVEN_Y, HAS_YM, HAS_YP = range(6)


def where_am_i():
    x = 4 * lax.axis_index("gx_0") + lax.axis_index("gx_1")
    y = 2 * lax.axis_index("gy_0") + lax.axis_index("gy_1")
    return x % 2 == 0, x > 0, x < 31, y % 2 == 0, y > 0, y < 7


class Sizes:
    def __init__(self, fine, coarse):
        self.fx, self.fy, self.fz = fine
        self.cx, self.cy, self.cz = coarse
        self.halves = self.cz // LANES
        self.x_coarse = 4 * self.fy
        self.x_plane = self.x_coarse + self.halves * 4 * self.cy
        self.x_rows = self.x_plane + self.cy
        self.x_fine_mats = self.x_rows
        self.x_coarse_mats = self.x_fine_mats + 2 * self.fy
        self.x_rows_mats = self.x_coarse_mats + 2 * self.halves * self.cy
        self.x_fine_beta = self.x_rows
        self.x_coarse_beta = self.x_fine_beta + 2 * self.fy
        self.x_spread = self.x_coarse_beta + self.halves * 2 * self.cy
        self.spread = self.cy + 8
        self.x_rows_beta = self.x_spread + 2 * self.spread
        self.fe, self.ce = self.fx + 4, self.cx + 4
        self.y_coarse = 2 * self.fe
        self.y_plane = self.y_coarse + self.halves * 2 * self.ce
        self.y_rows = self.y_plane + self.ce
        self.y_fine_mats = self.y_rows
        self.y_coarse_mats = self.y_fine_mats + self.fx
        self.y_rows_mats = self.y_coarse_mats + self.halves * self.cx
        self.y_fine_beta = self.y_rows
        self.y_coarse_beta = self.y_fine_beta + self.fe
        self.y_spread = self.y_coarse_beta + self.halves * self.ce
        self.y_rows_beta = self.y_spread + self.cx


def lanes_of(h):
    return slice(h * LANES, (h + 1) * LANES)


def put_strips(s, out, far, fine, coarse, at_f, at_c):
    near, second = jnp.where(far, 1, 0), jnp.where(far, 0, 1)
    for n, (c, row) in enumerate(((0, 0), (0, 1), (1, near), (2, near))):
        out[n * s.fy : (n + 1) * s.fy, :] = fine[c, at_f + row]
        line = coarse[c, at_c + row]
        for h in range(s.halves):
            base = s.x_coarse + (h * 4 + n) * s.cy
            out[base : base + s.cy, :] = line[:, lanes_of(h)]
    along_y, along_z = (coarse[c, at_c + second][:, 0:LANES] for c in (1, 2))
    lane = lax.broadcasted_iota(jnp.int32, along_y.shape, 1)
    plane = jnp.where(lane == 1, pltpu.roll(along_y, 1, 1), pltpu.roll(along_z, 2, 1))
    out[s.x_plane : s.x_plane + s.cy, :] = plane


def put_x(s, flags, outs, fine, coarse, betas=None, spread=None):
    even = flags[EVEN_X]
    for k, out in enumerate(outs):
        far = even if k == 0 else jnp.logical_not(even)
        start_f = jnp.where(far, s.fx - 2, 0)
        start_c = jnp.where(far, s.cx - 2, 0)
        put_strips(s, out, far, fine, coarse, start_f, start_c)
        if betas is None:
            continue
        strip = betas[0][pl.ds(start_f, 2), :, :]
        out[s.x_fine_beta : s.x_coarse_beta, :] = strip.reshape(2 * s.fy, LANES)
        strip = betas[1][pl.ds(start_c, 2), :, :]
        for h in range(s.halves):
            base = s.x_coarse_beta + h * 2 * s.cy
            out[base : base + 2 * s.cy, :] = strip[:, :, lanes_of(h)].reshape(2 * s.cy, LANES)
        start = jnp.where(far, s.cx + 2, 0)
        out[s.x_spread : s.x_rows_beta, :] = spread[pl.ds(start, 2)].reshape(2 * s.spread, LANES)


def first_kernel(s, fine, coarse, rig_f, met_f, rig_c, met_c, out_a, out_b, *scratch):
    strip_f, strip_c, line_f, line_c, sems = scratch
    flags = where_am_i()
    copies = []

    def fetch(source, target):
        copies.append(pltpu.make_async_copy(source, target, sems.at[len(copies)]))
        copies[-1].start()

    even = flags[EVEN_X]
    for k in range(2):
        far = even if k == 0 else jnp.logical_not(even)
        fetch(fine.at[:, pl.ds(jnp.where(far, s.fx - 2, 0), 2)], strip_f.at[k])
        fetch(coarse.at[:, pl.ds(jnp.where(far, s.cx - 2, 0), 2)], strip_c.at[k])
        for m, (of_f, of_c) in enumerate(((rig_f, rig_c), (met_f, met_c))):
            fetch(of_f.at[jnp.where(far, s.fx - 1, 0)], line_f.at[k, m])
            fetch(of_c.at[jnp.where(far, s.cx - 1, 0)], line_c.at[k, m])
    for copy in copies:
        copy.wait()
    for k, out in enumerate((out_a, out_b)):
        far = even if k == 0 else jnp.logical_not(even)
        put_strips(s, out, far, strip_f.at[k], strip_c.at[k], 0, 0)
        for m in range(2):
            base = s.x_fine_mats + m * s.fy
            out[base : base + s.fy, :] = line_f[k, m]
            for h in range(s.halves):
                base = s.x_coarse_mats + (m * s.halves + h) * s.cy
                out[base : base + s.cy, :] = line_c[k, m, :, lanes_of(h)]


def sides(flags, even, has_low, has_high, a, b):
    low = jnp.where(flags[even], b, a)
    high = jnp.where(flags[even], a, b)
    low = jnp.where(flags[has_low], low, 0.0)
    high = jnp.where(flags[has_high], high, 0.0)
    return low, high


def middle_kernel(s, step, *refs):
    flags = where_am_i()
    fine, coarse, *mats, in_a, in_b = refs[:-2] if step != 1 else refs[:-3]
    out_a, out_b = refs[-2:] if step != 1 else refs[-3:-1]
    even = flags[EVEN_Y]

    def put(index, low, high):
        out_a[index] = jnp.where(even, high, low)
        out_b[index] = jnp.where(even, low, high)

    def put_one(index, m, low, high):
        out_a[index, m : m + 1, :] = jnp.where(even, high, low)
        out_b[index, m : m + 1, :] = jnp.where(even, low, high)

    def came(first, count):
        rows = slice(first, first + count)
        return sides(flags, EVEN_X, HAS_XM, HAS_XP, in_a[rows, :], in_b[rows, :])

    def level(own, x, y, x_base, y_base, y_size, plane):
        both, single = y_base, y_base + y_size
        here = pl.ds(both + 2, x)
        put(here, own(1, slice(0, 2)), own(1, slice(y - 2, y)))
        for m, c in enumerate((0, 2)):
            here = pl.ds(single + 2, x)
            put_one(here, m, own(c, slice(0, 1)), own(c, slice(y - 1, y)))
            if plane:
                here = pl.ds(s.y_plane + 2, x)
                put_one(here, m, own(c, slice(1, 2)), own(c, slice(y - 2, y - 1)))
        for side in range(2):
            for k in range(2):
                place = k if side == 0 else x + 2 + k
                near = k == 1 - side

                def row(c, first, count):
                    if c == 0:
                        return came(x_base + k * y + first, count)[side]
                    if near:
                        return came(x_base + (1 + c) * y + first, count)[side]
                    return pltpu.roll(came(s.x_plane + first, count)[side], LANES - c, 1)

                if near or plane:
                    put(both + place, row(1, 0, 2), row(1, y - 2, 2))
                for m, c in enumerate((0, 2)):
                    if c == 0 or near or plane:
                        put_one(single + place, m, row(c, 0, 1), row(c, y - 1, 1))
                    if plane:
                        put_one(s.y_plane + place, m, row(c, 1, 1), row(c, y - 2, 1))

    def field(own, x, y, x_base, y_base):
        put(pl.ds(y_base + 2, x), own(slice(0, 2)), own(slice(y - 2, y)))
        for k in range(2):
            low, high = came(x_base + k * y, 2), came(x_base + (k + 1) * y - 2, 2)
            for side in range(2):
                put(y_base + (k if side == 0 else x + 2 + k), low[side], high[side])

    level(lambda c, r: fine[c, :, r, :], s.fx, s.fy, 0, 0, s.fe, False)
    for h in range(s.halves):
        at = lanes_of(h)
        x_base, y_base = s.x_coarse + h * 4 * s.cy, s.y_coarse + h * 2 * s.ce
        level(lambda c, r: coarse[c, :, r, at], s.cx, s.cy, x_base, y_base, s.ce, h == 0)
    if step == 0:
        rig_f, met_f, rig_c, met_c = mats
        for m, (of_f, of_c) in enumerate(((rig_f, rig_c), (met_f, met_c))):
            low, high = of_f[:, 0:1, :], of_f[:, s.fy - 1 : s.fy, :]
            where = pl.ds(s.y_fine_mats, s.fx)
            out_a[where, m : m + 1, :] = jnp.where(even, high, low)
            out_b[where, m : m + 1, :] = jnp.where(even, low, high)
            for h in range(s.halves):
                low, high = of_c[:, 0:1, lanes_of(h)], of_c[:, s.cy - 1 : s.cy, lanes_of(h)]
                where = pl.ds(s.y_coarse_mats + h * s.cx, s.cx)
                out_a[where, m : m + 1, :] = jnp.where(even, high, low)
                out_b[where, m : m + 1, :] = jnp.where(even, low, high)
    if step == 1:
        beta_f, beta_c, spread = mats
        field(lambda r: beta_f[:, r, :], s.fx, s.fy, s.x_fine_beta, s.y_fine_beta)
        for h in range(s.halves):
            at = lanes_of(h)
            x_base, y_base = s.x_coarse_beta + h * 2 * s.cy, s.y_coarse_beta + h * s.ce
            field(lambda r: beta_c[:, r, at], s.cx, s.cy, x_base, y_base)
        total = refs[-1]
        total[...] = spread[2 : 2 + s.cx]
        for k in range(2):
            rows = slice(s.x_spread + k * s.spread, s.x_spread + (k + 1) * s.spread)
            low, high = sides(flags, EVEN_X, HAS_XM, HAS_XP, in_a[rows, :], in_b[rows, :])
            total[k] += low
            total[s.cx - 2 + k] += high
        put(pl.ds(s.y_spread, s.cx), total[:, 0:2, :], total[:, s.cy + 2 : s.cy + 4, :])


def up_one(x):
    return pltpu.roll(x, x.shape[-1] - 1, x.ndim - 1)


def down_one(x):
    return pltpu.roll(x, 1, x.ndim - 1)


def own_kernel(density, lame, rigidity, metric, inverse, c1, c2, weight, above, first, beta):
    inv = 1.0 / metric[...]
    inverse[...] = inv
    over = 1.0 / density[...]
    c1[...] = inv * over
    c2[...] = (lame[...] + rigidity[...]) * over
    weight[...] = density[...] * metric[...]
    v = rigidity[...] * inv
    lane = lax.broadcasted_iota(jnp.int32, v.shape, 2)
    above[...] = jnp.where(lane == v.shape[2] - 1, v, 0.5 * (v + up_one(v)))
    first[...] = v[:, :, 0:LANES]
    beta[...] = (lame[...] + rigidity[...]) * metric[...]


def slope(f, up, down, lane):
    last = f.shape[-1] - 1
    return jnp.where(lane == 0, up - f, jnp.where(lane == last, f - down, 0.5 * (up - down)))


def slope_transposed(q, lane):
    last = q.shape[-1] - 1
    half = jnp.where((lane == 0) | (lane == last), q, 0.5 * q)
    down = jnp.where(lane == 0, -half, down_one(half))
    return down - jnp.where(lane == last, -half, up_one(half))


def fill_beta(s, flags, own, ext, x_in, y_in, fine):
    x, y, e = (s.fx, s.fy, s.fe) if fine else (s.cx, s.cy, s.ce)
    ext[2 : 2 + x, 8 : 8 + y, :] = own[...]
    for h in range(1 if fine else s.halves):
        at = lanes_of(h)
        base = s.x_fine_beta if fine else s.x_coarse_beta + h * 2 * y
        rows = slice(base, base + 2 * y)
        low, high = sides(flags, EVEN_X, HAS_XM, HAS_XP, x_in[0][rows, :], x_in[1][rows, :])
        ext[0:2, 8 : 8 + y, at] = low.reshape(2, y, LANES)
        ext[x + 2 : x + 4, 8 : 8 + y, at] = high.reshape(2, y, LANES)
        start = s.y_fine_beta if fine else s.y_coarse_beta + h * e
        rows = slice(start, start + e)
        low, high = sides(flags, EVEN_Y, HAS_YM, HAS_YP, y_in[0][rows], y_in[1][rows])
        ext[:, 6:8, at] = low
        ext[:, 8 + y : 10 + y, at] = high


def fill_transposed(x, y, ext, beta, inv_ext, psi):
    z = ext.shape[-1]
    lane = lax.broadcasted_iota(jnp.int32, (y + 2, z), 1)
    wide, low, high = slice(7, 9 + y), slice(6, 8 + y), slice(8, 10 + y)

    def row(r, carry):
        along_x = ext[0, r, wide, :] * beta[r, wide, :]
        along_x -= ext[0, r + 2, wide, :] * beta[r + 2, wide, :]
        along_y = ext[1, r + 1, low, :] * beta[r + 1, low, :]
        along_y -= ext[1, r + 1, high, :] * beta[r + 1, high, :]
        inv = inv_ext[r, 0 : 2 + y, :]
        column = inv * beta[r + 1, wide, :] * ext[2, r + 1, wide, :]
        total = 0.5 * along_x + 0.5 * along_y + slope_transposed(column, lane)
        psi[r, wide, :] = jnp.where(inv > 0.0, total, 0.0)
        return carry

    lax.fori_loop(0, x + 2, row, 0, unroll=True)


def fill_displacement(s, flags, own, ext, x_in, y_in, fine, halves=None):
    x, y, e = (s.fx, s.fy, s.fe) if fine else (s.cx, s.cy, s.ce)
    halves = 1 if fine else halves or s.halves
    ext[:, 2 : 2 + x, 8 : 8 + y, :] = own[:, :, :, 0 : halves * LANES]
    mid = slice(8, 8 + y)

    def from_x(first, rows):
        rows = slice(first, first + rows)
        return sides(flags, EVEN_X, HAS_XM, HAS_XP, x_in[0][rows, :], x_in[1][rows, :])

    def from_y(first):
        rows = slice(first, first + e)
        return sides(flags, EVEN_Y, HAS_YM, HAS_YP, y_in[0][rows], y_in[1][rows])

    for h in range(halves):
        at = lanes_of(h)
        base = 0 if fine else s.x_coarse + h * 4 * y
        low, high = from_x(base, 2 * y)
        ext[0, 0:2, mid, at] = low.reshape(2, y, LANES)
        ext[0, x + 2 : x + 4, mid, at] = high.reshape(2, y, LANES)
        for c in (1, 2):
            ext[c, 1, mid, at], ext[c, x + 2, mid, at] = from_x(base + (1 + c) * y, y)
        start = 0 if fine else s.y_coarse + h * 2 * e
        ext[1, :, 6:8, at], ext[1, :, 8 + y : 10 + y, at] = from_y(start)
        low, high = from_y(start + e)
        for m, c in enumerate((0, 2)):
            ext[c, :, 7:8, at] = low[:, m : m + 1, :]
            ext[c, :, 8 + y : 9 + y, at] = high[:, m : m + 1, :]
    if fine:
        return
    at = lanes_of(0)
    low, high = from_x(s.x_plane, y)
    for c in (1, 2):
        ext[c, 0, mid, at] = pltpu.roll(low, LANES - c, 1)
        ext[c, x + 3, mid, at] = pltpu.roll(high, LANES - c, 1)
    low, high = from_y(s.y_plane)
    for m, c in enumerate((0, 2)):
        ext[c, :, 6:7, at] = low[:, m : m + 1, :]
        ext[c, :, 9 + y : 10 + y, at] = high[:, m : m + 1, :]


def fill_materials(s, flags, rigidity, metric, inverse, wide_ext, inv_ext, x_in, y_in, fine):
    x, y = (s.fx, s.fy) if fine else (s.cx, s.cy)
    wide_ext[1 : 1 + x, 1 : 1 + y, :] = rigidity[...] * metric[...]
    inv_ext[1 : 1 + x, 1 : 1 + y, :] = inverse[...]
    for h in range(1 if fine else s.halves):
        at = lanes_of(h)
        got = []
        for m in range(2):
            base = s.x_fine_mats + m * y if fine else s.x_coarse_mats + (m * s.halves + h) * y
            rows = slice(base, base + y)
            even = flags[EVEN_X]
            a, b = x_in[0][rows, :], x_in[1][rows, :]
            got.append((jnp.where(even, b, a), jnp.where(even, a, b)))
        for side, (flag, place) in enumerate(((HAS_XM, 0), (HAS_XP, x + 1))):
            rig, met = got[0][side], got[1][side]
            wide_ext[place, 1 : 1 + y, at] = jnp.where(flags[flag], rig * met, 0.0)
            inv_ext[place, 1 : 1 + y, at] = jnp.where(flags[flag], 1.0 / met, 0.0)
        start = s.y_fine_mats if fine else s.y_coarse_mats + h * x
        rows = slice(start, start + x)
        got = []
        for m in range(2):
            even = flags[EVEN_Y]
            a, b = y_in[0][rows, m : m + 1, :], y_in[1][rows, m : m + 1, :]
            got.append((jnp.where(even, b, a), jnp.where(even, a, b)))
        for side, (flag, place) in enumerate(((HAS_YM, 0), (HAS_YP, 1 + y))):
            rig, met = got[0][side], got[1][side]
            wide_ext[1 : 1 + x, place : place + 1, at] = jnp.where(flags[flag], rig * met, 0.0)
            inv_ext[1 : 1 + x, place : place + 1, at] = jnp.where(flags[flag], 1.0 / met, 0.0)


def fill_divergence(x, y, ext, inv_ext, div):
    z = ext.shape[-1]
    lane = lax.broadcasted_iota(jnp.int32, (y + 2, z), 1)

    def row(r, carry):
        along_x = ext[0, r + 2, 7 : 9 + y, :] - ext[0, r, 7 : 9 + y, :]
        along_y = ext[1, r + 1, 8 : 10 + y, :] - ext[1, r + 1, 6 : 8 + y, :]
        f = ext[2, r + 1, 7 : 9 + y, :]
        inv = inv_ext[r, 0 : 2 + y, :]
        total = 0.5 * along_x + 0.5 * along_y + inv * slope(f, up_one(f), down_one(f), lane)
        div[r, 7 : 9 + y, :] = jnp.where(inv > 0.0, total, 0.0)
        return carry

    lax.fori_loop(0, x + 2, row, 0, unroll=True)


def update(x, y, ext, wide_ext, inv_ext, div, prev, coef, new, ghosts, psi=None):
    c1, c2, weight, above, vertical = coef
    z = ext.shape[-1]
    lane = lax.broadcasted_iota(jnp.int32, (y, z), 1)
    mid, left, right, own = slice(8, 8 + y), slice(7, 7 + y), slice(9, 9 + y), slice(1, 1 + y)

    def row(i, totals):
        wide = wide_ext[i + 1, own, :]
        w_xp = 0.5 * (wide + wide_ext[i + 2, own, :])
        w_xm = 0.5 * (wide_ext[i, own, :] + wide)
        w_yp = 0.5 * (wide + wide_ext[i + 1, 2 : 2 + y, :])
        w_ym = 0.5 * (wide_ext[i + 1, 0:y, :] + wide)
        inv = inv_ext[i + 1, own, :]
        f = div[i + 1, mid, :]
        gradient = (
            0.5 * (div[i + 2, mid, :] - div[i, mid, :]),
            0.5 * (div[i + 1, right, :] - div[i + 1, left, :]),
            inv * slope(f, up_one(f), down_one(f), lane),
        )
        if psi is not None:
            transposed = (
                0.5 * (psi[i, mid, :] - psi[i + 2, mid, :]),
                0.5 * (psi[i + 1, left, :] - psi[i + 1, right, :]),
                slope_transposed(inv * psi[i + 1, mid, :], lane),
            )
        top, bottom, top_next = ghosts(i)
        k1, k2, dm, va = c1[i], c2[i], weight[i], above[i]
        first = vertical[i, :, 0:1]
        inner, squares, cross = (jnp.zeros((y, z), jnp.float32) for _ in range(3))
        for c in range(3):
            u = ext[c, i + 2, mid, :]
            flux = w_xp * (ext[c, i + 3, mid, :] - u) - w_xm * (u - ext[c, i + 1, mid, :])
            flux += w_yp * (ext[c, i + 2, right, :] - u) - w_ym * (u - ext[c, i + 2, left, :])
            over = va * (jnp.where(lane == z - 1, 0.0, up_one(u)) - u)
            entry = 0.0 if top is None else first * u[:, 0:1]
            flux += over - jnp.where(lane == 0, entry, down_one(over))
            if top is None:
                ghost = jnp.where(lane == z - 1, va * bottom(c), 0.0)
            else:
                ghost = jnp.where(lane == 0, first * top(c), 0.0)
            rate = (flux + ghost) * k1 + k2 * gradient[c]
            updated = 2.0 * u - prev[c, i] + STEP * rate
            change = updated - u
            inner += change * change - STEP * updated * rate
            new[c, i] = updated
            if psi is not None:
                squares += change * change
                cross += updated * (flux + transposed[c])
                if top is not None:
                    cross += jnp.where(lane == 0, first * u[:, 0:1] * top_next(c), 0.0)
        total = totals[0] + dm * inner
        if psi is None:
            return (total,)
        return total, totals[1] + (dm * squares - STEP * cross)

    start = (jnp.zeros((y, z), jnp.float32),) * (1 if psi is None else 2)
    return lax.fori_loop(0, x, row, start, unroll=4)


def double_plane(s, ext_c, double):
    lane = lax.broadcasted_iota(jnp.int32, (s.cy + 4, LANES), 1)
    table = jnp.zeros((s.cy + 4, LANES), jnp.float32)
    for i in range(s.ce):
        e0, e1, e2 = (ext_c[c, i, 6 : 10 + s.cy, 0:LANES] for c in range(3))
        e1, e2 = pltpu.roll(e1, 1, 1), pltpu.roll(e2, 2, 1)
        plane = jnp.where(lane == 0, e0, jnp.where(lane == 1, e1, e2))
        for k in (2 * i, 2 * i + 1):
            there = pltpu.roll(plane, 4 * k, 1) if k else plane
            table = jnp.where(lane // 4 == k, there, table)
    for j in range(s.cy + 4):
        double[2 * j : 2 * j + 2, :] = jnp.broadcast_to(table[j : j + 1, :], (2, LANES))


def add_pairs(s, fine, pairs):
    for c in range(3):
        for i in range(s.cx):
            pairs[c, i] = fine[c, 2 * i] + fine[c, 2 * i + 1]


def node_weights(s, offs):
    node = (s.fy, LANES)
    node_lane = lax.broadcasted_iota(jnp.int32, node, 1)
    near_x = jnp.where(node_lane // 4 % 2 == 0, 0.75, 0.25)
    near_y = jnp.where(lax.broadcasted_iota(jnp.int32, node, 0) % 2 == 0, 0.75, 0.25)
    code = offs[...]
    weights_x, weights_y = (
        [
            jnp.where(off == shift, near, 0.0) + jnp.where(off == shift - 1, 1.0 - near, 0.0)
            for shift in (-1, 0, 1, 2)
        ]
        for off, near in ((code // 4 - 1, near_x), (code % 4 - 1, near_y))
    )
    return weights_x, weights_y


def bottom_ghosts(s, weights, double, moved):
    weights_x, weights_y = weights
    node = (s.fy, LANES)
    ghosts = jnp.zeros(node, jnp.float32)
    for a in range(4):
        moved[a] = pltpu.roll(double[...], LANES - 8 * (1 + a), 1)
        line = jnp.zeros(node, jnp.float32)
        for b in range(4):
            line += weights_y[b] * moved[a, 2 * b + 2 : 2 * b + 2 + s.fy, :]
        ghosts += weights_x[a] * line
    return lambda i: (None, lambda c: pltpu.roll(ghosts, LANES - 1 - c - 4 * i, 1), None)


def top_ghosts(s, pairs, pairs_next=None):
    def mean(of, i):
        def top(c):
            both = of[c, i, pl.ds(0, s.cy, stride=2), :] + of[c, i, pl.ds(1, s.cy, stride=2), :]
            return 0.25 * both[:, LANES - 1 :]

        return top

    return lambda i: (mean(pairs, i), None, mean(pairs_next, i) if pairs_next is not None else None)


def step_kernel(s, step, cells, *refs):
    flags = where_am_i()
    refs = list(refs)

    def take(n):
        out = refs[:n]
        del refs[:n]
        return out

    fine, coarse, fine_prev, coarse_prev, offs = take(5)
    coef_f, coef_c = take(5), take(5)
    if step == 0:
        rig_f, met_f, inverse_f, rig_c, met_c, inverse_c = take(6)
    else:
        wide_f, inv_f, wide_c, inv_c = take(4)
    beta_own = take(2)
    if step == 1:
        energy_in, spread_in = take(2)
    x_in, y_in = take(2), take(2)
    new_f, new_c, energy = take(3)
    x_out = take(2)
    if step == 0:
        wide_f, inv_f, wide_c, inv_c, spread_out = take(5)
    ext_f, ext_c, div_f, div_c, double, moved, pairs = take(7)

    fill_displacement(s, flags, fine, ext_f, x_in, y_in, True)
    fill_displacement(s, flags, coarse, ext_c, x_in, y_in, False)
    if step == 0:
        fill_materials(s, flags, rig_f, met_f, inverse_f, wide_f, inv_f, x_in, y_in, True)
        fill_materials(s, flags, rig_c, met_c, inverse_c, wide_c, inv_c, x_in, y_in, False)

    double_plane(s, ext_c, double)
    add_pairs(s, fine, pairs)
    fill_divergence(s.fx, s.fy, ext_f, inv_f, div_f)
    fill_divergence(s.cx, s.cy, ext_c, inv_c, div_c)
    psi_f = psi_c = None
    if step == 1:
        psi_f, psi_c, all_beta_f, all_beta_c, pairs_next, spread = take(6)
        fill_beta(s, flags, beta_own[0], all_beta_f, x_in, y_in, True)
        fill_beta(s, flags, beta_own[1], all_beta_c, x_in, y_in, False)
        fill_transposed(s.fx, s.fy, ext_f, all_beta_f, inv_f, psi_f)
        fill_transposed(s.cx, s.cy, ext_c, all_beta_c, inv_c, psi_c)

    weights = node_weights(s, offs)
    fine_ghosts = bottom_ghosts(s, weights, double, moved)
    coarse_ghosts = top_ghosts(s, pairs, pairs_next if step == 1 else None)
    sums_f = update(
        s.fx, s.fy, ext_f, wide_f, inv_f, div_f, fine_prev, coef_f, new_f, fine_ghosts, psi_f
    )
    if step == 1:
        add_pairs(s, new_f, pairs_next)
    sums_c = update(
        s.cx, s.cy, ext_c, wide_c, inv_c, div_c, coarse_prev, coef_c, new_c, coarse_ghosts, psi_c
    )
    place = lax.broadcasted_iota(jnp.int32, (8, LANES), 0)
    table = jnp.zeros((8, LANES), jnp.float32) if step == 0 else energy_in[...]
    table = jnp.where(place == step, jnp.sum(sums_f[0]) / cells[0], table)
    table = jnp.where(place == STEPS + step, jnp.sum(sums_c[0]) / cells[1], table)
    if step == 0:
        weights_x, weights_y = weights
        node = (s.fy, LANES)
        node_lane = lax.broadcasted_iota(jnp.int32, node, 1)
        q = jnp.zeros(node, jnp.float32)
        for i in range(s.fx):
            for c in range(3):
                there = pltpu.roll(coef_f[3][i] * new_f[c, i], 4 * i + c + 1, 1)
                q = jnp.where(node_lane == 4 * i + c, there, q)
        moved[...] = jnp.zeros(moved.shape, jnp.float32)
        for a in range(4):
            part = weights_x[a] * q
            for b in range(4):
                moved[a, 2 * b + 2 : 2 * b + 2 + s.fy, :] += weights_y[b] * part
        double[...] = sum(pltpu.roll(moved[a], 8 * (1 + a), 1) for a in range(4))
        rows = s.cy + 4
        both = double[pl.ds(0, rows, stride=2), :] + double[pl.ds(1, rows, stride=2), :]
        for i in range(s.ce):
            there = pltpu.roll(both, LANES - 8 * i, 1) if i else both
            spread_out[i, 0:rows, :] = there + pltpu.roll(there, LANES - 4, 1)
            spread_out[i, rows:, :] = jnp.zeros((s.spread - rows, LANES), jnp.float32)
        put_x(s, flags, x_out, new_f, new_c, beta_own, spread_out)
    if step == 1:
        spread[...] = spread_in[:, 2 : 2 + s.cy, :]
        rows = pl.ds(s.y_spread, s.cx)
        low, high = sides(flags, EVEN_Y, HAS_YM, HAS_YP, y_in[0][rows], y_in[1][rows])
        spread[:, 0:2, :] += low
        spread[:, s.cy - 2 : s.cy, :] += high
        joined = jnp.zeros((s.cy, LANES), jnp.float32)
        for i in range(s.cx):
            for c in range(3):
                weights = spread[i] if c == 0 else pltpu.roll(spread[i], LANES - c, 1)
                joined += new_c[c, i, :, 0:LANES] * weights
        joined = jnp.sum(joined[:, 0:1])
        table = jnp.where(place == 2, (jnp.sum(sums_f[1]) - STEP * joined) / cells[0], table)
        table = jnp.where(place == STEPS + 2, jnp.sum(sums_c[1]) / cells[1], table)
        put_x(s, flags, x_out, new_f, new_c)
    energy[...] = table


def final_fine_kernel(s, fine, coarse, prev, offs, *refs):
    coef, (wide, inv, xa, xb, ya, yb, new) = refs[:5], refs[5:12]
    ext_f, ext_c, div, double, moved = refs[12:]
    flags = where_am_i()
    fill_displacement(s, flags, fine, ext_f, (xa, xb), (ya, yb), True)
    fill_displacement(s, flags, coarse, ext_c, (xa, xb), (ya, yb), False, 1)
    double_plane(s, ext_c, double)
    fill_divergence(s.fx, s.fy, ext_f, inv, div)
    ghosts = bottom_ghosts(s, node_weights(s, offs), double, moved)
    update(s.fx, s.fy, ext_f, wide, inv, div, prev, coef, new, ghosts)


def final_coarse_kernel(s, fine, coarse, prev, *refs):
    coef, (wide, inv, xa, xb, ya, yb, new) = refs[:5], refs[5:12]
    ext, div, pairs = refs[12:]
    fill_displacement(s, where_am_i(), coarse, ext, (xa, xb), (ya, yb), False)
    add_pairs(s, fine, pairs)
    fill_divergence(s.cx, s.cy, ext, inv, div)
    update(s.cx, s.cy, ext, wide, inv, div, prev, coef, new, top_ghosts(s, pairs))


VMEM = pl.BlockSpec(memory_space=pltpu.VMEM)
HBM = pl.BlockSpec(memory_space=pltpu.HBM)


def call(kernel, shapes, flops, *args, scratch=(), spec=VMEM, sems=0):
    shapes = [jax.ShapeDtypeStruct(shape, jnp.float32) for shape in shapes]
    scratch = [pltpu.VMEM(shape, jnp.float32) for shape in scratch]
    if sems:
        scratch.append(pltpu.SemaphoreType.DMA((sems,)))
    return pl.pallas_call(
        kernel,
        out_shape=shapes,
        in_specs=[spec] * len(args),
        out_specs=[VMEM] * len(shapes),
        scratch_shapes=scratch,
        compiler_params=pltpu.CompilerParams(vmem_limit_bytes=VMEM_LIMIT),
        cost_estimate=pl.CostEstimate(flops=flops, bytes_accessed=1 << 20, transcendentals=0),
    )(*args)


def swap_pairs(mesh, move):
    sizes = list(mesh.shape.values())
    pairs = []
    for source in range(math.prod(sizes)):
        rest, at = source, []
        for size in reversed(sizes):
            at.insert(0, rest % size)
            rest //= size
        target = 0
        for index, size in zip(move(*at), sizes, strict=True):
            target = target * size + index
        pairs.append((source, target))
    return pairs


def beside_x(z, x, y, core):
    return z, x ^ 1, y, core


def across_x(z, x, y, core):
    place = 4 * z + x
    if place in (0, 31):
        return z, x, y, core ^ 1
    place += 1 if place % 2 else -1
    return place // 4, place % 4, y, core


def beside_y(z, x, y, core):
    return z, x, y, core ^ 1


def across_y(z, x, y, core):
    place = (2 * y + core + (1 if core else -1)) % 8
    return z, x, place // 2, place % 2


TOTAL = (
    lambda z, x, y, core: (z ^ 7, x, y, core),
    lambda z, x, y, core: (z, x, y, core ^ 1),
    lambda z, x, y, core: (z ^ 2, x, y, core ^ 1),
    lambda z, x, y, core: (z, x, y ^ 1, core ^ 1),
    lambda z, x, y, core: (z, x ^ 1, y, core ^ 1),
    lambda z, x, y, core: (z ^ 1, x, y, core ^ 1),
    lambda z, x, y, core: (z, x ^ 3, y, core ^ 1),
    lambda z, x, y, core: (z, x, y ^ 3, core ^ 1),
)


def per_device(
    mesh,
    fine_disp,
    fine_prev,
    coarse_disp,
    coarse_prev,
    fine_density,
    fine_lame,
    fine_rigidity,
    fine_metric,
    coarse_density,
    coarse_lame,
    coarse_rigidity,
    coarse_metric,
    offsets,
):
    fine_shape, coarse_shape = fine_metric.shape, coarse_metric.shape
    s = Sizes(fine_shape, coarse_shape)
    count_x, count_y = lax.axis_size(GX), lax.axis_size(GY)

    def swap(value, move):
        return lax.ppermute(value, ALL, swap_pairs(mesh, move))

    def swap_both(pair, beside, across):
        second = swap(pair[1], across)
        first = swap(pair[0], beside)
        return [pltpu.with_memory_space_constraint(x, pltpu.VMEM) for x in (first, second)]

    offs = offsets[0] * 4 + offsets[1] + 5
    offs = jnp.pad(jnp.repeat(offs.T, 4, axis=1), ((0, 0), (0, LANES - 4 * s.fx)))
    x_out = call(
        functools.partial(first_kernel, s),
        [(s.x_rows_mats, LANES)] * 2,
        1000,
        *(
            pltpu.with_memory_space_constraint(x, pltpu.HBM)
            for x in (
                fine_disp,
                coarse_disp,
                fine_rigidity,
                fine_metric,
                coarse_rigidity,
                coarse_metric,
            )
        ),
        scratch=[
            (2, 3, 2, s.fy, s.fz),
            (2, 3, 2, s.cy, s.cz),
            (2, 2, s.fy, s.fz),
            (2, 2, s.cy, s.cz),
        ],
        spec=HBM,
        sems=12,
    )
    own = []
    for density, lame, rigidity, metric in (
        (fine_density, fine_lame, fine_rigidity, fine_metric),
        (coarse_density, coarse_lame, coarse_rigidity, coarse_metric),
    ):
        own.append(
            call(
                own_kernel,
                [metric.shape] * 5 + [metric.shape[:2] + (LANES,), metric.shape],
                2_000_000,
                density,
                lame,
                rigidity,
                metric,
            )
        )
    inverse_f, *coef_f, beta_f = own[0]
    inverse_c, *coef_c, beta_c = own[1]

    fine, coarse = fine_disp, coarse_disp
    fine_ext = (s.fx + 2, s.fy + 2, s.fz)
    coarse_ext = (s.cx + 2, s.cy + 2, s.cz)
    scratch = [
        (3, s.fe, s.fy + 16, s.fz),
        (3, s.ce, s.cy + 16, s.cz),
        (s.fx + 2, s.fy + 16, s.fz),
        (s.cx + 2, s.cy + 16, s.cz),
        (2 * (s.cy + 4), LANES),
        (4, 2 * (s.cy + 4), LANES),
        (3, s.cx, s.fy, LANES),
    ]
    cells = [count_x * count_y * s.fx * s.fy * s.fz, count_x * count_y * s.cx * s.cy * s.cz]
    spread = (s.ce, s.spread, LANES)
    for step in range(STEPS):
        x_in = swap_both(x_out, beside_x, across_x)
        if step == 2:
            for k, move in enumerate(TOTAL):
                other = swap(energy, move)
                if k < len(TOTAL) - 1:
                    energy = energy + other
        shapes = [((s.y_rows_mats, s.y_rows_beta, s.y_rows)[step], 2, LANES)] * 2
        if step == 0:
            mats = [fine_rigidity, fine_metric, coarse_rigidity, coarse_metric]
        if step == 1:
            mats = [beta_f, beta_c, spread_own]
            shapes.append((s.cx,) + spread[1:])
        y_out = call(
            functools.partial(middle_kernel, s, step),
            shapes,
            1000,
            fine,
            coarse,
            *(mats if step < 2 else ()),
            *x_in,
        )
        y_in = swap_both(y_out[:2], beside_y, across_y)
        if step == 2:
            wide_f, inv_f, wide_c, inv_c = ext_mats
            (fine_final,) = call(
                functools.partial(final_fine_kernel, s),
                [fine.shape],
                2_000_000,
                fine,
                coarse,
                fine_prev,
                offs,
                *coef_f,
                wide_f,
                inv_f,
                *x_in,
                *y_in,
                scratch=[scratch[0], scratch[1][:3] + (LANES,), scratch[2], *scratch[4:6]],
            )
            (coarse_final,) = call(
                functools.partial(final_coarse_kernel, s),
                [coarse.shape],
                2_000_000,
                fine,
                coarse,
                coarse_prev,
                *coef_c,
                wide_c,
                inv_c,
                *x_in,
                *y_in,
                scratch=[scratch[1], scratch[3], scratch[6]],
            )
            break
        shapes = [fine.shape, coarse.shape, (8, LANES)]
        shapes += [((s.x_rows_beta, s.x_rows)[step], LANES)] * 2
        more_scratch = []
        if step == 0:
            extra = [fine_rigidity, fine_metric, inverse_f, coarse_rigidity, coarse_metric, inverse_c]
            extra += [beta_f, beta_c]
            shapes += [fine_ext, fine_ext, coarse_ext, coarse_ext, spread]
        else:
            extra = list(ext_mats)
        if step == 1:
            extra += [beta_f, beta_c, energy, y_out[2]]
            more_scratch = [
                scratch[2],
                scratch[3],
                scratch[0][1:],
                scratch[1][1:],
                scratch[6],
                (s.cx, s.cy, LANES),
            ]
        outs = call(
            functools.partial(step_kernel, s, step, cells),
            shapes,
            4_000_000,
            fine,
            coarse,
            fine_prev,
            coarse_prev,
            offs,
            *coef_f,
            *coef_c,
            *extra,
            *x_in,
            *y_in,
            scratch=scratch + more_scratch,
        )
        fine_prev, coarse_prev = fine, coarse
        fine, coarse, energy = outs[:3]
        x_out = outs[3:5]
        if step == 0:
            *ext_mats, spread_own = outs[5:]
    other, fine, coarse = lax.optimization_barrier((other, fine_final, coarse_final))
    energy = energy + other
    energy = energy[: 2 * STEPS, 0].reshape(2, STEPS).T
    return fine, coarse, energy


def solution(mesh):
    finer = Mesh(mesh.devices.reshape(8, 4, 4, 2), ALL)
    level, cell = P(None, GX, GY, None), P(GX, GY, None)
    in_specs = (level,) * 4 + (cell,) * 8 + (P(None, GX, GY),)

    def body(*args):
        return per_device(finer, *args)

    return jax.shard_map(
        body, mesh=finer, in_specs=in_specs, out_specs=(level, level, P()), check_vma=False
    )
```

```python
import functools
import math

import jax
import jax.numpy as jnp
from jax import lax
from jax.experimental import pallas as pl
from jax.experimental.pallas import tpu as pltpu
from jax.sharding import Mesh
from jax.sharding import PartitionSpec as P

STEPS = 3
GX = ("gx_0", "gx_1")
GY = ("gy_0", "gy_1")
ALL = GX + GY
STEP = 0.15
LANES = 128
VMEM_LIMIT = 20 * 1024 * 1024

EVEN_X, HAS_XM, HAS_XP, EVEN_Y, HAS_YM, HAS_YP = range(6)


def where_am_i():
    x = 4 * lax.axis_index("gx_0") + lax.axis_index("gx_1")
    y = 2 * lax.axis_index("gy_0") + lax.axis_index("gy_1")
    return x % 2 == 0, x > 0, x < 31, y % 2 == 0, y > 0, y < 7


class Sizes:
    def __init__(self, fine, coarse):
        self.fx, self.fy, self.fz = fine
        self.cx, self.cy, self.cz = coarse
        self.halves = self.cz // LANES
        self.x_coarse = 4 * self.fy
        self.x_plane = self.x_coarse + self.halves * 4 * self.cy
        self.x_rows = self.x_plane + self.cy
        self.x_fine_mats = self.x_rows
        self.x_coarse_mats = self.x_fine_mats + 2 * self.fy
        self.x_rows_mats = self.x_coarse_mats + 2 * self.halves * self.cy
        self.x_fine_beta = self.x_rows
        self.x_coarse_beta = self.x_fine_beta + 2 * self.fy
        self.x_spread = self.x_coarse_beta + self.halves * 2 * self.cy
        self.spread = self.cy + 8
        self.x_rows_beta = self.x_spread + 2 * self.spread
        self.fe, self.ce = self.fx + 4, self.cx + 4
        self.y_coarse = 2 * self.fe
        self.y_plane = self.y_coarse + self.halves * 2 * self.ce
        self.y_rows = self.y_plane + self.ce
        self.y_fine_mats = self.y_rows
        self.y_coarse_mats = self.y_fine_mats + self.fx
        self.y_rows_mats = self.y_coarse_mats + self.halves * self.cx
        self.y_fine_beta = self.y_rows
        self.y_coarse_beta = self.y_fine_beta + self.fe
        self.y_spread = self.y_coarse_beta + self.halves * self.ce
        self.y_rows_beta = self.y_spread + self.cx


def lanes_of(h):
    return slice(h * LANES, (h + 1) * LANES)


def put_strips(s, out, far, fine, coarse, at_f, at_c):
    near, second = jnp.where(far, 1, 0), jnp.where(far, 0, 1)
    for n, (c, row) in enumerate(((0, 0), (0, 1), (1, near), (2, near))):
        out[n * s.fy : (n + 1) * s.fy, :] = fine[c, at_f + row]
        line = coarse[c, at_c + row]
        for h in range(s.halves):
            base = s.x_coarse + (h * 4 + n) * s.cy
            out[base : base + s.cy, :] = line[:, lanes_of(h)]
    along_y, along_z = (coarse[c, at_c + second][:, 0:LANES] for c in (1, 2))
    lane = lax.broadcasted_iota(jnp.int32, along_y.shape, 1)
    plane = jnp.where(lane == 1, pltpu.roll(along_y, 1, 1), pltpu.roll(along_z, 2, 1))
    out[s.x_plane : s.x_plane + s.cy, :] = plane


def put_x(s, flags, outs, fine, coarse, betas=None, spread=None):
    even = flags[EVEN_X]
    for k, out in enumerate(outs):
        far = even if k == 0 else jnp.logical_not(even)
        start_f = jnp.where(far, s.fx - 2, 0)
        start_c = jnp.where(far, s.cx - 2, 0)
        put_strips(s, out, far, fine, coarse, start_f, start_c)
        if betas is None:
            continue
        strip = betas[0][pl.ds(start_f, 2), :, :]
        out[s.x_fine_beta : s.x_coarse_beta, :] = strip.reshape(2 * s.fy, LANES)
        strip = betas[1][pl.ds(start_c, 2), :, :]
        for h in range(s.halves):
            base = s.x_coarse_beta + h * 2 * s.cy
            out[base : base + 2 * s.cy, :] = strip[:, :, lanes_of(h)].reshape(2 * s.cy, LANES)
        start = jnp.where(far, s.cx + 2, 0)
        out[s.x_spread : s.x_rows_beta, :] = spread[pl.ds(start, 2)].reshape(2 * s.spread, LANES)


def first_kernel(s, fine, coarse, rig_f, met_f, rig_c, met_c, out_a, out_b, *scratch):
    strip_f, strip_c, line_f, line_c, sems = scratch
    flags = where_am_i()
    copies = []

    def fetch(source, target):
        copies.append(pltpu.make_async_copy(source, target, sems.at[len(copies)]))
        copies[-1].start()

    even = flags[EVEN_X]
    for k in range(2):
        far = even if k == 0 else jnp.logical_not(even)
        fetch(fine.at[:, pl.ds(jnp.where(far, s.fx - 2, 0), 2)], strip_f.at[k])
        fetch(coarse.at[:, pl.ds(jnp.where(far, s.cx - 2, 0), 2)], strip_c.at[k])
        for m, (of_f, of_c) in enumerate(((rig_f, rig_c), (met_f, met_c))):
            fetch(of_f.at[jnp.where(far, s.fx - 1, 0)], line_f.at[k, m])
            fetch(of_c.at[jnp.where(far, s.cx - 1, 0)], line_c.at[k, m])
    for copy in copies:
        copy.wait()
    for k, out in enumerate((out_a, out_b)):
        far = even if k == 0 else jnp.logical_not(even)
        put_strips(s, out, far, strip_f.at[k], strip_c.at[k], 0, 0)
        for m in range(2):
            base = s.x_fine_mats + m * s.fy
            out[base : base + s.fy, :] = line_f[k, m]
            for h in range(s.halves):
                base = s.x_coarse_mats + (m * s.halves + h) * s.cy
                out[base : base + s.cy, :] = line_c[k, m, :, lanes_of(h)]


def sides(flags, even, has_low, has_high, a, b):
    low = jnp.where(flags[even], b, a)
    high = jnp.where(flags[even], a, b)
    low = jnp.where(flags[has_low], low, 0.0)
    high = jnp.where(flags[has_high], high, 0.0)
    return low, high


def middle_kernel(s, step, *refs):
    flags = where_am_i()
    fine, coarse, *mats, in_a, in_b = refs[:-2] if step != 1 else refs[:-3]
    out_a, out_b = refs[-2:] if step != 1 else refs[-3:-1]
    even = flags[EVEN_Y]

    def put(index, low, high):
        out_a[index] = jnp.where(even, high, low)
        out_b[index] = jnp.where(even, low, high)

    def put_one(index, m, low, high):
        out_a[index, m : m + 1, :] = jnp.where(even, high, low)
        out_b[index, m : m + 1, :] = jnp.where(even, low, high)

    def came(first, count):
        rows = slice(first, first + count)
        return sides(flags, EVEN_X, HAS_XM, HAS_XP, in_a[rows, :], in_b[rows, :])

    def level(own, x, y, x_base, y_base, y_size, plane):
        both, single = y_base, y_base + y_size
        here = pl.ds(both + 2, x)
        put(here, own(1, slice(0, 2)), own(1, slice(y - 2, y)))
        for m, c in enumerate((0, 2)):
            here = pl.ds(single + 2, x)
            put_one(here, m, own(c, slice(0, 1)), own(c, slice(y - 1, y)))
            if plane:
                here = pl.ds(s.y_plane + 2, x)
                put_one(here, m, own(c, slice(1, 2)), own(c, slice(y - 2, y - 1)))
        for side in range(2):
            for k in range(2):
                place = k if side == 0 else x + 2 + k
                near = k == 1 - side

                def row(c, first, count):
                    if c == 0:
                        return came(x_base + k * y + first, count)[side]
                    if near:
                        return came(x_base + (1 + c) * y + first, count)[side]
                    return pltpu.roll(came(s.x_plane + first, count)[side], LANES - c, 1)

                if near or plane:
                    put(both + place, row(1, 0, 2), row(1, y - 2, 2))
                for m, c in enumerate((0, 2)):
                    if c == 0 or near or plane:
                        put_one(single + place, m, row(c, 0, 1), row(c, y - 1, 1))
                    if plane:
                        put_one(s.y_plane + place, m, row(c, 1, 1), row(c, y - 2, 1))

    def field(own, x, y, x_base, y_base):
        put(pl.ds(y_base + 2, x), own(slice(0, 2)), own(slice(y - 2, y)))
        for k in range(2):
            low, high = came(x_base + k * y, 2), came(x_base + (k + 1) * y - 2, 2)
            for side in range(2):
                put(y_base + (k if side == 0 else x + 2 + k), low[side], high[side])

    level(lambda c, r: fine[c, :, r, :], s.fx, s.fy, 0, 0, s.fe, False)
    for h in range(s.halves):
        at = lanes_of(h)
        x_base, y_base = s.x_coarse + h * 4 * s.cy, s.y_coarse + h * 2 * s.ce
        level(lambda c, r: coarse[c, :, r, at], s.cx, s.cy, x_base, y_base, s.ce, h == 0)
    if step == 0:
        rig_f, met_f, rig_c, met_c = mats
        for m, (of_f, of_c) in enumerate(((rig_f, rig_c), (met_f, met_c))):
            low, high = of_f[:, 0:1, :], of_f[:, s.fy - 1 : s.fy, :]
            where = pl.ds(s.y_fine_mats, s.fx)
            out_a[where, m : m + 1, :] = jnp.where(even, high, low)
            out_b[where, m : m + 1, :] = jnp.where(even, low, high)
            for h in range(s.halves):
                low, high = of_c[:, 0:1, lanes_of(h)], of_c[:, s.cy - 1 : s.cy, lanes_of(h)]
                where = pl.ds(s.y_coarse_mats + h * s.cx, s.cx)
                out_a[where, m : m + 1, :] = jnp.where(even, high, low)
                out_b[where, m : m + 1, :] = jnp.where(even, low, high)
    if step == 1:
        beta_f, beta_c, spread = mats
        field(lambda r: beta_f[:, r, :], s.fx, s.fy, s.x_fine_beta, s.y_fine_beta)
        for h in range(s.halves):
            at = lanes_of(h)
            x_base, y_base = s.x_coarse_beta + h * 2 * s.cy, s.y_coarse_beta + h * s.ce
            field(lambda r: beta_c[:, r, at], s.cx, s.cy, x_base, y_base)
        total = refs[-1]
        total[...] = spread[2 : 2 + s.cx]
        for k in range(2):
            rows = slice(s.x_spread + k * s.spread, s.x_spread + (k + 1) * s.spread)
            low, high = sides(flags, EVEN_X, HAS_XM, HAS_XP, in_a[rows, :], in_b[rows, :])
            total[k] += low
            total[s.cx - 2 + k] += high
        put(pl.ds(s.y_spread, s.cx), total[:, 0:2, :], total[:, s.cy + 2 : s.cy + 4, :])


def up_one(x):
    return pltpu.roll(x, x.shape[-1] - 1, x.ndim - 1)


def down_one(x):
    return pltpu.roll(x, 1, x.ndim - 1)


def edge_factor(shape, first, last):
    lane = first + lax.broadcasted_iota(jnp.int32, shape, len(shape) - 1)
    return jnp.where((lane == 0) | (lane == last), 2.0, 1.0)


def own_kernel(density, lame, rigidity, metric, inverse, c1, c2, weight, above, first, beta):
    inv = 1.0 / metric[...]
    last = inv.shape[2] - 1
    inverse[...] = inv * edge_factor(inv.shape, 0, last)
    over = 1.0 / density[...]
    c1[...] = (0.5 * STEP) * (inv * over)
    c2[...] = (0.25 * STEP) * ((lame[...] + rigidity[...]) * over)
    weight[...] = density[...] * metric[...]
    v = rigidity[...] * inv
    lane = lax.broadcasted_iota(jnp.int32, v.shape, 2)
    above[...] = v + jnp.where(lane == last, v, up_one(v))
    first[...] = 2.0 * v[:, :, 0:LANES]
    beta[...] = 0.5 * ((lame[...] + rigidity[...]) * metric[...])


def difference(f, lane):
    up = jnp.where(lane == f.shape[-1] - 1, f, up_one(f))
    return up - jnp.where(lane == 0, f, down_one(f))


def difference_transposed(q, lane):
    down = jnp.where(lane == 0, -q, down_one(q))
    return down - jnp.where(lane == q.shape[-1] - 1, -q, up_one(q))


def fill_beta(s, flags, own, ext, x_in, y_in, fine):
    x, y, e = (s.fx, s.fy, s.fe) if fine else (s.cx, s.cy, s.ce)
    ext[2 : 2 + x, 8 : 8 + y, :] = own[...]
    for h in range(1 if fine else s.halves):
        at = lanes_of(h)
        base = s.x_fine_beta if fine else s.x_coarse_beta + h * 2 * y
        rows = slice(base, base + 2 * y)
        low, high = sides(flags, EVEN_X, HAS_XM, HAS_XP, x_in[0][rows, :], x_in[1][rows, :])
        ext[0:2, 8 : 8 + y, at] = low.reshape(2, y, LANES)
        ext[x + 2 : x + 4, 8 : 8 + y, at] = high.reshape(2, y, LANES)
        start = s.y_fine_beta if fine else s.y_coarse_beta + h * e
        rows = slice(start, start + e)
        low, high = sides(flags, EVEN_Y, HAS_YM, HAS_YP, y_in[0][rows], y_in[1][rows])
        ext[:, 6:8, at] = low
        ext[:, 8 + y : 10 + y, at] = high


def fill_transposed(x, y, ext, beta, inv_ext, psi):
    z = ext.shape[-1]
    lane = lax.broadcasted_iota(jnp.int32, (y + 2, z), 1)
    wide, low, high = slice(7, 9 + y), slice(6, 8 + y), slice(8, 10 + y)

    def row(r, carry):
        along_x = ext[0, r, wide, :] * beta[r, wide, :]
        along_x -= ext[0, r + 2, wide, :] * beta[r + 2, wide, :]
        along_y = ext[1, r + 1, low, :] * beta[r + 1, low, :]
        along_y -= ext[1, r + 1, high, :] * beta[r + 1, high, :]
        inv = inv_ext[r, 0 : 2 + y, :]
        column = inv * beta[r + 1, wide, :] * ext[2, r + 1, wide, :]
        total = along_x + along_y + difference_transposed(column, lane)
        psi[r, wide, :] = jnp.where(inv > 0.0, total, 0.0)
        return carry

    lax.fori_loop(0, x + 2, row, 0, unroll=True)


def fill_displacement(s, flags, own, ext, x_in, y_in, fine, halves=None):
    x, y, e = (s.fx, s.fy, s.fe) if fine else (s.cx, s.cy, s.ce)
    halves = 1 if fine else halves or s.halves
    ext[:, 2 : 2 + x, 8 : 8 + y, :] = own[:, :, :, 0 : halves * LANES]
    mid = slice(8, 8 + y)

    def from_x(first, rows):
        rows = slice(first, first + rows)
        return sides(flags, EVEN_X, HAS_XM, HAS_XP, x_in[0][rows, :], x_in[1][rows, :])

    def from_y(first):
        rows = slice(first, first + e)
        return sides(flags, EVEN_Y, HAS_YM, HAS_YP, y_in[0][rows], y_in[1][rows])

    for h in range(halves):
        at = lanes_of(h)
        base = 0 if fine else s.x_coarse + h * 4 * y
        low, high = from_x(base, 2 * y)
        ext[0, 0:2, mid, at] = low.reshape(2, y, LANES)
        ext[0, x + 2 : x + 4, mid, at] = high.reshape(2, y, LANES)
        for c in (1, 2):
            ext[c, 1, mid, at], ext[c, x + 2, mid, at] = from_x(base + (1 + c) * y, y)
        start = 0 if fine else s.y_coarse + h * 2 * e
        ext[1, :, 6:8, at], ext[1, :, 8 + y : 10 + y, at] = from_y(start)
        low, high = from_y(start + e)
        for m, c in enumerate((0, 2)):
            ext[c, :, 7:8, at] = low[:, m : m + 1, :]
            ext[c, :, 8 + y : 9 + y, at] = high[:, m : m + 1, :]
    if fine:
        return
    at = lanes_of(0)
    low, high = from_x(s.x_plane, y)
    for c in (1, 2):
        ext[c, 0, mid, at] = pltpu.roll(low, LANES - c, 1)
        ext[c, x + 3, mid, at] = pltpu.roll(high, LANES - c, 1)
    low, high = from_y(s.y_plane)
    for m, c in enumerate((0, 2)):
        ext[c, :, 6:7, at] = low[:, m : m + 1, :]
        ext[c, :, 9 + y : 10 + y, at] = high[:, m : m + 1, :]


def fill_materials(s, flags, rigidity, metric, inverse, wide_ext, inv_ext, x_in, y_in, fine):
    x, y = (s.fx, s.fy) if fine else (s.cx, s.cy)
    own_z = metric.shape[2]
    wide_ext[1 : 1 + x, 1 : 1 + y, :] = rigidity[...] * metric[...]
    inv_ext[1 : 1 + x, 1 : 1 + y, :] = inverse[...]
    for h in range(1 if fine else s.halves):
        at = lanes_of(h)
        edge = edge_factor((y, LANES), h * LANES, own_z - 1)
        got = []
        for m in range(2):
            base = s.x_fine_mats + m * y if fine else s.x_coarse_mats + (m * s.halves + h) * y
            rows = slice(base, base + y)
            even = flags[EVEN_X]
            a, b = x_in[0][rows, :], x_in[1][rows, :]
            got.append((jnp.where(even, b, a), jnp.where(even, a, b)))
        for side, (flag, place) in enumerate(((HAS_XM, 0), (HAS_XP, x + 1))):
            rig, met = got[0][side], got[1][side]
            wide_ext[place, 1 : 1 + y, at] = jnp.where(flags[flag], rig * met, 0.0)
            inv_ext[place, 1 : 1 + y, at] = jnp.where(flags[flag], edge / met, 0.0)
        start = s.y_fine_mats if fine else s.y_coarse_mats + h * x
        rows = slice(start, start + x)
        got = []
        for m in range(2):
            even = flags[EVEN_Y]
            a, b = y_in[0][rows, m : m + 1, :], y_in[1][rows, m : m + 1, :]
            got.append((jnp.where(even, b, a), jnp.where(even, a, b)))
        for side, (flag, place) in enumerate(((HAS_YM, 0), (HAS_YP, 1 + y))):
            rig, met = got[0][side], got[1][side]
            wide_ext[1 : 1 + x, place : place + 1, at] = jnp.where(flags[flag], rig * met, 0.0)
            inv_ext[1 : 1 + x, place : place + 1, at] = jnp.where(flags[flag], edge[None, 0:1] / met, 0.0)


def fill_divergence(x, y, ext, inv_ext, div):
    z = ext.shape[-1]
    lane = lax.broadcasted_iota(jnp.int32, (y + 2, z), 1)

    def row(r, carry):
        along_x = ext[0, r + 2, 7 : 9 + y, :] - ext[0, r, 7 : 9 + y, :]
        along_y = ext[1, r + 1, 8 : 10 + y, :] - ext[1, r + 1, 6 : 8 + y, :]
        f = ext[2, r + 1, 7 : 9 + y, :]
        inv = inv_ext[r, 0 : 2 + y, :]
        total = along_x + along_y + inv * difference(f, lane)
        div[r, 7 : 9 + y, :] = jnp.where(inv > 0.0, total, 0.0)
        return carry

    lax.fori_loop(0, x + 2, row, 0, unroll=True)


def update(x, y, ext, wide_ext, inv_ext, div, prev, coef, new, ghosts, psi=None):
    c1, c2, weight, above, vertical = coef
    z = ext.shape[-1]
    lane = lax.broadcasted_iota(jnp.int32, (y, z), 1)
    mid, left, right, own = slice(8, 8 + y), slice(7, 7 + y), slice(9, 9 + y), slice(1, 1 + y)

    def row(i, totals):
        wide = wide_ext[i + 1, own, :]
        w_xp = wide + wide_ext[i + 2, own, :]
        w_xm = wide_ext[i, own, :] + wide
        w_yp = wide + wide_ext[i + 1, 2 : 2 + y, :]
        w_ym = wide_ext[i + 1, 0:y, :] + wide
        inv = inv_ext[i + 1, own, :]
        gradient = (
            div[i + 2, mid, :] - div[i, mid, :],
            div[i + 1, right, :] - div[i + 1, left, :],
            inv * difference(div[i + 1, mid, :], lane),
        )
        if psi is not None:
            transposed = (
                psi[i, mid, :] - psi[i + 2, mid, :],
                psi[i + 1, left, :] - psi[i + 1, right, :],
                difference_transposed(inv * psi[i + 1, mid, :], lane),
            )
        top, bottom, top_next = ghosts(i)
        k1, k2, dm, va = c1[i], c2[i], weight[i], above[i]
        first = vertical[i, :, 0:1]
        inner, squares, cross = (jnp.zeros((y, z), jnp.float32) for _ in range(3))
        for c in range(3):
            u = ext[c, i + 2, mid, :]
            flux = w_xp * (ext[c, i + 3, mid, :] - u) - w_xm * (u - ext[c, i + 1, mid, :])
            flux += w_yp * (ext[c, i + 2, right, :] - u) - w_ym * (u - ext[c, i + 2, left, :])
            below = entry = 0.0
            if psi is None:
                below = 0.0 if bottom is None else bottom(c)
                entry = 0.0 if top is None else first * (u[:, 0:1] - top(c))
            elif top is not None:
                entry = first * u[:, 0:1]
            over = va * (jnp.where(lane == z - 1, below, up_one(u)) - u)
            flux += over - jnp.where(lane == 0, entry, down_one(over))
            whole = flux
            if psi is not None:
                if top is None:
                    whole = flux + jnp.where(lane == z - 1, va * bottom(c), 0.0)
                else:
                    whole = flux + jnp.where(lane == 0, first * top(c), 0.0)
            push = whole * k1 + k2 * gradient[c]
            before = prev[c, i]
            change = u - before
            inner += change * change - before * push
            change += push
            updated = u + change
            new[c, i] = updated
            if psi is not None:
                squares += change * change
                cross += updated * (flux + transposed[c])
                if top is not None:
                    cross += jnp.where(lane == 0, first * u[:, 0:1] * top_next(c), 0.0)
        total = totals[0] + dm * inner
        if psi is None:
            return (total,)
        return total, totals[1] + (dm * squares - (0.5 * STEP) * cross)

    start = (jnp.zeros((y, z), jnp.float32),) * (1 if psi is None else 2)
    return lax.fori_loop(0, x, row, start, unroll=4)


def double_plane(s, ext_c, double):
    lane = lax.broadcasted_iota(jnp.int32, (s.cy + 4, LANES), 1)
    table = jnp.zeros((s.cy + 4, LANES), jnp.float32)
    for i in range(s.ce):
        e0, e1, e2 = (ext_c[c, i, 6 : 10 + s.cy, 0:LANES] for c in range(3))
        e1, e2 = pltpu.roll(e1, 1, 1), pltpu.roll(e2, 2, 1)
        plane = jnp.where(lane == 0, e0, jnp.where(lane == 1, e1, e2))
        for k in (2 * i, 2 * i + 1):
            there = pltpu.roll(plane, 4 * k, 1) if k else plane
            table = jnp.where(lane // 4 == k, there, table)
    for j in range(s.cy + 4):
        double[2 * j : 2 * j + 2, :] = jnp.broadcast_to(table[j : j + 1, :], (2, LANES))


def add_pairs(s, fine, pairs):
    for c in range(3):
        for i in range(s.cx):
            pairs[c, i] = fine[c, 2 * i] + fine[c, 2 * i + 1]


def node_weights(s, offs):
    node = (s.fy, LANES)
    node_lane = lax.broadcasted_iota(jnp.int32, node, 1)
    near_x = jnp.where(node_lane // 4 % 2 == 0, 0.75, 0.25)
    near_y = jnp.where(lax.broadcasted_iota(jnp.int32, node, 0) % 2 == 0, 0.75, 0.25)
    code = offs[...]
    weights_x, weights_y = (
        [
            jnp.where(off == shift, near, 0.0) + jnp.where(off == shift - 1, 1.0 - near, 0.0)
            for shift in (-1, 0, 1, 2)
        ]
        for off, near in ((code // 4 - 1, near_x), (code % 4 - 1, near_y))
    )
    return weights_x, weights_y


def bottom_ghosts(s, weights, double, moved):
    weights_x, weights_y = weights
    node = (s.fy, LANES)
    ghosts = jnp.zeros(node, jnp.float32)
    for a in range(4):
        moved[a] = pltpu.roll(double[...], LANES - 8 * (1 + a), 1)
        line = jnp.zeros(node, jnp.float32)
        for b in range(4):
            line += weights_y[b] * moved[a, 2 * b + 2 : 2 * b + 2 + s.fy, :]
        ghosts += weights_x[a] * line
    return lambda i: (None, lambda c: pltpu.roll(ghosts, LANES - 1 - c - 4 * i, 1), None)


def top_ghosts(s, pairs, pairs_next=None):
    def mean(of, i):
        def top(c):
            both = of[c, i, pl.ds(0, s.cy, stride=2), :] + of[c, i, pl.ds(1, s.cy, stride=2), :]
            return 0.25 * both[:, LANES - 1 :]

        return top

    return lambda i: (mean(pairs, i), None, mean(pairs_next, i) if pairs_next is not None else None)


def step_kernel(s, step, cells, *refs):
    flags = where_am_i()
    refs = list(refs)

    def take(n):
        out = refs[:n]
        del refs[:n]
        return out

    fine, coarse, fine_prev, coarse_prev, offs = take(5)
    coef_f, coef_c = take(5), take(5)
    if step == 0:
        rig_f, met_f, inverse_f, rig_c, met_c, inverse_c = take(6)
    else:
        wide_f, inv_f, wide_c, inv_c = take(4)
    beta_own = take(2)
    if step == 1:
        energy_in, spread_in = take(2)
    x_in, y_in = take(2), take(2)
    new_f, new_c, energy = take(3)
    x_out = take(2)
    if step == 0:
        wide_f, inv_f, wide_c, inv_c, spread_out = take(5)
    ext_f, ext_c, div_f, div_c, double, moved, pairs = take(7)

    fill_displacement(s, flags, fine, ext_f, x_in, y_in, True)
    fill_displacement(s, flags, coarse, ext_c, x_in, y_in, False)
    if step == 0:
        fill_materials(s, flags, rig_f, met_f, inverse_f, wide_f, inv_f, x_in, y_in, True)
        fill_materials(s, flags, rig_c, met_c, inverse_c, wide_c, inv_c, x_in, y_in, False)

    double_plane(s, ext_c, double)
    add_pairs(s, fine, pairs)
    fill_divergence(s.fx, s.fy, ext_f, inv_f, div_f)
    fill_divergence(s.cx, s.cy, ext_c, inv_c, div_c)
    psi_f = psi_c = None
    if step == 1:
        psi_f, psi_c, all_beta_f, all_beta_c, pairs_next, spread = take(6)
        fill_beta(s, flags, beta_own[0], all_beta_f, x_in, y_in, True)
        fill_beta(s, flags, beta_own[1], all_beta_c, x_in, y_in, False)
        fill_transposed(s.fx, s.fy, ext_f, all_beta_f, inv_f, psi_f)
        fill_transposed(s.cx, s.cy, ext_c, all_beta_c, inv_c, psi_c)

    weights = node_weights(s, offs)
    fine_ghosts = bottom_ghosts(s, weights, double, moved)
    coarse_ghosts = top_ghosts(s, pairs, pairs_next if step == 1 else None)
    sums_f = update(
        s.fx, s.fy, ext_f, wide_f, inv_f, div_f, fine_prev, coef_f, new_f, fine_ghosts, psi_f
    )
    if step == 1:
        add_pairs(s, new_f, pairs_next)
    sums_c = update(
        s.cx, s.cy, ext_c, wide_c, inv_c, div_c, coarse_prev, coef_c, new_c, coarse_ghosts, psi_c
    )
    place = lax.broadcasted_iota(jnp.int32, (8, LANES), 0)
    table = jnp.zeros((8, LANES), jnp.float32) if step == 0 else energy_in[...]
    table = jnp.where(place == step, jnp.sum(sums_f[0]) / cells[0], table)
    table = jnp.where(place == STEPS + step, jnp.sum(sums_c[0]) / cells[1], table)
    if step == 0:
        weights_x, weights_y = weights
        node = (s.fy, LANES)
        node_lane = lax.broadcasted_iota(jnp.int32, node, 1)
        q = jnp.zeros(node, jnp.float32)
        for i in range(s.fx):
            for c in range(3):
                there = pltpu.roll(coef_f[3][i] * new_f[c, i], 4 * i + c + 1, 1)
                q = jnp.where(node_lane == 4 * i + c, there, q)
        moved[...] = jnp.zeros(moved.shape, jnp.float32)
        for a in range(4):
            part = weights_x[a] * q
            for b in range(4):
                moved[a, 2 * b + 2 : 2 * b + 2 + s.fy, :] += weights_y[b] * part
        double[...] = sum(pltpu.roll(moved[a], 8 * (1 + a), 1) for a in range(4))
        rows = s.cy + 4
        both = double[pl.ds(0, rows, stride=2), :] + double[pl.ds(1, rows, stride=2), :]
        for i in range(s.ce):
            there = pltpu.roll(both, LANES - 8 * i, 1) if i else both
            spread_out[i, 0:rows, :] = there + pltpu.roll(there, LANES - 4, 1)
            spread_out[i, rows:, :] = jnp.zeros((s.spread - rows, LANES), jnp.float32)
        put_x(s, flags, x_out, new_f, new_c, beta_own, spread_out)
    if step == 1:
        spread[...] = spread_in[:, 2 : 2 + s.cy, :]
        rows = pl.ds(s.y_spread, s.cx)
        low, high = sides(flags, EVEN_Y, HAS_YM, HAS_YP, y_in[0][rows], y_in[1][rows])
        spread[:, 0:2, :] += low
        spread[:, s.cy - 2 : s.cy, :] += high
        joined = jnp.zeros((s.cy, LANES), jnp.float32)
        for i in range(s.cx):
            for c in range(3):
                weights = spread[i] if c == 0 else pltpu.roll(spread[i], LANES - c, 1)
                joined += new_c[c, i, :, 0:LANES] * weights
        joined = jnp.sum(joined[:, 0:1])
        table = jnp.where(place == 2, (jnp.sum(sums_f[1]) - (0.5 * STEP) * joined) / cells[0], table)
        table = jnp.where(place == STEPS + 2, jnp.sum(sums_c[1]) / cells[1], table)
        put_x(s, flags, x_out, new_f, new_c)
    energy[...] = table


def final_fine_kernel(s, fine, coarse, prev, offs, *refs):
    coef, (wide, inv, xa, xb, ya, yb, new) = refs[:5], refs[5:12]
    ext_f, ext_c, div, double, moved = refs[12:]
    flags = where_am_i()
    fill_displacement(s, flags, fine, ext_f, (xa, xb), (ya, yb), True)
    fill_displacement(s, flags, coarse, ext_c, (xa, xb), (ya, yb), False, 1)
    double_plane(s, ext_c, double)
    fill_divergence(s.fx, s.fy, ext_f, inv, div)
    ghosts = bottom_ghosts(s, node_weights(s, offs), double, moved)
    update(s.fx, s.fy, ext_f, wide, inv, div, prev, coef, new, ghosts)


def final_coarse_kernel(s, fine, coarse, prev, *refs):
    coef, (wide, inv, xa, xb, ya, yb, new) = refs[:5], refs[5:12]
    ext, div, pairs = refs[12:]
    fill_displacement(s, where_am_i(), coarse, ext, (xa, xb), (ya, yb), False)
    add_pairs(s, fine, pairs)
    fill_divergence(s.cx, s.cy, ext, inv, div)
    update(s.cx, s.cy, ext, wide, inv, div, prev, coef, new, top_ghosts(s, pairs))


VMEM = pl.BlockSpec(memory_space=pltpu.VMEM)
HBM = pl.BlockSpec(memory_space=pltpu.HBM)


def call(kernel, shapes, flops, *args, scratch=(), spec=VMEM, sems=0):
    shapes = [jax.ShapeDtypeStruct(shape, jnp.float32) for shape in shapes]
    scratch = [pltpu.VMEM(shape, jnp.float32) for shape in scratch]
    if sems:
        scratch.append(pltpu.SemaphoreType.DMA((sems,)))
    return pl.pallas_call(
        kernel,
        out_shape=shapes,
        in_specs=[spec] * len(args),
        out_specs=[VMEM] * len(shapes),
        scratch_shapes=scratch,
        compiler_params=pltpu.CompilerParams(vmem_limit_bytes=VMEM_LIMIT),
        cost_estimate=pl.CostEstimate(flops=flops, bytes_accessed=1 << 20, transcendentals=0),
    )(*args)


def swap_pairs(mesh, move):
    sizes = list(mesh.shape.values())
    pairs = []
    for source in range(math.prod(sizes)):
        rest, at = source, []
        for size in reversed(sizes):
            at.insert(0, rest % size)
            rest //= size
        target = 0
        for index, size in zip(move(*at), sizes, strict=True):
            target = target * size + index
        pairs.append((source, target))
    return pairs


def beside_x(z, x, y, core):
    return z, x ^ 1, y, core


def across_x(z, x, y, core):
    place = 4 * z + x
    if place in (0, 31):
        return z, x, y, core ^ 1
    place += 1 if place % 2 else -1
    return place // 4, place % 4, y, core


def beside_y(z, x, y, core):
    return z, x, y, core ^ 1


def across_y(z, x, y, core):
    place = (2 * y + core + (1 if core else -1)) % 8
    return z, x, place // 2, place % 2


TOTAL = (
    lambda z, x, y, core: (z ^ 7, x, y, core),
    lambda z, x, y, core: (z, x, y, core ^ 1),
    lambda z, x, y, core: (z ^ 2, x, y, core ^ 1),
    lambda z, x, y, core: (z, x, y ^ 1, core ^ 1),
    lambda z, x, y, core: (z, x ^ 1, y, core ^ 1),
    lambda z, x, y, core: (z ^ 1, x, y, core ^ 1),
    lambda z, x, y, core: (z, x ^ 3, y, core ^ 1),
    lambda z, x, y, core: (z, x, y ^ 3, core ^ 1),
)


def per_device(
    mesh,
    fine_disp,
    fine_prev,
    coarse_disp,
    coarse_prev,
    fine_density,
    fine_lame,
    fine_rigidity,
    fine_metric,
    coarse_density,
    coarse_lame,
    coarse_rigidity,
    coarse_metric,
    offsets,
):
    fine_shape, coarse_shape = fine_metric.shape, coarse_metric.shape
    s = Sizes(fine_shape, coarse_shape)
    count_x, count_y = lax.axis_size(GX), lax.axis_size(GY)

    def swap(value, move):
        return lax.ppermute(value, ALL, swap_pairs(mesh, move))

    def swap_both(pair, beside, across):
        second = swap(pair[1], across)
        first = swap(pair[0], beside)
        return [pltpu.with_memory_space_constraint(x, pltpu.VMEM) for x in (first, second)]

    offs = offsets[0] * 4 + offsets[1] + 5
    offs = jnp.pad(jnp.repeat(offs.T, 4, axis=1), ((0, 0), (0, LANES - 4 * s.fx)))
    x_out = call(
        functools.partial(first_kernel, s),
        [(s.x_rows_mats, LANES)] * 2,
        1000,
        *(
            pltpu.with_memory_space_constraint(x, pltpu.HBM)
            for x in (
                fine_disp,
                coarse_disp,
                fine_rigidity,
                fine_metric,
                coarse_rigidity,
                coarse_metric,
            )
        ),
        scratch=[
            (2, 3, 2, s.fy, s.fz),
            (2, 3, 2, s.cy, s.cz),
            (2, 2, s.fy, s.fz),
            (2, 2, s.cy, s.cz),
        ],
        spec=HBM,
        sems=12,
    )
    own = []
    for density, lame, rigidity, metric in (
        (fine_density, fine_lame, fine_rigidity, fine_metric),
        (coarse_density, coarse_lame, coarse_rigidity, coarse_metric),
    ):
        own.append(
            call(
                own_kernel,
                [metric.shape] * 5 + [metric.shape[:2] + (LANES,), metric.shape],
                2_000_000,
                density,
                lame,
                rigidity,
                metric,
            )
        )
    inverse_f, *coef_f, beta_f = own[0]
    inverse_c, *coef_c, beta_c = own[1]

    fine, coarse = fine_disp, coarse_disp
    fine_ext = (s.fx + 2, s.fy + 2, s.fz)
    coarse_ext = (s.cx + 2, s.cy + 2, s.cz)
    scratch = [
        (3, s.fe, s.fy + 16, s.fz),
        (3, s.ce, s.cy + 16, s.cz),
        (s.fx + 2, s.fy + 16, s.fz),
        (s.cx + 2, s.cy + 16, s.cz),
        (2 * (s.cy + 4), LANES),
        (4, 2 * (s.cy + 4), LANES),
        (3, s.cx, s.fy, LANES),
    ]
    cells = [count_x * count_y * s.fx * s.fy * s.fz, count_x * count_y * s.cx * s.cy * s.cz]
    spread = (s.ce, s.spread, LANES)
    for step in range(STEPS):
        x_in = swap_both(x_out, beside_x, across_x)
        if step == 2:
            for k, move in enumerate(TOTAL):
                other = swap(energy, move)
                if k < len(TOTAL) - 1:
                    energy = energy + other
        shapes = [((s.y_rows_mats, s.y_rows_beta, s.y_rows)[step], 2, LANES)] * 2
        if step == 0:
            mats = [fine_rigidity, fine_metric, coarse_rigidity, coarse_metric]
        if step == 1:
            mats = [beta_f, beta_c, spread_own]
            shapes.append((s.cx,) + spread[1:])
        y_out = call(
            functools.partial(middle_kernel, s, step),
            shapes,
            1000,
            fine,
            coarse,
            *(mats if step < 2 else ()),
            *x_in,
        )
        y_in = swap_both(y_out[:2], beside_y, across_y)
        if step == 2:
            wide_f, inv_f, wide_c, inv_c = ext_mats
            (fine_final,) = call(
                functools.partial(final_fine_kernel, s),
                [fine.shape],
                2_000_000,
                fine,
                coarse,
                fine_prev,
                offs,
                *coef_f,
                wide_f,
                inv_f,
                *x_in,
                *y_in,
                scratch=[scratch[0], scratch[1][:3] + (LANES,), scratch[2], *scratch[4:6]],
            )
            (coarse_final,) = call(
                functools.partial(final_coarse_kernel, s),
                [coarse.shape],
                2_000_000,
                fine,
                coarse,
                coarse_prev,
                *coef_c,
                wide_c,
                inv_c,
                *x_in,
                *y_in,
                scratch=[scratch[1], scratch[3], scratch[6]],
            )
            break
        shapes = [fine.shape, coarse.shape, (8, LANES)]
        shapes += [((s.x_rows_beta, s.x_rows)[step], LANES)] * 2
        more_scratch = []
        if step == 0:
            extra = [fine_rigidity, fine_metric, inverse_f, coarse_rigidity, coarse_metric, inverse_c]
            extra += [beta_f, beta_c]
            shapes += [fine_ext, fine_ext, coarse_ext, coarse_ext, spread]
        else:
            extra = list(ext_mats)
        if step == 1:
            extra += [beta_f, beta_c, energy, y_out[2]]
            more_scratch = [
                scratch[2],
                scratch[3],
                scratch[0][1:],
                scratch[1][1:],
                scratch[6],
                (s.cx, s.cy, LANES),
            ]
        outs = call(
            functools.partial(step_kernel, s, step, cells),
            shapes,
            4_000_000,
            fine,
            coarse,
            fine_prev,
            coarse_prev,
            offs,
            *coef_f,
            *coef_c,
            *extra,
            *x_in,
            *y_in,
            scratch=scratch + more_scratch,
        )
        fine_prev, coarse_prev = fine, coarse
        fine, coarse, energy = outs[:3]
        x_out = outs[3:5]
        if step == 0:
            *ext_mats, spread_own = outs[5:]
    other, fine, coarse = lax.optimization_barrier((other, fine_final, coarse_final))
    energy = energy + other
    energy = energy[: 2 * STEPS, 0].reshape(2, STEPS).T
    return fine, coarse, energy


def solution(mesh):
    finer = Mesh(mesh.devices.reshape(8, 4, 4, 2), ALL)
    level, cell = P(None, GX, GY, None), P(GX, GY, None)
    in_specs = (level,) * 4 + (cell,) * 8 + (P(None, GX, GY),)

    def body(*args):
        return per_device(finer, *args)

    return jax.shard_map(
        body, mesh=finer, in_specs=in_specs, out_specs=(level, level, P()), check_vma=False
    )
```

```python
import functools
import math

import jax
import jax.numpy as jnp
from jax import lax
from jax.experimental import pallas as pl
from jax.experimental.pallas import tpu as pltpu
from jax.sharding import Mesh
from jax.sharding import PartitionSpec as P

STEPS = 3
GX = ("gx_0", "gx_1")
GY = ("gy_0", "gy_1")
ALL = GX + GY
STEP = 0.15
LANES = 128
VMEM_LIMIT = 20 * 1024 * 1024

EVEN_X, HAS_XM, HAS_XP, EVEN_Y, HAS_YM, HAS_YP = range(6)


def where_am_i():
    x = 4 * lax.axis_index("gx_0") + lax.axis_index("gx_1")
    y = 2 * lax.axis_index("gy_0") + lax.axis_index("gy_1")
    return x % 2 == 0, x > 0, x < 31, y % 2 == 0, y > 0, y < 7


class Sizes:
    def __init__(self, fine, coarse):
        self.fx, self.fy, self.fz = fine
        self.cx, self.cy, self.cz = coarse
        self.halves = self.cz // LANES
        self.x_coarse = 4 * self.fy
        self.x_plane = self.x_coarse + self.halves * 4 * self.cy
        self.x_rows = self.x_plane + self.cy
        self.x_fine_mats = self.x_rows
        self.x_coarse_mats = self.x_fine_mats + 2 * self.fy
        self.x_rows_mats = self.x_coarse_mats + 2 * self.halves * self.cy
        self.x_fine_beta = self.x_rows
        self.x_coarse_beta = self.x_fine_beta + 2 * self.fy
        self.x_spread = self.x_coarse_beta + self.halves * 2 * self.cy
        self.spread = self.cy + 8
        self.x_rows_beta = self.x_spread + 2 * self.spread
        self.fe, self.ce = self.fx + 4, self.cx + 4
        self.y_coarse = 2 * self.fe
        self.y_plane = self.y_coarse + self.halves * 2 * self.ce
        self.y_rows = self.y_plane + self.ce
        self.y_fine_mats = self.y_rows
        self.y_coarse_mats = self.y_fine_mats + self.fx
        self.y_rows_mats = self.y_coarse_mats + self.halves * self.cx
        self.y_fine_beta = self.y_rows
        self.y_coarse_beta = self.y_fine_beta + self.fe
        self.y_rows_beta = self.y_coarse_beta + self.halves * self.ce
        self.f_coarse = 2
        self.f_plane = self.f_coarse + 2 * self.halves
        self.f_beta = self.f_plane + 1
        self.corner_rows = 4 * self.f_beta
        self.corner_spread = 4 * (self.f_beta + 1 + self.halves)
        self.corner_rows_beta = self.corner_spread + self.cx


def lanes_of(h):
    return slice(h * LANES, (h + 1) * LANES)


def put_strips(s, out, far, fine, coarse, at_f, at_c):
    near, second = jnp.where(far, 1, 0), jnp.where(far, 0, 1)
    for n, (c, row) in enumerate(((0, 0), (0, 1), (1, near), (2, near))):
        out[n * s.fy : (n + 1) * s.fy, :] = fine[c, at_f + row]
        line = coarse[c, at_c + row]
        for h in range(s.halves):
            base = s.x_coarse + (h * 4 + n) * s.cy
            out[base : base + s.cy, :] = line[:, lanes_of(h)]
    along_y, along_z = (coarse[c, at_c + second][:, 0:LANES] for c in (1, 2))
    lane = lax.broadcasted_iota(jnp.int32, along_y.shape, 1)
    plane = jnp.where(lane == 1, pltpu.roll(along_y, 1, 1), pltpu.roll(along_z, 2, 1))
    out[s.x_plane : s.x_plane + s.cy, :] = plane


def put_x(s, flags, outs, fine, coarse, betas=None, spread=None):
    even = flags[EVEN_X]
    for k, out in enumerate(outs):
        far = even if k == 0 else jnp.logical_not(even)
        start_f = jnp.where(far, s.fx - 2, 0)
        start_c = jnp.where(far, s.cx - 2, 0)
        put_strips(s, out, far, fine, coarse, start_f, start_c)
        if betas is None:
            continue
        strip = betas[0][pl.ds(start_f, 2), :, :]
        out[s.x_fine_beta : s.x_coarse_beta, :] = strip.reshape(2 * s.fy, LANES)
        strip = betas[1][pl.ds(start_c, 2), :, :]
        for h in range(s.halves):
            base = s.x_coarse_beta + h * 2 * s.cy
            out[base : base + 2 * s.cy, :] = strip[:, :, lanes_of(h)].reshape(2 * s.cy, LANES)
        start = jnp.where(far, s.cx + 2, 0)
        out[s.x_spread : s.x_rows_beta, :] = spread[pl.ds(start, 2)].reshape(2 * s.spread, LANES)


def first_kernel(s, fine, coarse, rig_f, met_f, rig_c, met_c, out_a, out_b, *scratch):
    strip_f, strip_c, line_f, line_c, sems = scratch
    flags = where_am_i()
    copies = []

    def fetch(source, target):
        copies.append(pltpu.make_async_copy(source, target, sems.at[len(copies)]))
        copies[-1].start()

    even = flags[EVEN_X]
    for k in range(2):
        far = even if k == 0 else jnp.logical_not(even)
        fetch(fine.at[:, pl.ds(jnp.where(far, s.fx - 2, 0), 2)], strip_f.at[k])
        fetch(coarse.at[:, pl.ds(jnp.where(far, s.cx - 2, 0), 2)], strip_c.at[k])
        for m, (of_f, of_c) in enumerate(((rig_f, rig_c), (met_f, met_c))):
            fetch(of_f.at[jnp.where(far, s.fx - 1, 0)], line_f.at[k, m])
            fetch(of_c.at[jnp.where(far, s.cx - 1, 0)], line_c.at[k, m])
    for copy in copies:
        copy.wait()
    for k, out in enumerate((out_a, out_b)):
        far = even if k == 0 else jnp.logical_not(even)
        put_strips(s, out, far, strip_f.at[k], strip_c.at[k], 0, 0)
        for m in range(2):
            base = s.x_fine_mats + m * s.fy
            out[base : base + s.fy, :] = line_f[k, m]
            for h in range(s.halves):
                base = s.x_coarse_mats + (m * s.halves + h) * s.cy
                out[base : base + s.cy, :] = line_c[k, m, :, lanes_of(h)]


def sides(flags, even, has_low, has_high, a, b):
    low = jnp.where(flags[even], b, a)
    high = jnp.where(flags[even], a, b)
    low = jnp.where(flags[has_low], low, 0.0)
    high = jnp.where(flags[has_high], high, 0.0)
    return low, high


def y_kernel(s, step, part, *refs):
    flags = where_am_i()
    refs = list(refs)
    even = flags[EVEN_Y]
    has_own, has_corners = part != "corners", part != "own"
    if has_own:
        fine, coarse = refs[:2]
        mats = refs[2:-2] if part == "own" else []
    if has_corners:
        total = refs.pop() if step == 1 else None
        in_a, in_b = refs[-4:-2]
        spread = refs[0]
    out_a, out_b = refs[-2:]

    def put(index, low, high):
        out_a[index] = jnp.where(even, high, low)
        out_b[index] = jnp.where(even, low, high)

    def put_one(index, m, low, high):
        out_a[index, m : m + 1, :] = jnp.where(even, high, low)
        out_b[index, m : m + 1, :] = jnp.where(even, low, high)

    def came(first, count):
        rows = slice(first, first + count)
        return sides(flags, EVEN_X, HAS_XM, HAS_XP, in_a[rows, :], in_b[rows, :])

    def corner(base, field, x, side, k):
        return 4 * field + 2 * side + k if part == "corners" else base + side * (x + 2) + k

    def level(own, x, y, x_base, y_base, y_size, field, plane):
        both, single = y_base, y_base + y_size
        if has_own:
            put(pl.ds(both + 2, x), own(1, slice(0, 2)), own(1, slice(y - 2, y)))
            for m, c in enumerate((0, 2)):
                here = pl.ds(single + 2, x)
                put_one(here, m, own(c, slice(0, 1)), own(c, slice(y - 1, y)))
                if plane:
                    here = pl.ds(s.y_plane + 2, x)
                    put_one(here, m, own(c, slice(1, 2)), own(c, slice(y - 2, y - 1)))
        for side, k in ((0, 0), (0, 1), (1, 0), (1, 1)) if has_corners else ():
            near = k == 1 - side

            def row(c, first, count):
                if c == 0:
                    return came(x_base + k * y + first, count)[side]
                if near:
                    return came(x_base + (1 + c) * y + first, count)[side]
                return pltpu.roll(came(s.x_plane + first, count)[side], LANES - c, 1)

            if near or plane:
                put(corner(both, field, x, side, k), row(1, 0, 2), row(1, y - 2, 2))
            for m, c in enumerate((0, 2)):
                if c == 0 or near or plane:
                    here = corner(single, field + 1, x, side, k)
                    put_one(here, m, row(c, 0, 1), row(c, y - 1, 1))
                if plane:
                    here = corner(s.y_plane, s.f_plane, x, side, k)
                    put_one(here, m, row(c, 1, 1), row(c, y - 2, 1))

    def two_deep(own, x, y, x_base, y_base, field):
        if has_own:
            put(pl.ds(y_base + 2, x), own(slice(0, 2)), own(slice(y - 2, y)))
        for k in range(2) if has_corners else ():
            low, high = came(x_base + k * y, 2), came(x_base + (k + 1) * y - 2, 2)
            for side in range(2):
                put(corner(y_base, field, x, side, k), low[side], high[side])

    level(lambda c, r: fine[c, :, r, :], s.fx, s.fy, 0, 0, s.fe, 0, False)
    for h in range(s.halves):
        x_base, y_base = s.x_coarse + h * 4 * s.cy, s.y_coarse + h * 2 * s.ce
        field = s.f_coarse + 2 * h
        at = lanes_of(h)
        level(
            lambda c, r: coarse[c, :, r, at], s.cx, s.cy, x_base, y_base, s.ce, field, h == 0
        )
    if step == 0 and has_own:
        rig_f, met_f, rig_c, met_c = mats
        for m, (of_f, of_c) in enumerate(((rig_f, rig_c), (met_f, met_c))):
            here = pl.ds(s.y_fine_mats, s.fx)
            put_one(here, m, of_f[:, 0:1, :], of_f[:, s.fy - 1 : s.fy, :])
            for h in range(s.halves):
                here = pl.ds(s.y_coarse_mats + h * s.cx, s.cx)
                low, high = of_c[:, 0:1, lanes_of(h)], of_c[:, s.cy - 1 : s.cy, lanes_of(h)]
                put_one(here, m, low, high)
    if step == 1:
        beta_f, beta_c = mats if has_own else (None, None)
        x_base, y_base = s.x_fine_beta, s.y_fine_beta
        two_deep(lambda r: beta_f[:, r, :], s.fx, s.fy, x_base, y_base, s.f_beta)
        for h in range(s.halves):
            at = lanes_of(h)
            x_base, y_base = s.x_coarse_beta + h * 2 * s.cy, s.y_coarse_beta + h * s.ce
            field = s.f_beta + 1 + h
            two_deep(lambda r: beta_c[:, r, at], s.cx, s.cy, x_base, y_base, field)
    if step == 1 and has_corners:
        total[...] = spread[2 : 2 + s.cx]
        for k in range(2):
            low, high = came(s.x_spread + k * s.spread, s.spread)
            total[k] += low
            total[s.cx - 2 + k] += high
        here = pl.ds(s.corner_spread, s.cx)
        put(here, total[:, 0:2, :], total[:, s.cy + 2 : s.cy + 4, :])


def up_one(x):
    return pltpu.roll(x, x.shape[-1] - 1, x.ndim - 1)


def down_one(x):
    return pltpu.roll(x, 1, x.ndim - 1)


def edge_factor(shape, first, last):
    lane = first + lax.broadcasted_iota(jnp.int32, shape, len(shape) - 1)
    return jnp.where((lane == 0) | (lane == last), 2.0, 1.0)


def own_kernel(density, lame, rigidity, metric, inverse, c1, c2, weight, above, first, beta):
    inv = 1.0 / metric[...]
    last = inv.shape[2] - 1
    inverse[...] = inv * edge_factor(inv.shape, 0, last)
    over = 1.0 / density[...]
    c1[...] = (0.5 * STEP) * (inv * over)
    c2[...] = (0.25 * STEP) * ((lame[...] + rigidity[...]) * over)
    weight[...] = density[...] * metric[...]
    v = rigidity[...] * inv
    lane = lax.broadcasted_iota(jnp.int32, v.shape, 2)
    above[...] = v + jnp.where(lane == last, v, up_one(v))
    first[...] = 2.0 * v[:, :, 0:LANES]
    beta[...] = 0.5 * ((lame[...] + rigidity[...]) * metric[...])


def difference(f, lane):
    up = jnp.where(lane == f.shape[-1] - 1, f, up_one(f))
    return up - jnp.where(lane == 0, f, down_one(f))


def difference_transposed(q, lane):
    down = jnp.where(lane == 0, -q, down_one(q))
    return down - jnp.where(lane == q.shape[-1] - 1, -q, up_one(q))


def y_pieces(flags, y_in, start, x, field):
    def taken(a, b):
        return sides(flags, EVEN_Y, HAS_YM, HAS_YP, a, b)

    if len(y_in) == 2:
        rows = slice(start, start + x + 4)
        return [(slice(0, x + 4), *taken(y_in[0][rows], y_in[1][rows]))]
    rows = slice(start + 2, start + 2 + x)
    out = [(slice(2, 2 + x), *taken(y_in[0][rows], y_in[1][rows]))]
    for side in range(2):
        rows = slice(4 * field + 2 * side, 4 * field + 2 * side + 2)
        at = slice(side * (x + 2), side * (x + 2) + 2)
        out.append((at, *taken(y_in[2][rows], y_in[3][rows])))
    return out


def fill_beta(s, flags, own, ext, x_in, y_in, fine):
    x, y, e = (s.fx, s.fy, s.fe) if fine else (s.cx, s.cy, s.ce)
    ext[2 : 2 + x, 8 : 8 + y, :] = own[...]
    for h in range(1 if fine else s.halves):
        at = lanes_of(h)
        base = s.x_fine_beta if fine else s.x_coarse_beta + h * 2 * y
        rows = slice(base, base + 2 * y)
        low, high = sides(flags, EVEN_X, HAS_XM, HAS_XP, x_in[0][rows, :], x_in[1][rows, :])
        ext[0:2, 8 : 8 + y, at] = low.reshape(2, y, LANES)
        ext[x + 2 : x + 4, 8 : 8 + y, at] = high.reshape(2, y, LANES)
        start = s.y_fine_beta if fine else s.y_coarse_beta + h * e
        field = s.f_beta if fine else s.f_beta + 1 + h
        for i, low, high in y_pieces(flags, y_in, start, x, field):
            ext[i, 6:8, at] = low
            ext[i, 8 + y : 10 + y, at] = high


def fill_transposed(x, y, ext, beta, inv_ext, psi):
    z = ext.shape[-1]
    lane = lax.broadcasted_iota(jnp.int32, (y + 2, z), 1)
    wide, low, high = slice(7, 9 + y), slice(6, 8 + y), slice(8, 10 + y)

    def row(r, carry):
        along_x = ext[0, r, wide, :] * beta[r, wide, :]
        along_x -= ext[0, r + 2, wide, :] * beta[r + 2, wide, :]
        along_y = ext[1, r + 1, low, :] * beta[r + 1, low, :]
        along_y -= ext[1, r + 1, high, :] * beta[r + 1, high, :]
        inv = inv_ext[r, 0 : 2 + y, :]
        column = inv * beta[r + 1, wide, :] * ext[2, r + 1, wide, :]
        total = along_x + along_y + difference_transposed(column, lane)
        psi[r, wide, :] = jnp.where(inv > 0.0, total, 0.0)
        return carry

    lax.fori_loop(0, x + 2, row, 0, unroll=True)


def fill_displacement(s, flags, own, ext, x_in, y_in, fine, halves=None):
    x, y, e = (s.fx, s.fy, s.fe) if fine else (s.cx, s.cy, s.ce)
    halves = 1 if fine else halves or s.halves
    ext[:, 2 : 2 + x, 8 : 8 + y, :] = own[:, :, :, 0 : halves * LANES]
    mid = slice(8, 8 + y)

    def from_x(first, rows):
        rows = slice(first, first + rows)
        return sides(flags, EVEN_X, HAS_XM, HAS_XP, x_in[0][rows, :], x_in[1][rows, :])

    for h in range(halves):
        at = lanes_of(h)
        base = 0 if fine else s.x_coarse + h * 4 * y
        low, high = from_x(base, 2 * y)
        ext[0, 0:2, mid, at] = low.reshape(2, y, LANES)
        ext[0, x + 2 : x + 4, mid, at] = high.reshape(2, y, LANES)
        for c in (1, 2):
            ext[c, 1, mid, at], ext[c, x + 2, mid, at] = from_x(base + (1 + c) * y, y)
        start = 0 if fine else s.y_coarse + h * 2 * e
        field = 0 if fine else s.f_coarse + 2 * h
        for i, low, high in y_pieces(flags, y_in, start, x, field):
            ext[1, i, 6:8, at] = low
            ext[1, i, 8 + y : 10 + y, at] = high
        for i, low, high in y_pieces(flags, y_in, start + e, x, field + 1):
            for m, c in enumerate((0, 2)):
                ext[c, i, 7:8, at] = low[:, m : m + 1, :]
                ext[c, i, 8 + y : 9 + y, at] = high[:, m : m + 1, :]
    if fine:
        return
    at = lanes_of(0)
    low, high = from_x(s.x_plane, y)
    for c in (1, 2):
        ext[c, 0, mid, at] = pltpu.roll(low, LANES - c, 1)
        ext[c, x + 3, mid, at] = pltpu.roll(high, LANES - c, 1)
    for i, low, high in y_pieces(flags, y_in, s.y_plane, x, s.f_plane):
        for m, c in enumerate((0, 2)):
            ext[c, i, 6:7, at] = low[:, m : m + 1, :]
            ext[c, i, 9 + y : 10 + y, at] = high[:, m : m + 1, :]


def fill_materials(s, flags, rigidity, metric, inverse, wide_ext, inv_ext, x_in, y_in, fine):
    x, y = (s.fx, s.fy) if fine else (s.cx, s.cy)
    own_z = metric.shape[2]
    wide_ext[1 : 1 + x, 1 : 1 + y, :] = rigidity[...] * metric[...]
    inv_ext[1 : 1 + x, 1 : 1 + y, :] = inverse[...]
    for h in range(1 if fine else s.halves):
        at = lanes_of(h)
        edge = edge_factor((y, LANES), h * LANES, own_z - 1)
        got = []
        for m in range(2):
            base = s.x_fine_mats + m * y if fine else s.x_coarse_mats + (m * s.halves + h) * y
            rows = slice(base, base + y)
            even = flags[EVEN_X]
            a, b = x_in[0][rows, :], x_in[1][rows, :]
            got.append((jnp.where(even, b, a), jnp.where(even, a, b)))
        for side, (flag, place) in enumerate(((HAS_XM, 0), (HAS_XP, x + 1))):
            rig, met = got[0][side], got[1][side]
            wide_ext[place, 1 : 1 + y, at] = jnp.where(flags[flag], rig * met, 0.0)
            inv_ext[place, 1 : 1 + y, at] = jnp.where(flags[flag], edge / met, 0.0)
        start = s.y_fine_mats if fine else s.y_coarse_mats + h * x
        rows = slice(start, start + x)
        got = []
        for m in range(2):
            even = flags[EVEN_Y]
            a, b = y_in[0][rows, m : m + 1, :], y_in[1][rows, m : m + 1, :]
            got.append((jnp.where(even, b, a), jnp.where(even, a, b)))
        for side, (flag, place) in enumerate(((HAS_YM, 0), (HAS_YP, 1 + y))):
            rig, met = got[0][side], got[1][side]
            wide_ext[1 : 1 + x, place : place + 1, at] = jnp.where(flags[flag], rig * met, 0.0)
            inv_ext[1 : 1 + x, place : place + 1, at] = jnp.where(flags[flag], edge[None, 0:1] / met, 0.0)


def fill_divergence(x, y, ext, inv_ext, div):
    z = ext.shape[-1]
    lane = lax.broadcasted_iota(jnp.int32, (y + 2, z), 1)

    def row(r, carry):
        along_x = ext[0, r + 2, 7 : 9 + y, :] - ext[0, r, 7 : 9 + y, :]
        along_y = ext[1, r + 1, 8 : 10 + y, :] - ext[1, r + 1, 6 : 8 + y, :]
        f = ext[2, r + 1, 7 : 9 + y, :]
        inv = inv_ext[r, 0 : 2 + y, :]
        total = along_x + along_y + inv * difference(f, lane)
        div[r, 7 : 9 + y, :] = jnp.where(inv > 0.0, total, 0.0)
        return carry

    lax.fori_loop(0, x + 2, row, 0, unroll=True)


def update(x, y, ext, wide_ext, inv_ext, div, prev, coef, new, ghosts, psi=None):
    c1, c2, weight, above, vertical = coef
    z = ext.shape[-1]
    lane = lax.broadcasted_iota(jnp.int32, (y, z), 1)
    mid, left, right, own = slice(8, 8 + y), slice(7, 7 + y), slice(9, 9 + y), slice(1, 1 + y)

    def row(i, totals):
        wide = wide_ext[i + 1, own, :]
        w_xp = wide + wide_ext[i + 2, own, :]
        w_xm = wide_ext[i, own, :] + wide
        w_yp = wide + wide_ext[i + 1, 2 : 2 + y, :]
        w_ym = wide_ext[i + 1, 0:y, :] + wide
        inv = inv_ext[i + 1, own, :]
        gradient = (
            div[i + 2, mid, :] - div[i, mid, :],
            div[i + 1, right, :] - div[i + 1, left, :],
            inv * difference(div[i + 1, mid, :], lane),
        )
        if psi is not None:
            transposed = (
                psi[i, mid, :] - psi[i + 2, mid, :],
                psi[i + 1, left, :] - psi[i + 1, right, :],
                difference_transposed(inv * psi[i + 1, mid, :], lane),
            )
        top, bottom, top_next = ghosts(i)
        k1, k2, dm, va = c1[i], c2[i], weight[i], above[i]
        first = vertical[i, :, 0:1]
        inner, squares, cross = (jnp.zeros((y, z), jnp.float32) for _ in range(3))
        for c in range(3):
            u = ext[c, i + 2, mid, :]
            flux = w_xp * (ext[c, i + 3, mid, :] - u) - w_xm * (u - ext[c, i + 1, mid, :])
            flux += w_yp * (ext[c, i + 2, right, :] - u) - w_ym * (u - ext[c, i + 2, left, :])
            below = entry = 0.0
            if psi is None:
                below = 0.0 if bottom is None else bottom(c)
                entry = 0.0 if top is None else first * (u[:, 0:1] - top(c))
            elif top is not None:
                entry = first * u[:, 0:1]
            over = va * (jnp.where(lane == z - 1, below, up_one(u)) - u)
            flux += over - jnp.where(lane == 0, entry, down_one(over))
            whole = flux
            if psi is not None:
                if top is None:
                    whole = flux + jnp.where(lane == z - 1, va * bottom(c), 0.0)
                else:
                    whole = flux + jnp.where(lane == 0, first * top(c), 0.0)
            push = whole * k1 + k2 * gradient[c]
            before = prev[c, i]
            change = u - before
            inner += change * change - before * push
            change += push
            updated = u + change
            new[c, i] = updated
            if psi is not None:
                squares += change * change
                cross += updated * (flux + transposed[c])
                if top is not None:
                    cross += jnp.where(lane == 0, first * u[:, 0:1] * top_next(c), 0.0)
        total = totals[0] + dm * inner
        if psi is None:
            return (total,)
        return total, totals[1] + (dm * squares - (0.5 * STEP) * cross)

    start = (jnp.zeros((y, z), jnp.float32),) * (1 if psi is None else 2)
    return lax.fori_loop(0, x, row, start, unroll=4)


def double_plane(s, ext_c, double):
    lane = lax.broadcasted_iota(jnp.int32, (s.cy + 4, LANES), 1)
    table = jnp.zeros((s.cy + 4, LANES), jnp.float32)
    for i in range(s.ce):
        e0, e1, e2 = (ext_c[c, i, 6 : 10 + s.cy, 0:LANES] for c in range(3))
        e1, e2 = pltpu.roll(e1, 1, 1), pltpu.roll(e2, 2, 1)
        plane = jnp.where(lane == 0, e0, jnp.where(lane == 1, e1, e2))
        for k in (2 * i, 2 * i + 1):
            there = pltpu.roll(plane, 4 * k, 1) if k else plane
            table = jnp.where(lane // 4 == k, there, table)
    for j in range(s.cy + 4):
        double[2 * j : 2 * j + 2, :] = jnp.broadcast_to(table[j : j + 1, :], (2, LANES))


def add_pairs(s, fine, pairs):
    for c in range(3):
        for i in range(s.cx):
            pairs[c, i] = fine[c, 2 * i] + fine[c, 2 * i + 1]


def node_weights(s, offs):
    node = (s.fy, LANES)
    node_lane = lax.broadcasted_iota(jnp.int32, node, 1)
    near_x = jnp.where(node_lane // 4 % 2 == 0, 0.75, 0.25)
    near_y = jnp.where(lax.broadcasted_iota(jnp.int32, node, 0) % 2 == 0, 0.75, 0.25)
    code = offs[...]
    weights_x, weights_y = (
        [
            jnp.where(off == shift, near, 0.0) + jnp.where(off == shift - 1, 1.0 - near, 0.0)
            for shift in (-1, 0, 1, 2)
        ]
        for off, near in ((code // 4 - 1, near_x), (code % 4 - 1, near_y))
    )
    return weights_x, weights_y


def bottom_ghosts(s, weights, double, moved):
    weights_x, weights_y = weights
    node = (s.fy, LANES)
    ghosts = jnp.zeros(node, jnp.float32)
    for a in range(4):
        moved[a] = pltpu.roll(double[...], LANES - 8 * (1 + a), 1)
        line = jnp.zeros(node, jnp.float32)
        for b in range(4):
            line += weights_y[b] * moved[a, 2 * b + 2 : 2 * b + 2 + s.fy, :]
        ghosts += weights_x[a] * line
    return lambda i: (None, lambda c: pltpu.roll(ghosts, LANES - 1 - c - 4 * i, 1), None)


def top_ghosts(s, pairs, pairs_next=None):
    def mean(of, i):
        def top(c):
            both = of[c, i, pl.ds(0, s.cy, stride=2), :] + of[c, i, pl.ds(1, s.cy, stride=2), :]
            return 0.25 * both[:, LANES - 1 :]

        return top

    return lambda i: (mean(pairs, i), None, mean(pairs_next, i) if pairs_next is not None else None)


def step_kernel(s, step, cells, *refs):
    flags = where_am_i()
    refs = list(refs)

    def take(n):
        out = refs[:n]
        del refs[:n]
        return out

    fine, coarse, fine_prev, coarse_prev, offs = take(5)
    coef_f, coef_c = take(5), take(5)
    if step == 0:
        rig_f, met_f, inverse_f, rig_c, met_c, inverse_c = take(6)
    else:
        wide_f, inv_f, wide_c, inv_c = take(4)
    beta_own = take(2)
    if step == 1:
        energy_in, spread_in = take(2)
    x_in, y_in = take(2), take(4)
    new_f, new_c, energy = take(3)
    x_out = take(2)
    if step == 0:
        wide_f, inv_f, wide_c, inv_c, spread_out = take(5)
    ext_f, ext_c, div_f, div_c, double, moved, pairs = take(7)

    fill_displacement(s, flags, fine, ext_f, x_in, y_in, True)
    fill_displacement(s, flags, coarse, ext_c, x_in, y_in, False)
    if step == 0:
        fill_materials(s, flags, rig_f, met_f, inverse_f, wide_f, inv_f, x_in, y_in, True)
        fill_materials(s, flags, rig_c, met_c, inverse_c, wide_c, inv_c, x_in, y_in, False)

    double_plane(s, ext_c, double)
    add_pairs(s, fine, pairs)
    fill_divergence(s.fx, s.fy, ext_f, inv_f, div_f)
    fill_divergence(s.cx, s.cy, ext_c, inv_c, div_c)
    psi_f = psi_c = None
    if step == 1:
        psi_f, psi_c, all_beta_f, all_beta_c, pairs_next, spread = take(6)
        fill_beta(s, flags, beta_own[0], all_beta_f, x_in, y_in, True)
        fill_beta(s, flags, beta_own[1], all_beta_c, x_in, y_in, False)
        fill_transposed(s.fx, s.fy, ext_f, all_beta_f, inv_f, psi_f)
        fill_transposed(s.cx, s.cy, ext_c, all_beta_c, inv_c, psi_c)

    weights = node_weights(s, offs)
    fine_ghosts = bottom_ghosts(s, weights, double, moved)
    coarse_ghosts = top_ghosts(s, pairs, pairs_next if step == 1 else None)
    sums_f = update(
        s.fx, s.fy, ext_f, wide_f, inv_f, div_f, fine_prev, coef_f, new_f, fine_ghosts, psi_f
    )
    if step == 1:
        add_pairs(s, new_f, pairs_next)
    sums_c = update(
        s.cx, s.cy, ext_c, wide_c, inv_c, div_c, coarse_prev, coef_c, new_c, coarse_ghosts, psi_c
    )
    place = lax.broadcasted_iota(jnp.int32, (8, LANES), 0)
    table = jnp.zeros((8, LANES), jnp.float32) if step == 0 else energy_in[...]
    table = jnp.where(place == step, jnp.sum(sums_f[0]) / cells[0], table)
    table = jnp.where(place == STEPS + step, jnp.sum(sums_c[0]) / cells[1], table)
    if step == 0:
        weights_x, weights_y = weights
        node = (s.fy, LANES)
        node_lane = lax.broadcasted_iota(jnp.int32, node, 1)
        q = jnp.zeros(node, jnp.float32)
        for i in range(s.fx):
            for c in range(3):
                there = pltpu.roll(coef_f[3][i] * new_f[c, i], 4 * i + c + 1, 1)
                q = jnp.where(node_lane == 4 * i + c, there, q)
        moved[...] = jnp.zeros(moved.shape, jnp.float32)
        for a in range(4):
            part = weights_x[a] * q
            for b in range(4):
                moved[a, 2 * b + 2 : 2 * b + 2 + s.fy, :] += weights_y[b] * part
        double[...] = sum(pltpu.roll(moved[a], 8 * (1 + a), 1) for a in range(4))
        rows = s.cy + 4
        both = double[pl.ds(0, rows, stride=2), :] + double[pl.ds(1, rows, stride=2), :]
        for i in range(s.ce):
            there = pltpu.roll(both, LANES - 8 * i, 1) if i else both
            spread_out[i, 0:rows, :] = there + pltpu.roll(there, LANES - 4, 1)
            spread_out[i, rows:, :] = jnp.zeros((s.spread - rows, LANES), jnp.float32)
        put_x(s, flags, x_out, new_f, new_c, beta_own, spread_out)
    if step == 1:
        spread[...] = spread_in[:, 2 : 2 + s.cy, :]
        rows = pl.ds(s.corner_spread, s.cx)
        low, high = sides(flags, EVEN_Y, HAS_YM, HAS_YP, y_in[2][rows], y_in[3][rows])
        spread[:, 0:2, :] += low
        spread[:, s.cy - 2 : s.cy, :] += high
        joined = jnp.zeros((s.cy, LANES), jnp.float32)
        for i in range(s.cx):
            for c in range(3):
                weights = spread[i] if c == 0 else pltpu.roll(spread[i], LANES - c, 1)
                joined += new_c[c, i, :, 0:LANES] * weights
        joined = jnp.sum(joined[:, 0:1])
        table = jnp.where(place == 2, (jnp.sum(sums_f[1]) - (0.5 * STEP) * joined) / cells[0], table)
        table = jnp.where(place == STEPS + 2, jnp.sum(sums_c[1]) / cells[1], table)
        put_x(s, flags, x_out, new_f, new_c)
    energy[...] = table


def final_fine_kernel(s, fine, coarse, prev, offs, *refs):
    coef, (wide, inv, xa, xb, ya, yb, new) = refs[:5], refs[5:12]
    ext_f, ext_c, div, double, moved = refs[12:]
    flags = where_am_i()
    fill_displacement(s, flags, fine, ext_f, (xa, xb), (ya, yb), True)
    fill_displacement(s, flags, coarse, ext_c, (xa, xb), (ya, yb), False, 1)
    double_plane(s, ext_c, double)
    fill_divergence(s.fx, s.fy, ext_f, inv, div)
    ghosts = bottom_ghosts(s, node_weights(s, offs), double, moved)
    update(s.fx, s.fy, ext_f, wide, inv, div, prev, coef, new, ghosts)


def final_coarse_kernel(s, fine, coarse, prev, *refs):
    coef, (wide, inv, xa, xb, ya, yb, new) = refs[:5], refs[5:12]
    ext, div, pairs = refs[12:]
    fill_displacement(s, where_am_i(), coarse, ext, (xa, xb), (ya, yb), False)
    add_pairs(s, fine, pairs)
    fill_divergence(s.cx, s.cy, ext, inv, div)
    update(s.cx, s.cy, ext, wide, inv, div, prev, coef, new, top_ghosts(s, pairs))


VMEM = pl.BlockSpec(memory_space=pltpu.VMEM)
HBM = pl.BlockSpec(memory_space=pltpu.HBM)


def call(kernel, shapes, flops, *args, scratch=(), spec=VMEM, sems=0):
    shapes = [jax.ShapeDtypeStruct(shape, jnp.float32) for shape in shapes]
    scratch = [pltpu.VMEM(shape, jnp.float32) for shape in scratch]
    if sems:
        scratch.append(pltpu.SemaphoreType.DMA((sems,)))
    return pl.pallas_call(
        kernel,
        out_shape=shapes,
        in_specs=[spec] * len(args),
        out_specs=[VMEM] * len(shapes),
        scratch_shapes=scratch,
        compiler_params=pltpu.CompilerParams(vmem_limit_bytes=VMEM_LIMIT),
        cost_estimate=pl.CostEstimate(flops=flops, bytes_accessed=1 << 20, transcendentals=0),
    )(*args)


def swap_pairs(mesh, move):
    sizes = list(mesh.shape.values())
    pairs = []
    for source in range(math.prod(sizes)):
        rest, at = source, []
        for size in reversed(sizes):
            at.insert(0, rest % size)
            rest //= size
        target = 0
        for index, size in zip(move(*at), sizes, strict=True):
            target = target * size + index
        pairs.append((source, target))
    return pairs


def beside_x(z, x, y, core):
    return z, x ^ 1, y, core


def across_x(z, x, y, core):
    place = 4 * z + x
    if place in (0, 31):
        return z, x, y, core ^ 1
    place += 1 if place % 2 else -1
    return place // 4, place % 4, y, core


def beside_y(z, x, y, core):
    return z, x, y, core ^ 1


def across_y(z, x, y, core):
    place = (2 * y + core + (1 if core else -1)) % 8
    return z, x, place // 2, place % 2


TOTAL = (
    lambda z, x, y, core: (z ^ 7, x, y, core),
    lambda z, x, y, core: (z, x, y, core ^ 1),
    lambda z, x, y, core: (z ^ 2, x, y, core ^ 1),
    lambda z, x, y, core: (z, x, y ^ 1, core ^ 1),
    lambda z, x, y, core: (z, x ^ 1, y, core ^ 1),
    lambda z, x, y, core: (z ^ 1, x, y, core ^ 1),
    lambda z, x, y, core: (z, x ^ 3, y, core ^ 1),
    lambda z, x, y, core: (z, x, y ^ 3, core ^ 1),
)


def per_device(
    mesh,
    fine_disp,
    fine_prev,
    coarse_disp,
    coarse_prev,
    fine_density,
    fine_lame,
    fine_rigidity,
    fine_metric,
    coarse_density,
    coarse_lame,
    coarse_rigidity,
    coarse_metric,
    offsets,
):
    fine_shape, coarse_shape = fine_metric.shape, coarse_metric.shape
    s = Sizes(fine_shape, coarse_shape)
    count_x, count_y = lax.axis_size(GX), lax.axis_size(GY)

    def swap(value, move):
        return lax.ppermute(value, ALL, swap_pairs(mesh, move))

    def swap_both(pair, beside, across):
        second = swap(pair[1], across)
        first = swap(pair[0], beside)
        return [pltpu.with_memory_space_constraint(x, pltpu.VMEM) for x in (first, second)]

    offs = offsets[0] * 4 + offsets[1] + 5
    offs = jnp.pad(jnp.repeat(offs.T, 4, axis=1), ((0, 0), (0, LANES - 4 * s.fx)))
    x_out = call(
        functools.partial(first_kernel, s),
        [(s.x_rows_mats, LANES)] * 2,
        1000,
        *(
            pltpu.with_memory_space_constraint(x, pltpu.HBM)
            for x in (
                fine_disp,
                coarse_disp,
                fine_rigidity,
                fine_metric,
                coarse_rigidity,
                coarse_metric,
            )
        ),
        scratch=[
            (2, 3, 2, s.fy, s.fz),
            (2, 3, 2, s.cy, s.cz),
            (2, 2, s.fy, s.fz),
            (2, 2, s.cy, s.cz),
        ],
        spec=HBM,
        sems=12,
    )
    own = []
    for density, lame, rigidity, metric in (
        (fine_density, fine_lame, fine_rigidity, fine_metric),
        (coarse_density, coarse_lame, coarse_rigidity, coarse_metric),
    ):
        own.append(
            call(
                own_kernel,
                [metric.shape] * 5 + [metric.shape[:2] + (LANES,), metric.shape],
                2_000_000,
                density,
                lame,
                rigidity,
                metric,
            )
        )
    inverse_f, *coef_f, beta_f = own[0]
    inverse_c, *coef_c, beta_c = own[1]

    fine, coarse = fine_disp, coarse_disp
    fine_ext = (s.fx + 2, s.fy + 2, s.fz)
    coarse_ext = (s.cx + 2, s.cy + 2, s.cz)
    scratch = [
        (3, s.fe, s.fy + 16, s.fz),
        (3, s.ce, s.cy + 16, s.cz),
        (s.fx + 2, s.fy + 16, s.fz),
        (s.cx + 2, s.cy + 16, s.cz),
        (2 * (s.cy + 4), LANES),
        (4, 2 * (s.cy + 4), LANES),
        (3, s.cx, s.fy, LANES),
    ]
    cells = [count_x * count_y * s.fx * s.fy * s.fz, count_x * count_y * s.cx * s.cy * s.cz]
    spread = (s.ce, s.spread, LANES)
    for step in range(STEPS):
        x_in = swap_both(x_out, beside_x, across_x)
        if step == 2:
            for k, move in enumerate(TOTAL):
                other = swap(energy, move)
                if k < len(TOTAL) - 1:
                    energy = energy + other

        def y_strips(part, shapes, *args):
            kernel = functools.partial(y_kernel, s, step, part)
            return call(kernel, shapes, 500_000, *args)

        pairs = [(s.y_rows_mats, s.y_rows_beta, s.y_rows)[step], 2, LANES]
        if step == 2:
            y_out = y_strips("all", [tuple(pairs)] * 2, fine, coarse, *x_in)
            y_in = swap_both(y_out, beside_y, across_y)
        else:
            if step == 0:
                mats = [fine_rigidity, fine_metric, coarse_rigidity, coarse_metric]
                more, shapes = [], [(s.corner_rows, 2, LANES)] * 2
            else:
                mats = [beta_f, beta_c]
                more, shapes = [spread_own], [(s.corner_rows_beta, 2, LANES)] * 2
                shapes.append((s.cx,) + spread[1:])
            y_out = y_strips("own", [tuple(pairs)] * 2, fine, coarse, *mats)
            y_in = swap_both(y_out, beside_y, across_y)
            y_out = y_strips("corners", shapes, *more, *x_in)
            y_in += swap_both(y_out[:2], beside_y, across_y)
        if step == 2:
            wide_f, inv_f, wide_c, inv_c = ext_mats
            (fine_final,) = call(
                functools.partial(final_fine_kernel, s),
                [fine.shape],
                2_000_000,
                fine,
                coarse,
                fine_prev,
                offs,
                *coef_f,
                wide_f,
                inv_f,
                *x_in,
                *y_in,
                scratch=[scratch[0], scratch[1][:3] + (LANES,), scratch[2], *scratch[4:6]],
            )
            (coarse_final,) = call(
                functools.partial(final_coarse_kernel, s),
                [coarse.shape],
                2_000_000,
                fine,
                coarse,
                coarse_prev,
                *coef_c,
                wide_c,
                inv_c,
                *x_in,
                *y_in,
                scratch=[scratch[1], scratch[3], scratch[6]],
            )
            break
        shapes = [fine.shape, coarse.shape, (8, LANES)]
        shapes += [((s.x_rows_beta, s.x_rows)[step], LANES)] * 2
        more_scratch = []
        if step == 0:
            extra = [fine_rigidity, fine_metric, inverse_f, coarse_rigidity, coarse_metric, inverse_c]
            extra += [beta_f, beta_c]
            shapes += [fine_ext, fine_ext, coarse_ext, coarse_ext, spread]
        else:
            extra = list(ext_mats)
        if step == 1:
            extra += [beta_f, beta_c, energy, y_out[2]]
            more_scratch = [
                scratch[2],
                scratch[3],
                scratch[0][1:],
                scratch[1][1:],
                scratch[6],
                (s.cx, s.cy, LANES),
            ]
        outs = call(
            functools.partial(step_kernel, s, step, cells),
            shapes,
            4_000_000,
            fine,
            coarse,
            fine_prev,
            coarse_prev,
            offs,
            *coef_f,
            *coef_c,
            *extra,
            *x_in,
            *y_in,
            scratch=scratch + more_scratch,
        )
        fine_prev, coarse_prev = fine, coarse
        fine, coarse, energy = outs[:3]
        x_out = outs[3:5]
        if step == 0:
            *ext_mats, spread_own = outs[5:]
    other, fine, coarse = lax.optimization_barrier((other, fine_final, coarse_final))
    energy = energy + other
    energy = energy[: 2 * STEPS, 0].reshape(2, STEPS).T
    return fine, coarse, energy


def solution(mesh):
    finer = Mesh(mesh.devices.reshape(8, 4, 4, 2), ALL)
    level, cell = P(None, GX, GY, None), P(GX, GY, None)
    in_specs = (level,) * 4 + (cell,) * 8 + (P(None, GX, GY),)

    def body(*args):
        return per_device(finer, *args)

    return jax.shard_map(
        body, mesh=finer, in_specs=in_specs, out_specs=(level, level, P()), check_vma=False
    )
```

```python
import functools
import math

import jax
import jax.numpy as jnp
from jax import lax
from jax.experimental import pallas as pl
from jax.experimental.pallas import tpu as pltpu
from jax.sharding import Mesh
from jax.sharding import PartitionSpec as P

STEPS = 3
GX = ("gx_0", "gx_1")
GY = ("gy_0", "gy_1")
ALL = GX + GY
STEP = 0.15
LANES = 128
VMEM_LIMIT = 20 * 1024 * 1024

EVEN_X, HAS_XM, HAS_XP, EVEN_Y, HAS_YM, HAS_YP = range(6)


def where_am_i():
    x = 4 * lax.axis_index("gx_0") + lax.axis_index("gx_1")
    y = 2 * lax.axis_index("gy_0") + lax.axis_index("gy_1")
    return x % 2 == 0, x > 0, x < 31, y % 2 == 0, y > 0, y < 7


class Sizes:
    def __init__(self, fine, coarse):
        self.fx, self.fy, self.fz = fine
        self.cx, self.cy, self.cz = coarse
        self.halves = self.cz // LANES
        self.x_coarse = 4 * self.fy
        self.x_plane = self.x_coarse + self.halves * 4 * self.cy
        self.x_rows = self.x_plane + self.cy
        self.x_fine_mats = self.x_rows
        self.x_coarse_mats = self.x_fine_mats + 2 * self.fy
        self.x_rows_mats = self.x_coarse_mats + 2 * self.halves * self.cy
        self.x_fine_beta = self.x_rows
        self.x_coarse_beta = self.x_fine_beta + 2 * self.fy
        self.x_spread = self.x_coarse_beta + self.halves * 2 * self.cy
        self.spread = self.cy + 8
        self.x_rows_beta = self.x_spread + 2 * self.spread
        self.fe, self.ce = self.fx + 4, self.cx + 4
        self.y_coarse = 2 * self.fe
        self.y_plane = self.y_coarse + self.halves * 2 * self.ce
        self.y_rows = self.y_plane + self.ce
        self.y_fine_mats = self.y_rows
        self.y_coarse_mats = self.y_fine_mats + self.fx
        self.y_rows_mats = self.y_coarse_mats + self.halves * self.cx
        self.y_fine_beta = self.y_rows
        self.y_coarse_beta = self.y_fine_beta + self.fe
        self.y_rows_beta = self.y_coarse_beta + self.halves * self.ce
        self.f_coarse = 2
        self.f_plane = self.f_coarse + 2 * self.halves
        self.f_beta = self.f_plane + 1
        self.corner_rows = 4 * self.f_beta
        self.corner_spread = 4 * (self.f_beta + 1 + self.halves)
        self.corner_rows_beta = self.corner_spread + self.cx


def lanes_of(h):
    return slice(h * LANES, (h + 1) * LANES)


def put_strips(s, out, far, fine, coarse, at_f, at_c):
    near, second = jnp.where(far, 1, 0), jnp.where(far, 0, 1)
    for n, (c, row) in enumerate(((0, 0), (0, 1), (1, near), (2, near))):
        out[n * s.fy : (n + 1) * s.fy, :] = fine[c, at_f + row]
        line = coarse[c, at_c + row]
        for h in range(s.halves):
            base = s.x_coarse + (h * 4 + n) * s.cy
            out[base : base + s.cy, :] = line[:, lanes_of(h)]
    along_y, along_z = (coarse[c, at_c + second][:, 0:LANES] for c in (1, 2))
    lane = lax.broadcasted_iota(jnp.int32, along_y.shape, 1)
    plane = jnp.where(lane == 1, pltpu.roll(along_y, 1, 1), pltpu.roll(along_z, 2, 1))
    out[s.x_plane : s.x_plane + s.cy, :] = plane


def put_x(s, flags, outs, fine, coarse, betas=None, spread=None):
    even = flags[EVEN_X]
    for k, out in enumerate(outs):
        far = even if k == 0 else jnp.logical_not(even)
        start_f = jnp.where(far, s.fx - 2, 0)
        start_c = jnp.where(far, s.cx - 2, 0)
        put_strips(s, out, far, fine, coarse, start_f, start_c)
        if betas is None:
            continue
        strip = betas[0][pl.ds(start_f, 2), :, :]
        out[s.x_fine_beta : s.x_coarse_beta, :] = strip.reshape(2 * s.fy, LANES)
        strip = betas[1][pl.ds(start_c, 2), :, :]
        for h in range(s.halves):
            base = s.x_coarse_beta + h * 2 * s.cy
            out[base : base + 2 * s.cy, :] = strip[:, :, lanes_of(h)].reshape(2 * s.cy, LANES)
        start = jnp.where(far, s.cx + 2, 0)
        out[s.x_spread : s.x_rows_beta, :] = spread[pl.ds(start, 2)].reshape(2 * s.spread, LANES)


def first_kernel(s, fine, coarse, rig_f, met_f, rig_c, met_c, out_a, out_b, *scratch):
    strip_f, strip_c, line_f, line_c, sems = scratch
    flags = where_am_i()
    copies = []

    def fetch(source, target):
        copies.append(pltpu.make_async_copy(source, target, sems.at[len(copies)]))
        copies[-1].start()

    even = flags[EVEN_X]
    for k in range(2):
        far = even if k == 0 else jnp.logical_not(even)
        fetch(fine.at[:, pl.ds(jnp.where(far, s.fx - 2, 0), 2)], strip_f.at[k])
        fetch(coarse.at[:, pl.ds(jnp.where(far, s.cx - 2, 0), 2)], strip_c.at[k])
        for m, (of_f, of_c) in enumerate(((rig_f, rig_c), (met_f, met_c))):
            fetch(of_f.at[jnp.where(far, s.fx - 1, 0)], line_f.at[k, m])
            fetch(of_c.at[jnp.where(far, s.cx - 1, 0)], line_c.at[k, m])
    for copy in copies:
        copy.wait()
    for k, out in enumerate((out_a, out_b)):
        far = even if k == 0 else jnp.logical_not(even)
        put_strips(s, out, far, strip_f.at[k], strip_c.at[k], 0, 0)
        for m in range(2):
            base = s.x_fine_mats + m * s.fy
            out[base : base + s.fy, :] = line_f[k, m]
            for h in range(s.halves):
                base = s.x_coarse_mats + (m * s.halves + h) * s.cy
                out[base : base + s.cy, :] = line_c[k, m, :, lanes_of(h)]


def sides(flags, even, has_low, has_high, a, b):
    low = jnp.where(flags[even], b, a)
    high = jnp.where(flags[even], a, b)
    low = jnp.where(flags[has_low], low, 0.0)
    high = jnp.where(flags[has_high], high, 0.0)
    return low, high


def y_kernel(s, step, part, *refs):
    flags = where_am_i()
    refs = list(refs)
    even = flags[EVEN_Y]
    has_own, has_corners = part != "corners", part != "own"
    if has_own:
        fine, coarse = refs[:2]
        mats = refs[2:-2] if part == "own" else []
    if has_corners:
        total = refs.pop() if step == 1 else None
        in_a, in_b = refs[-4:-2]
        spread = refs[0]
    out_a, out_b = refs[-2:]

    def put(index, low, high):
        out_a[index] = jnp.where(even, high, low)
        out_b[index] = jnp.where(even, low, high)

    def put_one(index, m, low, high):
        out_a[index, m : m + 1, :] = jnp.where(even, high, low)
        out_b[index, m : m + 1, :] = jnp.where(even, low, high)

    def came(first, count):
        rows = slice(first, first + count)
        return sides(flags, EVEN_X, HAS_XM, HAS_XP, in_a[rows, :], in_b[rows, :])

    def corner(base, field, x, side, k):
        return 4 * field + 2 * side + k if part == "corners" else base + side * (x + 2) + k

    def level(own, x, y, x_base, y_base, y_size, field, plane):
        both, single = y_base, y_base + y_size
        if has_own:
            put(pl.ds(both + 2, x), own(1, slice(0, 2)), own(1, slice(y - 2, y)))
            for m, c in enumerate((0, 2)):
                here = pl.ds(single + 2, x)
                put_one(here, m, own(c, slice(0, 1)), own(c, slice(y - 1, y)))
                if plane:
                    here = pl.ds(s.y_plane + 2, x)
                    put_one(here, m, own(c, slice(1, 2)), own(c, slice(y - 2, y - 1)))
        for side, k in ((0, 0), (0, 1), (1, 0), (1, 1)) if has_corners else ():
            near = k == 1 - side

            def row(c, first, count):
                if c == 0:
                    return came(x_base + k * y + first, count)[side]
                if near:
                    return came(x_base + (1 + c) * y + first, count)[side]
                return pltpu.roll(came(s.x_plane + first, count)[side], LANES - c, 1)

            if near or plane:
                put(corner(both, field, x, side, k), row(1, 0, 2), row(1, y - 2, 2))
            for m, c in enumerate((0, 2)):
                if c == 0 or near or plane:
                    here = corner(single, field + 1, x, side, k)
                    put_one(here, m, row(c, 0, 1), row(c, y - 1, 1))
                if plane:
                    here = corner(s.y_plane, s.f_plane, x, side, k)
                    put_one(here, m, row(c, 1, 1), row(c, y - 2, 1))

    def two_deep(own, x, y, x_base, y_base, field):
        if has_own:
            put(pl.ds(y_base + 2, x), own(slice(0, 2)), own(slice(y - 2, y)))
        for k in range(2) if has_corners else ():
            low, high = came(x_base + k * y, 2), came(x_base + (k + 1) * y - 2, 2)
            for side in range(2):
                put(corner(y_base, field, x, side, k), low[side], high[side])

    level(lambda c, r: fine[c, :, r, :], s.fx, s.fy, 0, 0, s.fe, 0, False)
    for h in range(s.halves):
        x_base, y_base = s.x_coarse + h * 4 * s.cy, s.y_coarse + h * 2 * s.ce
        field = s.f_coarse + 2 * h
        at = lanes_of(h)
        level(
            lambda c, r: coarse[c, :, r, at], s.cx, s.cy, x_base, y_base, s.ce, field, h == 0
        )
    if step == 0 and has_own:
        rig_f, met_f, rig_c, met_c = mats
        for m, (of_f, of_c) in enumerate(((rig_f, rig_c), (met_f, met_c))):
            here = pl.ds(s.y_fine_mats, s.fx)
            put_one(here, m, of_f[:, 0:1, :], of_f[:, s.fy - 1 : s.fy, :])
            for h in range(s.halves):
                here = pl.ds(s.y_coarse_mats + h * s.cx, s.cx)
                low, high = of_c[:, 0:1, lanes_of(h)], of_c[:, s.cy - 1 : s.cy, lanes_of(h)]
                put_one(here, m, low, high)
    if step == 1:
        beta_f, beta_c = mats if has_own else (None, None)
        x_base, y_base = s.x_fine_beta, s.y_fine_beta
        two_deep(lambda r: beta_f[:, r, :], s.fx, s.fy, x_base, y_base, s.f_beta)
        for h in range(s.halves):
            at = lanes_of(h)
            x_base, y_base = s.x_coarse_beta + h * 2 * s.cy, s.y_coarse_beta + h * s.ce
            field = s.f_beta + 1 + h
            two_deep(lambda r: beta_c[:, r, at], s.cx, s.cy, x_base, y_base, field)
    if step == 1 and has_corners:
        total[...] = spread[2 : 2 + s.cx]
        for k in range(2):
            low, high = came(s.x_spread + k * s.spread, s.spread)
            total[k] += low
            total[s.cx - 2 + k] += high
        here = pl.ds(s.corner_spread, s.cx)
        put(here, total[:, 0:2, :], total[:, s.cy + 2 : s.cy + 4, :])


def up_one(x):
    return pltpu.roll(x, x.shape[-1] - 1, x.ndim - 1)


def down_one(x):
    return pltpu.roll(x, 1, x.ndim - 1)


def edge_factor(shape, first, last):
    lane = first + lax.broadcasted_iota(jnp.int32, shape, len(shape) - 1)
    return jnp.where((lane == 0) | (lane == last), 2.0, 1.0)


def own_kernel(density, lame, rigidity, metric, inverse, c1, c2, weight, above, first, beta):
    inv = 1.0 / metric[...]
    last = inv.shape[2] - 1
    inverse[...] = inv * edge_factor(inv.shape, 0, last)
    over = 1.0 / density[...]
    c1[...] = (0.5 * STEP) * (inv * over)
    c2[...] = (0.25 * STEP) * ((lame[...] + rigidity[...]) * over)
    weight[...] = density[...] * metric[...]
    v = rigidity[...] * inv
    lane = lax.broadcasted_iota(jnp.int32, v.shape, 2)
    above[...] = v + jnp.where(lane == last, v, up_one(v))
    first[...] = 2.0 * v[:, :, 0:LANES]
    beta[...] = 0.5 * ((lame[...] + rigidity[...]) * metric[...])


def difference(f, lane):
    up = jnp.where(lane == f.shape[-1] - 1, f, up_one(f))
    return up - jnp.where(lane == 0, f, down_one(f))


def difference_transposed(q, lane):
    down = jnp.where(lane == 0, -q, down_one(q))
    return down - jnp.where(lane == q.shape[-1] - 1, -q, up_one(q))


def y_pieces(flags, y_in, start, x, field):
    def taken(a, b):
        return sides(flags, EVEN_Y, HAS_YM, HAS_YP, a, b)

    if len(y_in) == 2:
        rows = slice(start, start + x + 4)
        return [(slice(0, x + 4), *taken(y_in[0][rows], y_in[1][rows]))]
    rows = slice(start + 2, start + 2 + x)
    out = [(slice(2, 2 + x), *taken(y_in[0][rows], y_in[1][rows]))]
    for side in range(2 if y_in[2] is not None else 0):
        rows = slice(4 * field + 2 * side, 4 * field + 2 * side + 2)
        at = slice(side * (x + 2), side * (x + 2) + 2)
        out.append((at, *taken(y_in[2][rows], y_in[3][rows])))
    return out


def fill_beta(s, flags, own, ext, x_in, y_in, fine):
    x, y, e = (s.fx, s.fy, s.fe) if fine else (s.cx, s.cy, s.ce)
    ext[2 : 2 + x, 8 : 8 + y, :] = own[...]
    for h in range(1 if fine else s.halves):
        at = lanes_of(h)
        base = s.x_fine_beta if fine else s.x_coarse_beta + h * 2 * y
        rows = slice(base, base + 2 * y)
        low, high = sides(flags, EVEN_X, HAS_XM, HAS_XP, x_in[0][rows, :], x_in[1][rows, :])
        ext[0:2, 8 : 8 + y, at] = low.reshape(2, y, LANES)
        ext[x + 2 : x + 4, 8 : 8 + y, at] = high.reshape(2, y, LANES)
        start = s.y_fine_beta if fine else s.y_coarse_beta + h * e
        field = s.f_beta if fine else s.f_beta + 1 + h
        for i, low, high in y_pieces(flags, y_in, start, x, field):
            ext[i, 6:8, at] = low
            ext[i, 8 + y : 10 + y, at] = high


def fill_transposed(y, ext, beta, inv_ext, psi, rows):
    z = ext.shape[-1]
    lane = lax.broadcasted_iota(jnp.int32, (y + 2, z), 1)
    wide, low, high = slice(7, 9 + y), slice(6, 8 + y), slice(8, 10 + y)

    for r in rows:
        along_x = ext[0, r, wide, :] * beta[r, wide, :]
        along_x -= ext[0, r + 2, wide, :] * beta[r + 2, wide, :]
        along_y = ext[1, r + 1, low, :] * beta[r + 1, low, :]
        along_y -= ext[1, r + 1, high, :] * beta[r + 1, high, :]
        inv = inv_ext[r, 0 : 2 + y, :]
        column = inv * beta[r + 1, wide, :] * ext[2, r + 1, wide, :]
        total = along_x + along_y + difference_transposed(column, lane)
        psi[r, wide, :] = jnp.where(inv > 0.0, total, 0.0)


def fill_displacement(s, flags, own, ext, x_in, y_in, fine, halves=None):
    x, y, e = (s.fx, s.fy, s.fe) if fine else (s.cx, s.cy, s.ce)
    halves = 1 if fine else halves or s.halves
    ext[:, 2 : 2 + x, 8 : 8 + y, :] = own[:, :, :, 0 : halves * LANES]
    mid = slice(8, 8 + y)

    def from_x(first, rows):
        rows = slice(first, first + rows)
        return sides(flags, EVEN_X, HAS_XM, HAS_XP, x_in[0][rows, :], x_in[1][rows, :])

    for h in range(halves):
        at = lanes_of(h)
        base = 0 if fine else s.x_coarse + h * 4 * y
        low, high = from_x(base, 2 * y)
        ext[0, 0:2, mid, at] = low.reshape(2, y, LANES)
        ext[0, x + 2 : x + 4, mid, at] = high.reshape(2, y, LANES)
        for c in (1, 2):
            ext[c, 1, mid, at], ext[c, x + 2, mid, at] = from_x(base + (1 + c) * y, y)
        start = 0 if fine else s.y_coarse + h * 2 * e
        field = 0 if fine else s.f_coarse + 2 * h
        for i, low, high in y_pieces(flags, y_in, start, x, field):
            ext[1, i, 6:8, at] = low
            ext[1, i, 8 + y : 10 + y, at] = high
        for i, low, high in y_pieces(flags, y_in, start + e, x, field + 1):
            for m, c in enumerate((0, 2)):
                ext[c, i, 7:8, at] = low[:, m : m + 1, :]
                ext[c, i, 8 + y : 9 + y, at] = high[:, m : m + 1, :]
    if fine:
        return
    at = lanes_of(0)
    low, high = from_x(s.x_plane, y)
    for c in (1, 2):
        ext[c, 0, mid, at] = pltpu.roll(low, LANES - c, 1)
        ext[c, x + 3, mid, at] = pltpu.roll(high, LANES - c, 1)
    for i, low, high in y_pieces(flags, y_in, s.y_plane, x, s.f_plane):
        for m, c in enumerate((0, 2)):
            ext[c, i, 6:7, at] = low[:, m : m + 1, :]
            ext[c, i, 9 + y : 10 + y, at] = high[:, m : m + 1, :]


def fill_materials(s, flags, rigidity, metric, inverse, wide_ext, inv_ext, x_in, y_in, fine):
    x, y = (s.fx, s.fy) if fine else (s.cx, s.cy)
    own_z = metric.shape[2]
    wide_ext[1 : 1 + x, 1 : 1 + y, :] = rigidity[...] * metric[...]
    inv_ext[1 : 1 + x, 1 : 1 + y, :] = inverse[...]
    for h in range(1 if fine else s.halves):
        at = lanes_of(h)
        edge = edge_factor((y, LANES), h * LANES, own_z - 1)
        got = []
        for m in range(2):
            base = s.x_fine_mats + m * y if fine else s.x_coarse_mats + (m * s.halves + h) * y
            rows = slice(base, base + y)
            even = flags[EVEN_X]
            a, b = x_in[0][rows, :], x_in[1][rows, :]
            got.append((jnp.where(even, b, a), jnp.where(even, a, b)))
        for side, (flag, place) in enumerate(((HAS_XM, 0), (HAS_XP, x + 1))):
            rig, met = got[0][side], got[1][side]
            wide_ext[place, 1 : 1 + y, at] = jnp.where(flags[flag], rig * met, 0.0)
            inv_ext[place, 1 : 1 + y, at] = jnp.where(flags[flag], edge / met, 0.0)
        start = s.y_fine_mats if fine else s.y_coarse_mats + h * x
        rows = slice(start, start + x)
        got = []
        for m in range(2):
            even = flags[EVEN_Y]
            a, b = y_in[0][rows, m : m + 1, :], y_in[1][rows, m : m + 1, :]
            got.append((jnp.where(even, b, a), jnp.where(even, a, b)))
        for side, (flag, place) in enumerate(((HAS_YM, 0), (HAS_YP, 1 + y))):
            rig, met = got[0][side], got[1][side]
            wide_ext[1 : 1 + x, place : place + 1, at] = jnp.where(flags[flag], rig * met, 0.0)
            inv_ext[1 : 1 + x, place : place + 1, at] = jnp.where(flags[flag], edge[None, 0:1] / met, 0.0)


def fill_divergence(x, y, ext, inv_ext, div, rows=None):
    z = ext.shape[-1]
    lane = lax.broadcasted_iota(jnp.int32, (y + 2, z), 1)

    for r in rows or range(x + 2):
        along_x = ext[0, r + 2, 7 : 9 + y, :] - ext[0, r, 7 : 9 + y, :]
        along_y = ext[1, r + 1, 8 : 10 + y, :] - ext[1, r + 1, 6 : 8 + y, :]
        f = ext[2, r + 1, 7 : 9 + y, :]
        inv = inv_ext[r, 0 : 2 + y, :]
        total = along_x + along_y + inv * difference(f, lane)
        div[r, 7 : 9 + y, :] = jnp.where(inv > 0.0, total, 0.0)


def update(x, y, ext, wide_ext, inv_ext, div, prev, coef, new, ghosts, psi=None, rows=None):
    c1, c2, weight, above, vertical = coef
    z = ext.shape[-1]
    lane = lax.broadcasted_iota(jnp.int32, (y, z), 1)
    mid, left, right, own = slice(8, 8 + y), slice(7, 7 + y), slice(9, 9 + y), slice(1, 1 + y)

    def row(i, totals):
        wide = wide_ext[i + 1, own, :]
        w_xp = wide + wide_ext[i + 2, own, :]
        w_xm = wide_ext[i, own, :] + wide
        w_yp = wide + wide_ext[i + 1, 2 : 2 + y, :]
        w_ym = wide_ext[i + 1, 0:y, :] + wide
        inv = inv_ext[i + 1, own, :]
        gradient = (
            div[i + 2, mid, :] - div[i, mid, :],
            div[i + 1, right, :] - div[i + 1, left, :],
            inv * difference(div[i + 1, mid, :], lane),
        )
        if psi is not None:
            transposed = (
                psi[i, mid, :] - psi[i + 2, mid, :],
                psi[i + 1, left, :] - psi[i + 1, right, :],
                difference_transposed(inv * psi[i + 1, mid, :], lane),
            )
        top, bottom, top_next = ghosts(i)
        k1, k2, dm, va = c1[i], c2[i], weight[i], above[i]
        first = vertical[i, :, 0:1]
        inner, squares, cross = (jnp.zeros((y, z), jnp.float32) for _ in range(3))
        for c in range(3):
            u = ext[c, i + 2, mid, :]
            flux = w_xp * (ext[c, i + 3, mid, :] - u) - w_xm * (u - ext[c, i + 1, mid, :])
            flux += w_yp * (ext[c, i + 2, right, :] - u) - w_ym * (u - ext[c, i + 2, left, :])
            below = entry = 0.0
            if psi is None:
                below = 0.0 if bottom is None else bottom(c)
                entry = 0.0 if top is None else first * (u[:, 0:1] - top(c))
            elif top is not None:
                entry = first * u[:, 0:1]
            over = va * (jnp.where(lane == z - 1, below, up_one(u)) - u)
            flux += over - jnp.where(lane == 0, entry, down_one(over))
            whole = flux
            if psi is not None:
                if top is None:
                    whole = flux + jnp.where(lane == z - 1, va * bottom(c), 0.0)
                else:
                    whole = flux + jnp.where(lane == 0, first * top(c), 0.0)
            push = whole * k1 + k2 * gradient[c]
            before = prev[c, i]
            change = u - before
            inner += change * change - before * push
            change += push
            updated = u + change
            new[c, i] = updated
            if psi is not None:
                squares += change * change
                cross += updated * (flux + transposed[c])
                if top is not None:
                    cross += jnp.where(lane == 0, first * u[:, 0:1] * top_next(c), 0.0)
        total = totals[0] + dm * inner
        if psi is None:
            return (total,)
        return total, totals[1] + (dm * squares - (0.5 * STEP) * cross)

    start = (jnp.zeros((y, z), jnp.float32),) * (1 if psi is None else 2)
    count, index, unroll = rows or (x, lambda k: k, 4)
    return lax.fori_loop(0, count, lambda k, t: row(index(k), t), start, unroll=unroll)


def double_plane(s, ext_c, double):
    lane = lax.broadcasted_iota(jnp.int32, (s.cy + 4, LANES), 1)
    table = jnp.zeros((s.cy + 4, LANES), jnp.float32)
    for i in range(s.ce):
        e0, e1, e2 = (ext_c[c, i, 6 : 10 + s.cy, 0:LANES] for c in range(3))
        e1, e2 = pltpu.roll(e1, 1, 1), pltpu.roll(e2, 2, 1)
        plane = jnp.where(lane == 0, e0, jnp.where(lane == 1, e1, e2))
        for k in (2 * i, 2 * i + 1):
            there = pltpu.roll(plane, 4 * k, 1) if k else plane
            table = jnp.where(lane // 4 == k, there, table)
    for j in range(s.cy + 4):
        double[2 * j : 2 * j + 2, :] = jnp.broadcast_to(table[j : j + 1, :], (2, LANES))


def add_pairs(s, fine, pairs):
    for c in range(3):
        for i in range(s.cx):
            pairs[c, i] = fine[c, 2 * i] + fine[c, 2 * i + 1]


def node_weights(s, offs):
    node = (s.fy, LANES)
    node_lane = lax.broadcasted_iota(jnp.int32, node, 1)
    near_x = jnp.where(node_lane // 4 % 2 == 0, 0.75, 0.25)
    near_y = jnp.where(lax.broadcasted_iota(jnp.int32, node, 0) % 2 == 0, 0.75, 0.25)
    code = offs[...]
    weights_x, weights_y = (
        [
            jnp.where(off == shift, near, 0.0) + jnp.where(off == shift - 1, 1.0 - near, 0.0)
            for shift in (-1, 0, 1, 2)
        ]
        for off, near in ((code // 4 - 1, near_x), (code % 4 - 1, near_y))
    )
    return weights_x, weights_y


def bottom_ghosts(s, weights, double, moved):
    weights_x, weights_y = weights
    node = (s.fy, LANES)
    ghosts = jnp.zeros(node, jnp.float32)
    for a in range(4):
        moved[a] = pltpu.roll(double[...], LANES - 8 * (1 + a), 1)
        line = jnp.zeros(node, jnp.float32)
        for b in range(4):
            line += weights_y[b] * moved[a, 2 * b + 2 : 2 * b + 2 + s.fy, :]
        ghosts += weights_x[a] * line
    return lambda i: (None, lambda c: pltpu.roll(ghosts, LANES - 1 - c - 4 * i, 1), None)


def top_ghosts(s, pairs, pairs_next=None):
    def mean(of, i):
        def top(c):
            both = of[c, i, pl.ds(0, s.cy, stride=2), :] + of[c, i, pl.ds(1, s.cy, stride=2), :]
            return 0.25 * both[:, LANES - 1 :]

        return top

    return lambda i: (mean(pairs, i), None, mean(pairs_next, i) if pairs_next is not None else None)


INNER_F, OUTER_F = (10, lambda k: k + 2, 5), (6, lambda k: jnp.where(k < 2, k, k + 10), 3)
INNER_C, OUTER_C = (4, lambda k: k + 1, 4), (4, lambda k: jnp.where(k < 1, k, k + 4), 4)
INNER_DIV_F, OUTER_DIV_F = tuple(range(2, 14)), (0, 1, 2, 3, *range(12, 18))
INNER_DIV_C, OUTER_DIV_C = tuple(range(1, 7)), (0, 1, 2, *range(5, 10))


def step_kernel(s, step, inner, cells, *refs):
    flags = where_am_i()
    refs = list(refs)

    def take(n):
        out = refs[:n]
        del refs[:n]
        return out

    fine, coarse, fine_prev, coarse_prev, offs = take(5)
    coef_f, coef_c = take(5), take(5)
    makes_mats = inner and step == 0
    if makes_mats:
        rig_f, met_f, inverse_f, rig_c, met_c, inverse_c = take(6)
    else:
        wide_f, inv_f, wide_c, inv_c = take(4)
    beta_own = take(2)
    table_in = take(1)[0] if step == 1 or not inner else None
    if not inner:
        done_f, done_c = take(2)
    if step == 1 and not inner:
        (spread_in,) = take(1)
    x_in = take(2)
    y_in = take(2) + [None, None] if inner else take(4)
    new_f, new_c, energy = take(3)
    if not inner:
        x_out = take(2)
    if makes_mats:
        wide_f, inv_f, wide_c, inv_c = take(4)
    if step == 0 and not inner:
        (spread_out,) = take(1)
    ext_f, ext_c, div_f, div_c, double, moved, pairs = take(7)

    fill_displacement(s, flags, fine, ext_f, x_in, y_in, True)
    fill_displacement(s, flags, coarse, ext_c, x_in, y_in, False)
    if makes_mats:
        fill_materials(s, flags, rig_f, met_f, inverse_f, wide_f, inv_f, x_in, y_in, True)
        fill_materials(s, flags, rig_c, met_c, inverse_c, wide_c, inv_c, x_in, y_in, False)
    double_plane(s, ext_c, double)
    add_pairs(s, fine, pairs)
    rows_f, rows_c = (INNER_F, INNER_C) if inner else (OUTER_F, OUTER_C)
    lines_f, lines_c = (INNER_DIV_F, INNER_DIV_C) if inner else (OUTER_DIV_F, OUTER_DIV_C)
    fill_divergence(s.fx, s.fy, ext_f, inv_f, div_f, lines_f)
    fill_divergence(s.cx, s.cy, ext_c, inv_c, div_c, lines_c)
    psi_f = psi_c = pairs_next = None
    if step == 1:
        psi_f, psi_c, all_beta_f, all_beta_c, pairs_next, spread = take(6)
        fill_beta(s, flags, beta_own[0], all_beta_f, x_in, y_in, True)
        fill_beta(s, flags, beta_own[1], all_beta_c, x_in, y_in, False)
        fill_transposed(s.fy, ext_f, all_beta_f, inv_f, psi_f, lines_f)
        fill_transposed(s.cy, ext_c, all_beta_c, inv_c, psi_c, lines_c)
    if not inner:
        new_f[:, 2:12] = done_f[:, 2:12]
        new_c[:, 1:5] = done_c[:, 1:5]

    weights = node_weights(s, offs)
    ghosts_f = bottom_ghosts(s, weights, double, moved)
    ghosts_c = top_ghosts(s, pairs, pairs_next)
    sums_f = update(
        s.fx, s.fy, ext_f, wide_f, inv_f, div_f, fine_prev, coef_f, new_f, ghosts_f, psi_f, rows_f
    )
    if step == 1:
        add_pairs(s, new_f, pairs_next)
    sums_c = update(
        s.cx, s.cy, ext_c, wide_c, inv_c, div_c, coarse_prev, coef_c, new_c, ghosts_c, psi_c, rows_c
    )
    place = lax.broadcasted_iota(jnp.int32, (8, LANES), 0)
    table = jnp.zeros((8, LANES), jnp.float32) if table_in is None else table_in[...]
    adds = [(step, jnp.sum(sums_f[0]) / cells[0]), (STEPS + step, jnp.sum(sums_c[0]) / cells[1])]
    if step == 1:
        adds.append((2, jnp.sum(sums_f[1]) / cells[0]))
        adds.append((STEPS + 2, jnp.sum(sums_c[1]) / cells[1]))
    if step == 0 and not inner:
        weights_x, weights_y = weights
        node = (s.fy, LANES)
        node_lane = lax.broadcasted_iota(jnp.int32, node, 1)
        q = jnp.zeros(node, jnp.float32)
        for i in range(s.fx):
            for c in range(3):
                there = pltpu.roll(coef_f[3][i] * new_f[c, i], 4 * i + c + 1, 1)
                q = jnp.where(node_lane == 4 * i + c, there, q)
        moved[...] = jnp.zeros(moved.shape, jnp.float32)
        for a in range(4):
            part = weights_x[a] * q
            for b in range(4):
                moved[a, 2 * b + 2 : 2 * b + 2 + s.fy, :] += weights_y[b] * part
        double[...] = sum(pltpu.roll(moved[a], 8 * (1 + a), 1) for a in range(4))
        rows = s.cy + 4
        both = double[pl.ds(0, rows, stride=2), :] + double[pl.ds(1, rows, stride=2), :]
        for i in range(s.ce):
            there = pltpu.roll(both, LANES - 8 * i, 1) if i else both
            spread_out[i, 0:rows, :] = there + pltpu.roll(there, LANES - 4, 1)
            spread_out[i, rows:, :] = jnp.zeros((s.spread - rows, LANES), jnp.float32)
        put_x(s, flags, x_out, new_f, new_c, beta_own, spread_out)
    if step == 1 and not inner:
        spread[...] = spread_in[:, 2 : 2 + s.cy, :]
        rows = pl.ds(s.corner_spread, s.cx)
        low, high = sides(flags, EVEN_Y, HAS_YM, HAS_YP, y_in[2][rows], y_in[3][rows])
        spread[:, 0:2, :] += low
        spread[:, s.cy - 2 : s.cy, :] += high
        joined = jnp.zeros((s.cy, LANES), jnp.float32)
        for i in range(s.cx):
            for c in range(3):
                line = spread[i] if c == 0 else pltpu.roll(spread[i], LANES - c, 1)
                joined += new_c[c, i, :, 0:LANES] * line
        adds.append((2, (-0.5 * STEP) * jnp.sum(joined[:, 0:1]) / cells[0]))
        put_x(s, flags, x_out, new_f, new_c)
    for row, value in adds:
        table = table + jnp.where(place == row, value, 0.0)
    energy[...] = table


def final_fine_kernel(s, fine, coarse, prev, offs, *refs):
    coef, (wide, inv, xa, xb, ya, yb, new) = refs[:5], refs[5:12]
    ext_f, ext_c, div, double, moved = refs[12:]
    flags = where_am_i()
    fill_displacement(s, flags, fine, ext_f, (xa, xb), (ya, yb), True)
    fill_displacement(s, flags, coarse, ext_c, (xa, xb), (ya, yb), False, 1)
    double_plane(s, ext_c, double)
    fill_divergence(s.fx, s.fy, ext_f, inv, div)
    ghosts = bottom_ghosts(s, node_weights(s, offs), double, moved)
    update(s.fx, s.fy, ext_f, wide, inv, div, prev, coef, new, ghosts)


def final_coarse_kernel(s, fine, coarse, prev, *refs):
    coef, (wide, inv, xa, xb, ya, yb, new) = refs[:5], refs[5:12]
    ext, div, pairs = refs[12:]
    fill_displacement(s, where_am_i(), coarse, ext, (xa, xb), (ya, yb), False)
    add_pairs(s, fine, pairs)
    fill_divergence(s.cx, s.cy, ext, inv, div)
    update(s.cx, s.cy, ext, wide, inv, div, prev, coef, new, top_ghosts(s, pairs))


VMEM = pl.BlockSpec(memory_space=pltpu.VMEM)
HBM = pl.BlockSpec(memory_space=pltpu.HBM)


def call(kernel, shapes, flops, *args, scratch=(), spec=VMEM, sems=0):
    shapes = [jax.ShapeDtypeStruct(shape, jnp.float32) for shape in shapes]
    scratch = [pltpu.VMEM(shape, jnp.float32) for shape in scratch]
    if sems:
        scratch.append(pltpu.SemaphoreType.DMA((sems,)))
    return pl.pallas_call(
        kernel,
        out_shape=shapes,
        in_specs=[spec] * len(args),
        out_specs=[VMEM] * len(shapes),
        scratch_shapes=scratch,
        compiler_params=pltpu.CompilerParams(vmem_limit_bytes=VMEM_LIMIT),
        cost_estimate=pl.CostEstimate(flops=flops, bytes_accessed=1 << 20, transcendentals=0),
    )(*args)


def swap_pairs(mesh, move):
    sizes = list(mesh.shape.values())
    pairs = []
    for source in range(math.prod(sizes)):
        rest, at = source, []
        for size in reversed(sizes):
            at.insert(0, rest % size)
            rest //= size
        target = 0
        for index, size in zip(move(*at), sizes, strict=True):
            target = target * size + index
        pairs.append((source, target))
    return pairs


def beside_x(z, x, y, core):
    return z, x ^ 1, y, core


def across_x(z, x, y, core):
    place = 4 * z + x
    if place in (0, 31):
        return z, x, y, core ^ 1
    place += 1 if place % 2 else -1
    return place // 4, place % 4, y, core


def beside_y(z, x, y, core):
    return z, x, y, core ^ 1


def across_y(z, x, y, core):
    place = (2 * y + core + (1 if core else -1)) % 8
    return z, x, place // 2, place % 2


TOTAL = (
    lambda z, x, y, core: (z ^ 7, x, y, core),
    lambda z, x, y, core: (z, x, y, core ^ 1),
    lambda z, x, y, core: (z ^ 2, x, y, core ^ 1),
    lambda z, x, y, core: (z, x, y ^ 1, core ^ 1),
    lambda z, x, y, core: (z, x ^ 1, y, core ^ 1),
    lambda z, x, y, core: (z ^ 1, x, y, core ^ 1),
    lambda z, x, y, core: (z, x ^ 3, y, core ^ 1),
    lambda z, x, y, core: (z, x, y ^ 3, core ^ 1),
)


def per_device(
    mesh,
    fine_disp,
    fine_prev,
    coarse_disp,
    coarse_prev,
    fine_density,
    fine_lame,
    fine_rigidity,
    fine_metric,
    coarse_density,
    coarse_lame,
    coarse_rigidity,
    coarse_metric,
    offsets,
):
    fine_shape, coarse_shape = fine_metric.shape, coarse_metric.shape
    s = Sizes(fine_shape, coarse_shape)
    count_x, count_y = lax.axis_size(GX), lax.axis_size(GY)

    def swap(value, move):
        return lax.ppermute(value, ALL, swap_pairs(mesh, move))

    def swap_both(pair, beside, across):
        second = swap(pair[1], across)
        first = swap(pair[0], beside)
        return [pltpu.with_memory_space_constraint(x, pltpu.VMEM) for x in (first, second)]

    offs = offsets[0] * 4 + offsets[1] + 5
    offs = jnp.pad(jnp.repeat(offs.T, 4, axis=1), ((0, 0), (0, LANES - 4 * s.fx)))
    x_out = call(
        functools.partial(first_kernel, s),
        [(s.x_rows_mats, LANES)] * 2,
        1000,
        *(
            pltpu.with_memory_space_constraint(x, pltpu.HBM)
            for x in (
                fine_disp,
                coarse_disp,
                fine_rigidity,
                fine_metric,
                coarse_rigidity,
                coarse_metric,
            )
        ),
        scratch=[
            (2, 3, 2, s.fy, s.fz),
            (2, 3, 2, s.cy, s.cz),
            (2, 2, s.fy, s.fz),
            (2, 2, s.cy, s.cz),
        ],
        spec=HBM,
        sems=12,
    )
    own = []
    for density, lame, rigidity, metric in (
        (fine_density, fine_lame, fine_rigidity, fine_metric),
        (coarse_density, coarse_lame, coarse_rigidity, coarse_metric),
    ):
        own.append(
            call(
                own_kernel,
                [metric.shape] * 5 + [metric.shape[:2] + (LANES,), metric.shape],
                2_000_000,
                density,
                lame,
                rigidity,
                metric,
            )
        )
    inverse_f, *coef_f, beta_f = own[0]
    inverse_c, *coef_c, beta_c = own[1]

    fine, coarse = fine_disp, coarse_disp
    fine_ext = (s.fx + 2, s.fy + 2, s.fz)
    coarse_ext = (s.cx + 2, s.cy + 2, s.cz)
    scratch = [
        (3, s.fe, s.fy + 16, s.fz),
        (3, s.ce, s.cy + 16, s.cz),
        (s.fx + 2, s.fy + 16, s.fz),
        (s.cx + 2, s.cy + 16, s.cz),
        (2 * (s.cy + 4), LANES),
        (4, 2 * (s.cy + 4), LANES),
        (3, s.cx, s.fy, LANES),
    ]
    cells = [count_x * count_y * s.fx * s.fy * s.fz, count_x * count_y * s.cx * s.cy * s.cz]
    spread = (s.ce, s.spread, LANES)
    for step in range(STEPS):
        x_in = swap_both(x_out, beside_x, across_x)
        if step == 2:
            for k, move in enumerate(TOTAL):
                other = swap(energy, move)
                if k < len(TOTAL) - 1:
                    energy = energy + other

        def y_strips(part, shapes, *args):
            kernel = functools.partial(y_kernel, s, step, part)
            return call(kernel, shapes, 500_000, *args)

        pairs = [(s.y_rows_mats, s.y_rows_beta, s.y_rows)[step], 2, LANES]
        if step == 2:
            y_out = y_strips("all", [tuple(pairs)] * 2, fine, coarse, *x_in)
            y_in = swap_both(y_out, beside_y, across_y)
        else:
            if step == 0:
                mats = [fine_rigidity, fine_metric, coarse_rigidity, coarse_metric]
                more, shapes = [], [(s.corner_rows, 2, LANES)] * 2
            else:
                mats = [beta_f, beta_c]
                more, shapes = [spread_own], [(s.corner_rows_beta, 2, LANES)] * 2
                shapes.append((s.cx,) + spread[1:])
            y_out = y_strips("own", [tuple(pairs)] * 2, fine, coarse, *mats)
            y_in = swap_both(y_out, beside_y, across_y)
            y_out = y_strips("corners", shapes, *more, *x_in)
            y_in += swap_both(y_out[:2], beside_y, across_y)
        if step == 2:
            wide_f, inv_f, wide_c, inv_c = ext_mats
            (fine_final,) = call(
                functools.partial(final_fine_kernel, s),
                [fine.shape],
                2_000_000,
                fine,
                coarse,
                fine_prev,
                offs,
                *coef_f,
                wide_f,
                inv_f,
                *x_in,
                *y_in,
                scratch=[scratch[0], scratch[1][:3] + (LANES,), scratch[2], *scratch[4:6]],
            )
            (coarse_final,) = call(
                functools.partial(final_coarse_kernel, s),
                [coarse.shape],
                2_000_000,
                fine,
                coarse,
                coarse_prev,
                *coef_c,
                wide_c,
                inv_c,
                *x_in,
                *y_in,
                scratch=[scratch[1], scratch[3], scratch[6]],
            )
            break

        def part_of_step(inner, shapes, *args):
            return call(
                functools.partial(step_kernel, s, step, inner, cells),
                [fine.shape, coarse.shape, (8, LANES)] + shapes,
                2_000_000,
                fine,
                coarse,
                fine_prev,
                coarse_prev,
                offs,
                *coef_f,
                *coef_c,
                *args,
                scratch=scratch + (more_scratch if step == 1 else []),
            )

        more_scratch = [
            scratch[2],
            scratch[3],
            scratch[0][1:],
            scratch[1][1:],
            scratch[6],
            (s.cx, s.cy, LANES),
        ]
        betas = [beta_f, beta_c]
        if step == 0:
            raw = [fine_rigidity, fine_metric, inverse_f, coarse_rigidity, coarse_metric, inverse_c]
            shapes = [fine_ext, fine_ext, coarse_ext, coarse_ext]
            *done, energy, w_f, i_f, w_c, i_c = part_of_step(
                True, shapes, *raw, *betas, *x_in, *y_in[:2]
            )
            ext_mats = [w_f, i_f, w_c, i_c]
            shapes, added = [(s.x_rows_beta, LANES)] * 2 + [spread], []
        else:
            *done, energy = part_of_step(True, [], *ext_mats, *betas, energy, *x_in, *y_in[:2])
            shapes, added = [(s.x_rows, LANES)] * 2, [y_out[2]]
        outs = part_of_step(False, shapes, *ext_mats, *betas, energy, *done, *added, *x_in, *y_in)
        fine_prev, coarse_prev = fine, coarse
        fine, coarse, energy = outs[:3]
        x_out = outs[3:5]
        if step == 0:
            spread_own = outs[5]
    other, fine, coarse = lax.optimization_barrier((other, fine_final, coarse_final))
    energy = energy + other
    energy = energy[: 2 * STEPS, 0].reshape(2, STEPS).T
    return fine, coarse, energy


def solution(mesh):
    finer = Mesh(mesh.devices.reshape(8, 4, 4, 2), ALL)
    level, cell = P(None, GX, GY, None), P(GX, GY, None)
    in_specs = (level,) * 4 + (cell,) * 8 + (P(None, GX, GY),)

    def body(*args):
        return per_device(finer, *args)

    return jax.shard_map(
        body, mesh=finer, in_specs=in_specs, out_specs=(level, level, P()), check_vma=False
    )
```

```python
import functools
import math

import jax
import jax.numpy as jnp
from jax import lax
from jax.experimental import pallas as pl
from jax.experimental.pallas import tpu as pltpu
from jax.sharding import Mesh
from jax.sharding import PartitionSpec as P

STEPS = 3
GX = ("gx_0", "gx_1")
GY = ("gy_0", "gy_1")
ALL = GX + GY
STEP = 0.15
LANES = 128
VMEM_LIMIT = 20 * 1024 * 1024

EVEN_X, HAS_XM, HAS_XP, EVEN_Y, HAS_YM, HAS_YP = range(6)


def where_am_i():
    x = 4 * lax.axis_index("gx_0") + lax.axis_index("gx_1")
    y = 2 * lax.axis_index("gy_0") + lax.axis_index("gy_1")
    return x % 2 == 0, x > 0, x < 31, y % 2 == 0, y > 0, y < 7


class Sizes:
    def __init__(self, fine, coarse):
        self.fx, self.fy, self.fz = fine
        self.cx, self.cy, self.cz = coarse
        self.halves = self.cz // LANES
        self.x_coarse = 4 * self.fy
        self.x_plane = self.x_coarse + self.halves * 4 * self.cy
        self.x_rows = self.x_plane + self.cy
        self.x_fine_mats = self.x_rows
        self.x_coarse_mats = self.x_fine_mats + 2 * self.fy
        self.x_rows_mats = self.x_coarse_mats + 2 * self.halves * self.cy
        self.x_fine_beta = self.x_rows
        self.x_coarse_beta = self.x_fine_beta + 2 * self.fy
        self.x_spread = self.x_coarse_beta + self.halves * 2 * self.cy
        self.spread = self.cy + 8
        self.x_rows_beta = self.x_spread + 2 * self.spread
        self.fe, self.ce = self.fx + 4, self.cx + 4
        self.y_coarse = 2 * self.fe
        self.y_plane = self.y_coarse + self.halves * 2 * self.ce
        self.y_rows = self.y_plane + self.ce
        self.y_fine_mats = self.y_rows
        self.y_coarse_mats = self.y_fine_mats + self.fx
        self.y_rows_mats = self.y_coarse_mats + self.halves * self.cx
        self.y_fine_beta = self.y_rows
        self.y_coarse_beta = self.y_fine_beta + self.fe
        self.y_rows_beta = self.y_coarse_beta + self.halves * self.ce
        self.f_coarse = 2
        self.f_plane = self.f_coarse + 2 * self.halves
        self.f_beta = self.f_plane + 1
        self.corner_rows = 4 * self.f_beta
        self.corner_spread = 4 * (self.f_beta + 1 + self.halves)
        self.corner_rows_beta = self.corner_spread + self.cx


def lanes_of(h):
    return slice(h * LANES, (h + 1) * LANES)


def put_strips(s, out, far, fine, coarse, at_f, at_c):
    near, second = jnp.where(far, 1, 0), jnp.where(far, 0, 1)
    for n, (c, row) in enumerate(((0, 0), (0, 1), (1, near), (2, near))):
        out[n * s.fy : (n + 1) * s.fy, :] = fine[c, at_f + row]
        line = coarse[c, at_c + row]
        for h in range(s.halves):
            base = s.x_coarse + (h * 4 + n) * s.cy
            out[base : base + s.cy, :] = line[:, lanes_of(h)]
    along_y, along_z = (coarse[c, at_c + second][:, 0:LANES] for c in (1, 2))
    lane = lax.broadcasted_iota(jnp.int32, along_y.shape, 1)
    plane = jnp.where(lane == 1, pltpu.roll(along_y, 1, 1), pltpu.roll(along_z, 2, 1))
    out[s.x_plane : s.x_plane + s.cy, :] = plane


def put_x(s, flags, outs, fine, coarse, betas=None, spread=None):
    even = flags[EVEN_X]
    for k, out in enumerate(outs):
        far = even if k == 0 else jnp.logical_not(even)
        start_f = jnp.where(far, s.fx - 2, 0)
        start_c = jnp.where(far, s.cx - 2, 0)
        put_strips(s, out, far, fine, coarse, start_f, start_c)
        if betas is None:
            continue
        strip = betas[0][pl.ds(start_f, 2), :, :]
        out[s.x_fine_beta : s.x_coarse_beta, :] = strip.reshape(2 * s.fy, LANES)
        strip = betas[1][pl.ds(start_c, 2), :, :]
        for h in range(s.halves):
            base = s.x_coarse_beta + h * 2 * s.cy
            out[base : base + 2 * s.cy, :] = strip[:, :, lanes_of(h)].reshape(2 * s.cy, LANES)
        start = jnp.where(far, s.cx + 2, 0)
        out[s.x_spread : s.x_rows_beta, :] = spread[pl.ds(start, 2)].reshape(2 * s.spread, LANES)


def first_kernel(s, fine, coarse, rig_f, met_f, rig_c, met_c, out_a, out_b, *scratch):
    strip_f, strip_c, line_f, line_c, sems = scratch
    flags = where_am_i()
    copies = []

    def fetch(source, target):
        copies.append(pltpu.make_async_copy(source, target, sems.at[len(copies)]))
        copies[-1].start()

    even = flags[EVEN_X]
    for k in range(2):
        far = even if k == 0 else jnp.logical_not(even)
        fetch(fine.at[:, pl.ds(jnp.where(far, s.fx - 2, 0), 2)], strip_f.at[k])
        fetch(coarse.at[:, pl.ds(jnp.where(far, s.cx - 2, 0), 2)], strip_c.at[k])
        for m, (of_f, of_c) in enumerate(((rig_f, rig_c), (met_f, met_c))):
            fetch(of_f.at[jnp.where(far, s.fx - 1, 0)], line_f.at[k, m])
            fetch(of_c.at[jnp.where(far, s.cx - 1, 0)], line_c.at[k, m])
    for copy in copies:
        copy.wait()
    for k, out in enumerate((out_a, out_b)):
        far = even if k == 0 else jnp.logical_not(even)
        put_strips(s, out, far, strip_f.at[k], strip_c.at[k], 0, 0)
        for m in range(2):
            base = s.x_fine_mats + m * s.fy
            out[base : base + s.fy, :] = line_f[k, m]
            for h in range(s.halves):
                base = s.x_coarse_mats + (m * s.halves + h) * s.cy
                out[base : base + s.cy, :] = line_c[k, m, :, lanes_of(h)]


def sides(flags, even, has_low, has_high, a, b):
    low = jnp.where(flags[even], b, a)
    high = jnp.where(flags[even], a, b)
    low = jnp.where(flags[has_low], low, 0.0)
    high = jnp.where(flags[has_high], high, 0.0)
    return low, high


def y_kernel(s, step, part, *refs):
    flags = where_am_i()
    refs = list(refs)
    even = flags[EVEN_Y]
    has_own, has_corners = part != "corners", part != "own"
    if has_own:
        fine, coarse = refs[:2]
        mats = refs[2:-2] if part == "own" else []
    if has_corners:
        total = refs.pop() if step == 1 else None
        in_a, in_b = refs[-4:-2]
        spread = refs[0]
    out_a, out_b = refs[-2:]

    def put(index, low, high):
        out_a[index] = jnp.where(even, high, low)
        out_b[index] = jnp.where(even, low, high)

    def put_one(index, m, low, high):
        out_a[index, m : m + 1, :] = jnp.where(even, high, low)
        out_b[index, m : m + 1, :] = jnp.where(even, low, high)

    def came(first, count):
        rows = slice(first, first + count)
        return sides(flags, EVEN_X, HAS_XM, HAS_XP, in_a[rows, :], in_b[rows, :])

    def corner(base, field, x, side, k):
        return 4 * field + 2 * side + k if part == "corners" else base + side * (x + 2) + k

    def level(own, x, y, x_base, y_base, y_size, field, plane):
        both, single = y_base, y_base + y_size
        if has_own:
            put(pl.ds(both + 2, x), own(1, slice(0, 2)), own(1, slice(y - 2, y)))
            for m, c in enumerate((0, 2)):
                here = pl.ds(single + 2, x)
                put_one(here, m, own(c, slice(0, 1)), own(c, slice(y - 1, y)))
                if plane:
                    here = pl.ds(s.y_plane + 2, x)
                    put_one(here, m, own(c, slice(1, 2)), own(c, slice(y - 2, y - 1)))
        for side, k in ((0, 0), (0, 1), (1, 0), (1, 1)) if has_corners else ():
            near = k == 1 - side

            def row(c, first, count):
                if c == 0:
                    return came(x_base + k * y + first, count)[side]
                if near:
                    return came(x_base + (1 + c) * y + first, count)[side]
                return pltpu.roll(came(s.x_plane + first, count)[side], LANES - c, 1)

            if near or plane:
                put(corner(both, field, x, side, k), row(1, 0, 2), row(1, y - 2, 2))
            for m, c in enumerate((0, 2)):
                if c == 0 or near or plane:
                    here = corner(single, field + 1, x, side, k)
                    put_one(here, m, row(c, 0, 1), row(c, y - 1, 1))
                if plane:
                    here = corner(s.y_plane, s.f_plane, x, side, k)
                    put_one(here, m, row(c, 1, 1), row(c, y - 2, 1))

    def two_deep(own, x, y, x_base, y_base, field):
        if has_own:
            put(pl.ds(y_base + 2, x), own(slice(0, 2)), own(slice(y - 2, y)))
        for k in range(2) if has_corners else ():
            low, high = came(x_base + k * y, 2), came(x_base + (k + 1) * y - 2, 2)
            for side in range(2):
                put(corner(y_base, field, x, side, k), low[side], high[side])

    level(lambda c, r: fine[c, :, r, :], s.fx, s.fy, 0, 0, s.fe, 0, False)
    for h in range(s.halves):
        x_base, y_base = s.x_coarse + h * 4 * s.cy, s.y_coarse + h * 2 * s.ce
        field = s.f_coarse + 2 * h
        at = lanes_of(h)
        level(
            lambda c, r: coarse[c, :, r, at], s.cx, s.cy, x_base, y_base, s.ce, field, h == 0
        )
    if step == 0 and has_own:
        rig_f, met_f, rig_c, met_c = mats
        for m, (of_f, of_c) in enumerate(((rig_f, rig_c), (met_f, met_c))):
            here = pl.ds(s.y_fine_mats, s.fx)
            put_one(here, m, of_f[:, 0:1, :], of_f[:, s.fy - 1 : s.fy, :])
            for h in range(s.halves):
                here = pl.ds(s.y_coarse_mats + h * s.cx, s.cx)
                low, high = of_c[:, 0:1, lanes_of(h)], of_c[:, s.cy - 1 : s.cy, lanes_of(h)]
                put_one(here, m, low, high)
    if step == 1:
        beta_f, beta_c = mats if has_own else (None, None)
        x_base, y_base = s.x_fine_beta, s.y_fine_beta
        two_deep(lambda r: beta_f[:, r, :], s.fx, s.fy, x_base, y_base, s.f_beta)
        for h in range(s.halves):
            at = lanes_of(h)
            x_base, y_base = s.x_coarse_beta + h * 2 * s.cy, s.y_coarse_beta + h * s.ce
            field = s.f_beta + 1 + h
            two_deep(lambda r: beta_c[:, r, at], s.cx, s.cy, x_base, y_base, field)
    if step == 1 and has_corners:
        total[...] = spread[2 : 2 + s.cx]
        for k in range(2):
            low, high = came(s.x_spread + k * s.spread, s.spread)
            total[k] += low
            total[s.cx - 2 + k] += high
        here = pl.ds(s.corner_spread, s.cx)
        put(here, total[:, 0:2, :], total[:, s.cy + 2 : s.cy + 4, :])


def up_one(x):
    return pltpu.roll(x, x.shape[-1] - 1, x.ndim - 1)


def down_one(x):
    return pltpu.roll(x, 1, x.ndim - 1)


def edge_factor(shape, first, last):
    lane = first + lax.broadcasted_iota(jnp.int32, shape, len(shape) - 1)
    return jnp.where((lane == 0) | (lane == last), 2.0, 1.0)


def own_kernel(density, lame, rigidity, metric, inverse, c1, c2, weight, above, first, beta):
    inv = 1.0 / metric[...]
    last = inv.shape[2] - 1
    inverse[...] = inv * edge_factor(inv.shape, 0, last)
    over = 1.0 / density[...]
    c1[...] = (0.5 * STEP) * (inv * over)
    c2[...] = (0.25 * STEP) * ((lame[...] + rigidity[...]) * over)
    weight[...] = density[...] * metric[...]
    v = rigidity[...] * inv
    lane = lax.broadcasted_iota(jnp.int32, v.shape, 2)
    above[...] = v + jnp.where(lane == last, v, up_one(v))
    first[...] = 2.0 * v[:, :, 0:LANES]
    beta[...] = 0.5 * ((lame[...] + rigidity[...]) * metric[...])


def difference(f, lane):
    up = jnp.where(lane == f.shape[-1] - 1, f, up_one(f))
    return up - jnp.where(lane == 0, f, down_one(f))


def difference_transposed(q, lane):
    down = jnp.where(lane == 0, -q, down_one(q))
    return down - jnp.where(lane == q.shape[-1] - 1, -q, up_one(q))


def y_pieces(flags, y_in, start, x, field):
    def taken(a, b):
        return sides(flags, EVEN_Y, HAS_YM, HAS_YP, a, b)

    if len(y_in) == 2:
        rows = slice(start, start + x + 4)
        return [(slice(0, x + 4), *taken(y_in[0][rows], y_in[1][rows]))]
    rows = slice(start + 2, start + 2 + x)
    out = [(slice(2, 2 + x), *taken(y_in[0][rows], y_in[1][rows]))]
    for side in range(2 if y_in[2] is not None else 0):
        rows = slice(4 * field + 2 * side, 4 * field + 2 * side + 2)
        at = slice(side * (x + 2), side * (x + 2) + 2)
        out.append((at, *taken(y_in[2][rows], y_in[3][rows])))
    return out


def fill_beta(s, flags, own, ext, x_in, y_in, fine):
    x, y, e = (s.fx, s.fy, s.fe) if fine else (s.cx, s.cy, s.ce)
    ext[2 : 2 + x, 8 : 8 + y, :] = own[...]
    for h in range(1 if fine else s.halves):
        at = lanes_of(h)
        base = s.x_fine_beta if fine else s.x_coarse_beta + h * 2 * y
        rows = slice(base, base + 2 * y)
        low, high = sides(flags, EVEN_X, HAS_XM, HAS_XP, x_in[0][rows, :], x_in[1][rows, :])
        ext[0:2, 8 : 8 + y, at] = low.reshape(2, y, LANES)
        ext[x + 2 : x + 4, 8 : 8 + y, at] = high.reshape(2, y, LANES)
        start = s.y_fine_beta if fine else s.y_coarse_beta + h * e
        field = s.f_beta if fine else s.f_beta + 1 + h
        for i, low, high in y_pieces(flags, y_in, start, x, field):
            ext[i, 6:8, at] = low
            ext[i, 8 + y : 10 + y, at] = high


def fill_transposed(y, ext, beta, inv_ext, psi, rows):
    z = ext.shape[-1]
    lane = lax.broadcasted_iota(jnp.int32, (y + 2, z), 1)
    wide, low, high = slice(7, 9 + y), slice(6, 8 + y), slice(8, 10 + y)

    for r in rows:
        along_x = ext[0, r, wide, :] * beta[r, wide, :]
        along_x -= ext[0, r + 2, wide, :] * beta[r + 2, wide, :]
        along_y = ext[1, r + 1, low, :] * beta[r + 1, low, :]
        along_y -= ext[1, r + 1, high, :] * beta[r + 1, high, :]
        inv = inv_ext[r, 0 : 2 + y, :]
        column = inv * beta[r + 1, wide, :] * ext[2, r + 1, wide, :]
        total = along_x + along_y + difference_transposed(column, lane)
        psi[r, wide, :] = jnp.where(inv > 0.0, total, 0.0)


def fill_displacement(s, flags, own, ext, x_in, y_in, fine, halves=None):
    x, y, e = (s.fx, s.fy, s.fe) if fine else (s.cx, s.cy, s.ce)
    halves = 1 if fine else halves or s.halves
    ext[:, 2 : 2 + x, 8 : 8 + y, :] = own[:, :, :, 0 : halves * LANES]
    mid = slice(8, 8 + y)

    def from_x(first, rows):
        rows = slice(first, first + rows)
        return sides(flags, EVEN_X, HAS_XM, HAS_XP, x_in[0][rows, :], x_in[1][rows, :])

    for h in range(halves):
        at = lanes_of(h)
        base = 0 if fine else s.x_coarse + h * 4 * y
        low, high = from_x(base, 2 * y)
        ext[0, 0:2, mid, at] = low.reshape(2, y, LANES)
        ext[0, x + 2 : x + 4, mid, at] = high.reshape(2, y, LANES)
        for c in (1, 2):
            ext[c, 1, mid, at], ext[c, x + 2, mid, at] = from_x(base + (1 + c) * y, y)
        start = 0 if fine else s.y_coarse + h * 2 * e
        field = 0 if fine else s.f_coarse + 2 * h
        for i, low, high in y_pieces(flags, y_in, start, x, field):
            ext[1, i, 6:8, at] = low
            ext[1, i, 8 + y : 10 + y, at] = high
        for i, low, high in y_pieces(flags, y_in, start + e, x, field + 1):
            for m, c in enumerate((0, 2)):
                ext[c, i, 7:8, at] = low[:, m : m + 1, :]
                ext[c, i, 8 + y : 9 + y, at] = high[:, m : m + 1, :]
    if fine:
        return
    at = lanes_of(0)
    low, high = from_x(s.x_plane, y)
    for c in (1, 2):
        ext[c, 0, mid, at] = pltpu.roll(low, LANES - c, 1)
        ext[c, x + 3, mid, at] = pltpu.roll(high, LANES - c, 1)
    for i, low, high in y_pieces(flags, y_in, s.y_plane, x, s.f_plane):
        for m, c in enumerate((0, 2)):
            ext[c, i, 6:7, at] = low[:, m : m + 1, :]
            ext[c, i, 9 + y : 10 + y, at] = high[:, m : m + 1, :]


def fill_materials(s, flags, rigidity, metric, inverse, wide_ext, inv_ext, x_in, y_in, fine):
    x, y = (s.fx, s.fy) if fine else (s.cx, s.cy)
    own_z = metric.shape[2]
    wide_ext[1 : 1 + x, 1 : 1 + y, :] = rigidity[...] * metric[...]
    inv_ext[1 : 1 + x, 1 : 1 + y, :] = inverse[...]
    for h in range(1 if fine else s.halves):
        at = lanes_of(h)
        edge = edge_factor((y, LANES), h * LANES, own_z - 1)
        got = []
        for m in range(2):
            base = s.x_fine_mats + m * y if fine else s.x_coarse_mats + (m * s.halves + h) * y
            rows = slice(base, base + y)
            even = flags[EVEN_X]
            a, b = x_in[0][rows, :], x_in[1][rows, :]
            got.append((jnp.where(even, b, a), jnp.where(even, a, b)))
        for side, (flag, place) in enumerate(((HAS_XM, 0), (HAS_XP, x + 1))):
            rig, met = got[0][side], got[1][side]
            wide_ext[place, 1 : 1 + y, at] = jnp.where(flags[flag], rig * met, 0.0)
            inv_ext[place, 1 : 1 + y, at] = jnp.where(flags[flag], edge / met, 0.0)
        start = s.y_fine_mats if fine else s.y_coarse_mats + h * x
        rows = slice(start, start + x)
        got = []
        for m in range(2):
            even = flags[EVEN_Y]
            a, b = y_in[0][rows, m : m + 1, :], y_in[1][rows, m : m + 1, :]
            got.append((jnp.where(even, b, a), jnp.where(even, a, b)))
        for side, (flag, place) in enumerate(((HAS_YM, 0), (HAS_YP, 1 + y))):
            rig, met = got[0][side], got[1][side]
            wide_ext[1 : 1 + x, place : place + 1, at] = jnp.where(flags[flag], rig * met, 0.0)
            inv_ext[1 : 1 + x, place : place + 1, at] = jnp.where(flags[flag], edge[None, 0:1] / met, 0.0)


def fill_divergence(x, y, ext, inv_ext, div, rows=None):
    z = ext.shape[-1]
    lane = lax.broadcasted_iota(jnp.int32, (y + 2, z), 1)

    for r in rows or range(x + 2):
        along_x = ext[0, r + 2, 7 : 9 + y, :] - ext[0, r, 7 : 9 + y, :]
        along_y = ext[1, r + 1, 8 : 10 + y, :] - ext[1, r + 1, 6 : 8 + y, :]
        f = ext[2, r + 1, 7 : 9 + y, :]
        inv = inv_ext[r, 0 : 2 + y, :]
        total = along_x + along_y + inv * difference(f, lane)
        div[r, 7 : 9 + y, :] = jnp.where(inv > 0.0, total, 0.0)


def update(x, y, ext, wide_ext, inv_ext, div, prev, coef, new, ghosts, psi=None, rows=None):
    c1, c2, weight, above, vertical = coef
    z = ext.shape[-1]
    lane = lax.broadcasted_iota(jnp.int32, (y, z), 1)
    mid, left, right, own = slice(8, 8 + y), slice(7, 7 + y), slice(9, 9 + y), slice(1, 1 + y)

    def row(i, totals):
        wide = wide_ext[i + 1, own, :]
        w_xp = wide + wide_ext[i + 2, own, :]
        w_xm = wide_ext[i, own, :] + wide
        w_yp = wide + wide_ext[i + 1, 2 : 2 + y, :]
        w_ym = wide_ext[i + 1, 0:y, :] + wide
        inv = inv_ext[i + 1, own, :]
        gradient = (
            div[i + 2, mid, :] - div[i, mid, :],
            div[i + 1, right, :] - div[i + 1, left, :],
            inv * difference(div[i + 1, mid, :], lane),
        )
        if psi is not None:
            transposed = (
                psi[i, mid, :] - psi[i + 2, mid, :],
                psi[i + 1, left, :] - psi[i + 1, right, :],
                difference_transposed(inv * psi[i + 1, mid, :], lane),
            )
        top, bottom, top_next = ghosts(i)
        k1, k2, dm, va = c1[i], c2[i], weight[i], above[i]
        first = vertical[i, :, 0:1]
        inner, squares, cross = (jnp.zeros((y, z), jnp.float32) for _ in range(3))
        for c in range(3):
            u = ext[c, i + 2, mid, :]
            flux = w_xp * (ext[c, i + 3, mid, :] - u) - w_xm * (u - ext[c, i + 1, mid, :])
            flux += w_yp * (ext[c, i + 2, right, :] - u) - w_ym * (u - ext[c, i + 2, left, :])
            below = entry = 0.0
            if psi is None:
                below = 0.0 if bottom is None else bottom(c)
                entry = 0.0 if top is None else first * (u[:, 0:1] - top(c))
            elif top is not None:
                entry = first * u[:, 0:1]
            over = va * (jnp.where(lane == z - 1, below, up_one(u)) - u)
            flux += over - jnp.where(lane == 0, entry, down_one(over))
            whole = flux
            if psi is not None:
                if top is None:
                    whole = flux + jnp.where(lane == z - 1, va * bottom(c), 0.0)
                else:
                    whole = flux + jnp.where(lane == 0, first * top(c), 0.0)
            push = whole * k1 + k2 * gradient[c]
            before = prev[c, i]
            change = u - before
            inner += change * change - before * push
            change += push
            updated = u + change
            new[c, i] = updated
            if psi is not None:
                squares += change * change
                cross += updated * (flux + transposed[c])
                if top is not None:
                    cross += jnp.where(lane == 0, first * u[:, 0:1] * top_next(c), 0.0)
        total = totals[0] + dm * inner
        if psi is None:
            return (total,)
        return total, totals[1] + (dm * squares - (0.5 * STEP) * cross)

    start = (jnp.zeros((y, z), jnp.float32),) * (1 if psi is None else 2)
    count, index, unroll = rows or (x, lambda k: k, 4)
    return lax.fori_loop(0, count, lambda k, t: row(index(k), t), start, unroll=unroll)


def double_plane(s, ext_c, double):
    lane = lax.broadcasted_iota(jnp.int32, (s.cy + 4, LANES), 1)
    table = jnp.zeros((s.cy + 4, LANES), jnp.float32)
    for i in range(s.ce):
        e0, e1, e2 = (ext_c[c, i, 6 : 10 + s.cy, 0:LANES] for c in range(3))
        e1, e2 = pltpu.roll(e1, 1, 1), pltpu.roll(e2, 2, 1)
        plane = jnp.where(lane == 0, e0, jnp.where(lane == 1, e1, e2))
        for k in (2 * i, 2 * i + 1):
            there = pltpu.roll(plane, 4 * k, 1) if k else plane
            table = jnp.where(lane // 4 == k, there, table)
    for j in range(s.cy + 4):
        double[2 * j : 2 * j + 2, :] = jnp.broadcast_to(table[j : j + 1, :], (2, LANES))


def add_pairs(s, fine, pairs):
    for c in range(3):
        for i in range(s.cx):
            pairs[c, i] = fine[c, 2 * i] + fine[c, 2 * i + 1]


def node_weights(s, offs):
    node = (s.fy, LANES)
    node_lane = lax.broadcasted_iota(jnp.int32, node, 1)
    near_x = jnp.where(node_lane // 4 % 2 == 0, 0.75, 0.25)
    near_y = jnp.where(lax.broadcasted_iota(jnp.int32, node, 0) % 2 == 0, 0.75, 0.25)
    code = offs[...]
    weights_x, weights_y = (
        [
            jnp.where(off == shift, near, 0.0) + jnp.where(off == shift - 1, 1.0 - near, 0.0)
            for shift in (-1, 0, 1, 2)
        ]
        for off, near in ((code // 4 - 1, near_x), (code % 4 - 1, near_y))
    )
    return weights_x, weights_y


def bottom_ghosts(s, weights, double, moved):
    weights_x, weights_y = weights
    node = (s.fy, LANES)
    ghosts = jnp.zeros(node, jnp.float32)
    for a in range(4):
        moved[a] = pltpu.roll(double[...], LANES - 8 * (1 + a), 1)
        line = jnp.zeros(node, jnp.float32)
        for b in range(4):
            line += weights_y[b] * moved[a, 2 * b + 2 : 2 * b + 2 + s.fy, :]
        ghosts += weights_x[a] * line
    return lambda i: (None, lambda c: pltpu.roll(ghosts, LANES - 1 - c - 4 * i, 1), None)


def top_ghosts(s, pairs, pairs_next=None):
    def mean(of, i):
        def top(c):
            both = of[c, i, pl.ds(0, s.cy, stride=2), :] + of[c, i, pl.ds(1, s.cy, stride=2), :]
            return 0.25 * both[:, LANES - 1 :]

        return top

    return lambda i: (mean(pairs, i), None, mean(pairs_next, i) if pairs_next is not None else None)


INNER_F, OUTER_F = (10, lambda k: k + 2, 5), (6, lambda k: jnp.where(k < 2, k, k + 10), 3)
INNER_C, OUTER_C = (5, lambda k: k + 1, 5), (3, lambda k: jnp.where(k < 1, k, k + 5), 3)
INNER_DIV_F, OUTER_DIV_F = tuple(range(2, 14)), (0, 1, 2, 3, *range(12, 18))
INNER_DIV_C, OUTER_DIV_C = tuple(range(1, 8)), (0, 1, 2, *range(6, 10))


def step_kernel(s, step, inner, cells, *refs):
    flags = where_am_i()
    refs = list(refs)

    def take(n):
        out = refs[:n]
        del refs[:n]
        return out

    fine, coarse, fine_prev, coarse_prev, offs = take(5)
    coef_f, coef_c = take(5), take(5)
    makes_mats = inner and step == 0
    if makes_mats:
        rig_f, met_f, inverse_f, rig_c, met_c, inverse_c = take(6)
    else:
        wide_f, inv_f, wide_c, inv_c = take(4)
    beta_own = take(2)
    table_in = take(1)[0] if step == 1 or not inner else None
    if not inner:
        done_f, done_c = take(2)
    if step == 1 and not inner:
        (spread_in,) = take(1)
    x_in = take(2)
    y_in = take(2) + [None, None] if inner else take(4)
    new_f, new_c, energy = take(3)
    if not inner:
        x_out = take(2)
    if makes_mats:
        wide_f, inv_f, wide_c, inv_c = take(4)
    if step == 0 and not inner:
        (spread_out,) = take(1)
    ext_f, ext_c, div_f, div_c, double, moved, pairs = take(7)

    fill_displacement(s, flags, fine, ext_f, x_in, y_in, True)
    fill_displacement(s, flags, coarse, ext_c, x_in, y_in, False)
    if makes_mats:
        fill_materials(s, flags, rig_f, met_f, inverse_f, wide_f, inv_f, x_in, y_in, True)
        fill_materials(s, flags, rig_c, met_c, inverse_c, wide_c, inv_c, x_in, y_in, False)
    double_plane(s, ext_c, double)
    add_pairs(s, fine, pairs)
    rows_f, rows_c = (INNER_F, INNER_C) if inner else (OUTER_F, OUTER_C)
    lines_f, lines_c = (INNER_DIV_F, INNER_DIV_C) if inner else (OUTER_DIV_F, OUTER_DIV_C)
    fill_divergence(s.fx, s.fy, ext_f, inv_f, div_f, lines_f)
    fill_divergence(s.cx, s.cy, ext_c, inv_c, div_c, lines_c)
    psi_f = psi_c = pairs_next = None
    if step == 1:
        psi_f, psi_c, all_beta_f, all_beta_c, pairs_next, spread = take(6)
        fill_beta(s, flags, beta_own[0], all_beta_f, x_in, y_in, True)
        fill_beta(s, flags, beta_own[1], all_beta_c, x_in, y_in, False)
        fill_transposed(s.fy, ext_f, all_beta_f, inv_f, psi_f, lines_f)
        fill_transposed(s.cy, ext_c, all_beta_c, inv_c, psi_c, lines_c)
    if not inner:
        new_f[:, 2:12] = done_f[:, 2:12]
        new_c[:, 1:6] = done_c[:, 1:6]

    weights = node_weights(s, offs)
    ghosts_f = bottom_ghosts(s, weights, double, moved)
    ghosts_c = top_ghosts(s, pairs, pairs_next)
    sums_f = update(
        s.fx, s.fy, ext_f, wide_f, inv_f, div_f, fine_prev, coef_f, new_f, ghosts_f, psi_f, rows_f
    )
    if step == 1:
        add_pairs(s, new_f, pairs_next)
    sums_c = update(
        s.cx, s.cy, ext_c, wide_c, inv_c, div_c, coarse_prev, coef_c, new_c, ghosts_c, psi_c, rows_c
    )
    place = lax.broadcasted_iota(jnp.int32, (8, LANES), 0)
    table = jnp.zeros((8, LANES), jnp.float32) if table_in is None else table_in[...]
    adds = [(step, jnp.sum(sums_f[0]) / cells[0]), (STEPS + step, jnp.sum(sums_c[0]) / cells[1])]
    if step == 1:
        adds.append((2, jnp.sum(sums_f[1]) / cells[0]))
        adds.append((STEPS + 2, jnp.sum(sums_c[1]) / cells[1]))
    if step == 0 and not inner:
        weights_x, weights_y = weights
        node = (s.fy, LANES)
        node_lane = lax.broadcasted_iota(jnp.int32, node, 1)
        q = jnp.zeros(node, jnp.float32)
        for i in range(s.fx):
            for c in range(3):
                there = pltpu.roll(coef_f[3][i] * new_f[c, i], 4 * i + c + 1, 1)
                q = jnp.where(node_lane == 4 * i + c, there, q)
        moved[...] = jnp.zeros(moved.shape, jnp.float32)
        for a in range(4):
            part = weights_x[a] * q
            for b in range(4):
                moved[a, 2 * b + 2 : 2 * b + 2 + s.fy, :] += weights_y[b] * part
        double[...] = sum(pltpu.roll(moved[a], 8 * (1 + a), 1) for a in range(4))
        rows = s.cy + 4
        both = double[pl.ds(0, rows, stride=2), :] + double[pl.ds(1, rows, stride=2), :]
        for i in range(s.ce):
            there = pltpu.roll(both, LANES - 8 * i, 1) if i else both
            spread_out[i, 0:rows, :] = there + pltpu.roll(there, LANES - 4, 1)
            spread_out[i, rows:, :] = jnp.zeros((s.spread - rows, LANES), jnp.float32)
        put_x(s, flags, x_out, new_f, new_c, beta_own, spread_out)
    if step == 1 and not inner:
        spread[...] = spread_in[:, 2 : 2 + s.cy, :]
        rows = pl.ds(s.corner_spread, s.cx)
        low, high = sides(flags, EVEN_Y, HAS_YM, HAS_YP, y_in[2][rows], y_in[3][rows])
        spread[:, 0:2, :] += low
        spread[:, s.cy - 2 : s.cy, :] += high
        joined = jnp.zeros((s.cy, LANES), jnp.float32)
        for i in range(s.cx):
            for c in range(3):
                line = spread[i] if c == 0 else pltpu.roll(spread[i], LANES - c, 1)
                joined += new_c[c, i, :, 0:LANES] * line
        adds.append((2, (-0.5 * STEP) * jnp.sum(joined[:, 0:1]) / cells[0]))
        put_x(s, flags, x_out, new_f, new_c)
    for row, value in adds:
        table = table + jnp.where(place == row, value, 0.0)
    energy[...] = table


def final_fine_kernel(s, fine, coarse, prev, offs, *refs):
    coef, (wide, inv, xa, xb, ya, yb, new) = refs[:5], refs[5:12]
    ext_f, ext_c, div, double, moved = refs[12:]
    flags = where_am_i()
    fill_displacement(s, flags, fine, ext_f, (xa, xb), (ya, yb), True)
    fill_displacement(s, flags, coarse, ext_c, (xa, xb), (ya, yb), False, 1)
    double_plane(s, ext_c, double)
    fill_divergence(s.fx, s.fy, ext_f, inv, div)
    ghosts = bottom_ghosts(s, node_weights(s, offs), double, moved)
    update(s.fx, s.fy, ext_f, wide, inv, div, prev, coef, new, ghosts)


def final_coarse_kernel(s, fine, coarse, prev, *refs):
    coef, (wide, inv, xa, xb, ya, yb, new) = refs[:5], refs[5:12]
    ext, div, pairs = refs[12:]
    fill_displacement(s, where_am_i(), coarse, ext, (xa, xb), (ya, yb), False)
    add_pairs(s, fine, pairs)
    fill_divergence(s.cx, s.cy, ext, inv, div)
    update(s.cx, s.cy, ext, wide, inv, div, prev, coef, new, top_ghosts(s, pairs))


VMEM = pl.BlockSpec(memory_space=pltpu.VMEM)
HBM = pl.BlockSpec(memory_space=pltpu.HBM)


def call(kernel, shapes, flops, *args, scratch=(), spec=VMEM, sems=0):
    shapes = [jax.ShapeDtypeStruct(shape, jnp.float32) for shape in shapes]
    scratch = [pltpu.VMEM(shape, jnp.float32) for shape in scratch]
    if sems:
        scratch.append(pltpu.SemaphoreType.DMA((sems,)))
    return pl.pallas_call(
        kernel,
        out_shape=shapes,
        in_specs=[spec] * len(args),
        out_specs=[VMEM] * len(shapes),
        scratch_shapes=scratch,
        compiler_params=pltpu.CompilerParams(vmem_limit_bytes=VMEM_LIMIT),
        cost_estimate=pl.CostEstimate(flops=flops, bytes_accessed=1 << 20, transcendentals=0),
    )(*args)


def swap_pairs(mesh, move):
    sizes = list(mesh.shape.values())
    pairs = []
    for source in range(math.prod(sizes)):
        rest, at = source, []
        for size in reversed(sizes):
            at.insert(0, rest % size)
            rest //= size
        target = 0
        for index, size in zip(move(*at), sizes, strict=True):
            target = target * size + index
        pairs.append((source, target))
    return pairs


def beside_x(z, x, y, core):
    return z, x ^ 1, y, core


def across_x(z, x, y, core):
    place = 4 * z + x
    if place in (0, 31):
        return z, x, y, core ^ 1
    place += 1 if place % 2 else -1
    return place // 4, place % 4, y, core


def beside_y(z, x, y, core):
    return z, x, y, core ^ 1


def across_y(z, x, y, core):
    place = (2 * y + core + (1 if core else -1)) % 8
    return z, x, place // 2, place % 2


TOTAL = (
    lambda z, x, y, core: (z ^ 7, x, y, core),
    lambda z, x, y, core: (z, x, y, core ^ 1),
    lambda z, x, y, core: (z ^ 2, x, y, core ^ 1),
    lambda z, x, y, core: (z, x, y ^ 1, core ^ 1),
    lambda z, x, y, core: (z, x ^ 1, y, core ^ 1),
    lambda z, x, y, core: (z ^ 1, x, y, core ^ 1),
    lambda z, x, y, core: (z, x ^ 3, y, core ^ 1),
    lambda z, x, y, core: (z, x, y ^ 3, core ^ 1),
)


def per_device(
    mesh,
    fine_disp,
    fine_prev,
    coarse_disp,
    coarse_prev,
    fine_density,
    fine_lame,
    fine_rigidity,
    fine_metric,
    coarse_density,
    coarse_lame,
    coarse_rigidity,
    coarse_metric,
    offsets,
):
    fine_shape, coarse_shape = fine_metric.shape, coarse_metric.shape
    s = Sizes(fine_shape, coarse_shape)
    count_x, count_y = lax.axis_size(GX), lax.axis_size(GY)

    def swap(value, move):
        return lax.ppermute(value, ALL, swap_pairs(mesh, move))

    def swap_both(pair, beside, across):
        second = swap(pair[1], across)
        first = swap(pair[0], beside)
        return [pltpu.with_memory_space_constraint(x, pltpu.VMEM) for x in (first, second)]

    offs = offsets[0] * 4 + offsets[1] + 5
    offs = jnp.pad(jnp.repeat(offs.T, 4, axis=1), ((0, 0), (0, LANES - 4 * s.fx)))
    x_out = call(
        functools.partial(first_kernel, s),
        [(s.x_rows_mats, LANES)] * 2,
        1000,
        *(
            pltpu.with_memory_space_constraint(x, pltpu.HBM)
            for x in (
                fine_disp,
                coarse_disp,
                fine_rigidity,
                fine_metric,
                coarse_rigidity,
                coarse_metric,
            )
        ),
        scratch=[
            (2, 3, 2, s.fy, s.fz),
            (2, 3, 2, s.cy, s.cz),
            (2, 2, s.fy, s.fz),
            (2, 2, s.cy, s.cz),
        ],
        spec=HBM,
        sems=12,
    )
    own = []
    for density, lame, rigidity, metric in (
        (fine_density, fine_lame, fine_rigidity, fine_metric),
        (coarse_density, coarse_lame, coarse_rigidity, coarse_metric),
    ):
        own.append(
            call(
                own_kernel,
                [metric.shape] * 5 + [metric.shape[:2] + (LANES,), metric.shape],
                2_000_000,
                density,
                lame,
                rigidity,
                metric,
            )
        )
    inverse_f, *coef_f, beta_f = own[0]
    inverse_c, *coef_c, beta_c = own[1]

    fine, coarse = fine_disp, coarse_disp
    fine_ext = (s.fx + 2, s.fy + 2, s.fz)
    coarse_ext = (s.cx + 2, s.cy + 2, s.cz)
    scratch = [
        (3, s.fe, s.fy + 16, s.fz),
        (3, s.ce, s.cy + 16, s.cz),
        (s.fx + 2, s.fy + 16, s.fz),
        (s.cx + 2, s.cy + 16, s.cz),
        (2 * (s.cy + 4), LANES),
        (4, 2 * (s.cy + 4), LANES),
        (3, s.cx, s.fy, LANES),
    ]
    cells = [count_x * count_y * s.fx * s.fy * s.fz, count_x * count_y * s.cx * s.cy * s.cz]
    spread = (s.ce, s.spread, LANES)
    for step in range(STEPS):
        x_in = swap_both(x_out, beside_x, across_x)
        if step == 2:
            for k, move in enumerate(TOTAL):
                other = swap(energy, move)
                if k < len(TOTAL) - 1:
                    energy = energy + other

        def y_strips(part, shapes, *args):
            kernel = functools.partial(y_kernel, s, step, part)
            return call(kernel, shapes, 500_000, *args)

        pairs = [(s.y_rows_mats, s.y_rows_beta, s.y_rows)[step], 2, LANES]
        if step == 2:
            y_out = y_strips("all", [tuple(pairs)] * 2, fine, coarse, *x_in)
            y_in = swap_both(y_out, beside_y, across_y)
        else:
            if step == 0:
                mats = [fine_rigidity, fine_metric, coarse_rigidity, coarse_metric]
                more, shapes = [], [(s.corner_rows, 2, LANES)] * 2
            else:
                mats = [beta_f, beta_c]
                more, shapes = [spread_own], [(s.corner_rows_beta, 2, LANES)] * 2
                shapes.append((s.cx,) + spread[1:])
            y_out = y_strips("own", [tuple(pairs)] * 2, fine, coarse, *mats)
            y_in = swap_both(y_out, beside_y, across_y)
            y_out = y_strips("corners", shapes, *more, *x_in)
            y_in += swap_both(y_out[:2], beside_y, across_y)
        if step == 2:
            wide_f, inv_f, wide_c, inv_c = ext_mats
            (fine_final,) = call(
                functools.partial(final_fine_kernel, s),
                [fine.shape],
                2_000_000,
                fine,
                coarse,
                fine_prev,
                offs,
                *coef_f,
                wide_f,
                inv_f,
                *x_in,
                *y_in,
                scratch=[scratch[0], scratch[1][:3] + (LANES,), scratch[2], *scratch[4:6]],
            )
            (coarse_final,) = call(
                functools.partial(final_coarse_kernel, s),
                [coarse.shape],
                2_000_000,
                fine,
                coarse,
                coarse_prev,
                *coef_c,
                wide_c,
                inv_c,
                *x_in,
                *y_in,
                scratch=[scratch[1], scratch[3], scratch[6]],
            )
            break

        def part_of_step(inner, shapes, *args):
            return call(
                functools.partial(step_kernel, s, step, inner, cells),
                [fine.shape, coarse.shape, (8, LANES)] + shapes,
                2_000_000,
                fine,
                coarse,
                fine_prev,
                coarse_prev,
                offs,
                *coef_f,
                *coef_c,
                *args,
                scratch=scratch + (more_scratch if step == 1 else []),
            )

        more_scratch = [
            scratch[2],
            scratch[3],
            scratch[0][1:],
            scratch[1][1:],
            scratch[6],
            (s.cx, s.cy, LANES),
        ]
        betas = [beta_f, beta_c]
        if step == 0:
            raw = [fine_rigidity, fine_metric, inverse_f, coarse_rigidity, coarse_metric, inverse_c]
            shapes = [fine_ext, fine_ext, coarse_ext, coarse_ext]
            *done, energy, w_f, i_f, w_c, i_c = part_of_step(
                True, shapes, *raw, *betas, *x_in, *y_in[:2]
            )
            ext_mats = [w_f, i_f, w_c, i_c]
            shapes, added = [(s.x_rows_beta, LANES)] * 2 + [spread], []
        else:
            *done, energy = part_of_step(True, [], *ext_mats, *betas, energy, *x_in, *y_in[:2])
            shapes, added = [(s.x_rows, LANES)] * 2, [y_out[2]]
        outs = part_of_step(False, shapes, *ext_mats, *betas, energy, *done, *added, *x_in, *y_in)
        fine_prev, coarse_prev = fine, coarse
        fine, coarse, energy = outs[:3]
        x_out = outs[3:5]
        if step == 0:
            spread_own = outs[5]
    other, fine, coarse = lax.optimization_barrier((other, fine_final, coarse_final))
    energy = energy + other
    energy = energy[: 2 * STEPS, 0].reshape(2, STEPS).T
    return fine, coarse, energy


def solution(mesh):
    finer = Mesh(mesh.devices.reshape(8, 4, 4, 2), ALL)
    level, cell = P(None, GX, GY, None), P(GX, GY, None)
    in_specs = (level,) * 4 + (cell,) * 8 + (P(None, GX, GY),)

    def body(*args):
        return per_device(finer, *args)

    return jax.shard_map(
        body, mesh=finer, in_specs=in_specs, out_specs=(level, level, P()), check_vma=False
    )
```
